64 devices in a mesh: data: 4 (over x, y), seq: 16 (over z, core).
Axes of the slice: x: 2, y: 2, z: 8, core: 2. Of those that a mesh axis runs over, the one named last changes fastest.
The devices are a block of a 4x4x8 slice.
Arguments:
- dec_in: bfloat16 [8192, 768], P(('data', 'seq')), parts along dimension 0
- memory: bfloat16 [65536, 768], P(('data', 'seq')), parts along dimension 0
- mem_len: int32 [4], P('data'), parts along dimension 0
- grad_out: float32 [8192, 768], P(('data', 'seq')), parts along dimension 0
- norm_attn: bfloat16 [768], replicated
- wq_cross: bfloat16 [768, 12, 64], replicated
- wk_cross: bfloat16 [768, 12, 64], replicated
- wv_cross: bfloat16 [768, 12, 64], replicated
- wo_cross: bfloat16 [12, 64, 768], replicated
- norm_mlp: bfloat16 [768], replicated
- w_gate: bfloat16 [768, 2048], replicated
- w_up: bfloat16 [768, 2048], replicated
- w_down: bfloat16 [2048, 768], replicated
Outputs:
- output 1: float32 [8192, 768], P(('data', 'seq')), parts along dimension 0
- output 2: float32 [65536, 768], P(('data', 'seq')), parts along dimension 0
- output 3: float32 [3072], P('data'), parts along dimension 0
- output 4: float32 [3072, 12, 64], P('data'), parts along dimension 0
- output 5: float32 [3072, 12, 64], P('data'), parts along dimension 0
- output 6: float32 [3072, 12, 64], P('data'), parts along dimension 0
- output 7: float32 [48, 64, 768], P('data'), parts along dimension 0
- output 8: float32 [3072], P('data'), parts along dimension 0
- output 9: float32 [3072, 2048], P('data'), parts along dimension 0
- output 10: float32 [3072, 2048], P('data'), parts along dimension 0
- output 11: float32 [8192, 768], P('data'), parts along dimension 0
There are 4 independent parts. The reference program is written for one: setup_inputs(seed, part) draws one part's arguments, and reference() takes and returns one part's arrays. A program takes and returns all parts, laid end to end along the dimension named above; an argument that names none is the same for every part.
All inputs are finite; a program needn't handle non-finite values.
Results may differ from the reference program's by a relative error of at most 0.0157877.
Values are sent between devices in bfloat16 or wider.
A program may use at most 768 MiB of HBM per device.

```python
import functools
import jax
import jax.numpy as jnp
from jax import lax

TQ = 2048
TM = 16384
D = 768
HEADS = 12
KV_HEADS = 12
HEAD = 64
FF = 2048
QBLK = 128
SEGMENTS = 16


def setup_inputs(seed: int = 0, part: int = 0) -> dict:
    part_keys = jax.random.split(jax.random.fold_in(jax.random.key(seed), part), 5)
    shared_keys = jax.random.split(jax.random.key(seed + 1), 11)
    inv_width = D ** -0.5

    def normal_draw(key, shape, spread):
        return spread * jax.random.normal(key, shape, jnp.float32)

    topics = normal_draw(part_keys[1], (SEGMENTS, D), 1.0)
    memory = normal_draw(part_keys[2], (TM, D), 0.6) + 0.8 * jnp.repeat(topics, TM // SEGMENTS, axis=0)
    quarter = TM // 4
    mem_len = jax.random.randint(part_keys[3], (1,), quarter, TM - quarter + 1, dtype=jnp.int32)
    return {
        'dec_in': normal_draw(part_keys[0], (TQ, D), 1.0).astype(jnp.bfloat16),
        'memory': memory.astype(jnp.bfloat16),
        'mem_len': mem_len,
        'grad_out': normal_draw(part_keys[4], (TQ, D), 1.0),
        'norm_attn': (1.0 + normal_draw(shared_keys[0], (D,), 0.3)).astype(jnp.bfloat16),
        'wq_cross': normal_draw(shared_keys[1], (D, HEADS, HEAD), 1.2 * inv_width).astype(jnp.bfloat16),
        'wk_cross': normal_draw(shared_keys[2], (D, KV_HEADS, HEAD), 1.2 * inv_width).astype(jnp.bfloat16),
        'wv_cross': normal_draw(shared_keys[3], (D, KV_HEADS, HEAD), inv_width).astype(jnp.bfloat16),
        'wo_cross': normal_draw(shared_keys[4], (HEADS, HEAD, D), 1.5 * inv_width).astype(jnp.bfloat16),
        'norm_mlp': (1.0 + normal_draw(shared_keys[5], (D,), 0.3)).astype(jnp.bfloat16),
        'w_gate': normal_draw(shared_keys[6], (D, FF), inv_width).astype(jnp.bfloat16),
        'w_up': normal_draw(shared_keys[7], (D, FF), inv_width).astype(jnp.bfloat16),
        'w_down': normal_draw(shared_keys[8], (FF, D), FF ** -0.5).astype(jnp.bfloat16),
    }


def to_bf16(tensor):
    return tensor + lax.stop_gradient(tensor.astype(jnp.bfloat16).astype(jnp.float32) - tensor)


def rms_norm(tensor, gain):
    mean_sq = jnp.mean(tensor * tensor, axis=-1, keepdims=True)
    return tensor * lax.rsqrt(mean_sq + 1e-6) * gain


def layer_forward(valid_mask, dec_in, memory, norm_attn, wq_cross, wk_cross, wv_cross, wo_cross, norm_mlp, w_gate, w_up, w_down):
    normed = to_bf16(rms_norm(dec_in, norm_attn))
    dec_query = to_bf16(jnp.einsum('td,dhe->the', normed, wq_cross))
    dec_query = dec_query.reshape(TQ // QBLK, QBLK, KV_HEADS, HEADS // KV_HEADS, HEAD)
    mem_keys = to_bf16(jnp.einsum('td,dke->tke', memory, wk_cross))
    mem_vals = to_bf16(jnp.einsum('td,dke->tke', memory, wv_cross))

    def block_attention(query_block):
        scores = jnp.einsum('qkge,tke->qkgt', query_block, mem_keys) * (HEAD ** -0.5)
        scores = jnp.where(valid_mask, scores, -1e30)
        attn_prob = jax.nn.softmax(scores, axis=-1)
        return jnp.einsum('qkgt,tke->qkge', attn_prob, mem_vals)

    attended = to_bf16(lax.map(jax.checkpoint(block_attention), dec_query).reshape(TQ, HEADS, HEAD))
    hidden = to_bf16(dec_in + jnp.einsum('the,hed->td', attended, wo_cross))
    normed_mlp = to_bf16(rms_norm(hidden, norm_mlp))
    gate_pre = jnp.dot(normed_mlp, w_gate, preferred_element_type=jnp.float32)
    up_pre = jnp.dot(normed_mlp, w_up, preferred_element_type=jnp.float32)
    mlp_act = to_bf16(jax.nn.silu(gate_pre) * up_pre)
    return hidden + jnp.dot(mlp_act, w_down, preferred_element_type=jnp.float32)


def reference(dec_in, memory, mem_len, grad_out, norm_attn, wq_cross, wk_cross, wv_cross, wo_cross, norm_mlp, w_gate, w_up, w_down):
    valid_mask = jnp.arange(TM) < mem_len[0]
    primals = [tensor.astype(jnp.float32) for tensor in (dec_in, memory, norm_attn, wq_cross, wk_cross, wv_cross, wo_cross, norm_mlp, w_gate, w_up, w_down)]
    _, pullback = jax.vjp(functools.partial(layer_forward, valid_mask), *primals)
    (g_dec, g_mem, g_norm_attn, g_wq, g_wk, g_wv, g_wo, g_norm_mlp, g_gate, g_up, g_down) = pullback(grad_out.astype(jnp.float32))
    return (g_dec, g_mem, g_norm_attn, g_wq, g_wk, g_wv, g_wo, g_norm_mlp, g_gate, g_up, g_down)
```

```python
import functools
import math

import jax
import jax.numpy as jnp
from jax import lax
from jax.experimental import pallas as pl
from jax.experimental.pallas import tpu as pltpu
from jax.sharding import PartitionSpec as P

F32 = jnp.float32
BF16 = jnp.bfloat16
QT = 256
MC = 256
LOG2E = math.log2(math.e)
VMEM = pltpu.VMEM


def mm(a, b):
    return jnp.dot(a, b, preferred_element_type=F32)


def mm_bt(a, b):
    return lax.dot_general(a, b, (((1,), (1,)), ((), ())), preferred_element_type=F32)


def mm_at(a, b):
    return lax.dot_general(a, b, (((0,), (0,)), ((), ())), preferred_element_type=F32)


def rms_norm(tensor, gain):
    mean_sq = jnp.mean(tensor * tensor, axis=-1, keepdims=True)
    return tensor * lax.rsqrt(mean_sq + 1e-6) * gain


def gated_unit(gate_pre, up_pre):
    return jax.nn.silu(gate_pre) * up_pre


def split3(x):
    hi = lax.reduce_precision(x, 8, 7)
    rest = x - hi
    mid = lax.reduce_precision(rest, 8, 7)
    lo = rest - mid
    return hi.astype(BF16), mid.astype(BF16), lo.astype(BF16)


def fwd_kernel(heads, mem, queries, c, k_ref, ak_ref, vt_ref, qz_ref, aq_ref, o_ref, m_ref, l_ref, s_scr, mx_scr):
    nq = queries // QT
    n = heads * nq

    def step(ia, sa, ib, sb):
        if ia is not None:
            h = ia // nq
            qc = ia - h * nq
            rhs = jnp.concatenate([qz_ref[pl.ds(pl.multiple_of(h * 128, 128), 128), pl.ds(pl.multiple_of(qc * QT, QT), QT)], aq_ref[...]], axis=0)
            pair = pl.ds(pl.multiple_of((h // 2) * 128, 128), 128)
            mx = None
        if ib is not None:
            hb = ib // nq
            qb = ib - hb * nq
            m = jnp.max(mx_scr[sb], axis=0, keepdims=True)
            vrow = pl.ds(pl.multiple_of(hb * 64, 64), 64)
            ls = None
            acc = None
        for j in range(mem // MC):
            rows = slice(j * MC, (j + 1) * MC)
            if ia is not None:
                s = mm(jnp.concatenate([k_ref[rows, pair], ak_ref[rows, 0:16]], axis=1), rhs)
                s_scr[sa, rows, :] = s
                t = jnp.max(s.reshape(MC // 8, 8, QT), axis=0)
                mx = t if mx is None else jnp.maximum(mx, t)
            if ib is not None:
                pr = jnp.exp2((s_scr[sb, rows, :] - m) * c)
                t = jnp.sum(pr.reshape(MC // 8, 8, QT), axis=0)
                ls = t if ls is None else ls + t
                d = mm(vt_ref[vrow, rows], pr.astype(BF16))
                acc = d if acc is None else acc + d
        if ia is not None:
            mx_scr[sa] = mx
        if ib is not None:
            qs = pl.ds(pl.multiple_of(qb * QT, QT), QT)
            o_ref[vrow, qs] = acc
            m_ref[pl.ds(hb, 1), qs] = m
            l_ref[pl.ds(hb, 1), qs] = jnp.sum(ls, axis=0, keepdims=True)

    step(0, 0, None, None)

    def body(i, carry):
        step(2 * i + 1, 1, 2 * i, 0)
        step(jnp.minimum(2 * i + 2, n - 1), 0, 2 * i + 1, 1)
        return carry

    lax.fori_loop(0, n // 2, body, 0)


def bwd_kernel(heads, mem, queries, c, k_ref, v_ref, ak_ref, kt_ref, qz_ref, aq_ref, doz_ref, ad_ref, dkt_ref, dvt_ref, dqt_ref):
    nq = queries // QT
    nm = mem // MC
    dkt_ref[...] = jnp.zeros_like(dkt_ref)
    dvt_ref[...] = jnp.zeros_like(dvt_ref)

    def body(it, carry):
        h = it // nq
        qc = it - h * nq
        pair = h // 2
        qs = pl.ds(pl.multiple_of(qc * QT, QT), QT)
        hz = pl.ds(pl.multiple_of(h * 128, 128), 128)
        h64 = pl.ds(pl.multiple_of(h * 64, 64), 64)
        h16 = pl.ds(pl.multiple_of(h * 16, 16), 16)
        ps = pl.ds(pl.multiple_of(pair * 128, 128), 128)
        hz64 = pl.ds(pl.multiple_of(h * 128 + (h - 2 * pair) * 64, 64), 64)
        q_t = qz_ref[hz64, qs]
        do_t = doz_ref[hz64, qs]
        r1 = jnp.concatenate([qz_ref[hz, qs], aq_ref[h16, qs]], axis=0)
        r2 = jnp.concatenate([doz_ref[hz, qs], ad_ref[h16, qs]], axis=0)
        stage = {}
        dq = None
        for j in range(nm + 2):
            if j < nm:
                rows = slice(j * MC, (j + 1) * MC)
                ak = ak_ref[rows, 0:16]
                stage["a", j] = (mm(jnp.concatenate([k_ref[rows, ps], ak], axis=1), r1),
                                 mm(jnp.concatenate([v_ref[rows, ps], ak], axis=1), r2))
            if 1 <= j <= nm:
                s, dp = stage.pop(("a", j - 1))
                a = jnp.exp2(s * c)
                stage["b", j - 1] = (a.astype(BF16), (a * dp).astype(BF16))
            if j >= 2:
                rows = slice((j - 2) * MC, (j - 1) * MC)
                pb, ds = stage.pop(("b", j - 2))
                dvt_ref[h64, rows] += mm_bt(do_t, pb)
                dkt_ref[h64, rows] += mm_bt(q_t, ds)
                d = mm(kt_ref[h64, rows], ds)
                dq = d if dq is None else dq + d
        dqt_ref[h64, qs] = dq
        return carry

    lax.fori_loop(0, heads * nq, body, 0)


def vspec(n):
    return [pl.BlockSpec(memory_space=VMEM)] * n


def params():
    return pltpu.CompilerParams(vmem_limit_bytes=60 * 1024 * 1024)


def solution(mesh):
    group = mesh.shape['seq']
    row_spec = P(('data', 'seq'), None)
    part_vec = P('data')
    part_mat = P('data', None)
    part_cube = P('data', None, None)

    def device_step(dec_in, memory, mem_len, grad_out, norm_attn, wq, wk, wv, wo, norm_mlp, w_gate, w_up, w_down):
        rows, dim = dec_in.shape
        mem = memory.shape[0]
        heads, hd = wq.shape[1], wq.shape[2]
        inner = heads * hd
        queries = rows * group
        c = LOG2E * hd ** -0.5
        wq2, wk2, wv2 = (w.reshape(dim, inner) for w in (wq, wk, wv))
        wo2 = wo.reshape(inner, dim)
        gain1 = norm_attn.astype(F32)
        gain2 = norm_mlp.astype(F32)

        y_all = lax.all_gather(dec_in, 'seq', axis=0, tiled=True)
        go_all = lax.all_gather(grad_out.astype(BF16), 'seq', axis=0, tiled=True)
        x_all = y_all.astype(F32)
        n1_all = rms_norm(x_all, gain1).astype(BF16)
        q_t = lax.dot_general(wq2, n1_all, (((0,), (1,)), ((), ())), preferred_element_type=F32).astype(BF16)

        def pair_pad(t):
            t = t.reshape(heads // 2, 2, hd, queries)
            zero = jnp.zeros_like(t[:, 0])
            return jnp.stack([t[:, 0], zero, zero, t[:, 1]], axis=1).reshape(heads * 128, queries)

        qz = pair_pad(q_t)
        mem_k = mm(memory, wk2).astype(BF16)
        mem_v = mm(memory, wv2).astype(BF16)
        k_t = mem_k.T
        v_t = mem_v.T
        pos = lax.axis_index('seq') * mem + jnp.arange(mem)
        bias = jnp.where(pos < mem_len[0], 0.0, -1e30).astype(F32)
        lane = jnp.arange(128)
        ak = jnp.where(lane[None, :] == 0, bias[:, None], jnp.where(lane[None, :] < 4, 1.0, 0.0)).astype(BF16)
        aq0 = jnp.where(jnp.arange(16)[:, None] == 0, 1.0, 0.0).astype(BF16) * jnp.ones((1, QT), BF16)

        o_t, m_loc, l_loc = pl.pallas_call(
            functools.partial(fwd_kernel, heads, mem, queries, c),
            out_shape=(jax.ShapeDtypeStruct((inner, queries), F32), jax.ShapeDtypeStruct((heads, queries), F32), jax.ShapeDtypeStruct((heads, queries), F32)),
            in_specs=vspec(5), out_specs=tuple(vspec(3)),
            scratch_shapes=[VMEM((2, mem, QT), F32), VMEM((2, 8, QT), F32)],
            compiler_params=params(),
            cost_estimate=pl.CostEstimate(flops=4 * heads * mem * queries * 256, bytes_accessed=30 << 20, transcendentals=0),
            name="attn_fwd")(mem_k, ak, v_t, qz, aq0)
        m_all = lax.pmax(m_loc, 'seq')
        scale_loc = jnp.exp2((m_loc - m_all) * c)
        o_part = (o_t.reshape(heads, hd, queries) * scale_loc[:, None, :]).reshape(inner, queries).T
        l_part = (l_loc * scale_loc).T
        packed = jnp.concatenate([o_part, l_part, jnp.zeros((queries, 128 - heads), F32)], axis=1)
        summed = lax.psum_scatter(packed, 'seq', scatter_dimension=0, tiled=True)
        den = summed[:, inner:inner + heads]
        attended_f = (summed[:, :inner].reshape(rows, heads, hd) / den[:, :, None]).reshape(rows, inner)
        attended = attended_f.astype(BF16)
        m_own = lax.dynamic_slice_in_dim(m_all, lax.axis_index('seq') * rows, rows, axis=1).T
        lse = m_own + jnp.log2(den) / c

        x_in = dec_in.astype(F32)
        hidden = (x_in + mm(attended, wo2)).astype(BF16)
        n2_f, n2_pull = jax.vjp(rms_norm, hidden.astype(F32), gain2)
        n2 = n2_f.astype(BF16)
        gate_pre = mm(n2, w_gate)
        up_pre = mm(n2, w_up)
        _, gated_pull = jax.vjp(gated_unit, gate_pre, up_pre)
        grad_act = mm_bt(grad_out.astype(BF16), w_down)
        grad_gate, grad_up = gated_pull(grad_act)
        grad_n2 = mm_bt(grad_gate.astype(BF16), w_gate) + mm_bt(grad_up.astype(BF16), w_up)
        grad_h_norm, g_norm_mlp_part = n2_pull(grad_n2)
        grad_hidden = grad_out + grad_h_norm
        dh = grad_hidden.astype(BF16)
        d_att = mm_bt(dh, wo2)
        delta = jnp.sum((d_att * attended_f).reshape(rows, heads, hd), axis=-1)

        stats = jnp.concatenate(split3(-lse) + split3(-delta) + (jnp.zeros((rows, 128 - 6 * heads), BF16),), axis=1)
        gn = jnp.stack(split3(g_norm_mlp_part) + (jnp.zeros((dim,), BF16),) * 13)
        payload = jnp.concatenate([jnp.concatenate([dh, stats], axis=1), jnp.concatenate([gn, jnp.zeros((16, 128), BF16)], axis=1)], axis=0)
        gathered = lax.all_gather(payload, 'seq', axis=0, tiled=False)
        dh_all = gathered[:, :rows, :dim].reshape(queries, dim)
        st = gathered[:, :rows, dim:dim + 6 * heads].reshape(queries, 6, heads).transpose(2, 1, 0)
        g_norm_mlp = jnp.sum(gathered[:, rows:rows + 3, :dim].astype(F32), axis=(0, 1))
        one = jnp.ones((heads, 1, queries), BF16)
        pad = jnp.zeros((heads, 12, queries), BF16)
        aq = jnp.concatenate([one, st[:, 0:3], pad], axis=1).reshape(heads * 16, queries)
        ad = jnp.concatenate([0 * one, st[:, 3:6], pad], axis=1).reshape(heads * 16, queries)
        doz = pair_pad(mm_bt(wo2, dh_all).astype(BF16))

        dk_t, dv_t, dq_t = pl.pallas_call(
            functools.partial(bwd_kernel, heads, mem, queries, c),
            out_shape=(jax.ShapeDtypeStruct((inner, mem), F32), jax.ShapeDtypeStruct((inner, mem), F32), jax.ShapeDtypeStruct((inner, queries), F32)),
            in_specs=vspec(8), out_specs=tuple(vspec(3)),
            compiler_params=params(),
            cost_estimate=pl.CostEstimate(flops=10 * heads * mem * queries * 256, bytes_accessed=40 << 20, transcendentals=0),
            name="attn_bwd")(mem_k, mem_v, ak, k_t, qz, aq, doz, ad)
        att_all = lax.all_gather(attended, 'seq', axis=0, tiled=True)
        score_scale = hd ** -0.5
        dq = lax.psum_scatter(dq_t.T, 'seq', scatter_dimension=0, tiled=True) * score_scale
        dq_b = dq.astype(BF16)
        dq_all = lax.all_gather(dq_b, 'seq', axis=0, tiled=True)
        dkb = (dk_t * score_scale).astype(BF16)
        dvb = dv_t.astype(BF16)
        dkv = jnp.concatenate([dkb, dvb], axis=0)
        g_wkv = lax.psum(lax.dot_general(dkv, memory, (((1,), (0,)), ((), ())), preferred_element_type=F32), 'seq').T
        g_mem = lax.dot_general(dkv, jnp.concatenate([wk2, wv2], axis=1), (((0,), (1,)), ((), ())), preferred_element_type=F32)

        _, norm_pull = jax.vjp(rms_norm, x_in, gain1)
        grad_x_norm, _ = norm_pull(mm_bt(dq_b, wq2))
        g_dec = grad_hidden + grad_x_norm

        xhat = x_all * lax.rsqrt(jnp.mean(x_all * x_all, axis=-1, keepdims=True) + 1e-6)
        g_norm_attn = jnp.sum(mm_bt(dq_all, wq2) * xhat, axis=0)
        g_wq = mm_at(n1_all, dq_all)
        g_wo = mm_at(att_all, dh_all)
        h_all = (x_all + mm(att_all, wo2)).astype(BF16)
        n2_all = rms_norm(h_all.astype(F32), gain2).astype(BF16)
        mlp_f, pull_all = jax.vjp(gated_unit, mm(n2_all, w_gate), mm(n2_all, w_up))
        gg, gu = pull_all(mm_bt(go_all, w_down))
        g_down = mm_at(mlp_f.astype(BF16), go_all)
        g_gate = mm_at(n2_all, gg.astype(BF16))
        g_up = mm_at(n2_all, gu.astype(BF16))
        cube = (dim, heads, hd)
        return (g_dec, g_mem, g_norm_attn, g_wq.reshape(cube), g_wkv[:, :inner].reshape(cube), g_wkv[:, inner:].reshape(cube),
                g_wo.reshape(heads, hd, dim), g_norm_mlp, g_gate, g_up, g_down)

    return jax.shard_map(device_step, mesh=mesh,
                         in_specs=(row_spec, row_spec, part_vec, row_spec) + (P(),) * 9,
                         out_specs=(row_spec, row_spec, part_vec, part_cube, part_cube, part_cube, part_cube, part_vec, part_mat, part_mat, part_mat),
                         check_vma=False)
```

```python
import functools
import math

import jax
import jax.numpy as jnp
from jax import lax
from jax.experimental import pallas as pl
from jax.experimental.pallas import tpu as pltpu
from jax.sharding import PartitionSpec as P

F32 = jnp.float32
BF16 = jnp.bfloat16
QT = 256
MC = 256
LOG2E = math.log2(math.e)
VMEM = pltpu.VMEM
MESH = pl.DeviceIdType.MESH


def mm(a, b):
    return jnp.dot(a, b, preferred_element_type=F32)


def mm_bt(a, b):
    return lax.dot_general(a, b, (((1,), (1,)), ((), ())), preferred_element_type=F32)


def mm_at(a, b):
    return lax.dot_general(a, b, (((0,), (0,)), ((), ())), preferred_element_type=F32)


def rms_norm(tensor, gain):
    mean_sq = jnp.mean(tensor * tensor, axis=-1, keepdims=True)
    return tensor * lax.rsqrt(mean_sq + 1e-6) * gain


def gated_unit(gate_pre, up_pre):
    return jax.nn.silu(gate_pre) * up_pre


def split3(x):
    hi = lax.reduce_precision(x, 8, 7)
    rest = x - hi
    mid = lax.reduce_precision(rest, 8, 7)
    lo = rest - mid
    return hi.astype(BF16), mid.astype(BF16), lo.astype(BF16)


RIGHT, LEFT = 0, 1

class Ring:
    def __init__(self, chips):
        me = lax.axis_index('seq')
        self.chips = chips
        self.z = me // 2
        self.core = me - 2 * self.z
        self.partner = 2 * self.z + 1 - self.core
        self.next = (2 * self.chip(1) + self.core, 2 * self.chip(-1) + self.core)

    def chip(self, off):
        return lax.rem(self.z + off + self.chips, self.chips)

def remote(src, dst, ssem, rsem, dev):
    return pltpu.make_async_remote_copy(src_ref=src, dst_ref=dst, send_sem=ssem, recv_sem=rsem, device_id={'seq': dev}, device_id_type=MESH)

def enter(ring):
    barrier = pltpu.get_barrier_semaphore()
    for dev in (ring.partner, ring.next[0], ring.next[1]):
        pl.semaphore_signal(barrier, inc=1, device_id={'seq': dev}, device_id_type=MESH)
    pl.semaphore_wait(barrier, 3)

def fwd_kernel(dims, y_ref, m_ref, ak_ref, wq_ref, wk_ref, wv_ref, g_ref,
               yall_ref, att_ref, lse_ref,
               yg, mg, wqt, k_s, vt_s, qz, s_scr, mx_scr, part, rbuf, own, pown,
               agss, agrs, fss, frs, xss, xrs, rss, rrs):
    chips, rows, mem, dim, hc, c = dims
    QT = 2 * rows; T = 2 * mem; MC = min(256, mem); hh = hc // 2; inner = hc * 64
    HR = hh * 64; half_chips = chips // 2
    ring = Ring(chips); z = ring.z; core = ring.core
    hops = {(RIGHT, 0): half_chips, (RIGHT, 1): half_chips - 1, (LEFT, 0): half_chips - 1, (LEFT, 1): half_chips}
    sgn = (1, -1)
    sub = rows // 2
    enter(ring)

    mine = pl.ds(pl.multiple_of(core * mem, mem), mem)
    other = pl.ds(pl.multiple_of((1 - core) * mem, mem), mem)

    def mcopy():
        return remote(m_ref, mg, xss.at[0], xrs.at[0], ring.partner)

    def ag_desc(d, s, t):
        chip = ring.chip(-sgn[d] * (t - 1))
        src = y_ref.at[pl.ds(s * sub, sub)] if t == 1 else yg.at[chip, core, s]
        return remote(src, yg.at[chip, core, s], agss.at[d, s, t - 1], agrs.at[d, s, t - 1], ring.next[d])

    def ag_recv(d, s, t):
        slot = yg.at[ring.chip(-sgn[d] * t), core, s]
        return remote(slot, slot, agss.at[d, s, t - 1], agrs.at[d, s, t - 1], ring.next[d])

    def fw_desc(d, s, t):
        slot = yg.at[ring.chip(-sgn[d] * t), core, s]
        return remote(slot, slot, fss.at[d, s, t - 1], frs.at[d, s, t - 1], ring.partner)

    def fw_recv(d, s, t):
        slot = yg.at[ring.chip(-sgn[d] * t), 1 - core, s]
        return remote(slot, slot, fss.at[d, s, t - 1], frs.at[d, s, t - 1], ring.partner)

    def own_desc(s):
        return remote(y_ref.at[pl.ds(s * sub, sub)], yg.at[z, core, s], xss.at[1 + s], xrs.at[1 + s], ring.partner)

    def own_recv(s):
        slot = yg.at[z, 1 - core, s]
        return remote(slot, slot, xss.at[1 + s], xrs.at[1 + s], ring.partner)

    def serve(t):
        for d, s in ((RIGHT, 0), (LEFT, 1), (RIGHT, 1), (LEFT, 0)):
            if hops[d, s] >= t:
                ag_recv(d, s, t).wait_recv()
                if hops[d, s] > t:
                    ag_desc(d, s, t + 1).start()
                fw_desc(d, s, t).start()

    for d, s in ((RIGHT, 0), (LEFT, 1), (RIGHT, 1), (LEFT, 0)):
        ag_desc(d, s, 1).start()
    for s in range(2):
        own_desc(s).start()
    mcopy().start()
    for s in range(2):
        yg[z, core, s] = y_ref[s * sub:(s + 1) * sub, :]

    hcol = pl.ds(pl.multiple_of(core * inner, 128), inner)
    qz[...] = jnp.zeros_like(qz)
    wqt[...] = wq_ref[:, hcol].T
    wk = wk_ref[:, hcol]
    wvt = wv_ref[:, hcol].T

    def project(src, base):
        for j in range(mem // MC):
            r = pl.ds(pl.multiple_of(base + j * MC, MC), MC)
            blk = src[j * MC:(j + 1) * MC, :]
            k_s[r, :] = mm(blk, wk).astype(BF16)
            vt_s[:, r] = mm_bt(wvt, blk).astype(BF16)

    project(m_ref, core * mem)
    serve(1)
    mrecv = remote(mg, mg, xss.at[0], xrs.at[0], ring.partner)
    mrecv.wait_recv()
    project(mg, (1 - core) * mem)
    serve(2)
    gain = g_ref[...]

    def stats(ref, hl):
        return ref[HR + hl:HR + hl + 1, :], ref[HR + 8 + hl:HR + 9 + hl, :]

    def flash(chip):
        x = yg[chip].reshape(QT, dim).astype(F32)
        n1 = rms_norm(x, gain).astype(BF16)
        qt = mm_bt(wqt[...], n1).astype(BF16)
        for h in range(hc):
            lo = h * 128 + (h % 2) * 64
            qz[lo:lo + 64, :] = qt[h * 64:(h + 1) * 64]
        one_row = jnp.where(lax.broadcasted_iota(jnp.int32, (16, QT), 0) == 0, 1.0, 0.0).astype(BF16)

        def step(h, slot, hp, pslot):
            if h is not None:
                rhs = jnp.concatenate([qz[pl.ds(pl.multiple_of(h * 128, 128), 128), :], one_row], axis=0)
                pair = pl.ds(pl.multiple_of((h // 2) * 128, 128), 128)
                mx = None
            if hp is not None:
                m = jnp.max(mx_scr[pslot], axis=0, keepdims=True)
                vrow = pl.ds(pl.multiple_of(hp * 64, 64), 64)
                ls = None
                acc = None
            for j in range(T // MC):
                r = slice(j * MC, (j + 1) * MC)
                if h is not None:
                    s = mm(jnp.concatenate([k_s[r, pair], ak_ref[r, 0:16]], axis=1), rhs)
                    s_scr[slot, r, :] = s
                    t = jnp.max(s.reshape(MC // 8, 8, QT), axis=0)
                    mx = t if mx is None else jnp.maximum(mx, t)
                if hp is not None:
                    pr = jnp.exp2((s_scr[pslot, r, :] - m) * c)
                    t = jnp.sum(pr.reshape(MC // 8, 8, QT), axis=0)
                    ls = t if ls is None else ls + t
                    dd = mm(vt_s[vrow, r], pr.astype(BF16))
                    acc = dd if acc is None else acc + dd
            if h is not None:
                mx_scr[slot] = mx
            if hp is not None:
                half = hp // hh
                hl = hp - half * hh
                part[chip, half, pl.ds(pl.multiple_of(hl * 64, 64), 64), :] = acc
                part[chip, half, pl.ds(HR + hl, 1), :] = m
                part[chip, half, pl.ds(HR + 8 + hl, 1), :] = jnp.sum(ls, axis=0, keepdims=True)

        step(0, 0, None, None)
        if hc > 2:
            def pair_steps(i, carry):
                step(2 * i + 1, 1, 2 * i, 0)
                step(2 * i + 2, 0, 2 * i + 1, 1)
                return carry
            lax.fori_loop(0, hc // 2 - 1, pair_steps, 0)
        step(hc - 1, 1, hc - 2, 0)
        step(None, None, hc - 1, 1)

    def merge(dst, src):
        for hl in range(hh):
            m1, l1 = stats(dst, hl)
            m2, l2 = stats(src, hl)
            m = jnp.maximum(m1, m2)
            a = jnp.exp2((m1 - m) * c)
            b = jnp.exp2((m2 - m) * c)
            rr = slice(hl * 64, (hl + 1) * 64)
            dst[rr, :] = dst[rr, :] * a + src[rr, :] * b
            dst[HR + hl:HR + hl + 1, :] = m
            dst[HR + 8 + hl:HR + 9 + hl, :] = l1 * a + l2 * b

    def rs_desc(d, half, o):
        chip = ring.chip(sgn[d] * o)
        return remote(part.at[chip, half], rbuf.at[d, half, o - 1], rss.at[d, half, o - 1], rrs.at[d, half, o - 1], ring.next[d])

    def rs_recv(d, half, o):
        slot = rbuf.at[d, half, o]
        return remote(slot, slot, rss.at[d, half, o], rrs.at[d, half, o], ring.next[d])

    def rs_step(d, o):
        for half in ((0, 1) if d == RIGHT else (1, 0)):
            n = hops[d, half]
            if o > n:
                continue
            if o < n:
                rs_recv(d, half, o).wait_recv()
                merge(part.at[ring.chip(sgn[d] * o), half], rbuf.at[d, half, o])
            rs_desc(d, half, o).start()

    order = [0, 1, half_chips]
    for o in range(half_chips - 1, 1, -1):
        order += [o, -o]
    order += [-1]
    n = len(order)

    def ready(off):
        if off == 0:
            for s in range(2):
                own_recv(s).wait_recv()
            return
        for s in range(2):
            for d in (RIGHT, LEFT):
                t = -off * sgn[d] if off != half_chips else half_chips
                if 1 <= t <= hops[d, s] and (off == half_chips or t == abs(off)):
                    fw_recv(d, s, t).wait_recv()

    def body(i, carry):
        off = jnp.int32(order[-1])
        for kk in range(n - 1):
            off = jnp.where(i == kk, order[kk], off)
        for kk in range(n):
            @pl.when(i == kk)
            def _(kk=kk):
                if kk == 2:
                    for t in range(3, half_chips + 1):
                        serve(t)
                ready(order[kk])
        flash(ring.chip(off))
        for kk in range(2, n):
            @pl.when(i == kk)
            def _(kk=kk):
                o = order[kk]
                if o == half_chips:
                    rs_step(RIGHT, o); rs_step(LEFT, o)
                elif o > 0:
                    rs_step(RIGHT, o)
                elif o == -2:
                    rs_step(LEFT, 2); rs_step(RIGHT, 1)
                else:
                    rs_step(LEFT, -o)
        return carry
    lax.fori_loop(0, n, body, 0)

    for half in range(2):
        for d in (RIGHT, LEFT):
            rs_recv(d, half, 0).wait_recv()
            merge(part.at[z, half], rbuf.at[d, half, 0])
    for h in range(hc):
        half, hl = h // hh, h % hh
        m, l = stats(part.at[z, half], hl)
        own[h * 64:(h + 1) * 64, :] = part[z, half, hl * 64:(hl + 1) * 64, :] / l
        own[inner + h:inner + h + 1, :] = m + jnp.log2(l) / c
    qmine = pl.ds(pl.multiple_of(core * rows, rows), rows)
    qother = pl.ds(pl.multiple_of((1 - core) * rows, rows), rows)
    xo = remote(own.at[:, qother], pown, xss.at[3], xrs.at[3], ring.partner)
    xo.start()
    yall_ref[...] = yg[...].reshape(chips * QT, dim)
    hrow = pl.ds(pl.multiple_of(core * inner, inner), inner)
    orow = pl.ds(pl.multiple_of((1 - core) * inner, inner), inner)
    att_ref[hrow, :] = own[:inner, qmine]
    lse_ref[core] = own[inner:inner + 8, qmine]
    xo.wait()
    att_ref[orow, :] = pown[:inner, :]
    lse_ref[1 - core] = pown[inner:inner + 8, :]
    mcopy().wait_send()
    for s in range(2):
        own_desc(s).wait_send()
    for (d, s), nh in hops.items():
        for t in range(1, nh + 1):
            ag_desc(d, s, t).wait_send()
            fw_desc(d, s, t).wait_send()
            rs_desc(d, s, t).wait_send()

def fwd_call(dims, y, memory, ak, wq, wk, wv, gain):
    chips, rows, mem, dim, hc, c = dims
    hh = hc // 2; inner = hc * 64; QT = 2 * rows; T = 2 * mem; HR = hh * 64; h2 = chips // 2
    dma = pltpu.SemaphoreType.DMA
    v = pl.BlockSpec(memory_space=VMEM)
    return pl.pallas_call(
        functools.partial(fwd_kernel, dims),
        out_shape=(jax.ShapeDtypeStruct((chips * QT, dim), BF16), jax.ShapeDtypeStruct((2 * inner, rows), F32), jax.ShapeDtypeStruct((2, 8, rows), F32)),
        in_specs=[v] * 7, out_specs=(v,) * 3,
        scratch_shapes=[
            VMEM((chips, 2, 2, rows // 2, dim), BF16), VMEM((mem, dim), BF16), VMEM((inner, dim), BF16),
            VMEM((T, inner), BF16), VMEM((inner, T), BF16), VMEM((hc * 128, QT), BF16),
            VMEM((2, T, QT), F32), VMEM((2, 8, QT), F32), VMEM((chips, 2, HR + 16, QT), F32), VMEM((2, 2, h2, HR + 16, QT), F32),
            VMEM((inner + 8, QT), F32), VMEM((inner + 8, rows), F32),
            dma((2, 2, h2)), dma((2, 2, h2)), dma((2, 2, h2)), dma((2, 2, h2)), dma((4,)), dma((4,)), dma((2, 2, h2)), dma((2, 2, h2))],
        compiler_params=pltpu.CompilerParams(vmem_limit_bytes=60 * 1024 * 1024, collective_id=0, has_side_effects=True),
        cost_estimate=pl.CostEstimate(flops=10**10, bytes_accessed=30 << 20, transcendentals=0),
        name="attn_fwd")(y, memory, ak, wq, wk, wv, gain)


def bwd_kernel(heads, mem, queries, c, k_ref, v_ref, ak_ref, kt_ref, qz_ref, aq_ref, doz_ref, ad_ref, dkt_ref, dvt_ref, dqt_ref):
    nq = queries // QT
    nm = mem // MC
    dkt_ref[...] = jnp.zeros_like(dkt_ref)
    dvt_ref[...] = jnp.zeros_like(dvt_ref)

    def body(it, carry):
        h = it // nq
        qc = it - h * nq
        pair = h // 2
        qs = pl.ds(pl.multiple_of(qc * QT, QT), QT)
        hz = pl.ds(pl.multiple_of(h * 128, 128), 128)
        h64 = pl.ds(pl.multiple_of(h * 64, 64), 64)
        h16 = pl.ds(pl.multiple_of(h * 16, 16), 16)
        ps = pl.ds(pl.multiple_of(pair * 128, 128), 128)
        hz64 = pl.ds(pl.multiple_of(h * 128 + (h - 2 * pair) * 64, 64), 64)
        q_t = qz_ref[hz64, qs]
        do_t = doz_ref[hz64, qs]
        r1 = jnp.concatenate([qz_ref[hz, qs], aq_ref[h16, qs]], axis=0)
        r2 = jnp.concatenate([doz_ref[hz, qs], ad_ref[h16, qs]], axis=0)
        stage = {}
        dq = None
        for j in range(nm + 2):
            if j < nm:
                rows = slice(j * MC, (j + 1) * MC)
                ak = ak_ref[rows, 0:16]
                stage["a", j] = (mm(jnp.concatenate([k_ref[rows, ps], ak], axis=1), r1),
                                 mm(jnp.concatenate([v_ref[rows, ps], ak], axis=1), r2))
            if 1 <= j <= nm:
                s, dp = stage.pop(("a", j - 1))
                a = jnp.exp2(s * c)
                stage["b", j - 1] = (a.astype(BF16), (a * dp).astype(BF16))
            if j >= 2:
                rows = slice((j - 2) * MC, (j - 1) * MC)
                pb, ds = stage.pop(("b", j - 2))
                dvt_ref[h64, rows] += mm_bt(do_t, pb)
                dkt_ref[h64, rows] += mm_bt(q_t, ds)
                d = mm(kt_ref[h64, rows], ds)
                dq = d if dq is None else dq + d
        dqt_ref[h64, qs] = dq
        return carry

    lax.fori_loop(0, heads * nq, body, 0)


def vspec(n):
    return [pl.BlockSpec(memory_space=VMEM)] * n


def params():
    return pltpu.CompilerParams(vmem_limit_bytes=60 * 1024 * 1024)


def solution(mesh):
    group = mesh.shape['seq']
    row_spec = P(('data', 'seq'), None)
    part_vec = P('data')
    part_mat = P('data', None)
    part_cube = P('data', None, None)

    def device_step(dec_in, memory, mem_len, grad_out, norm_attn, wq, wk, wv, wo, norm_mlp, w_gate, w_up, w_down):
        rows, dim = dec_in.shape
        mem = memory.shape[0]
        heads, hd = wq.shape[1], wq.shape[2]
        inner = heads * hd
        queries = rows * group
        c = LOG2E * hd ** -0.5
        wq2, wk2, wv2 = (w.reshape(dim, inner) for w in (wq, wk, wv))
        wo2 = wo.reshape(inner, dim)
        gain1 = norm_attn.astype(F32)
        gain2 = norm_mlp.astype(F32)

        go_all = lax.all_gather(grad_out.astype(BF16), 'seq', axis=0, tiled=True)
        chips = group // 2
        seq = lax.axis_index('seq')
        lane = jnp.arange(128)

        def aux_lanes(start, count):
            pos = start + jnp.arange(count)
            bias = jnp.where(pos < mem_len[0], 0.0, -1e30).astype(F32)
            return jnp.where(lane[None, :] == 0, bias[:, None], jnp.where(lane[None, :] < 4, 1.0, 0.0)).astype(BF16)

        y_all, att_t, lse2 = fwd_call((chips, rows, mem, dim, heads // 2, c), dec_in, memory, aux_lanes((seq // 2) * 2 * mem, 2 * mem),
                                      wq2, wk2, wv2, gain1[None, :])
        attended_f = att_t.T
        attended = attended_f.astype(BF16)
        lse = jnp.concatenate([lse2[0, :heads // 2], lse2[1, :heads // 2]], axis=0).T
        x_all = y_all.astype(F32)
        n1_all = rms_norm(x_all, gain1).astype(BF16)
        q_t = lax.dot_general(wq2, n1_all, (((0,), (1,)), ((), ())), preferred_element_type=F32).astype(BF16)

        def pair_pad(t):
            t = t.reshape(heads // 2, 2, hd, queries)
            zero = jnp.zeros_like(t[:, 0])
            return jnp.stack([t[:, 0], zero, zero, t[:, 1]], axis=1).reshape(heads * 128, queries)

        qz = pair_pad(q_t)
        mem_k = mm(memory, wk2).astype(BF16)
        mem_v = mm(memory, wv2).astype(BF16)
        k_t = mem_k.T
        ak = aux_lanes(seq * mem, mem)

        x_in = dec_in.astype(F32)
        hidden = (x_in + mm(attended, wo2)).astype(BF16)
        n2_f, n2_pull = jax.vjp(rms_norm, hidden.astype(F32), gain2)
        n2 = n2_f.astype(BF16)
        gate_pre = mm(n2, w_gate)
        up_pre = mm(n2, w_up)
        _, gated_pull = jax.vjp(gated_unit, gate_pre, up_pre)
        grad_act = mm_bt(grad_out.astype(BF16), w_down)
        grad_gate, grad_up = gated_pull(grad_act)
        grad_n2 = mm_bt(grad_gate.astype(BF16), w_gate) + mm_bt(grad_up.astype(BF16), w_up)
        grad_h_norm, g_norm_mlp_part = n2_pull(grad_n2)
        grad_hidden = grad_out + grad_h_norm
        dh = grad_hidden.astype(BF16)
        d_att = mm_bt(dh, wo2)
        delta = jnp.sum((d_att * attended_f).reshape(rows, heads, hd), axis=-1)

        stats = jnp.concatenate(split3(-lse) + split3(-delta) + (jnp.zeros((rows, 128 - 6 * heads), BF16),), axis=1)
        gn = jnp.stack(split3(g_norm_mlp_part) + (jnp.zeros((dim,), BF16),) * 13)
        payload = jnp.concatenate([jnp.concatenate([dh, stats], axis=1), jnp.concatenate([gn, jnp.zeros((16, 128), BF16)], axis=1)], axis=0)
        gathered = lax.all_gather(payload, 'seq', axis=0, tiled=False)
        dh_all = gathered[:, :rows, :dim].reshape(queries, dim)
        st = gathered[:, :rows, dim:dim + 6 * heads].reshape(queries, 6, heads).transpose(2, 1, 0)
        g_norm_mlp = jnp.sum(gathered[:, rows:rows + 3, :dim].astype(F32), axis=(0, 1))
        one = jnp.ones((heads, 1, queries), BF16)
        pad = jnp.zeros((heads, 12, queries), BF16)
        aq = jnp.concatenate([one, st[:, 0:3], pad], axis=1).reshape(heads * 16, queries)
        ad = jnp.concatenate([0 * one, st[:, 3:6], pad], axis=1).reshape(heads * 16, queries)
        doz = pair_pad(mm_bt(wo2, dh_all).astype(BF16))

        dk_t, dv_t, dq_t = pl.pallas_call(
            functools.partial(bwd_kernel, heads, mem, queries, c),
            out_shape=(jax.ShapeDtypeStruct((inner, mem), F32), jax.ShapeDtypeStruct((inner, mem), F32), jax.ShapeDtypeStruct((inner, queries), F32)),
            in_specs=vspec(8), out_specs=tuple(vspec(3)),
            compiler_params=params(),
            cost_estimate=pl.CostEstimate(flops=10 * heads * mem * queries * 256, bytes_accessed=40 << 20, transcendentals=0),
            name="attn_bwd")(mem_k, mem_v, ak, k_t, qz, aq, doz, ad)
        att_all = lax.all_gather(attended, 'seq', axis=0, tiled=True)
        score_scale = hd ** -0.5
        dq = lax.psum_scatter(dq_t.T, 'seq', scatter_dimension=0, tiled=True) * score_scale
        dq_b = dq.astype(BF16)
        dq_all = lax.all_gather(dq_b, 'seq', axis=0, tiled=True)
        dkb = (dk_t * score_scale).astype(BF16)
        dvb = dv_t.astype(BF16)
        dkv = jnp.concatenate([dkb, dvb], axis=0)
        g_wkv = lax.psum(lax.dot_general(dkv, memory, (((1,), (0,)), ((), ())), preferred_element_type=F32), 'seq').T
        g_mem = lax.dot_general(dkv, jnp.concatenate([wk2, wv2], axis=1), (((0,), (1,)), ((), ())), preferred_element_type=F32)

        _, norm_pull = jax.vjp(rms_norm, x_in, gain1)
        grad_x_norm, _ = norm_pull(mm_bt(dq_b, wq2))
        g_dec = grad_hidden + grad_x_norm

        xhat = x_all * lax.rsqrt(jnp.mean(x_all * x_all, axis=-1, keepdims=True) + 1e-6)
        g_norm_attn = jnp.sum(mm_bt(dq_all, wq2) * xhat, axis=0)
        g_wq = mm_at(n1_all, dq_all)
        g_wo = mm_at(att_all, dh_all)
        h_all = (x_all + mm(att_all, wo2)).astype(BF16)
        n2_all = rms_norm(h_all.astype(F32), gain2).astype(BF16)
        mlp_f, pull_all = jax.vjp(gated_unit, mm(n2_all, w_gate), mm(n2_all, w_up))
        gg, gu = pull_all(mm_bt(go_all, w_down))
        g_down = mm_at(mlp_f.astype(BF16), go_all)
        g_gate = mm_at(n2_all, gg.astype(BF16))
        g_up = mm_at(n2_all, gu.astype(BF16))
        cube = (dim, heads, hd)
        return (g_dec, g_mem, g_norm_attn, g_wq.reshape(cube), g_wkv[:, :inner].reshape(cube), g_wkv[:, inner:].reshape(cube),
                g_wo.reshape(heads, hd, dim), g_norm_mlp, g_gate, g_up, g_down)

    return jax.shard_map(device_step, mesh=mesh,
                         in_specs=(row_spec, row_spec, part_vec, row_spec) + (P(),) * 9,
                         out_specs=(row_spec, row_spec, part_vec, part_cube, part_cube, part_cube, part_cube, part_vec, part_mat, part_mat, part_mat),
                         check_vma=False)
```

```python
import functools
import math

import jax
import jax.numpy as jnp
from jax import lax
from jax.experimental import pallas as pl
from jax.experimental.pallas import tpu as pltpu
from jax.sharding import PartitionSpec as P

F32 = jnp.float32
BF16 = jnp.bfloat16
LOG2E = math.log2(math.e)
VMEM = pltpu.VMEM
MESH = pl.DeviceIdType.MESH


def mm(a, b):
    return jnp.dot(a, b, preferred_element_type=F32)


def mm_bt(a, b):
    return lax.dot_general(a, b, (((1,), (1,)), ((), ())), preferred_element_type=F32)


def mm_at(a, b):
    return lax.dot_general(a, b, (((0,), (0,)), ((), ())), preferred_element_type=F32)


def rms_norm(tensor, gain):
    mean_sq = jnp.mean(tensor * tensor, axis=-1, keepdims=True)
    return tensor * lax.rsqrt(mean_sq + 1e-6) * gain


def gated_unit(gate_pre, up_pre):
    return jax.nn.silu(gate_pre) * up_pre


RIGHT, LEFT = 0, 1
DMA = pltpu.SemaphoreType.DMA


class Ring:
    def __init__(self, chips):
        me = lax.axis_index('seq')
        self.chips = chips
        self.far = chips // 2
        self.z = me // 2
        self.core = me - 2 * self.z
        self.partner = 2 * self.z + 1 - self.core
        self.next = (2 * self.chip(1) + self.core, 2 * self.chip(-1) + self.core)
        self.hops = {(RIGHT, 0): self.far, (LEFT, 1): self.far, (RIGHT, 1): self.far - 1, (LEFT, 0): self.far - 1}

    def chip(self, off):
        return lax.rem(self.z + off + self.chips, self.chips)

    def ahead(self, d, k):
        return self.chip(k if d == RIGHT else -k)

    def enter(self):
        barrier = pltpu.get_barrier_semaphore()
        for dev in (self.partner,) + self.next:
            pl.semaphore_signal(barrier, inc=1, device_id={'seq': dev}, device_id_type=MESH)
        pl.semaphore_wait(barrier, 3)


def remote(src, dst, ssem, rsem, dev):
    return pltpu.make_async_remote_copy(src_ref=src, dst_ref=dst, send_sem=ssem, recv_sem=rsem, device_id={'seq': dev}, device_id_type=MESH)


class Share:
    def __init__(self, ring, buf, src, sems):
        self.ring, self.buf, self.src = ring, buf, src
        self.ss, self.rs = sems

    def slot(self, chip, half):
        return self.buf.at[chip, half]

    def send(self, d, half, t):
        slot = self.slot(self.ring.ahead(d, 1 - t), half)
        src = self.src(half) if t == 1 else slot
        return remote(src, slot, self.ss.at[d, half, t - 1], self.rs.at[d, half, t - 1], self.ring.next[d])

    def recv(self, d, half, t):
        slot = self.slot(self.ring.ahead(d, -t), half)
        return remote(slot, slot, self.ss.at[d, half, t - 1], self.rs.at[d, half, t - 1], self.ring.next[d])

    def start(self):
        for d, half in self.ring.hops:
            self.send(d, half, 1).start()

    def came(self, d, half, t):
        pass

    def serve(self, t):
        for (d, half), n in self.ring.hops.items():
            if t <= n:
                self.recv(d, half, t).wait_recv()
                if t < n:
                    self.send(d, half, t + 1).start()
                self.came(d, half, t)

    def drain(self):
        for (d, half), n in self.ring.hops.items():
            for t in range(1, n + 1):
                self.send(d, half, t).wait_send()


class Rows(Share):
    def __init__(self, ring, buf, src, sems):
        super().__init__(ring, buf, src, sems[:2])
        self.fs, self.fr, self.os, self.orr = sems[2:]

    def slot(self, chip, half):
        return self.buf.at[chip, self.ring.core, half]

    def pslot(self, chip, half):
        return self.buf.at[chip, 1 - self.ring.core, half]

    def start(self):
        super().start()
        for half in range(2):
            self.own(half).start()

    def own(self, half):
        return remote(self.src(half), self.slot(self.ring.z, half), self.os.at[half], self.orr.at[half], self.ring.partner)

    def forward(self, d, half, t):
        slot = self.slot(self.ring.ahead(d, -t), half)
        return remote(slot, slot, self.fs.at[d, half, t - 1], self.fr.at[d, half, t - 1], self.ring.partner)

    def came(self, d, half, t):
        self.forward(d, half, t).start()

    def ready(self, off):
        ring = self.ring
        if off == 0:
            for half in range(2):
                slot = self.pslot(ring.z, half)
                remote(slot, slot, self.os.at[half], self.orr.at[half], ring.partner).wait_recv()
            return
        for (d, half), n in ring.hops.items():
            t = ring.far if abs(off) == ring.far else (-off if d == RIGHT else off)
            if 1 <= t <= n:
                slot = self.pslot(ring.ahead(d, -t), half)
                remote(slot, slot, self.fs.at[d, half, t - 1], self.fr.at[d, half, t - 1], ring.partner).wait_recv()

    def drain(self):
        super().drain()
        for half in range(2):
            self.own(half).wait_send()
        for (d, half), n in self.ring.hops.items():
            for t in range(1, n + 1):
                self.forward(d, half, t).wait_send()


class Reduce:
    def __init__(self, ring, part, rbuf, merge, sems):
        self.ring, self.part, self.rbuf, self.merge = ring, part, rbuf, merge
        self.ss, self.rs = sems

    def send(self, d, half, o):
        return remote(self.part.at[self.ring.ahead(d, o), half], self.rbuf.at[d, half, o - 1], self.ss.at[d, half, o - 1], self.rs.at[d, half, o - 1], self.ring.next[d])

    def recv(self, d, half, o):
        slot = self.rbuf.at[d, half, o]
        return remote(slot, slot, self.ss.at[d, half, o], self.rs.at[d, half, o], self.ring.next[d])

    def step(self, d, o):
        for half in ((0, 1) if d == RIGHT else (1, 0)):
            n = self.ring.hops[d, half]
            if o > n:
                continue
            if o < n:
                self.recv(d, half, o).wait_recv()
                self.merge(self.part.at[self.ring.ahead(d, o), half], self.rbuf.at[d, half, o])
            self.send(d, half, o).start()

    def both(self, o):
        self.step(RIGHT, o)
        self.step(LEFT, o)

    def final(self):
        for half in range(2):
            for d in (RIGHT, LEFT):
                self.recv(d, half, 0).wait_recv()
                self.merge(self.part.at[self.ring.z, half], self.rbuf.at[d, half, 0])

    def drain(self):
        for (d, half), n in self.ring.hops.items():
            for o in range(1, n + 1):
                self.send(d, half, o).wait_send()


def pick(i, values):
    out = jnp.int32(values[-1])
    for k, v in enumerate(values[:-1]):
        out = jnp.where(i == k, jnp.int32(v), out)
    return out


def add_into(dst, src):
    dst[...] = dst[...] + src[...]


def parts3(x):
    hi = x.astype(BF16)
    rest = x - hi.astype(F32)
    mid = rest.astype(BF16)
    lo = (rest - mid.astype(F32)).astype(BF16)
    return hi, mid, lo


def bwd_kernel(dims, dh_ref, own_ref, gn_ref, att_ref, go_ref, k_ref, v_ref, kt_ref, qz_ref, ak_ref, ma_ref, mb_ref, y_ref, wo_ref, wq_ref, wk_ref, wv_ref, g1_ref,
               gmem_ref, gwkv_ref, gwq_ref, gvec_ref, dqo_ref, attg, gog, dho,
               dhg, doz, aqs, ads, stb, dk, dv, dkv, dkvp, dqp, dqr, dqa, arp, arr, ara, pvec, pdq, spb,
               *sems):
    chips, rows, mem, dim, hc, c = dims
    QT = 2 * rows
    T = 2 * mem
    MC = min(256, mem)
    nm = T // MC
    inner = hc * 64
    np_ = hc // 2
    seg = 256 // chips // 2
    ring = Ring(chips)
    z, core, far = ring.z, ring.core, ring.far
    sems = list(sems)

    def take(n):
        out = sems[:n]
        del sems[:n]
        return out

    half_rows = rows // 2
    rsrc = lambda ref: (lambda half: ref.at[pl.ds(half * half_rows, half_rows)])
    dh_g = Rows(ring, dhg, rsrc(dh_ref), take(6))
    att_g = Rows(ring, attg, rsrc(att_ref), take(6))
    go_g = Rows(ring, gog, rsrc(go_ref), take(6))
    st_g = Share(ring, stb, lambda half: stb.at[z, half], take(2))
    dq_r = [Reduce(ring, dqp.at[p], dqr.at[p], add_into, take(2)) for p in range(np_)]
    dq_s = [Share(ring, dqa.at[p], lambda half, p=p: dqa.at[p, z, half], take(2)) for p in range(np_)]
    ar_r = [Reduce(ring, arp.at[p], arr.at[p], add_into, take(2)) for p in range(np_)]
    ar_s = [Share(ring, ara.at[p], lambda half, p=p: ara.at[p, z, half], take(2)) for p in range(np_)]
    xs, xr, ls = take(3)
    ring.enter()
    dh_g.start()
    locals_ = []
    for n, (ref, buf) in enumerate(((att_ref, attg), (go_ref, gog))):
        for half in range(2):
            cp = pltpu.make_async_copy(ref.at[pl.ds(half * half_rows, half_rows)], buf.at[z, core, half], ls.at[2 * n + half])
            cp.start()
            locals_.append(cp)
    for half in range(2):
        dhg[z, core, half] = dh_ref[half * half_rows:(half + 1) * half_rows, :]
    doz[...] = jnp.zeros_like(doz)
    hrow = pl.ds(pl.multiple_of(core * inner, inner), inner)
    orow = pl.ds(pl.multiple_of((1 - core) * inner, inner), inner)
    wo_h = wo_ref[hrow, :]

    def d_out(chip):
        return mm_bt(wo_h, dhg[chip].reshape(QT, dim))

    def lanes(chip):
        return pl.ds(pl.multiple_of(chip * QT, QT), QT)

    def prepare(chip, dot=None):
        dot = d_out(chip) if dot is None else dot
        dob = dot.astype(BF16)
        q = lanes(chip)
        row = lax.broadcasted_iota(jnp.int32, (16, QT), 0)
        for h in range(hc):
            lo = h * 128 + (h % 2) * 64
            doz[lo:lo + 64, q] = dob[h * 64:(h + 1) * 64]
            for ref, half, first in ((aqs, 0, 1.0), (ads, 1, 0.0)):
                a, b, e = (x.astype(F32) for x in parts3(stb[chip, half, h:h + 1, :]))
                ref[h * 16:(h + 1) * 16, q] = jnp.where(row == 0, first, jnp.where(row == 1, a, jnp.where(row == 2, b, jnp.where(row == 3, e, 0.0)))).astype(BF16)

    dh_g.ready(0)
    dot0 = d_out(z)
    prod = dot0 * own_ref[:inner, :]
    for h in range(hc):
        stb[z, 0, h:h + 1, :] = -own_ref[inner + h:inner + h + 1, :]
        stb[z, 1, h:h + 1, :] = -jnp.sum(prod[h * 64:(h + 1) * 64], axis=0, keepdims=True)
    stb[z, 0, hc:8, :] = gn_ref[0:8 - hc, :]
    stb[z, 1, hc:8, :] = gn_ref[8 - hc:16 - 2 * hc, :]
    st_g.start()
    prepare(z, dot0)

    def tile(h, chip, p, hl):
        q = lanes(chip)
        hz = pl.ds(pl.multiple_of(h * 128, 128), 128)
        h16 = pl.ds(pl.multiple_of(h * 16, 16), 16)
        ps = slice(p * 128, (p + 1) * 128)
        hr = pl.ds(pl.multiple_of(hl * 64, 64), 64)
        hz64 = pl.ds(pl.multiple_of(h * 128 + hl * 64, 64), 64)
        h64 = pl.ds(pl.multiple_of(h * 64, 64), 64)
        q_t = qz_ref[hz64, q]
        do_t = doz[hz64, q]
        r1 = jnp.concatenate([qz_ref[hz, q], aqs[h16, q]], axis=0)
        r2 = jnp.concatenate([doz[hz, q], ads[h16, q]], axis=0)
        stage = {}
        dq = None
        for j in range(nm + 2):
            if j < nm:
                r = slice(j * MC, (j + 1) * MC)
                ak = ak_ref[r, 0:16]
                stage["a", j] = (mm(jnp.concatenate([k_ref[r, ps], ak], axis=1), r1), mm(jnp.concatenate([v_ref[r, ps], ak], axis=1), r2))
            if 1 <= j <= nm:
                s, dp = stage.pop(("a", j - 1))
                a = jnp.exp2(s * c)
                stage["b", j - 1] = (a.astype(BF16), (a * dp).astype(BF16))
            if j >= 2:
                r = slice((j - 2) * MC, (j - 1) * MC)
                pb, ds = stage.pop(("b", j - 2))
                dv[hr, r] += mm_bt(do_t, pb)
                dk[hr, r] += mm_bt(q_t, ds)
                d = mm(kt_ref[h64, r], ds)
                dq = d if dq is None else dq + d
        dqp[p, chip, hl] = dq

    near = [0]
    for o in range(1, far):
        near += [o, -o]
    near += [far]
    far_first = [far] + [s * o for o in range(far - 1, 0, -1) for s in (1, -1)] + [0]
    scale = 0.125

    def run_pair(p, order, before, after):
        dk[...] = jnp.zeros_like(dk)
        dv[...] = jnp.zeros_like(dv)

        def body(i, carry):
            chip = ring.chip(pick(i, order))
            for kk, fn in sorted(before.items()):
                pl.when(i == kk)(functools.partial(fn, chip))
            lax.fori_loop(0, 2, lambda hl, cc: (tile(2 * p + hl, chip, p, hl), cc)[1], 0)
            for kk, fn in sorted(after.items()):
                pl.when(i == kk)(fn)
            return carry

        lax.fori_loop(0, chips, body, 0)
        dkb = (dk[...] * scale).astype(BF16)
        dvb = dv[...].astype(BF16)
        dkv[p, 0:128, :] = dkb
        dkv[p, 128:256, :] = dvb
        xp(p).start()
        for part in range(2):
            mine = pl.ds(pl.multiple_of(core * mem, mem), mem)
            other = pl.ds(pl.multiple_of((1 - core) * mem, mem), mem)
            g = mm(dkv[p, part * 128:(part + 1) * 128, mine], ma_ref[...]) + mm(dkv[p, part * 128:(part + 1) * 128, other], mb_ref[...])
            for n in range(128 // seg):
                row = part * 128 + n * seg
                arp[p, row // (2 * seg), (row // seg) % 2] = g[n * seg:(n + 1) * seg]

    other_cols = pl.ds(pl.multiple_of((1 - core) * mem, mem), mem)
    my_cols = pl.ds(pl.multiple_of(core * mem, mem), mem)

    def xp(p):
        return remote(dkv.at[p, :, other_cols], dkvp.at[p], xs.at[p], xr.at[p], ring.partner)

    def gate(off, t=None):
        def fn(chip):
            if t is not None:
                dh_g.serve(t)
                st_g.serve(t)
            dh_g.ready(off)
            prepare(chip)
        return fn

    before0 = {}
    for n, off in enumerate(near):
        if off:
            before0[n] = gate(off, abs(off) if off > 0 else None)
    run_pair(0, near, before0, {})

    def seq(*fns):
        def run(*_):
            for f in fns:
                f()
        return run

    part_ = functools.partial
    def bg_reduce(p, base):
        ev = {}
        for n, o in enumerate(range(far, 0, -1)):
            ev.setdefault(2 * n, []).extend([part_(dq_r[p].both, o), part_(ar_r[p].both, o)])
        return ev

    def finish_reduce(p):
        dq_r[p].final()
        ar_r[p].final()
        for half in range(2):
            dqa[p, z, half] = (dqp[p, z, half] * scale).astype(BF16)
            ara[p, z, half] = arp[p, z, half]
        dq_s[p].start()
        ar_s[p].start()
        xq(p).start()

    qother = pl.ds(pl.multiple_of((1 - core) * rows, rows), rows)

    def xq(p):
        return remote(dqa.at[p, z, :, :, qother], pdq.at[p], xs.at[np_ + p], xr.at[np_ + p], ring.partner)

    def merged(*evs):
        out = {}
        for ev in evs:
            for kk, fns in ev.items():
                out.setdefault(kk, []).extend(fns)
        return {kk: seq(*fns) for kk, fns in out.items()}

    def spread(g):
        return {2 * t - 1: [part_(g.serve, t)] for t in range(1, far + 1)}

    cp = pltpu.make_async_copy(dhg, dho, ls.at[4])
    cp.start()
    locals_.append(cp)
    att_g.start()
    run_pair(1, far_first, {}, merged(bg_reduce(0, 0), spread(att_g)))
    finish_reduce(0)
    go_g.start()
    tail = {0: [part_(dq_s[0].serve, 1), part_(ar_s[0].serve, 1)], 2: [part_(dq_s[0].serve, 2), part_(ar_s[0].serve, 2)], 4: [part_(dq_s[0].serve, 3), part_(ar_s[0].serve, 3)], 6: [part_(dq_s[0].serve, 4), part_(ar_s[0].serve, 4)]}
    inl = {}
    for n, off in enumerate(far_first):
        if off == far:
            inl[n] = [part_(dq_r[2].both, far)]
        elif off > 0:
            inl[n] = [part_(dq_r[2].step, RIGHT, off)]
        elif off < 0:
            inl[n] = [part_(dq_r[2].step, LEFT, -off)]
    run_pair(2, far_first, {}, merged(bg_reduce(1, 0), tail, spread(go_g), inl))
    finish_reduce(1)
    ar_r[2].both(far)
    dq_r[2].final()
    for half in range(2):
        dqa[2, z, half] = (dqp[2, z, half] * scale).astype(BF16)
    dq_s[2].start()
    xq(2).start()
    for p in range(np_):
        remote(dkvp.at[p], dkvp.at[p], xs.at[p], xr.at[p], ring.partner).wait_recv()
    step_fns = [[part_(ar_r[2].both, 3), part_(dq_s[1].serve, 1), part_(ar_s[1].serve, 1), part_(dq_s[2].serve, 1)],
                [part_(ar_r[2].both, 2), part_(dq_s[1].serve, 2), part_(ar_s[1].serve, 2), part_(dq_s[2].serve, 2)],
                [part_(ar_r[2].both, 1), part_(dq_s[1].serve, 3), part_(ar_s[1].serve, 3), part_(dq_s[2].serve, 3)],
                [part_(dq_s[1].serve, 4), part_(ar_s[1].serve, 4), part_(dq_s[2].serve, 4)]]
    nb = 4
    for b in range(nb):
        w = mem // nb
        cb = pl.ds(pl.multiple_of(core * mem + b * w, w), w)
        acc = None
        for p in range(np_):
            for part, w_ref in ((0, wk_ref), (1, wv_ref)):
                own_cols = pl.ds(pl.multiple_of(core * inner + p * 128, 128), 128)
                oth_cols = pl.ds(pl.multiple_of((1 - core) * inner + p * 128, 128), 128)
                e = slice(part * 128, (part + 1) * 128)
                d = mm(jnp.concatenate([w_ref[:, own_cols], w_ref[:, oth_cols]], axis=1),
                       jnp.concatenate([dkv[p, e, cb], dkvp[p, e, b * w:(b + 1) * w]], axis=0))
                acc = d if acc is None else acc + d
        gmem_ref[b * w:(b + 1) * w, :] = acc.T
        for f in step_fns[b]:
            f()
    ar_r[2].final()
    for half in range(2):
        ara[2, z, half] = arp[2, z, half]
    ar_s[2].start()
    gain = g1_ref[...]
    wqt = wq_ref[:, pl.ds(pl.multiple_of(core * inner, 128), inner)].T
    gvec = jnp.zeros((1, dim), F32)
    gvec2 = jnp.zeros((16 - 2 * hc, QT), F32)
    for ch in range(chips):
        x = y_ref[ch * QT:(ch + 1) * QT, :].astype(F32)
        xhat = x * lax.rsqrt(jnp.mean(x * x, axis=-1, keepdims=True) + 1e-6)
        n1 = (xhat * gain).astype(BF16)
        dqc = jnp.concatenate([dqa[p, ch].reshape(128, QT) for p in range(np_)], axis=0)
        dn = mm_at(dqc, wqt)
        d = mm(dqc, n1)
        if ch == 0:
            gwq_ref[core] = d
        else:
            gwq_ref[core] += d
        gvec = gvec + jnp.sum(dn * xhat, axis=0, keepdims=True)
        gvec2 = gvec2 + jnp.concatenate([stb[ch, 0, hc:8, :], stb[ch, 1, hc:8, :]], axis=0)
        if ch % 2 == 1:
            ar_s[2].serve(ch // 2 + 1)
    spb[0:1, :] = gvec
    for n in range(dim // QT):
        spb[1:2, n * QT:(n + 1) * QT] = gvec2[n:n + 1]
    cv = remote(spb, pvec, xs.at[2 * np_], xr.at[2 * np_], ring.partner)
    cq = remote(gwq_ref.at[core], gwq_ref.at[core], xs.at[2 * np_ + 1], xr.at[2 * np_ + 1], ring.partner)
    cv.start()
    cq.start()
    for p in range(np_):
        gwkv_ref[core, p] = ara[p]
    cw = [remote(ara.at[p], gwkv_ref.at[core, p], xs.at[2 * np_ + 2 + p], xr.at[2 * np_ + 2 + p], ring.partner) for p in range(np_)]
    for p in range(np_):
        cw[p].start()
    qmine = pl.ds(pl.multiple_of(core * rows, rows), rows)
    for p in range(np_):
        own_r = pl.ds(pl.multiple_of(core * inner + p * 128, 128), 128)
        oth_r = pl.ds(pl.multiple_of((1 - core) * inner + p * 128, 128), 128)
        dqo_ref[own_r, :] = dqa[p, z, :, :, qmine].reshape(128, rows)
        xq(p).wait()
        dqo_ref[oth_r, :] = pdq[p].reshape(128, rows)
    cv.wait()
    gvec_ref[...] = spb[0:2] + pvec[0:2]
    cq.wait()
    for p in range(np_):
        cw[p].wait()
        xp(p).wait_send()
    for g in (att_g, go_g):
        for off in near:
            g.ready(off)
    for cp in locals_:
        cp.wait()
    for obj in [dh_g, att_g, go_g, st_g] + dq_r + dq_s + ar_r + ar_s:
        obj.drain()


def bwd_call(dims, *args):
    chips, rows, mem, dim, hc, c = dims
    inner = hc * 64
    QT = 2 * rows
    T = 2 * mem
    np_ = hc // 2
    h2 = chips // 2
    seg = 256 // chips // 2
    v = pl.BlockSpec(memory_space=VMEM)
    hbm = pl.BlockSpec(memory_space=pl.ANY)
    s3 = (2, 2, h2)
    rows_sems = [DMA(s3)] * 4 + [DMA((2,))] * 2
    two = [DMA(s3)] * 2
    S = jax.ShapeDtypeStruct
    gshape = (chips, 2, 2, rows // 2, dim)
    return pl.pallas_call(
        functools.partial(bwd_kernel, dims),
        out_shape=(S((mem, dim), F32), S((2, np_, chips, 2, seg, dim), F32), S((2, inner, dim), F32), S((2, dim), F32), S((2 * inner, rows), BF16), S(gshape, BF16), S(gshape, BF16), S(gshape, BF16)),
        in_specs=[v] * 18, out_specs=(v,) * 5 + (hbm,) * 3,
        scratch_shapes=[
            VMEM(gshape, BF16), VMEM((hc * 128, chips * QT), BF16), VMEM((hc * 16, chips * QT), BF16), VMEM((hc * 16, chips * QT), BF16),
            VMEM((chips, 2, 8, QT), F32), VMEM((128, T), F32), VMEM((128, T), F32), VMEM((np_, 256, T), BF16), VMEM((np_, 256, mem), BF16),
            VMEM((np_, chips, 2, 64, QT), F32), VMEM((np_, 2, 2, h2, 64, QT), F32), VMEM((np_, chips, 2, 64, QT), BF16),
            VMEM((np_, chips, 2, seg, dim), F32), VMEM((np_, 2, 2, h2, seg, dim), F32), VMEM((np_, chips, 2, seg, dim), F32),
            VMEM((8, dim), F32), VMEM((np_, 2, 64, rows), BF16), VMEM((8, dim), F32)]
        + rows_sems * 3 + two * (1 + 4 * np_) + [DMA((3 * np_ + 2,))] * 2 + [DMA((5,))],
        compiler_params=pltpu.CompilerParams(vmem_limit_bytes=66_900_000, collective_id=1, has_side_effects=True),
        cost_estimate=pl.CostEstimate(flops=10**10, bytes_accessed=30 << 20, transcendentals=0),
        name="attn_bwd")(*args)

def fwd_kernel(dims, y_ref, m_ref, ak_ref, wq_ref, wk_ref, wv_ref, g_ref,
               own, att_ref, k_s, v_s, kt_s, qz, mg, yall,
               yg, wqt, vt_s, s_scr, mx_scr, part, rbuf, patt, satt, *sems):
    chips, rows, mem, dim, hc, c = dims
    QT = 2 * rows
    T = 2 * mem
    MC = min(256, mem)
    hh = hc // 2
    inner = hc * 64
    HR = hh * 64
    ring = Ring(chips)
    z, core, far = ring.z, ring.core, ring.far
    sub = rows // 2
    xs, xr, ls = sems[8:]
    y_g = Rows(ring, yg, lambda half: y_ref.at[pl.ds(half * sub, sub)], sems[:6])

    def merge(dst, src):
        for hl in range(hh):
            mr = slice(HR + hl, HR + hl + 1)
            lr = slice(HR + 8 + hl, HR + 9 + hl)
            m1, m2 = dst[mr, :], src[mr, :]
            m = jnp.maximum(m1, m2)
            a = jnp.exp2((m1 - m) * c)
            b = jnp.exp2((m2 - m) * c)
            rr = slice(hl * 64, (hl + 1) * 64)
            dst[rr, :] = dst[rr, :] * a + src[rr, :] * b
            dst[mr, :] = m
            dst[lr, :] = dst[lr, :] * a + src[lr, :] * b

    o_r = Reduce(ring, part, rbuf, merge, sems[6:8])
    ring.enter()
    y_g.start()
    mx_copy = remote(m_ref, mg, xs.at[0], xr.at[0], ring.partner)
    mx_copy.start()
    for half in range(2):
        yg[z, core, half] = y_ref[half * sub:(half + 1) * sub, :]
    hcol = pl.ds(pl.multiple_of(core * inner, 128), inner)
    qz[...] = jnp.zeros_like(qz)
    wqt[...] = wq_ref[:, hcol].T
    wk = wk_ref[:, hcol]
    wv = wv_ref[:, hcol]

    def project(src, base):
        for j in range(mem // MC):
            r = pl.ds(pl.multiple_of(base + j * MC, MC), MC)
            blk = src[j * MC:(j + 1) * MC, :]
            kb = mm(blk, wk).astype(BF16)
            vb = mm(blk, wv).astype(BF16)
            k_s[r, :] = kb
            v_s[r, :] = vb
            kt_s[:, r] = kb.T
            vt_s[:, r] = vb.T

    project(m_ref, core * mem)
    y_g.serve(1)
    mx_copy.wait_recv()
    project(mg, (1 - core) * mem)
    y_g.serve(2)
    gain = g_ref[...]

    def flash(chip):
        x = yg[chip].reshape(QT, dim).astype(F32)
        n1 = rms_norm(x, gain).astype(BF16)
        qt = mm_bt(wqt[...], n1).astype(BF16)
        q = pl.ds(pl.multiple_of(chip * QT, QT), QT)
        for h in range(hc):
            lo = h * 128 + (h % 2) * 64
            qz[lo:lo + 64, q] = qt[h * 64:(h + 1) * 64]
        one_row = jnp.where(lax.broadcasted_iota(jnp.int32, (16, QT), 0) == 0, 1.0, 0.0).astype(BF16)

        def step(h, slot, hp, pslot):
            if h is not None:
                rhs = jnp.concatenate([qz[pl.ds(pl.multiple_of(h * 128, 128), 128), q], one_row], axis=0)
                pair = pl.ds(pl.multiple_of((h // 2) * 128, 128), 128)
                mx = None
            if hp is not None:
                m = jnp.max(mx_scr[pslot], axis=0, keepdims=True)
                vrow = pl.ds(pl.multiple_of(hp * 64, 64), 64)
                ls_ = None
                acc = None
            for j in range(T // MC):
                r = slice(j * MC, (j + 1) * MC)
                if h is not None:
                    s = mm(jnp.concatenate([k_s[r, pair], ak_ref[r, 0:16]], axis=1), rhs)
                    s_scr[slot, r, :] = s
                    t = jnp.max(s.reshape(MC // 8, 8, QT), axis=0)
                    mx = t if mx is None else jnp.maximum(mx, t)
                if hp is not None:
                    pr = jnp.exp2((s_scr[pslot, r, :] - m) * c)
                    t = jnp.sum(pr.reshape(MC // 8, 8, QT), axis=0)
                    ls_ = t if ls_ is None else ls_ + t
                    dd = mm(vt_s[vrow, r], pr.astype(BF16))
                    acc = dd if acc is None else acc + dd
            if h is not None:
                mx_scr[slot] = mx
            if hp is not None:
                half = hp // hh
                hl = hp - half * hh
                part[chip, half, pl.ds(pl.multiple_of(hl * 64, 64), 64), :] = acc
                part[chip, half, pl.ds(HR + hl, 1), :] = m
                part[chip, half, pl.ds(HR + 8 + hl, 1), :] = jnp.sum(ls_, axis=0, keepdims=True)

        step(0, 0, None, None)
        if hc > 2:
            def pair_steps(i, carry):
                step(2 * i + 1, 1, 2 * i, 0)
                step(2 * i + 2, 0, 2 * i + 1, 1)
                return carry
            lax.fori_loop(0, hc // 2 - 1, pair_steps, 0)
        step(hc - 1, 1, hc - 2, 0)
        step(None, None, hc - 1, 1)

    order = [0, 1, far]
    for o in range(far - 1, 1, -1):
        order += [o, -o]
    order += [-1]

    def body(i, carry):
        for kk, off in enumerate(order):
            def get(kk=kk, off=off):
                if kk == 2:
                    for t in range(3, far + 1):
                        y_g.serve(t)
                y_g.ready(off)
            pl.when(i == kk)(get)
        flash(ring.chip(pick(i, order)))
        for kk, off in enumerate(order):
            if kk < 2:
                continue
            def put(off=off):
                if off == far:
                    o_r.both(far)
                elif off > 0:
                    o_r.step(RIGHT, off)
                else:
                    o_r.step(LEFT, -off)
                    if off == -2:
                        o_r.step(RIGHT, 1)
            pl.when(i == kk)(put)
        return carry

    lax.fori_loop(0, chips, body, 0)
    yc = pltpu.make_async_copy(yg, yall, ls.at[0])
    yc.start()
    o_r.final()
    qmine = pl.ds(pl.multiple_of(core * rows, rows), rows)
    qother = pl.ds(pl.multiple_of((1 - core) * rows, rows), rows)
    for h in range(hc):
        half, hl = h // hh, h % hh
        m = part[z, half, HR + hl:HR + hl + 1, :]
        l = part[z, half, HR + 8 + hl:HR + 9 + hl, :]
        o = part[z, half, hl * 64:(hl + 1) * 64, :] / l
        own[h * 64:(h + 1) * 64, :] = o
        own[inner + h:inner + h + 1, :] = m + jnp.log2(l) / c
    satt[...] = own[:inner, qother].astype(BF16)
    xo = remote(satt, patt, xs.at[1], xr.at[1], ring.partner)
    xo.start()
    att_ref[pl.ds(pl.multiple_of(core * inner, inner), inner), :] = own[:inner, qmine].astype(BF16)
    xo.wait()
    att_ref[pl.ds(pl.multiple_of((1 - core) * inner, inner), inner), :] = patt[...]
    mx_copy.wait_send()
    yc.wait()
    y_g.drain()
    o_r.drain()


def fwd_call(dims, *args):
    chips, rows, mem, dim, hc, c = dims
    hh = hc // 2
    inner = hc * 64
    QT = 2 * rows
    T = 2 * mem
    HR = hh * 64
    h2 = chips // 2
    v = pl.BlockSpec(memory_space=VMEM)
    S = jax.ShapeDtypeStruct
    s3 = (2, 2, h2)
    gshape = (chips, 2, 2, rows // 2, dim)
    return pl.pallas_call(
        functools.partial(fwd_kernel, dims),
        out_shape=(S((inner + 8, QT), F32), S((2 * inner, rows), BF16), S((T, inner), BF16), S((T, inner), BF16), S((inner, T), BF16),
                   S((hc * 128, chips * QT), BF16), S((mem, dim), BF16), S(gshape, BF16)),
        in_specs=[v] * 7, out_specs=(v,) * 7 + (pl.BlockSpec(memory_space=pl.ANY),),
        scratch_shapes=[
            VMEM(gshape, BF16), VMEM((inner, dim), BF16), VMEM((inner, T), BF16), VMEM((2, T, QT), F32), VMEM((2, 8, QT), F32),
            VMEM((chips, 2, HR + 16, QT), F32), VMEM((2, 2, h2, HR + 16, QT), F32), VMEM((inner, rows), BF16), VMEM((inner, rows), BF16)]
        + [DMA(s3)] * 4 + [DMA((2,))] * 2 + [DMA(s3)] * 2 + [DMA((2,))] * 2 + [DMA((1,))],
        compiler_params=pltpu.CompilerParams(vmem_limit_bytes=62 * 1024 * 1024, collective_id=0, has_side_effects=True),
        cost_estimate=pl.CostEstimate(flops=10**10, bytes_accessed=30 << 20, transcendentals=0),
        name="attn_fwd")(*args)

def solution(mesh):
    group = mesh.shape['seq']
    row_spec = P(('data', 'seq'), None)
    part_vec = P('data')
    part_mat = P('data', None)
    part_cube = P('data', None, None)

    def device_step(dec_in, memory, mem_len, grad_out, norm_attn, wq, wk, wv, wo, norm_mlp, w_gate, w_up, w_down):
        rows, dim = dec_in.shape
        mem = memory.shape[0]
        heads, hd = wq.shape[1], wq.shape[2]
        inner = heads * hd
        queries = rows * group
        chips = group // 2
        hc = heads // 2
        c = LOG2E * hd ** -0.5
        dims = (chips, rows, mem, dim, hc, c)
        wq2, wk2, wv2 = (w.reshape(dim, inner) for w in (wq, wk, wv))
        wo2 = wo.reshape(inner, dim)
        gain1 = norm_attn.astype(F32)
        gain2 = norm_mlp.astype(F32)

        pos = (lax.axis_index('seq') // 2) * 2 * mem + jnp.arange(2 * mem)
        bias = jnp.where(pos < mem_len[0], 0.0, -1e30).astype(F32)
        lane = jnp.arange(128)
        ak = jnp.where(lane[None, :] == 0, bias[:, None], jnp.where(lane[None, :] < 4, 1.0, 0.0)).astype(BF16)
        own, att_t, k_c, v_c, kt_c, qz, mem_p, y_all = fwd_call(dims, dec_in, memory, ak, wq2, wk2, wv2, gain1[None, :])
        y_all = y_all.reshape(queries, dim)
        attended = att_t.T

        x_in = dec_in.astype(F32)
        hidden = (x_in + mm(attended, wo2)).astype(BF16)
        n2_f, n2_pull = jax.vjp(rms_norm, hidden.astype(F32), gain2)
        n2 = n2_f.astype(BF16)
        gate_pre = mm(n2, w_gate)
        up_pre = mm(n2, w_up)
        _, gated_pull = jax.vjp(gated_unit, gate_pre, up_pre)
        go_b = grad_out.astype(BF16)
        grad_act = mm_bt(go_b, w_down)
        grad_gate, grad_up = gated_pull(grad_act)
        grad_n2 = mm_bt(grad_gate.astype(BF16), w_gate) + mm_bt(grad_up.astype(BF16), w_up)
        grad_h_norm, g_norm_mlp_part = n2_pull(grad_n2)
        grad_hidden = grad_out + grad_h_norm
        dh = grad_hidden.astype(BF16)
        gn = g_norm_mlp_part.reshape(-1, 2 * rows)
        gn = jnp.concatenate([gn, jnp.zeros((8 - gn.shape[0], 2 * rows), F32)], axis=0)

        g_mem, g_wkv, g_wq, gvec, dq_own, att_all, go_all, dh_all = bwd_call(
            dims, dh, own, gn, attended, go_b, k_c, v_c, kt_c, qz, ak, memory, mem_p, y_all, wo2, wq2, wk2, wv2, gain1[None, :])
        att_all, go_all, dh_all = (t.reshape(queries, dim) for t in (att_all, go_all, dh_all))
        _, norm_pull = jax.vjp(rms_norm, x_in, gain1)
        grad_x_norm, _ = norm_pull(mm_bt(dq_own.T, wq2))
        g_dec = grad_hidden + grad_x_norm

        x_all = y_all.astype(F32)
        g_wo = mm_at(att_all, dh_all)
        h_all = (x_all + mm(att_all, wo2)).astype(BF16)
        n2_all = rms_norm(h_all.astype(F32), gain2).astype(BF16)
        mlp_f, pull_all = jax.vjp(gated_unit, mm(n2_all, w_gate), mm(n2_all, w_up))
        gg, gu = pull_all(mm_bt(go_all, w_down))
        g_down = mm_at(mlp_f.astype(BF16), go_all)
        g_gate = mm_at(n2_all, gg.astype(BF16))
        g_up = mm_at(n2_all, gu.astype(BF16))
        cube = (dim, heads, hd)
        g_wkv = g_wkv.reshape(hc, 2, 128, dim)
        return (g_dec, g_mem, gvec[0], g_wq.reshape(inner, dim).T.reshape(cube), g_wkv[:, 0].reshape(inner, dim).T.reshape(cube),
                g_wkv[:, 1].reshape(inner, dim).T.reshape(cube), g_wo.reshape(heads, hd, dim), gvec[1], g_gate, g_up, g_down)

    return jax.shard_map(device_step, mesh=mesh,
                         in_specs=(row_spec, row_spec, part_vec, row_spec) + (P(),) * 9,
                         out_specs=(row_spec, row_spec, part_vec, part_cube, part_cube, part_cube, part_cube, part_vec, part_mat, part_mat, part_mat),
                         check_vma=False)
```

```python
import functools
import math

import jax
import jax.numpy as jnp
from jax import lax
from jax.experimental import pallas as pl
from jax.experimental.pallas import tpu as pltpu
from jax.sharding import PartitionSpec as P

F32 = jnp.float32
BF16 = jnp.bfloat16
LOG2E = math.log2(math.e)
VMEM = pltpu.VMEM
MESH = pl.DeviceIdType.MESH


def mm(a, b):
    return jnp.dot(a, b, preferred_element_type=F32)


def mm_bt(a, b):
    return lax.dot_general(a, b, (((1,), (1,)), ((), ())), preferred_element_type=F32)


def mm_at(a, b):
    return lax.dot_general(a, b, (((0,), (0,)), ((), ())), preferred_element_type=F32)


def rms_norm(tensor, gain):
    mean_sq = jnp.mean(tensor * tensor, axis=-1, keepdims=True)
    return tensor * lax.rsqrt(mean_sq + 1e-6) * gain


def gated_unit(gate_pre, up_pre):
    return jax.nn.silu(gate_pre) * up_pre


RIGHT, LEFT = 0, 1
DMA = pltpu.SemaphoreType.DMA


class Ring:
    def __init__(self, chips):
        me = lax.axis_index('seq')
        self.chips = chips
        self.far = chips // 2
        self.z = me // 2
        self.core = me - 2 * self.z
        self.partner = 2 * self.z + 1 - self.core
        self.next = (2 * self.chip(1) + self.core, 2 * self.chip(-1) + self.core)
        self.hops = {(RIGHT, 0): self.far, (LEFT, 1): self.far, (RIGHT, 1): self.far - 1, (LEFT, 0): self.far - 1}

    def chip(self, off):
        return lax.rem(self.z + off + self.chips, self.chips)

    def ahead(self, d, k):
        return self.chip(k if d == RIGHT else -k)

    def enter(self):
        barrier = pltpu.get_barrier_semaphore()
        for dev in (self.partner,) + self.next:
            pl.semaphore_signal(barrier, inc=1, device_id={'seq': dev}, device_id_type=MESH)
        pl.semaphore_wait(barrier, 3)


def remote(src, dst, ssem, rsem, dev):
    return pltpu.make_async_remote_copy(src_ref=src, dst_ref=dst, send_sem=ssem, recv_sem=rsem, device_id={'seq': dev}, device_id_type=MESH)


class Share:
    def __init__(self, ring, buf, src, sems):
        self.ring, self.buf, self.src = ring, buf, src
        self.ss, self.rs = sems

    def slot(self, chip, half):
        return self.buf.at[chip, half]

    def send(self, d, half, t):
        slot = self.slot(self.ring.ahead(d, 1 - t), half)
        src = self.src(half) if t == 1 else slot
        return remote(src, slot, self.ss.at[d, half, t - 1], self.rs.at[d, half, t - 1], self.ring.next[d])

    def recv(self, d, half, t):
        slot = self.slot(self.ring.ahead(d, -t), half)
        return remote(slot, slot, self.ss.at[d, half, t - 1], self.rs.at[d, half, t - 1], self.ring.next[d])

    def start(self):
        for d, half in self.ring.hops:
            self.send(d, half, 1).start()

    def came(self, d, half, t):
        pass

    def serve(self, t):
        for (d, half), n in self.ring.hops.items():
            if t <= n:
                self.recv(d, half, t).wait_recv()
                if t < n:
                    self.send(d, half, t + 1).start()
                self.came(d, half, t)

    def drain(self):
        for (d, half), n in self.ring.hops.items():
            for t in range(1, n + 1):
                self.send(d, half, t).wait_send()


class Rows(Share):
    def __init__(self, ring, buf, src, sems):
        super().__init__(ring, buf, src, sems[:2])
        self.fs, self.fr, self.os, self.orr = sems[2:]

    def slot(self, chip, half):
        return self.buf.at[chip, self.ring.core, half]

    def pslot(self, chip, half):
        return self.buf.at[chip, 1 - self.ring.core, half]

    def start(self):
        super().start()
        for half in range(2):
            self.own(half).start()

    def own(self, half):
        return remote(self.src(half), self.slot(self.ring.z, half), self.os.at[half], self.orr.at[half], self.ring.partner)

    def forward(self, d, half, t):
        slot = self.slot(self.ring.ahead(d, -t), half)
        return remote(slot, slot, self.fs.at[d, half, t - 1], self.fr.at[d, half, t - 1], self.ring.partner)

    def came(self, d, half, t):
        self.forward(d, half, t).start()

    def ready(self, off):
        ring = self.ring
        if off == 0:
            for half in range(2):
                slot = self.pslot(ring.z, half)
                remote(slot, slot, self.os.at[half], self.orr.at[half], ring.partner).wait_recv()
            return
        for (d, half), n in ring.hops.items():
            t = ring.far if abs(off) == ring.far else (-off if d == RIGHT else off)
            if 1 <= t <= n:
                slot = self.pslot(ring.ahead(d, -t), half)
                remote(slot, slot, self.fs.at[d, half, t - 1], self.fr.at[d, half, t - 1], ring.partner).wait_recv()

    def drain(self):
        super().drain()
        for half in range(2):
            self.own(half).wait_send()
        for (d, half), n in self.ring.hops.items():
            for t in range(1, n + 1):
                self.forward(d, half, t).wait_send()


class Reduce:
    def __init__(self, ring, part, rbuf, merge, sems):
        self.ring, self.part, self.rbuf, self.merge = ring, part, rbuf, merge
        self.ss, self.rs = sems

    def send(self, d, half, o):
        return remote(self.part.at[self.ring.ahead(d, o), half], self.rbuf.at[d, half, o - 1], self.ss.at[d, half, o - 1], self.rs.at[d, half, o - 1], self.ring.next[d])

    def recv(self, d, half, o):
        slot = self.rbuf.at[d, half, o]
        return remote(slot, slot, self.ss.at[d, half, o], self.rs.at[d, half, o], self.ring.next[d])

    def step(self, d, o):
        for half in ((0, 1) if d == RIGHT else (1, 0)):
            n = self.ring.hops[d, half]
            if o > n:
                continue
            if o < n:
                self.recv(d, half, o).wait_recv()
                self.merge(self.part.at[self.ring.ahead(d, o), half], self.rbuf.at[d, half, o])
            self.send(d, half, o).start()

    def both(self, o):
        self.step(RIGHT, o)
        self.step(LEFT, o)

    def final(self):
        for half in range(2):
            for d in (RIGHT, LEFT):
                self.recv(d, half, 0).wait_recv()
                self.merge(self.part.at[self.ring.z, half], self.rbuf.at[d, half, 0])

    def drain(self):
        for (d, half), n in self.ring.hops.items():
            for o in range(1, n + 1):
                self.send(d, half, o).wait_send()


def pick(i, values):
    out = jnp.int32(values[-1])
    for k, v in enumerate(values[:-1]):
        out = jnp.where(i == k, jnp.int32(v), out)
    return out


def add_into(dst, src):
    dst[...] = dst[...] + src[...]


def parts3(x):
    hi = x.astype(BF16)
    rest = x - hi.astype(F32)
    mid = rest.astype(BF16)
    lo = (rest - mid.astype(F32)).astype(BF16)
    return hi, mid, lo


def bwd_kernel(dims, dh_ref, own_ref, gn_ref, att_ref, go_ref, k_ref, v_ref, kt_ref, qz_ref, ak_ref, wo_ref, wq_ref, wk_ref, wv_ref, g1_ref, g2_ref,
               ma_hbm, mb_hbm, y_hbm, wg_hbm, wu_hbm, wd_hbm,
               gvec_ref, dqo_ref, gmem, gwkv, gwq, gwo, gdown, ggate, gup, attg, gog,
               dhg, doz, aqs, ads, stb, dk, dv, dkv, dkvp, dqp, dqr, dqa, arp, arr, ara, pvec, pdq, spb,
               msc, ybuf, abuf, wbuf, dbuf, wt, gst, gwo_s, gwq_s,
               *sems):
    chips, rows, mem, dim, hc, c, ff = dims
    QT = 2 * rows
    T = 2 * mem
    MC = min(256, mem)
    nm = T // MC
    inner = hc * 64
    np_ = hc // 2
    seg = 256 // chips // 2
    fh = ff // 2
    FT = wt.shape[1]
    nf = fh // FT
    ring = Ring(chips)
    z, core, far = ring.z, ring.core, ring.far
    sems = list(sems)

    def take(n):
        out = sems[:n]
        del sems[:n]
        return out

    half_rows = rows // 2
    rsrc = lambda ref: (lambda half: ref.at[pl.ds(half * half_rows, half_rows)])
    dh_g = Rows(ring, dhg, rsrc(dh_ref), take(6))
    att_g = Rows(ring, attg, rsrc(att_ref), take(6))
    go_g = Rows(ring, gog, rsrc(go_ref), take(6))
    st_g = Share(ring, stb, lambda half: stb.at[z, half], take(2))
    dq_r = [Reduce(ring, dqp.at[p], dqr.at[p], add_into, take(2)) for p in range(np_)]
    dq_s = [Share(ring, dqa.at[p], lambda half, p=p: dqa.at[p, z, half], take(2)) for p in range(np_)]
    ar_r = [Reduce(ring, arp.at[p], arr.at[p], add_into, take(2)) for p in range(np_)]
    ar_s = [Share(ring, ara.at[p], lambda half, p=p: ara.at[p, z, half], take(2)) for p in range(np_)]
    xs, xr, ls, gs, gr, gl, wsem, ysem = take(8)
    part_ = functools.partial
    ring.enter()
    dh_g.start()
    locals_ = []

    def local(src, dst, n):
        cp = pltpu.make_async_copy(src, dst, ls.at[n])
        cp.start()
        locals_.append(cp)
        return cp

    for n, (ref, buf) in enumerate(((att_ref, attg), (go_ref, gog))):
        for half in range(2):
            local(ref.at[pl.ds(half * half_rows, half_rows)], buf.at[z, core, half], 2 * n + half)
    m_loads = [pltpu.make_async_copy(src, msc.at[n, pl.ds(0, mem)], ls.at[4 + n]) for n, src in enumerate((ma_hbm, mb_hbm))]
    for cp in m_loads:
        cp.start()
    for half in range(2):
        dhg[z, core, half] = dh_ref[half * half_rows:(half + 1) * half_rows, :]
    doz[...] = jnp.zeros_like(doz)
    hrow = pl.ds(pl.multiple_of(core * inner, inner), inner)
    hcol = pl.ds(pl.multiple_of(core * inner, 128), inner)
    other_cols = pl.ds(pl.multiple_of((1 - core) * mem, mem), mem)
    my_cols = pl.ds(pl.multiple_of(core * mem, mem), mem)
    qmine = pl.ds(pl.multiple_of(core * rows, rows), rows)
    qother = pl.ds(pl.multiple_of((1 - core) * rows, rows), rows)

    def lanes(chip):
        return pl.ds(pl.multiple_of(chip * QT, QT), QT)

    def d_out(chip):
        return mm_bt(wo_ref[hrow, :], dhg[chip].reshape(QT, dim))

    def prepare(chip, dot=None):
        dot = d_out(chip) if dot is None else dot
        dob = dot.astype(BF16)
        q = lanes(chip)
        row = lax.broadcasted_iota(jnp.int32, (16, QT), 0)
        for h in range(hc):
            lo = h * 128 + (h % 2) * 64
            doz[lo:lo + 64, q] = dob[h * 64:(h + 1) * 64]
            for ref, half, first in ((aqs, 0, 1.0), (ads, 1, 0.0)):
                a, b, e = (x.astype(F32) for x in parts3(stb[chip, half, h:h + 1, :]))
                ref[h * 16:(h + 1) * 16, q] = jnp.where(row == 0, first, jnp.where(row == 1, a, jnp.where(row == 2, b, jnp.where(row == 3, e, 0.0)))).astype(BF16)

    dh_g.ready(0)
    dot0 = d_out(z)
    prod = dot0 * own_ref[:inner, :]
    for h in range(hc):
        stb[z, 0, h:h + 1, :] = -own_ref[inner + h:inner + h + 1, :]
        stb[z, 1, h:h + 1, :] = -jnp.sum(prod[h * 64:(h + 1) * 64], axis=0, keepdims=True)
    stb[z, 0, hc:8, :] = gn_ref[0:8 - hc, :]
    stb[z, 1, hc:8, :] = gn_ref[8 - hc:16 - 2 * hc, :]
    st_g.start()
    prepare(z, dot0)

    def tile(h, chip, p, hl):
        q = lanes(chip)
        hz = pl.ds(pl.multiple_of(h * 128, 128), 128)
        h16 = pl.ds(pl.multiple_of(h * 16, 16), 16)
        ps = slice(p * 128, (p + 1) * 128)
        hr = pl.ds(pl.multiple_of(hl * 64, 64), 64)
        hz64 = pl.ds(pl.multiple_of(h * 128 + hl * 64, 64), 64)
        h64 = pl.ds(pl.multiple_of(h * 64, 64), 64)
        q_t = qz_ref[hz64, q]
        do_t = doz[hz64, q]
        r1 = jnp.concatenate([qz_ref[hz, q], aqs[h16, q]], axis=0)
        r2 = jnp.concatenate([doz[hz, q], ads[h16, q]], axis=0)
        stage = {}
        dq = None
        for j in range(nm + 2):
            if j < nm:
                r = slice(j * MC, (j + 1) * MC)
                ak = ak_ref[r, 0:16]
                stage["a", j] = (mm(jnp.concatenate([k_ref[r, ps], ak], axis=1), r1), mm(jnp.concatenate([v_ref[r, ps], ak], axis=1), r2))
            if 1 <= j <= nm:
                s, dp = stage.pop(("a", j - 1))
                a = jnp.exp2(s * c)
                stage["b", j - 1] = (a.astype(BF16), (a * dp).astype(BF16))
            if j >= 2:
                r = slice((j - 2) * MC, (j - 1) * MC)
                pb, ds = stage.pop(("b", j - 2))
                dv[hr, r] += mm_bt(do_t, pb)
                dk[hr, r] += mm_bt(q_t, ds)
                d = mm(kt_ref[h64, r], ds)
                dq = d if dq is None else dq + d
        dqp[p, chip, hl] = dq

    near = [0]
    for o in range(1, far):
        near += [o, -o]
    near += [far]
    far_first = [far] + [s * o for o in range(far - 1, 0, -1) for s in (1, -1)] + [0]
    scale = 0.125

    def xp(p):
        return remote(dkv.at[p, :, other_cols], dkvp.at[p], xs.at[p], xr.at[p], ring.partner)

    def xq(p):
        return remote(dqa.at[p, z, :, :, qother], pdq.at[p], xs.at[np_ + p], xr.at[np_ + p], ring.partner)

    def at(i, events):
        for kk, fns in sorted(events.items()):
            def run(fns=fns):
                for f in fns:
                    f()
            pl.when(i == kk)(run)

    def run_pair(p, order, before, after):
        dk[...] = jnp.zeros_like(dk)
        dv[...] = jnp.zeros_like(dv)

        def body(i, carry):
            chip = ring.chip(pick(i, order))
            at(i, {kk: [part_(fn, chip)] for kk, fn in before.items()})
            lax.fori_loop(0, 2, lambda hl, cc: (tile(2 * p + hl, chip, p, hl), cc)[1], 0)
            at(i, after)
            return carry

        lax.fori_loop(0, chips, body, 0)
        dkv[p, 0:128, :] = (dk[...] * scale).astype(BF16)
        dkv[p, 128:256, :] = dv[...].astype(BF16)
        xp(p).start()
        if p == 0:
            for cp in m_loads:
                cp.wait()
        for part in range(2):
            e = slice(part * 128, (part + 1) * 128)
            g = mm(dkv[p, e, my_cols], msc[0, 0:mem]) + mm(dkv[p, e, other_cols], msc[1, 0:mem])
            for n in range(128 // seg):
                row = part * 128 + n * seg
                arp[p, row // (2 * seg), (row // seg) % 2] = g[n * seg:(n + 1) * seg]

    def gate(off, t=None):
        def fn(chip):
            if t is not None:
                dh_g.serve(t)
                st_g.serve(t)
            dh_g.ready(off)
            prepare(chip)
        return fn

    before0 = {}
    for n, off in enumerate(near):
        if off:
            before0[n] = gate(off, abs(off) if off > 0 else None)
    run_pair(0, near, before0, {})

    def reduce_events(p):
        return {2 * n: [part_(dq_r[p].both, o), part_(ar_r[p].both, o)] for n, o in enumerate(range(far, 0, -1))}

    def share_dq(p):
        for half in range(2):
            dqa[p, z, half] = (dqp[p, z, half] * scale).astype(BF16)
        dq_s[p].start()
        xq(p).start()

    def share_ar(p):
        for half in range(2):
            ara[p, z, half] = arp[p, z, half]
        ar_s[p].start()

    def finish(p):
        dq_r[p].final()
        ar_r[p].final()
        share_dq(p)
        share_ar(p)

    def merged(*evs):
        out = {}
        for ev in evs:
            for kk, fns in ev.items():
                out.setdefault(kk, []).extend(fns)
        return out

    def spread(g, first):
        return {2 * t - 2 + first: [part_(g.serve, t)] for t in range(1, far + 1)}

    att_g.start()
    run_pair(1, far_first, {}, merged(reduce_events(0), spread(att_g, 1)))
    finish(0)
    go_g.start()
    inl = {}
    for n, off in enumerate(far_first):
        if off == far:
            inl[n] = [part_(dq_r[2].both, far)]
        elif off > 0:
            inl[n] = [part_(dq_r[2].step, RIGHT, off)]
        elif off < 0:
            inl[n] = [part_(dq_r[2].step, LEFT, -off)]
    run_pair(2, far_first, {}, merged(inl, reduce_events(1), spread(dq_s[0], 0), spread(ar_s[0], 0), spread(go_g, 1)))
    ar_r[2].both(far)
    finish(1)
    dq_r[2].final()
    share_dq(2)

    for cp in locals_:
        cp.wait()
    for off in near:
        att_g.ready(off)
    gain2 = g2_ref[...]
    gwo_s[...] = jnp.zeros_like(gwo_s)

    def y_fetch(ch, slot):
        return pltpu.make_async_copy(y_hbm.at[ch], ybuf.at[slot], ysem.at[slot, 0])

    def fetch(ch, slot):
        return (y_fetch(ch, slot), pltpu.make_async_copy(attg.at[ch], abuf.at[slot], ysem.at[slot, 1]))

    def n2_at(ch):
        nh = chips // 2
        return ch // nh, pl.ds(pl.multiple_of((ch - nh * (ch // nh)) * QT, QT), QT)

    for cp in fetch(0, 0):
        cp.start()

    def hidden(ch, carry):
        slot = ch % 2
        for cp in fetch(ch, slot):
            cp.wait()

        @pl.when(ch + 1 < chips)
        def _():
            for cp in fetch(ch + 1, 1 - slot):
                cp.start()
        att = abuf[slot].reshape(QT, dim)
        h = (ybuf[slot].reshape(QT, dim).astype(F32) + mm(att, wo_ref[...])).astype(BF16)
        a, b = n2_at(ch)
        msc[a, b, :] = rms_norm(h.astype(F32), gain2).astype(BF16)
        ah = jnp.where(core == 0, att[:, :inner], att[:, inner:])
        gwo_s[...] += mm_at(ah, dhg[ch].reshape(QT, dim))
        at(ch, {1: [part_(ar_r[2].both, 3), part_(dq_s[1].serve, 1), part_(ar_s[1].serve, 1)],
                4: [part_(dq_s[2].serve, 1), part_(dq_s[1].serve, 2), part_(ar_s[1].serve, 2), part_(ar_r[2].both, 2)],
                7: [part_(dq_s[2].serve, 2), part_(dq_s[1].serve, 3), part_(ar_s[1].serve, 3)]})
        return carry

    lax.fori_loop(0, chips, hidden, 0)
    for off in near:
        go_g.ready(off)
    dh_g.drain()
    go_load = pltpu.make_async_copy(gog, dhg, ls.at[0])
    go_load.start()

    def partner_rows(buf, out, first, n, k):
        dst = out.at[pl.ds(pl.multiple_of(first, n), n)]
        return pltpu.make_async_copy(buf, dst, gl.at[k]), remote(buf, dst, gs.at[k], gr.at[k], ring.partner)

    def both_start(pair):
        pair[0].start()
        pair[1].start()

    def both_wait(pair):
        pair[0].wait()
        pair[1].wait()

    wo_out = partner_rows(gwo_s, gwo, core * inner, inner, 3 * nf)
    both_start(wo_out)

    def w_fetch(f, slot):
        cols = pl.ds(pl.multiple_of(core * fh + f * FT, FT), FT)
        return (pltpu.make_async_copy(wg_hbm.at[:, cols], wbuf.at[slot, 0], wsem.at[slot, 0]),
                pltpu.make_async_copy(wu_hbm.at[:, cols], wbuf.at[slot, 1], wsem.at[slot, 1]),
                pltpu.make_async_copy(wd_hbm.at[cols], dbuf.at[slot], wsem.at[slot, 2]))

    for cp in w_fetch(0, 0):
        cp.start()
    go_load.wait()
    f_events = {0: [part_(ar_r[2].both, 1), part_(dq_s[2].serve, 3), part_(dq_s[1].serve, 4), part_(ar_s[1].serve, 4)],
                1: [ar_r[2].final, part_(share_ar, 2), part_(dq_s[2].serve, 4)]}
    f_events2 = {2: [part_(ar_s[2].serve, 1), part_(ar_s[2].serve, 2)],
                 3: [part_(ar_s[2].serve, 3), part_(ar_s[2].serve, 4)]}
    outs3 = (gdown, ggate, gup)

    def mlp(f, carry):
        slot = f % 2
        for cp in w_fetch(f, slot):
            cp.wait()

        @pl.when(f + 1 < nf)
        def _():
            for cp in w_fetch(f + 1, 1 - slot):
                cp.start()
        for n in range(2):
            wt[n] = wbuf[slot, n].T

        def act_chunk(ch, cc):
            a, b = n2_at(ch)
            n2 = msc[a, b, :]
            g = mm_bt(wt[0], n2)
            u = mm_bt(wt[1], n2)
            ga = mm_bt(dbuf[slot], dhg[ch].reshape(QT, dim))
            sig = jax.nn.sigmoid(g)
            si = g * sig
            q = lanes(ch)
            doz[0:FT, q] = (si * u).astype(BF16)
            doz[FT:2 * FT, q] = (ga * u * (sig + si * (1.0 - sig))).astype(BF16)
            doz[2 * FT:3 * FT, q] = (ga * si).astype(BF16)
            return cc

        lax.fori_loop(0, chips, act_chunk, 0)
        at(f, f_events)
        for n in range(3):
            @pl.when(f > 0)
            def _(n=n):
                both_wait(partner_rows(gst.at[n, pl.ds(0, FT)], outs3[n], core * fh + (f - 1) * FT, FT, n * nf + f - 1))
            acc = None
            for ch in range(chips):
                if n == 0:
                    rhs = dhg[ch].reshape(QT, dim)
                else:
                    nh = chips // 2
                    rhs = msc[ch // nh, (ch % nh) * QT:(ch % nh + 1) * QT, :]
                d = mm(doz[n * FT:(n + 1) * FT, ch * QT:(ch + 1) * QT], rhs)
                acc = d if acc is None else acc + d
            gst[n, 0:FT] = acc
            both_start(partner_rows(gst.at[n, pl.ds(0, FT)], outs3[n], core * fh + f * FT, FT, n * nf + f))
        at(f, f_events2)
        return carry

    lax.fori_loop(0, nf, mlp, 0)
    for p in range(np_):
        local(ara.at[p], gwkv.at[core, p], 1 + p)
    cw = [remote(ara.at[p], gwkv.at[core, p], xs.at[2 * np_ + 2 + p], xr.at[2 * np_ + 2 + p], ring.partner) for p in range(np_)]
    for p in range(np_):
        cw[p].start()

    gain = g1_ref[...]
    wqt = wq_ref[:, hcol].T
    y_fetch(0, 0).start()
    spb[...] = jnp.zeros_like(spb)

    def query(ch, carry):
        slot = ch % 2
        y_fetch(ch, slot).wait()

        @pl.when(ch + 1 < chips)
        def _():
            y_fetch(ch + 1, 1 - slot).start()
        x = ybuf[slot].reshape(QT, dim).astype(F32)
        xhat = x * lax.rsqrt(jnp.mean(x * x, axis=-1, keepdims=True) + 1e-6)
        n1 = (xhat * gain).astype(BF16)
        dqc = jnp.concatenate([dqa[p, ch].reshape(128, QT) for p in range(np_)], axis=0)
        dn = mm_at(dqc, wqt)
        d = mm(dqc, n1)

        @pl.when(ch == 0)
        def _():
            gwq_s[...] = d

        @pl.when(ch > 0)
        def _():
            gwq_s[...] += d
        spb[0:1, :] += jnp.sum(dn * xhat, axis=0, keepdims=True)
        return carry

    lax.fori_loop(0, chips, query, 0)
    gvec2 = jnp.zeros((16 - 2 * hc, QT), F32)
    for ch in range(chips):
        gvec2 = gvec2 + jnp.concatenate([stb[ch, 0, hc:8, :], stb[ch, 1, hc:8, :]], axis=0)
    for n in range(dim // QT):
        spb[1:2, n * QT:(n + 1) * QT] = gvec2[n:n + 1]
    cv = remote(spb, pvec, xs.at[2 * np_], xr.at[2 * np_], ring.partner)
    cv.start()
    wq_out = partner_rows(gwq_s, gwq, core * inner, inner, 3 * nf + 1)
    both_start(wq_out)

    for p in range(np_):
        remote(dkvp.at[p], dkvp.at[p], xs.at[p], xr.at[p], ring.partner).wait_recv()
    nb = 4
    w = mem // nb
    gm = lambda b: pltpu.make_async_copy(gst.at[b % 3, pl.ds(0, w)], gmem.at[pl.ds(b * w, w)], gl.at[3 * nf + 2 + b % 3])
    for b in range(nb):
        if b < 3:
            both_wait(partner_rows(gst.at[b, pl.ds(0, FT)], outs3[b], core * fh + (nf - 1) * FT, FT, b * nf + nf - 1))
        else:
            gm(b - 3).wait()
        cb = pl.ds(pl.multiple_of(core * mem + b * w, w), w)
        acc = None
        for p in range(np_):
            for part, w_ref in ((0, wk_ref), (1, wv_ref)):
                own_cols = pl.ds(pl.multiple_of(core * inner + p * 128, 128), 128)
                oth_cols = pl.ds(pl.multiple_of((1 - core) * inner + p * 128, 128), 128)
                e = slice(part * 128, (part + 1) * 128)
                d = mm(jnp.concatenate([w_ref[:, own_cols], w_ref[:, oth_cols]], axis=1),
                       jnp.concatenate([dkv[p, e, cb], dkvp[p, e, b * w:(b + 1) * w]], axis=0))
                acc = d if acc is None else acc + d
        gst[b % 3, 0:w] = acc.T
        gm(b).start()
    for p in range(np_):
        own_r = pl.ds(pl.multiple_of(core * inner + p * 128, 128), 128)
        oth_r = pl.ds(pl.multiple_of((1 - core) * inner + p * 128, 128), 128)
        dqo_ref[own_r, :] = dqa[p, z, :, :, qmine].reshape(128, rows)
        xq(p).wait()
        dqo_ref[oth_r, :] = pdq[p].reshape(128, rows)
        xp(p).wait_send()
    cv.wait()
    gvec_ref[...] = spb[0:2] + pvec[0:2]
    both_wait(wo_out)
    both_wait(wq_out)
    for p in range(np_):
        cw[p].wait()
    for cp in locals_[4:]:
        cp.wait()
    for b in range(nb - 3, nb):
        gm(b).wait()
    for obj in [att_g, go_g, st_g] + dq_r + dq_s + ar_r + ar_s:
        obj.drain()


def bwd_call(dims, *args):
    chips, rows, mem, dim, hc, c, ff = dims
    inner = hc * 64
    QT = 2 * rows
    T = 2 * mem
    np_ = hc // 2
    h2 = chips // 2
    seg = 256 // chips // 2
    FT = ff // 8
    v = pl.BlockSpec(memory_space=VMEM)
    hbm = pl.BlockSpec(memory_space=pl.ANY)
    s3 = (2, 2, h2)
    rows_sems = [DMA(s3)] * 4 + [DMA((2,))] * 2
    two = [DMA(s3)] * 2
    S = jax.ShapeDtypeStruct
    gshape = (chips, 2, 2, rows // 2, dim)
    return pl.pallas_call(
        functools.partial(bwd_kernel, dims),
        out_shape=(S((2, dim), F32), S((2 * inner, rows), BF16), S((mem, dim), F32), S((2, np_, chips, 2, seg, dim), F32), S((2 * inner, dim), F32), S((2 * inner, dim), F32),
                   S((ff, dim), F32), S((ff, dim), F32), S((ff, dim), F32), S(gshape, BF16), S(gshape, BF16)),
        in_specs=[v] * 16 + [hbm] * 6, out_specs=(v,) * 2 + (hbm,) * 9,
        scratch_shapes=[
            VMEM(gshape, BF16), VMEM((max(hc * 128, 3 * FT), chips * QT), BF16), VMEM((hc * 16, chips * QT), BF16), VMEM((hc * 16, chips * QT), BF16),
            VMEM((chips, 2, 8, QT), F32), VMEM((128, T), F32), VMEM((128, T), F32), VMEM((np_, 256, T), BF16), VMEM((np_, 256, mem), BF16),
            VMEM((np_, chips, 2, 64, QT), F32), VMEM((np_, 2, 2, h2, 64, QT), F32), VMEM((np_, chips, 2, 64, QT), BF16),
            VMEM((np_, chips, 2, seg, dim), F32), VMEM((np_, 2, 2, h2, seg, dim), F32), VMEM((np_, chips, 2, seg, dim), F32),
            VMEM((8, dim), F32), VMEM((np_, 2, 64, rows), BF16), VMEM((8, dim), F32),
            VMEM((2, max(mem, chips * rows), dim), BF16), VMEM((2, 2, 2, rows // 2, dim), BF16), VMEM((2, 2, 2, rows // 2, dim), BF16),
            VMEM((2, 2, dim, FT), BF16), VMEM((2, FT, dim), BF16), VMEM((2, FT, dim), BF16), VMEM((3, max(FT, mem // 4), dim), F32), VMEM((inner, dim), F32), VMEM((inner, dim), F32)]
        + rows_sems * 3 + two * (1 + 4 * np_) + [DMA((3 * np_ + 2,))] * 2 + [DMA((6,)), DMA((14,)), DMA((14,)), DMA((17,)), DMA((2, 3)), DMA((2, 2))],
        compiler_params=pltpu.CompilerParams(vmem_limit_bytes=66_900_000, collective_id=1, has_side_effects=True),
        cost_estimate=pl.CostEstimate(flops=10**10, bytes_accessed=30 << 20, transcendentals=0),
        name="attn_bwd")(*args)


def fwd_kernel(dims, y_ref, m_ref, ak_ref, wq_ref, wk_ref, wv_ref, g_ref,
               own, att_ref, k_s, v_s, kt_s, qz, mg, yall,
               yg, wqt, vt_s, s_scr, mx_scr, part, rbuf, patt, satt, *sems):
    chips, rows, mem, dim, hc, c = dims
    QT = 2 * rows
    T = 2 * mem
    MC = min(256, mem)
    hh = hc // 2
    inner = hc * 64
    HR = hh * 64
    ring = Ring(chips)
    z, core, far = ring.z, ring.core, ring.far
    sub = rows // 2
    xs, xr, ls = sems[8:]
    y_g = Rows(ring, yg, lambda half: y_ref.at[pl.ds(half * sub, sub)], sems[:6])

    def merge(dst, src):
        for hl in range(hh):
            mr = slice(HR + hl, HR + hl + 1)
            lr = slice(HR + 8 + hl, HR + 9 + hl)
            m1, m2 = dst[mr, :], src[mr, :]
            m = jnp.maximum(m1, m2)
            a = jnp.exp2((m1 - m) * c)
            b = jnp.exp2((m2 - m) * c)
            rr = slice(hl * 64, (hl + 1) * 64)
            dst[rr, :] = dst[rr, :] * a + src[rr, :] * b
            dst[mr, :] = m
            dst[lr, :] = dst[lr, :] * a + src[lr, :] * b

    o_r = Reduce(ring, part, rbuf, merge, sems[6:8])
    ring.enter()
    y_g.start()
    mx_copy = remote(m_ref, mg, xs.at[0], xr.at[0], ring.partner)
    mx_copy.start()
    for half in range(2):
        yg[z, core, half] = y_ref[half * sub:(half + 1) * sub, :]
    hcol = pl.ds(pl.multiple_of(core * inner, 128), inner)
    qz[...] = jnp.zeros_like(qz)
    wqt[...] = wq_ref[:, hcol].T
    wk = wk_ref[:, hcol]
    wv = wv_ref[:, hcol]

    def project(src, base):
        for j in range(mem // MC):
            r = pl.ds(pl.multiple_of(base + j * MC, MC), MC)
            blk = src[j * MC:(j + 1) * MC, :]
            kb = mm(blk, wk).astype(BF16)
            vb = mm(blk, wv).astype(BF16)
            k_s[r, :] = kb
            v_s[r, :] = vb
            kt_s[:, r] = kb.T
            vt_s[:, r] = vb.T

    project(m_ref, core * mem)
    y_g.serve(1)
    mx_copy.wait_recv()
    project(mg, (1 - core) * mem)
    y_g.serve(2)
    gain = g_ref[...]

    def flash(chip):
        x = yg[chip].reshape(QT, dim).astype(F32)
        n1 = rms_norm(x, gain).astype(BF16)
        qt = mm_bt(wqt[...], n1).astype(BF16)
        q = pl.ds(pl.multiple_of(chip * QT, QT), QT)
        for h in range(hc):
            lo = h * 128 + (h % 2) * 64
            qz[lo:lo + 64, q] = qt[h * 64:(h + 1) * 64]
        one_row = jnp.where(lax.broadcasted_iota(jnp.int32, (16, QT), 0) == 0, 1.0, 0.0).astype(BF16)

        def step(h, slot, hp, pslot):
            if h is not None:
                rhs = jnp.concatenate([qz[pl.ds(pl.multiple_of(h * 128, 128), 128), q], one_row], axis=0)
                pair = pl.ds(pl.multiple_of((h // 2) * 128, 128), 128)
                mx = None
            if hp is not None:
                m = jnp.max(mx_scr[pslot], axis=0, keepdims=True)
                vrow = pl.ds(pl.multiple_of(hp * 64, 64), 64)
                ls_ = None
                acc = None
            for j in range(T // MC):
                r = slice(j * MC, (j + 1) * MC)
                if h is not None:
                    s = mm(jnp.concatenate([k_s[r, pair], ak_ref[r, 0:16]], axis=1), rhs)
                    s_scr[slot, r, :] = s
                    t = jnp.max(s.reshape(MC // 8, 8, QT), axis=0)
                    mx = t if mx is None else jnp.maximum(mx, t)
                if hp is not None:
                    pr = jnp.exp2((s_scr[pslot, r, :] - m) * c)
                    t = jnp.sum(pr.reshape(MC // 8, 8, QT), axis=0)
                    ls_ = t if ls_ is None else ls_ + t
                    dd = mm(vt_s[vrow, r], pr.astype(BF16))
                    acc = dd if acc is None else acc + dd
            if h is not None:
                mx_scr[slot] = mx
            if hp is not None:
                half = hp // hh
                hl = hp - half * hh
                part[chip, half, pl.ds(pl.multiple_of(hl * 64, 64), 64), :] = acc
                part[chip, half, pl.ds(HR + hl, 1), :] = m
                part[chip, half, pl.ds(HR + 8 + hl, 1), :] = jnp.sum(ls_, axis=0, keepdims=True)

        step(0, 0, None, None)
        if hc > 2:
            def pair_steps(i, carry):
                step(2 * i + 1, 1, 2 * i, 0)
                step(2 * i + 2, 0, 2 * i + 1, 1)
                return carry
            lax.fori_loop(0, hc // 2 - 1, pair_steps, 0)
        step(hc - 1, 1, hc - 2, 0)
        step(None, None, hc - 1, 1)

    order = [0, 1, far]
    for o in range(far - 1, 1, -1):
        order += [o, -o]
    order += [-1]

    def body(i, carry):
        for kk, off in enumerate(order):
            def get(kk=kk, off=off):
                if kk == 2:
                    for t in range(3, far + 1):
                        y_g.serve(t)
                y_g.ready(off)
            pl.when(i == kk)(get)
        flash(ring.chip(pick(i, order)))
        for kk, off in enumerate(order):
            if kk < 2:
                continue
            def put(off=off):
                if off == far:
                    o_r.both(far)
                elif off > 0:
                    o_r.step(RIGHT, off)
                else:
                    o_r.step(LEFT, -off)
                    if off == -2:
                        o_r.step(RIGHT, 1)
            pl.when(i == kk)(put)
        return carry

    lax.fori_loop(0, chips, body, 0)
    yc = pltpu.make_async_copy(yg, yall, ls.at[0])
    yc.start()
    o_r.final()
    qmine = pl.ds(pl.multiple_of(core * rows, rows), rows)
    qother = pl.ds(pl.multiple_of((1 - core) * rows, rows), rows)
    for h in range(hc):
        half, hl = h // hh, h % hh
        m = part[z, half, HR + hl:HR + hl + 1, :]
        l = part[z, half, HR + 8 + hl:HR + 9 + hl, :]
        o = part[z, half, hl * 64:(hl + 1) * 64, :] / l
        own[h * 64:(h + 1) * 64, :] = o
        own[inner + h:inner + h + 1, :] = m + jnp.log2(l) / c
    satt[...] = own[:inner, qother].astype(BF16)
    xo = remote(satt, patt, xs.at[1], xr.at[1], ring.partner)
    xo.start()
    att_ref[pl.ds(pl.multiple_of(core * inner, inner), inner), :] = own[:inner, qmine].astype(BF16)
    xo.wait()
    att_ref[pl.ds(pl.multiple_of((1 - core) * inner, inner), inner), :] = patt[...]
    mx_copy.wait_send()
    yc.wait()
    y_g.drain()
    o_r.drain()


def fwd_call(dims, *args):
    chips, rows, mem, dim, hc, c = dims
    hh = hc // 2
    inner = hc * 64
    QT = 2 * rows
    T = 2 * mem
    HR = hh * 64
    h2 = chips // 2
    v = pl.BlockSpec(memory_space=VMEM)
    S = jax.ShapeDtypeStruct
    s3 = (2, 2, h2)
    gshape = (chips, 2, 2, rows // 2, dim)
    return pl.pallas_call(
        functools.partial(fwd_kernel, dims),
        out_shape=(S((inner + 8, QT), F32), S((2 * inner, rows), BF16), S((T, inner), BF16), S((T, inner), BF16), S((inner, T), BF16),
                   S((hc * 128, chips * QT), BF16), S((mem, dim), BF16), S(gshape, BF16)),
        in_specs=[v] * 7, out_specs=(v,) * 7 + (pl.BlockSpec(memory_space=pl.ANY),),
        scratch_shapes=[
            VMEM(gshape, BF16), VMEM((inner, dim), BF16), VMEM((inner, T), BF16), VMEM((2, T, QT), F32), VMEM((2, 8, QT), F32),
            VMEM((chips, 2, HR + 16, QT), F32), VMEM((2, 2, h2, HR + 16, QT), F32), VMEM((inner, rows), BF16), VMEM((inner, rows), BF16)]
        + [DMA(s3)] * 4 + [DMA((2,))] * 2 + [DMA(s3)] * 2 + [DMA((2,))] * 2 + [DMA((1,))],
        compiler_params=pltpu.CompilerParams(vmem_limit_bytes=62 * 1024 * 1024, collective_id=0, has_side_effects=True),
        cost_estimate=pl.CostEstimate(flops=10**10, bytes_accessed=30 << 20, transcendentals=0),
        name="attn_fwd")(*args)

def solution(mesh):
    group = mesh.shape['seq']
    row_spec = P(('data', 'seq'), None)
    part_vec = P('data')
    part_mat = P('data', None)
    part_cube = P('data', None, None)

    def device_step(dec_in, memory, mem_len, grad_out, norm_attn, wq, wk, wv, wo, norm_mlp, w_gate, w_up, w_down):
        rows, dim = dec_in.shape
        mem = memory.shape[0]
        heads, hd = wq.shape[1], wq.shape[2]
        inner = heads * hd
        chips = group // 2
        hc = heads // 2
        c = LOG2E * hd ** -0.5
        dims = (chips, rows, mem, dim, hc, c)
        wq2, wk2, wv2 = (w.reshape(dim, inner) for w in (wq, wk, wv))
        wo2 = wo.reshape(inner, dim)
        gain1 = norm_attn.astype(F32)
        gain2 = norm_mlp.astype(F32)

        pos = (lax.axis_index('seq') // 2) * 2 * mem + jnp.arange(2 * mem)
        bias = jnp.where(pos < mem_len[0], 0.0, -1e30).astype(F32)
        lane = jnp.arange(128)
        ak = jnp.where(lane[None, :] == 0, bias[:, None], jnp.where(lane[None, :] < 4, 1.0, 0.0)).astype(BF16)
        own, att_t, k_c, v_c, kt_c, qz, mem_p, y_all = fwd_call(dims, dec_in, memory, ak, wq2, wk2, wv2, gain1[None, :])
        attended = att_t.T

        x_in = dec_in.astype(F32)
        hidden = (x_in + mm(attended, wo2)).astype(BF16)
        n2_f, n2_pull = jax.vjp(rms_norm, hidden.astype(F32), gain2)
        n2 = n2_f.astype(BF16)
        gate_pre = mm(n2, w_gate)
        up_pre = mm(n2, w_up)
        _, gated_pull = jax.vjp(gated_unit, gate_pre, up_pre)
        go_b = grad_out.astype(BF16)
        grad_act = mm_bt(go_b, w_down)
        grad_gate, grad_up = gated_pull(grad_act)
        grad_n2 = mm_bt(grad_gate.astype(BF16), w_gate) + mm_bt(grad_up.astype(BF16), w_up)
        grad_h_norm, g_norm_mlp_part = n2_pull(grad_n2)
        grad_hidden = grad_out + grad_h_norm
        dh = grad_hidden.astype(BF16)
        gn = g_norm_mlp_part.reshape(-1, 2 * rows)
        gn = jnp.concatenate([gn, jnp.zeros((8 - gn.shape[0], 2 * rows), F32)], axis=0)

        gvec, dq_own, g_mem, g_wkv, g_wq, g_wo, g_down, g_gate, g_up, _, _ = bwd_call(
            dims + (w_gate.shape[1],), dh, own, gn, attended, go_b, k_c, v_c, kt_c, qz, ak, wo2, wq2, wk2, wv2, gain1[None, :], gain2[None, :],
            memory, mem_p, y_all, w_gate, w_up, w_down)
        _, norm_pull = jax.vjp(rms_norm, x_in, gain1)
        grad_x_norm, _ = norm_pull(mm_bt(dq_own.T, wq2))
        g_dec = grad_hidden + grad_x_norm
        cube = (dim, heads, hd)
        g_wkv = g_wkv.reshape(hc, 2, 128, dim)
        return (g_dec, g_mem, gvec[0], g_wq.T.reshape(cube), g_wkv[:, 0].reshape(inner, dim).T.reshape(cube),
                g_wkv[:, 1].reshape(inner, dim).T.reshape(cube), g_wo.reshape(heads, hd, dim), gvec[1], g_gate.T, g_up.T, g_down)

    return jax.shard_map(device_step, mesh=mesh,
                         in_specs=(row_spec, row_spec, part_vec, row_spec) + (P(),) * 9,
                         out_specs=(row_spec, row_spec, part_vec, part_cube, part_cube, part_cube, part_cube, part_vec, part_mat, part_mat, part_mat),
                         check_vma=False)
```

```python
import functools
import math

import jax
import jax.numpy as jnp
from jax import lax
from jax.experimental import pallas as pl
from jax.experimental.pallas import tpu as pltpu
from jax.sharding import PartitionSpec as P

F32 = jnp.float32
BF16 = jnp.bfloat16
LOG2E = math.log2(math.e)
VMEM = pltpu.VMEM
MESH = pl.DeviceIdType.MESH


def mm(a, b):
    return jnp.dot(a, b, preferred_element_type=F32)


def mm_bt(a, b):
    return lax.dot_general(a, b, (((1,), (1,)), ((), ())), preferred_element_type=F32)


def mm_at(a, b):
    return lax.dot_general(a, b, (((0,), (0,)), ((), ())), preferred_element_type=F32)


def rms_norm(tensor, gain):
    mean_sq = jnp.mean(tensor * tensor, axis=-1, keepdims=True)
    return tensor * lax.rsqrt(mean_sq + 1e-6) * gain


RIGHT, LEFT = 0, 1
DMA = pltpu.SemaphoreType.DMA

FWD_ORDER = [(0, 0), (0, 1), (1, 0), (1, 1), (-3, 0), (3, 1), (4, 0), (4, 1), (3, 0), (-3, 1), (2, 0), (-2, 1), (2, 1), (-2, 0), (-1, 1), (-1, 0)]
BWD_ORDER = [0, 1, -1, 4, 3, -3, 2, -2]
FWD_PLAN = {
    ("b", 11): [("y", 1, 1, 3), ("y", 1, 0, 3), ("go", 0, 0, 1)],
    ("b", 12): [("go", 1, 1, 1)],
    ("b", 14): [("o", 1, 0, 3), ("go", 0, 1, 1)],
    ("b", 17): [("o", 0, 1, 3), ("go", 1, 0, 1)],
    ("b", 19): [("go", 1, 1, 2)],
    ("b", 20): [("o", 0, 0, 4)],
    ("b", 23): [("o", 1, 1, 4)],
    ("b", 29): [("go", 0, 0, 2)],
    ("b", 30): [("go", 1, 0, 2)],
    ("b", 32): [("go", 0, 1, 2)],
    ("b", 33): [("go", 1, 1, 3)],
    ("b", 36): [("o", 0, 0, 3)],
    ("b", 37): [("o", 1, 1, 3)],
    ("b", 38): [("o", 0, 1, 2)],
    ("b", 4): [("y", 0, 0, 2), ("y", 1, 1, 2)],
    ("b", 40): [("go", 1, 0, 3)],
    ("b", 41): [("o", 1, 0, 2), ("go", 0, 1, 3)],
    ("b", 42): [("go", 1, 1, 4)],
    ("b", 7): [("y", 0, 1, 2), ("y", 1, 0, 2)],
    ("b", 8): [("go", "start")],
    ("r", 3): [("y", 0, 0, 3), ("y", 0, 1, 3)],
    ("r", 5): [("y", 0, 0, 4), ("y", 1, 1, 4)],
    ("s", 1): [("y", 0, 0, 1), ("y", 1, 1, 1)],
    ("s", 2): [("y", 0, 1, 1), ("y", 1, 0, 1)],
    ("t", 1): [("o", 0, 0, 2), ("o", 1, 1, 2), ("o", 0, 1, 1), ("o", 1, 0, 1), ("o", 0, 0, 1), ("o", 1, 1, 1), ("o", 0, 1, 0), ("o", 1, 0, 0), ("o", 0, 0, 0), ("o", 1, 1, 0)],
    ("t", 2): [("go", 0, 0, 3)],
    ("t", 6): [("go", 0, 0, 4)],
}
BWD_PLAN = {
    ("b", 1): [("dh", 0, 0, 1), ("dh", 1, 1, 1)],
    ("b", 11): [("dh", 0, 1, 3), ("dh", 1, 0, 3), ("st", 0, 0, 3), ("st", 1, 1, 3), ("st", 0, 1, 3), ("st", 1, 0, 3)],
    ("b", 13): [("dh", 0, 0, 4), ("dh", 1, 1, 4), ("att", "start"), ("st", 0, 0, 4), ("st", 1, 1, 4)],
    ("b", 17): [("att", 0, 0, 1), ("att", 1, 1, 1)],
    ("b", 19): [("att", 0, 1, 1), ("att", 1, 0, 1)],
    ("b", 21): [("att", 0, 0, 2), ("att", 1, 1, 2)],
    ("b", 23): [("dq", 0, 0, 4), ("dq", 1, 1, 4), ("att", 0, 1, 2), ("att", 1, 0, 2)],
    ("b", 25): [("att", 0, 0, 3), ("att", 1, 1, 3)],
    ("b", 29): [("dq", 0, 0, 3), ("dq", 0, 1, 3)],
    ("b", 3): [("dh", 0, 1, 1), ("dh", 1, 0, 1), ("st", 0, 0, 1), ("st", 1, 1, 1), ("st", 0, 1, 1), ("st", 1, 0, 1)],
    ("b", 30): [("att", 0, 1, 3), ("att", 1, 0, 3)],
    ("b", 32): [("att", 0, 0, 4), ("att", 1, 1, 4)],
    ("b", 35): [("dq", 1, 1, 3), ("dq", 1, 0, 3)],
    ("b", 41): [("dq", 0, 0, 2), ("dq", 0, 1, 2)],
    ("b", 47): [("dq", 1, 1, 2), ("dq", 1, 0, 2), ("dq", 0, 0, 1)],
    ("b", 5): [("dh", 0, 0, 2), ("dh", 1, 1, 2)],
    ("b", 7): [("dh", 0, 1, 2), ("dh", 1, 0, 2), ("st", 0, 0, 2), ("st", 1, 1, 2), ("st", 0, 1, 2), ("st", 1, 0, 2)],
    ("b", 9): [("dh", 0, 0, 3), ("dh", 1, 1, 3)],
    ("f", 0): [("ar0", 1, 0, 2), ("ar0", 1, 1, 3)],
    ("f", 10): [("ar1", 0, 0, 2)],
    ("f", 12): [("ar2", 0, 1, 1)],
    ("f", 14): [("ar2", 0, 0, 2)],
    ("f", 16): [("dq", 1, 0, 0), ("dqs", "start"), ("ar0", 0, 1, 0)],
    ("f", 17): [("ar0", 0, 0, 1), ("ar0", 1, 0, 1), ("ar1", 0, 1, 0), ("ar0", 1, 1, 2), ("ar1", 0, 0, 1), ("ar1", 1, 0, 1)],
    ("f", 18): [("ar2", 0, 1, 0), ("ar1", 1, 1, 2)],
    ("f", 2): [("ar1", 1, 0, 2)],
    ("f", 20): [("ar2", 0, 0, 1), ("ar2", 1, 0, 1)],
    ("f", 22): [("ar2", 1, 1, 2)],
    ("f", 23): [("dqs", 0, 0, 1)],
    ("f", 25): [("dqs", 1, 1, 1)],
    ("f", 26): [("ar0", 0, 0, 0), ("ar1", 0, 0, 0), ("ar0", 1, 0, 0), ("dqs", 0, 1, 1), ("dqs", 1, 0, 1)],
    ("f", 28): [("ar2", 0, 0, 0), ("ar0", 1, 1, 1)],
    ("f", 3): [("ar1", 1, 1, 3)],
    ("f", 30): [("ar1", 1, 0, 0)],
    ("f", 31): [("dqs", 0, 0, 2), ("ar1", 1, 1, 1)],
    ("f", 33): [("ar2", 1, 0, 0)],
    ("f", 35): [("ar2", 1, 1, 1), ("dqs", 0, 1, 2), ("dqs", 1, 1, 2), ("dqs", 0, 0, 3)],
    ("f", 5): [("dq", 0, 1, 0), ("ar2", 1, 0, 2)],
    ("f", 6): [("ar2", 0, 1, 2)],
    ("f", 7): [("ar2", 1, 1, 3)],
    ("f", 8): [("ar2", 0, 0, 3), ("ar0", 0, 1, 1), ("ar0", 0, 0, 2)],
    ("f", 9): [("dq", 1, 1, 0), ("ar1", 0, 1, 1)],
    ("h", 2): [("dq", 1, 1, 1)],
    ("h", 3): [("dq", 0, 0, 0)],
    ("h", 4): [("ar0", 0, 1, 2)],
    ("h", 5): [("ar0", 0, 0, 3)],
    ("h", 6): [("ar1", 0, 1, 2)],
    ("h", 7): [("dq", 1, 0, 1), ("ar1", 0, 0, 3)],
    ("m", 1): [("ar0", 1, 1, 0), ("as0", "start"), ("dqs", 1, 0, 2)],
    ("m", 2): [("ar1", 1, 1, 0), ("as1", "start")],
    ("m", 3): [("ar2", 1, 1, 0), ("as2", "start"), ("dqs", 0, 1, 3)],
    ("m", 4): [("dqs", 1, 1, 3), ("dqs", 0, 0, 4), ("dqs", 1, 0, 3), ("dqs", 1, 1, 4)],
    ("p", 0): [("ar0", 0, 1, 3), ("ar0", 1, 0, 3), ("ar0", 0, 0, 4), ("ar0", 1, 1, 4)],
    ("p", 1): [("ar1", 0, 1, 3), ("ar1", 1, 0, 3), ("ar1", 0, 0, 4), ("ar1", 1, 1, 4), ("dq", 0, 1, 1)],
    ("p", 2): [("ar2", 0, 1, 3), ("ar2", 1, 0, 3), ("ar2", 0, 0, 4), ("ar2", 1, 1, 4)],
    ("q", 0): [("as0", 1, 1, 1), ("as0", 0, 0, 1), ("as0", 1, 0, 1), ("as0", 0, 1, 1), ("as1", 0, 0, 1), ("as1", 0, 1, 1), ("as1", 1, 1, 1), ("as2", 0, 0, 1), ("as1", 1, 0, 1), ("as2", 0, 1, 1), ("as2", 1, 1, 1), ("as2", 1, 0, 1)],
    ("q", 6): [("as0", 1, 1, 2), ("as0", 0, 0, 2)],
    ("q", 8): [("as0", 1, 0, 2), ("as0", 0, 1, 2), ("as1", 1, 1, 2), ("as1", 0, 0, 2), ("as1", 1, 0, 2), ("as1", 0, 1, 2), ("as2", 1, 1, 2), ("as2", 0, 0, 2), ("as2", 1, 0, 2), ("as2", 0, 1, 2), ("as0", 1, 1, 3), ("as0", 0, 0, 3), ("as0", 1, 0, 3), ("as0", 0, 1, 3), ("as1", 1, 1, 3), ("as1", 0, 0, 3), ("as1", 1, 0, 3), ("as1", 0, 1, 3), ("as2", 1, 1, 3), ("as2", 0, 0, 3), ("as2", 1, 0, 3), ("as2", 0, 1, 3), ("as0", 1, 1, 4), ("as0", 0, 0, 4), ("as1", 1, 1, 4), ("as1", 0, 0, 4), ("as2", 1, 1, 4), ("as2", 0, 0, 4)],
}


class Ring:
    def __init__(self, chips):
        me = lax.axis_index('seq')
        self.chips = chips
        self.far = chips // 2
        self.z = me // 2
        self.core = me - 2 * self.z
        self.partner = 2 * self.z + 1 - self.core
        self.next = (2 * self.chip(1) + self.core, 2 * self.chip(-1) + self.core)
        self.hops = {(RIGHT, 0): self.far, (LEFT, 1): self.far, (RIGHT, 1): self.far - 1, (LEFT, 0): self.far - 1}

    def chip(self, off):
        return lax.rem(self.z + off + self.chips, self.chips)

    def ahead(self, d, k):
        return self.chip(k if d == RIGHT else -k)

    def enter(self):
        barrier = pltpu.get_barrier_semaphore()
        for dev in (self.partner,) + self.next:
            pl.semaphore_signal(barrier, inc=1, device_id={'seq': dev}, device_id_type=MESH)
        pl.semaphore_wait(barrier, 3)


def remote(src, dst, ssem, rsem, dev):
    return pltpu.make_async_remote_copy(src_ref=src, dst_ref=dst, send_sem=ssem, recv_sem=rsem, device_id={'seq': dev}, device_id_type=MESH)


class Share:
    def __init__(self, ring, buf, src, sems):
        self.ring, self.buf, self.src = ring, buf, src
        self.ss, self.rs = sems

    def slot(self, chip, half):
        return self.buf.at[chip, half]

    def send(self, d, half, t):
        slot = self.slot(self.ring.ahead(d, 1 - t), half)
        src = self.src(half) if t == 1 else slot
        return remote(src, slot, self.ss.at[d, half, t - 1], self.rs.at[d, half, t - 1], self.ring.next[d])

    def recv(self, d, half, t):
        slot = self.slot(self.ring.ahead(d, -t), half)
        return remote(slot, slot, self.ss.at[d, half, t - 1], self.rs.at[d, half, t - 1], self.ring.next[d])

    def start(self):
        for d, half in self.ring.hops:
            self.send(d, half, 1).start()

    def came(self, d, half, t):
        pass

    def move(self, d, half, t):
        self.recv(d, half, t).wait_recv()
        if t < self.ring.hops[d, half]:
            self.send(d, half, t + 1).start()
        self.came(d, half, t)

    def drain(self):
        for (d, half), n in self.ring.hops.items():
            for t in range(1, n + 1):
                self.send(d, half, t).wait_send()


class Rows(Share):
    def __init__(self, ring, buf, src, sems):
        super().__init__(ring, buf, src, sems[:2])
        self.fs, self.fr, self.os, self.orr = sems[2:]

    def slot(self, chip, half):
        return self.buf.at[chip, self.ring.core, half]

    def pslot(self, chip, half):
        return self.buf.at[chip, 1 - self.ring.core, half]

    def start(self):
        super().start()
        for half in range(2):
            self.own(half).start()

    def own(self, half):
        return remote(self.src(half), self.slot(self.ring.z, half), self.os.at[half], self.orr.at[half], self.ring.partner)

    def forward(self, d, half, t):
        slot = self.slot(self.ring.ahead(d, -t), half)
        return remote(slot, slot, self.fs.at[d, half, t - 1], self.fr.at[d, half, t - 1], self.ring.partner)

    def came(self, d, half, t):
        self.forward(d, half, t).start()

    def ready(self, off):
        ring = self.ring
        if off == 0:
            for half in range(2):
                slot = self.pslot(ring.z, half)
                remote(slot, slot, self.os.at[half], self.orr.at[half], ring.partner).wait_recv()
            return
        for (d, half), n in ring.hops.items():
            t = ring.far if abs(off) == ring.far else (-off if d == RIGHT else off)
            if 1 <= t <= n:
                slot = self.pslot(ring.ahead(d, -t), half)
                remote(slot, slot, self.fs.at[d, half, t - 1], self.fr.at[d, half, t - 1], ring.partner).wait_recv()

    def drain(self):
        super().drain()
        for half in range(2):
            self.own(half).wait_send()
        for (d, half), n in self.ring.hops.items():
            for t in range(1, n + 1):
                self.forward(d, half, t).wait_send()


class Reduce:
    def __init__(self, ring, part, rbuf, merge, sems):
        self.ring, self.part, self.rbuf, self.merge = ring, part, rbuf, merge
        self.ss, self.rs = sems

    def send(self, d, half, o):
        return remote(self.part.at[self.ring.ahead(d, o), half], self.rbuf.at[d, half, o - 1], self.ss.at[d, half, o - 1], self.rs.at[d, half, o - 1], self.ring.next[d])

    def recv(self, d, half, o):
        slot = self.rbuf.at[d, half, o]
        return remote(slot, slot, self.ss.at[d, half, o], self.rs.at[d, half, o], self.ring.next[d])

    def move(self, d, half, o):
        if o < self.ring.hops[d, half]:
            self.recv(d, half, o).wait_recv()
            self.merge(self.part.at[self.ring.ahead(d, o), half], self.rbuf.at[d, half, o])
        if o > 0:
            self.send(d, half, o).start()

    def drain(self):
        for (d, half), n in self.ring.hops.items():
            for o in range(1, n + 1):
                self.send(d, half, o).wait_send()


def pick(i, values):
    out = jnp.int32(values[-1])
    for k, v in enumerate(values[:-1]):
        out = jnp.where(i == k, jnp.int32(v), out)
    return out


def dispatch(index, table):
    def branch(keys):
        if len(keys) == 1:
            def run():
                for fn in table[keys[0]]:
                    fn()
            pl.when(index == keys[0])(run)
            return
        low, high = keys[:len(keys) // 2], keys[len(keys) // 2:]
        pl.when(index < high[0])(functools.partial(branch, low))
        pl.when(index >= high[0])(functools.partial(branch, high))
    if table:
        branch(sorted(table))


def add_into(dst, src):
    dst[...] = dst[...] + src[...]


def parts3(x):
    hi = x.astype(BF16)
    rest = x - hi.astype(F32)
    mid = rest.astype(BF16)
    lo = (rest - mid.astype(F32)).astype(BF16)
    return hi, mid, lo


def bwd_kernel(dims, dh_ref, own_ref, gn_ref, att_ref, ak_ref, g1_ref, g2_ref,
               k_hbm, v_hbm, kt_hbm, qz_hbm, wo_hbm, wq_hbm, wk_hbm, wv_hbm, ma_hbm, mb_hbm, y_hbm, gog, wg_hbm, wu_hbm, wd_hbm,
               gvec_ref, dqo_ref, gmem, gwkv, gwq, gwo, gdown, ggate, gup, attg,
               k_ref, v_ref, kt_ref, qz_ref, wo_ref, wq_ref, wk_ref, wv_ref,
               dhg, doz, aqs, ads, stb, dk, dv, dkv, dkvp, dqp, dqr, dqa, arp, arr, ara, pvec, pdq, spb,
               msc, ybuf, abuf, wbuf, dbuf, wt, gst, gsw, gwo_s, gwq_s,
               *sems):
    chips, rows, mem, dim, hc, c, ff = dims
    QT = 2 * rows
    T = 2 * mem
    MC = min(256, mem)
    nm = T // MC
    inner = hc * 64
    np_ = hc // 2
    seg = 256 // chips // 2
    fh = ff // 2
    FT = wt.shape[1]
    nf = fh // FT
    ring = Ring(chips)
    z, core, far = ring.z, ring.core, ring.far
    sems = list(sems)

    def take(n):
        out = sems[:n]
        del sems[:n]
        return out

    half_rows = rows // 2
    hh = hc // 2
    part_ = functools.partial
    rsrc = lambda ref: (lambda half: ref.at[pl.ds(half * half_rows, half_rows)])
    dh_g = Rows(ring, dhg, rsrc(dh_ref), take(6))
    att_g = Rows(ring, attg, rsrc(att_ref), take(6))
    st_g = Share(ring, stb, lambda half: stb.at[z, half], take(2))
    dq_r = Reduce(ring, dqp, dqr, add_into, take(2))
    dq_s = Share(ring, dqa, lambda half: dqa.at[z, half], take(2))
    ar_r = [Reduce(ring, arp.at[p], arr.at[p], add_into, take(2)) for p in range(np_)]
    ar_s = [Share(ring, ara.at[p], lambda half, p=p: ara.at[p, z, half], take(2)) for p in range(np_)]
    xs, xr, ls, gs, gr, gl, wsem, ysem, lsem = take(9)
    loads = [pltpu.make_async_copy(src, dst, lsem.at[n]) for n, (src, dst) in enumerate((
        (wo_hbm, wo_ref), (k_hbm, k_ref), (v_hbm, v_ref), (kt_hbm, kt_ref), (qz_hbm, qz_ref),
        (ma_hbm, msc.at[0, pl.ds(0, mem)]), (mb_hbm, msc.at[1, pl.ds(0, mem)]), (wq_hbm, wq_ref), (wk_hbm, wk_ref), (wv_hbm, wv_ref)))]
    for cp in loads:
        cp.start()
    ring.enter()
    dh_g.start()
    locals_ = [pltpu.make_async_copy(att_ref.at[pl.ds(half * half_rows, half_rows)], attg.at[z, core, half], ls.at[half]) for half in range(2)]
    for cp in locals_:
        cp.start()
    for half in range(2):
        dhg[z, core, half] = dh_ref[half * half_rows:(half + 1) * half_rows, :]
    doz[...] = jnp.zeros_like(doz)
    hrow = pl.ds(pl.multiple_of(core * inner, inner), inner)
    hcol = pl.ds(pl.multiple_of(core * inner, 128), inner)
    other_cols = pl.ds(pl.multiple_of((1 - core) * mem, mem), mem)
    my_cols = pl.ds(pl.multiple_of(core * mem, mem), mem)
    qmine = pl.ds(pl.multiple_of(core * rows, rows), rows)
    qother = pl.ds(pl.multiple_of((1 - core) * rows, rows), rows)

    def lanes(chip):
        return pl.ds(pl.multiple_of(chip * QT, QT), QT)

    def d_out(chip):
        return mm_bt(wo_ref[hrow, :], dhg[chip].reshape(QT, dim))

    def prepare(chip, dot=None):
        dot = d_out(chip) if dot is None else dot
        dob = dot.astype(BF16)
        q = lanes(chip)
        row = lax.broadcasted_iota(jnp.int32, (16, QT), 0)
        for h in range(hc):
            lo = h * 128 + (h % 2) * 64
            doz[lo:lo + 64, q] = dob[h * 64:(h + 1) * 64]
            for ref, half, first in ((aqs, 0, 1.0), (ads, 1, 0.0)):
                a, b, e = (x.astype(F32) for x in parts3(stb[chip, half, h:h + 1, :]))
                ref[h * 16:(h + 1) * 16, q] = jnp.where(row == 0, first, jnp.where(row == 1, a, jnp.where(row == 2, b, jnp.where(row == 3, e, 0.0)))).astype(BF16)

    dh_g.ready(0)
    loads[0].wait()
    dot0 = d_out(z)
    prod = dot0 * own_ref[:inner, :]
    for h in range(hc):
        stb[z, 0, h:h + 1, :] = -own_ref[inner + h:inner + h + 1, :]
        stb[z, 1, h:h + 1, :] = -jnp.sum(prod[h * 64:(h + 1) * 64], axis=0, keepdims=True)
    stb[z, 0, hc:8, :] = gn_ref[0:8 - hc, :]
    stb[z, 1, hc:8, :] = gn_ref[8 - hc:16 - 2 * hc, :]
    st_g.start()
    prepare(z, dot0)
    dk[...] = jnp.zeros_like(dk)
    dv[...] = jnp.zeros_like(dv)
    for cp in loads[1:]:
        cp.wait()

    def tile(h, chip):
        pair = h // 2
        q = lanes(chip)
        hz = pl.ds(pl.multiple_of(h * 128, 128), 128)
        h16 = pl.ds(pl.multiple_of(h * 16, 16), 16)
        ps = pl.ds(pl.multiple_of(pair * 128, 128), 128)
        hz64 = pl.ds(pl.multiple_of(h * 128 + (h - 2 * pair) * 64, 64), 64)
        h64 = pl.ds(pl.multiple_of(h * 64, 64), 64)
        hr = h64
        q_t = qz_ref[hz64, q]
        do_t = doz[hz64, q]
        r1 = jnp.concatenate([qz_ref[hz, q], aqs[h16, q]], axis=0)
        r2 = jnp.concatenate([doz[hz, q], ads[h16, q]], axis=0)
        stage = {}
        dq = None
        for j in range(nm + 2):
            if j < nm:
                r = slice(j * MC, (j + 1) * MC)
                ak = ak_ref[r, 0:16]
                stage["a", j] = (mm(jnp.concatenate([k_ref[r, ps], ak], axis=1), r1), mm(jnp.concatenate([v_ref[r, ps], ak], axis=1), r2))
            if 1 <= j <= nm:
                s, dp = stage.pop(("a", j - 1))
                a = jnp.exp2(s * c)
                stage["b", j - 1] = (a.astype(BF16), (a * dp).astype(BF16))
            if j >= 2:
                r = slice((j - 2) * MC, (j - 1) * MC)
                pb, ds = stage.pop(("b", j - 2))
                dv[hr, r] += mm_bt(do_t, pb)
                dk[hr, r] += mm_bt(q_t, ds)
                d = mm(kt_ref[h64, r], ds)
                dq = d if dq is None else dq + d
        half = h // hh
        dqp[chip, half, pl.ds(pl.multiple_of((h - half * hh) * 64, 64), 64), :] = dq

    scale = 0.125

    def xp(p):
        return remote(dkv.at[p, :, other_cols], dkvp.at[p], xs.at[p], xr.at[p], ring.partner)

    def xq():
        return remote(dqa.at[z, :, :, qother], pdq, xs.at[np_], xr.at[np_], ring.partner)

    def share_dq():
        for half in range(2):
            dqa[z, half] = (dqp[z, half] * scale).astype(BF16)
        dq_s.start()
        xq().start()

    def share_ar(p):
        for half in range(2):
            ara[p, z, half] = arp[p, z, half]
        ar_s[p].start()

    moves = {"dh": dh_g, "st": st_g, "att": att_g, "dq": dq_r, "dqs": dq_s}
    begins = {"att": att_g.start, "dqs": share_dq}
    for p in range(np_):
        moves[f"ar{p}"] = ar_r[p]
        moves[f"as{p}"] = ar_s[p]
        begins[f"as{p}"] = part_(share_ar, p)

    def acts(*point):
        return [begins[e[0]] if e[1] == "start" else part_(moves[e[0]].move, *e[1:]) for e in BWD_PLAN.get(point, [])]

    def run(*point):
        for fn in acts(*point):
            fn()

    def table(kind, n):
        return {k: acts(kind, k) for k in range(n) if acts(kind, k)}

    offs = BWD_ORDER

    def body(it, carry):
        i = it // hc
        h = it - i * hc
        chip = ring.chip(pick(i, offs))
        dispatch(it, {k * hc: acts("r", k) + [part_(dh_g.ready, offs[k])] for k in range(1, chips)})
        pl.when((h == 0) & (it > 0))(part_(prepare, chip))
        tile(h, chip)
        dispatch(it, table("b", chips * hc))
        return carry

    lax.fori_loop(0, chips * hc, body, 0)
    for p in range(np_):
        r = slice(p * 128, (p + 1) * 128)
        dkv[p, 0:128, :] = (dk[r, :] * scale).astype(BF16)
        dkv[p, 128:256, :] = dv[r, :].astype(BF16)
        xp(p).start()
        g = mm(dkv[p, :, my_cols], msc[0, 0:mem]) + mm(dkv[p, :, other_cols], msc[1, 0:mem])
        for n in range(256 // seg):
            arp[p, n // 2, n % 2] = g[n * seg:(n + 1) * seg]
        run("p", p)
    run("p", np_)
    near = range(1 - far, far + 1)

    for cp in locals_:
        cp.wait()
    for off in near:
        att_g.ready(off)
    gain2 = g2_ref[...]
    gwo_s[...] = jnp.zeros_like(gwo_s)

    def y_fetch(ch, slot):
        return pltpu.make_async_copy(y_hbm.at[ch], ybuf.at[slot], ysem.at[slot, 0])

    def fetch(ch, slot):
        return (y_fetch(ch, slot), pltpu.make_async_copy(attg.at[ch], abuf.at[slot], ysem.at[slot, 1]))

    for cp in fetch(0, 0):
        cp.start()

    def hidden(ch, carry):
        slot = ch % 2
        for cp in fetch(ch, slot):
            cp.wait()

        @pl.when(ch + 1 < chips)
        def _():
            for cp in fetch(ch + 1, 1 - slot):
                cp.start()
        att = abuf[slot].reshape(QT, dim)
        h = (ybuf[slot].reshape(QT, dim).astype(F32) + mm(att, wo_ref[...])).astype(BF16)
        qz_ref[0:dim, lanes(ch)] = rms_norm(h.astype(F32), gain2).astype(BF16).T
        ah = jnp.where(core == 0, att[:, :inner], att[:, inner:])
        gwo_s[...] += mm_at(ah, dhg[ch].reshape(QT, dim))
        dispatch(ch, table("h", chips))
        return carry

    lax.fori_loop(0, chips, hidden, 0)
    dh_g.drain()
    go_load = pltpu.make_async_copy(gog, dhg, ls.at[0])
    go_load.start()

    def partner_block(buf, dst, k):
        return pltpu.make_async_copy(buf, dst, gl.at[k]), remote(buf, dst, gs.at[k], gr.at[k], ring.partner)

    def both_start(pair):
        pair[0].start()
        pair[1].start()

    def both_wait(pair):
        pair[0].wait()
        pair[1].wait()

    wo_out = partner_block(gwo_s, gwo.at[hrow], 3 * nf)
    both_start(wo_out)

    def w_fetch(f, slot):
        cols = pl.ds(pl.multiple_of(core * fh + f * FT, FT), FT)
        return (pltpu.make_async_copy(wg_hbm.at[:, cols], wbuf.at[slot, 0], wsem.at[slot, 0]),
                pltpu.make_async_copy(wu_hbm.at[:, cols], wbuf.at[slot, 1], wsem.at[slot, 1]),
                pltpu.make_async_copy(wd_hbm.at[cols], dbuf.at[slot], wsem.at[slot, 2]))

    for cp in w_fetch(0, 0):
        cp.start()
    go_load.wait()
    f_table = table("f", 9 * nf)

    def block(f, n):
        if n == 0:
            return partner_block(gst.at[0, pl.ds(0, FT)], gdown.at[pl.ds(pl.multiple_of(core * fh + f * FT, FT), FT)], f)
        return partner_block(gsw.at[n - 1], (ggate, gup)[n - 1].at[:, pl.ds(pl.multiple_of(core * fh + f * FT, FT), FT)], n * nf + f)

    def mlp(f, carry):
        slot = f % 2
        for cp in w_fetch(f, slot):
            cp.wait()

        @pl.when(f + 1 < nf)
        def _():
            for cp in w_fetch(f + 1, 1 - slot):
                cp.start()
        for n in range(2):
            wt[n] = wbuf[slot, n].T

        def act_chunk(ch, cc):
            q = lanes(ch)
            n2t = qz_ref[0:dim, q]
            g = mm(wt[0], n2t)
            u = mm(wt[1], n2t)
            ga = mm_bt(dbuf[slot], dhg[ch].reshape(QT, dim))
            sig = jax.nn.sigmoid(g)
            si = g * sig
            doz[0:FT, q] = (si * u).astype(BF16)
            doz[FT:2 * FT, q] = (ga * u * (sig + si * (1.0 - sig))).astype(BF16)
            doz[2 * FT:3 * FT, q] = (ga * si).astype(BF16)
            dispatch(f * 9 + ch, f_table)
            return cc

        lax.fori_loop(0, chips, act_chunk, 0)

        @pl.when(f > 0)
        def _():
            for n in range(3):
                both_wait(block(f - 1, n))
        acc = [None] * 3
        for ch in range(chips):
            q = slice(ch * QT, (ch + 1) * QT)
            n2t = qz_ref[0:dim, q]
            for n, d in enumerate((mm(doz[0:FT, q], dhg[ch].reshape(QT, dim)), mm_bt(n2t, doz[FT:2 * FT, q]), mm_bt(n2t, doz[2 * FT:3 * FT, q]))):
                acc[n] = d if acc[n] is None else acc[n] + d
        gst[0, 0:FT] = acc[0]
        gsw[0] = acc[1]
        gsw[1] = acc[2]
        for n in range(3):
            both_start(block(f, n))
        dispatch(f * 9 + 8, f_table)
        return carry

    lax.fori_loop(0, nf, mlp, 0)
    for p in range(np_):
        remote(dkvp.at[p], dkvp.at[p], xs.at[p], xr.at[p], ring.partner).wait_recv()
    nb = 4
    w = mem // nb
    gm = lambda b: pltpu.make_async_copy(gst.at[b % 2, pl.ds(0, w)], gmem.at[pl.ds(b * w, w)], gl.at[3 * nf + 2 + b % 2])
    for n in range(3):
        both_wait(block(nf - 1, n))
    for b in range(nb):
        if b > 1:
            gm(b - 2).wait()
        cb = pl.ds(pl.multiple_of(core * mem + b * w, w), w)
        acc = None
        for p in range(np_):
            own_e = pl.ds(pl.multiple_of(core * inner + p * 128, 128), 128)
            oth_e = pl.ds(pl.multiple_of((1 - core) * inner + p * 128, 128), 128)
            for part, w_ref in ((0, wk_ref), (1, wv_ref)):
                e = slice(part * 128, (part + 1) * 128)
                lhs = jnp.concatenate([dkv[p, e, cb], dkvp[p, e, b * w:(b + 1) * w]], axis=0)
                rhs = jnp.concatenate([w_ref[:, own_e], w_ref[:, oth_e]], axis=1)
                d = mm_bt(lhs.T, rhs)
                acc = d if acc is None else acc + d
        gst[b % 2, 0:w] = acc
        gm(b).start()
        run("m", b)
    run("m", nb)

    gain = g1_ref[...]
    y_fetch(0, 0).start()
    spb[...] = jnp.zeros_like(spb)
    gwq_s[...] = jnp.zeros_like(gwq_s)
    wq_h = wq_ref[:, hcol]

    def query(ch, carry):
        slot = ch % 2
        y_fetch(ch, slot).wait()

        @pl.when(ch + 1 < chips)
        def _():
            y_fetch(ch + 1, 1 - slot).start()
        x = ybuf[slot].reshape(QT, dim).astype(F32)
        xhat = x * lax.rsqrt(jnp.mean(x * x, axis=-1, keepdims=True) + 1e-6)
        n1 = (xhat * gain).astype(BF16)
        dqc = dqa[ch].reshape(inner, QT)
        dn = mm_bt(dqc.T, wq_h)
        gwq_s[...] += mm(dqc, n1)
        spb[0:1, :] += jnp.sum(dn * xhat, axis=0, keepdims=True)
        dispatch(ch, table("q", chips))
        return carry

    lax.fori_loop(0, chips, query, 0)
    gvec2 = jnp.zeros((16 - 2 * hc, QT), F32)
    for ch in range(chips):
        gvec2 = gvec2 + jnp.concatenate([stb[ch, 0, hc:8, :], stb[ch, 1, hc:8, :]], axis=0)
    for n in range(dim // QT):
        spb[1:2, n * QT:(n + 1) * QT] = gvec2[n:n + 1]
    cv = remote(spb, pvec, xs.at[np_ + 1], xr.at[np_ + 1], ring.partner)
    cv.start()
    wq_out = partner_block(gwq_s, gwq.at[hrow], 3 * nf + 1)
    both_start(wq_out)
    own_r = pl.ds(pl.multiple_of(core * inner, inner), inner)
    oth_r = pl.ds(pl.multiple_of((1 - core) * inner, inner), inner)
    dqo_ref[own_r, :] = dqa[z, :, :, qmine].reshape(inner, rows)
    xq().wait()
    dqo_ref[oth_r, :] = pdq[...].reshape(inner, rows)
    run("q", chips)
    wkv_out = [pltpu.make_async_copy(ara.at[p], gwkv.at[core, p], ls.at[2 + p]) for p in range(np_)]
    wkv_out += [remote(ara.at[p], gwkv.at[core, p], xs.at[np_ + 2 + p], xr.at[np_ + 2 + p], ring.partner) for p in range(np_)]
    for cp in wkv_out:
        cp.start()
    for p in range(np_):
        xp(p).wait_send()
    cv.wait()
    gvec_ref[...] = spb[0:2] + pvec[0:2]
    both_wait(wo_out)
    both_wait(wq_out)
    for cp in wkv_out:
        cp.wait()
    for b in range(nb - 2, nb):
        gm(b).wait()
    for obj in [att_g, st_g, dq_r, dq_s] + ar_r + ar_s:
        obj.drain()


def bwd_call(dims, *args):
    chips, rows, mem, dim, hc, c, ff = dims
    inner = hc * 64
    QT = 2 * rows
    T = 2 * mem
    np_ = hc // 2
    h2 = chips // 2
    seg = 256 // chips // 2
    FT = ff // 8
    v = pl.BlockSpec(memory_space=VMEM)
    hbm = pl.BlockSpec(memory_space=pl.ANY)
    s3 = (2, 2, h2)
    rows_sems = [DMA(s3)] * 4 + [DMA((2,))] * 2
    two = [DMA(s3)] * 2
    S = jax.ShapeDtypeStruct
    gshape = (chips, 2, 2, rows // 2, dim)
    cols = chips * QT
    wsq = VMEM((dim, 2 * inner), BF16)
    return pl.pallas_call(
        functools.partial(bwd_kernel, dims),
        out_shape=(S((2, dim), F32), S((2 * inner, rows), BF16), S((mem, dim), F32), S((2, np_, chips, 2, seg, dim), F32), S((2 * inner, dim), F32), S((2 * inner, dim), F32),
                   S((ff, dim), F32), S((dim, ff), F32), S((dim, ff), F32), S(gshape, BF16)),
        in_specs=[v] * 7 + [hbm] * 15, out_specs=(v,) * 2 + (hbm,) * 8,
        scratch_shapes=[
            VMEM((T, inner), BF16), VMEM((T, inner), BF16), VMEM((inner, T), BF16), VMEM((hc * 128, cols), BF16), VMEM((2 * inner, dim), BF16), wsq, wsq, wsq,
            VMEM(gshape, BF16), VMEM((max(hc * 128, 3 * FT), cols), BF16), VMEM((hc * 16, cols), BF16), VMEM((hc * 16, cols), BF16),
            VMEM((chips, 2, 8, QT), F32), VMEM((inner, T), F32), VMEM((inner, T), F32), VMEM((np_, 256, T), BF16), VMEM((np_, 256, mem), BF16),
            VMEM((chips, 2, inner // 2, QT), F32), VMEM((2, 2, h2, inner // 2, QT), F32), VMEM((chips, 2, inner // 2, QT), BF16),
            VMEM((np_, chips, 2, seg, dim), F32), VMEM((np_, 2, 2, h2, seg, dim), F32), VMEM((np_, chips, 2, seg, dim), F32),
            VMEM((8, dim), F32), VMEM((2, inner // 2, rows), BF16), VMEM((8, dim), F32),
            VMEM((2, mem, dim), BF16), VMEM((2, 2, 2, rows // 2, dim), BF16), VMEM((2, 2, 2, rows // 2, dim), BF16),
            VMEM((2, 2, dim, FT), BF16), VMEM((2, FT, dim), BF16), VMEM((2, FT, dim), BF16), VMEM((2, max(FT, mem // 4), dim), F32), VMEM((2, dim, FT), F32),
            VMEM((inner, dim), F32), VMEM((inner, dim), F32)]
        + rows_sems * 2 + two * (3 + 2 * np_) + [DMA((2 * np_ + 2,))] * 2 + [DMA((2 + np_,)), DMA((14,)), DMA((14,)), DMA((16,)), DMA((2, 3)), DMA((2, 2)), DMA((10,))],
        compiler_params=pltpu.CompilerParams(vmem_limit_bytes=66_900_000, collective_id=1, has_side_effects=True),
        cost_estimate=pl.CostEstimate(flops=10**10, bytes_accessed=30 << 20, transcendentals=0),
        name="attn_bwd")(*args)


def fwd_kernel(dims, y_ref, go_ref, m_ref, ak_ref, wq_ref, wk_ref, wv_ref, g1_ref, g2_ref, wo_hbm, wg_hbm, wu_hbm, wd_hbm,
               own, att_ref, dh_ref, gh_ref, gn_ref, k_s, v_s, kt_s, qz, mg, yall, gog,
               yg, wqt, vt_s, s_scr, mx_scr, part, rbuf, patt, satt, gob, attt, wo_s, wg_s, wu_s, wd_s, *sems):
    chips, rows, mem, dim, hc, c, ff = dims
    QT = 2 * rows
    T = 2 * mem
    MC = min(256, mem)
    hh = hc // 2
    inner = hc * 64
    HR = hh * 64
    ring = Ring(chips)
    z, core, far = ring.z, ring.core, ring.far
    sub = rows // 2
    part_ = functools.partial
    xs, xr, ls = sems[14:]
    rsrc = lambda ref: (lambda half: ref.at[pl.ds(half * sub, sub)])
    y_g = Rows(ring, yg, rsrc(y_ref), sems[:6])
    go_g = Rows(ring, gog, rsrc(gob), sems[6:12])

    def merge(dst, src):
        for hl in range(hh):
            mr = slice(HR + hl, HR + hl + 1)
            lr = slice(HR + 8 + hl, HR + 9 + hl)
            m1, m2 = dst[mr, :], src[mr, :]
            m = jnp.maximum(m1, m2)
            a = jnp.exp2((m1 - m) * c)
            b = jnp.exp2((m2 - m) * c)
            rr = slice(hl * 64, (hl + 1) * 64)
            dst[rr, :] = dst[rr, :] * a + src[rr, :] * b
            dst[mr, :] = m
            dst[lr, :] = dst[lr, :] * a + src[lr, :] * b

    o_r = Reduce(ring, part, rbuf, merge, sems[12:14])
    loads = [pltpu.make_async_copy(src, dst, ls.at[1 + n]) for n, (src, dst) in enumerate(((wo_hbm, wo_s), (wg_hbm, wg_s), (wu_hbm, wu_s), (wd_hbm, wd_s)))]
    ring.enter()
    y_g.start()
    mx_copy = remote(m_ref, mg, xs.at[0], xr.at[0], ring.partner)
    mx_copy.start()
    for cp in loads:
        cp.start()
    gob[...] = go_ref[...].astype(BF16)
    for half in range(2):
        yg[z, core, half] = y_ref[half * sub:(half + 1) * sub, :]
    hcol = pl.ds(pl.multiple_of(core * inner, 128), inner)
    qz[...] = jnp.zeros_like(qz)
    wqt[...] = wq_ref[:, hcol].T
    wk = wk_ref[:, hcol]
    wv = wv_ref[:, hcol]

    moves = {"y": y_g, "go": go_g, "o": o_r}

    def acts(*point):
        return [go_g.start if e[1] == "start" else part_(moves[e[0]].move, *e[1:]) for e in FWD_PLAN.get(point, [])]

    def run(*point):
        for fn in acts(*point):
            fn()

    def project(src, base, blocks):
        for j in blocks:
            r = pl.ds(pl.multiple_of(base + j * MC, MC), MC)
            blk = src[j * MC:(j + 1) * MC, :]
            kb = mm(blk, wk).astype(BF16)
            vb = mm(blk, wv).astype(BF16)
            k_s[r, :] = kb
            v_s[r, :] = vb
            kt_s[:, r] = kb.T
            vt_s[:, r] = vb.T

    nb = mem // MC
    project(m_ref, core * mem, range(nb))
    run("s", 0)
    mx_copy.wait_recv()
    project(mg, (1 - core) * mem, range(nb // 2))
    run("s", 1)
    project(mg, (1 - core) * mem, range(nb // 2, nb))
    run("s", 2)
    gain = g1_ref[...]
    one_row = jnp.where(lax.broadcasted_iota(jnp.int32, (16, QT), 0) == 0, 1.0, 0.0).astype(BF16)

    def lanes(chip):
        return pl.ds(pl.multiple_of(chip * QT, QT), QT)

    def prep(chip):
        n1 = rms_norm(yg[chip].reshape(QT, dim).astype(F32), gain).astype(BF16)
        qt = mm_bt(wqt[...], n1).astype(BF16)
        for h in range(hc):
            lo = h * 128 + (h % 2) * 64
            qz[lo:lo + 64, lanes(chip)] = qt[h * 64:(h + 1) * 64]

    def step(new, slot, old, pslot):
        if new is not None:
            chip, h = new
            rhs = jnp.concatenate([qz[pl.ds(pl.multiple_of(h * 128, 128), 128), lanes(chip)], one_row], axis=0)
            pair = pl.ds(pl.multiple_of((h // 2) * 128, 128), 128)
            mx = None
        if old is not None:
            ochip, half, hl = old
            m = jnp.max(mx_scr[pslot], axis=0, keepdims=True)
            vrow = pl.ds(pl.multiple_of((half * hh + hl) * 64, 64), 64)
            ls_ = None
            acc = None
        for j in range(T // MC):
            r = slice(j * MC, (j + 1) * MC)
            if new is not None:
                s = mm(jnp.concatenate([k_s[r, pair], ak_ref[r, 0:16]], axis=1), rhs)
                s_scr[slot, r, :] = s
                t = jnp.max(s.reshape(MC // 8, 8, QT), axis=0)
                mx = t if mx is None else jnp.maximum(mx, t)
            if old is not None:
                pr = jnp.exp2((s_scr[pslot, r, :] - m) * c)
                t = jnp.sum(pr.reshape(MC // 8, 8, QT), axis=0)
                ls_ = t if ls_ is None else ls_ + t
                dd = mm(vt_s[vrow, r], pr.astype(BF16))
                acc = dd if acc is None else acc + dd
        if new is not None:
            mx_scr[slot] = mx
        if old is not None:
            part[ochip, half, hl * 64:(hl + 1) * 64, :] = acc
            part[ochip, half, HR + hl:HR + hl + 1, :] = m
            part[ochip, half, HR + 8 + hl:HR + 9 + hl, :] = jnp.sum(ls_, axis=0, keepdims=True)

    offs = [o for o, _ in FWD_ORDER]
    halves = [h for _, h in FWD_ORDER]
    n = len(offs)
    fresh = [int(k + 1 < n and offs[k + 1] not in offs[:k + 1]) for k in range(n)]
    run("s", 3)
    y_g.ready(0)
    prep(z)
    step((z, halves[0] * hh), 0, None, None)

    def body(i, carry):
        i2 = jnp.minimum(i + 1, n - 1)
        chip, half = ring.chip(pick(i, offs)), pick(i, halves)
        chip2, half2 = ring.chip(pick(i2, offs)), pick(i2, halves)
        for k in range(hh):
            slot = (i * hh + k) % 2
            if k == hh - 1:
                dispatch(i, {kk: acts("r", kk) + [part_(y_g.ready, offs[kk + 1])] for kk in range(n) if fresh[kk]})
                pl.when(pick(i, fresh) == 1)(part_(prep, chip2))
                new = (chip2, half2 * hh)
            else:
                new = (chip, half * hh + k + 1)
            step(new, 1 - slot, (chip, half, k), slot)
            dispatch(i, {kk: acts("b", kk * hh + k) for kk in range(n) if acts("b", kk * hh + k)})
        return carry

    gl = [pltpu.make_async_copy(gob.at[pl.ds(half * sub, sub)], gog.at[z, core, half], ls.at[5 + half]) for half in range(2)]
    for cp in gl:
        cp.start()
    lax.fori_loop(0, n, body, 0)
    yc = pltpu.make_async_copy(yg, yall, ls.at[0])
    yc.start()
    run("t", 0)
    run("t", 1)
    qmine = pl.ds(pl.multiple_of(core * rows, rows), rows)
    qother = pl.ds(pl.multiple_of((1 - core) * rows, rows), rows)
    for h in range(hc):
        half, hl = h // hh, h % hh
        m = part[z, half, HR + hl:HR + hl + 1, :]
        l = part[z, half, HR + 8 + hl:HR + 9 + hl, :]
        own[h * 64:(h + 1) * 64, :] = part[z, half, hl * 64:(hl + 1) * 64, :] / l
        own[inner + h:inner + h + 1, :] = m + jnp.log2(l) / c
    satt[...] = own[:inner, qother].astype(BF16)
    xo = remote(satt, patt, xs.at[1], xr.at[1], ring.partner)
    xo.start()
    attt[pl.ds(pl.multiple_of(core * inner, inner), inner), :] = own[:inner, qmine].astype(BF16)
    for cp in loads:
        cp.wait()
    run("t", 2)
    xo.wait()
    attt[pl.ds(pl.multiple_of((1 - core) * inner, inner), inner), :] = patt[...]

    att = attt[...].T
    att_ref[...] = att
    gain2 = g2_ref[...]
    run("t", 3)
    hid = (y_ref[...].astype(F32) + mm(att, wo_s[...])).astype(BF16).astype(F32)
    inv = lax.rsqrt(jnp.mean(hid * hid, axis=-1, keepdims=True) + 1e-6)
    hhat = hid * inv
    n2 = (hhat * gain2).astype(BF16)
    gb = gob[...]
    dn = None
    fb = ff // 4
    for f in range(ff // fb):
        cols = slice(f * fb, (f + 1) * fb)
        wg, wu = wg_s[:, cols], wu_s[:, cols]
        g = mm(n2, wg)
        u = mm(n2, wu)
        ga = mm_bt(gb, wd_s[cols, :])
        sig = jax.nn.sigmoid(g)
        si = g * sig
        d = mm_bt((ga * u * (sig + si * (1.0 - sig))).astype(BF16), wg) + mm_bt((ga * si).astype(BF16), wu)
        dn = d if dn is None else dn + d
        run("t", 4 + f)
    gsum = jnp.sum(dn * hhat, axis=0, keepdims=True)
    gn_ref[...] = jnp.zeros_like(gn_ref)
    for k in range(dim // QT):
        gn_ref[k:k + 1, :] = gsum[:, k * QT:(k + 1) * QT]
    t = dn * gain2
    gh = go_ref[...] + inv * (t - hhat * jnp.mean(t * hhat, axis=-1, keepdims=True))
    gh_ref[...] = gh
    dh_ref[...] = gh.astype(BF16)
    run("t", 8)
    for off in range(-far + 1, far + 1):
        go_g.ready(off)
    mx_copy.wait_send()
    for cp in [yc] + gl:
        cp.wait()
    for obj in (y_g, go_g, o_r):
        obj.drain()


def fwd_call(dims, *args):
    chips, rows, mem, dim, hc, c, ff = dims
    hh = hc // 2
    inner = hc * 64
    QT = 2 * rows
    T = 2 * mem
    HR = hh * 64
    h2 = chips // 2
    v = pl.BlockSpec(memory_space=VMEM)
    hbm = pl.BlockSpec(memory_space=pl.ANY)
    S = jax.ShapeDtypeStruct
    s3 = (2, 2, h2)
    gshape = (chips, 2, 2, rows // 2, dim)
    rows_sems = [DMA(s3)] * 4 + [DMA((2,))] * 2
    return pl.pallas_call(
        functools.partial(fwd_kernel, dims),
        out_shape=(S((inner + 8, QT), F32), S((rows, 2 * inner), BF16), S((rows, dim), BF16), S((rows, dim), F32), S((8, QT), F32),
                   S((T, inner), BF16), S((T, inner), BF16), S((inner, T), BF16), S((hc * 128, chips * QT), BF16), S((mem, dim), BF16), S(gshape, BF16), S(gshape, BF16)),
        in_specs=[v] * 9 + [hbm] * 4, out_specs=(v,) * 10 + (hbm,) * 2,
        scratch_shapes=[
            VMEM(gshape, BF16), VMEM((inner, dim), BF16), VMEM((inner, T), BF16), VMEM((2, T, QT), F32), VMEM((2, 8, QT), F32),
            VMEM((chips, 2, HR + 16, QT), F32), VMEM((2, 2, h2, HR + 16, QT), F32), VMEM((inner, rows), BF16), VMEM((inner, rows), BF16),
            VMEM((rows, dim), BF16), VMEM((2 * inner, rows), BF16), VMEM((2 * inner, dim), BF16), VMEM((dim, ff), BF16), VMEM((dim, ff), BF16), VMEM((ff, dim), BF16)]
        + rows_sems * 2 + [DMA(s3)] * 2 + [DMA((2,))] * 2 + [DMA((7,))],
        compiler_params=pltpu.CompilerParams(vmem_limit_bytes=62 * 1024 * 1024, collective_id=0, has_side_effects=True),
        cost_estimate=pl.CostEstimate(flops=10**10, bytes_accessed=30 << 20, transcendentals=0),
        name="attn_fwd")(*args)


def solution(mesh):
    group = mesh.shape['seq']
    row_spec = P(('data', 'seq'), None)
    part_vec = P('data')
    part_mat = P('data', None)
    part_cube = P('data', None, None)

    def device_step(dec_in, memory, mem_len, grad_out, norm_attn, wq, wk, wv, wo, norm_mlp, w_gate, w_up, w_down):
        rows, dim = dec_in.shape
        mem = memory.shape[0]
        heads, hd = wq.shape[1], wq.shape[2]
        inner = heads * hd
        chips = group // 2
        hc = heads // 2
        c = LOG2E * hd ** -0.5
        dims = (chips, rows, mem, dim, hc, c, w_gate.shape[1])
        wq2, wk2, wv2 = (w.reshape(dim, inner) for w in (wq, wk, wv))
        wo2 = wo.reshape(inner, dim)
        gain1 = norm_attn.astype(F32)
        gain2 = norm_mlp.astype(F32)[None, :]

        pos = (lax.axis_index('seq') // 2) * 2 * mem + jnp.arange(2 * mem)
        bias = jnp.where(pos < mem_len[0], 0.0, -1e30).astype(F32)
        lane = jnp.arange(128)
        ak = jnp.where(lane[None, :] == 0, bias[:, None], jnp.where(lane[None, :] < 4, 1.0, 0.0)).astype(BF16)
        own, attended, dh, grad_hidden, gn, k_c, v_c, kt_c, qz, mem_p, y_all, go_all = fwd_call(
            dims, dec_in, grad_out, memory, ak, wq2, wk2, wv2, gain1[None, :], gain2, wo2, w_gate, w_up, w_down)
        gvec, dq_own, g_mem, g_wkv, g_wq, g_wo, g_down, g_gate, g_up, _ = bwd_call(
            dims, dh, own, gn, attended, ak, gain1[None, :], gain2,
            k_c, v_c, kt_c, qz, wo2, wq2, wk2, wv2, memory, mem_p, y_all, go_all, w_gate, w_up, w_down)
        x_in = dec_in.astype(F32)
        _, norm_pull = jax.vjp(rms_norm, x_in, gain1)
        grad_x_norm, _ = norm_pull(mm_bt(dq_own.T, wq2))
        g_dec = grad_hidden + grad_x_norm
        cube = (dim, heads, hd)
        g_wkv = g_wkv.reshape(hc, 2, 128, dim)
        return (g_dec, g_mem, gvec[0], g_wq.T.reshape(cube), g_wkv[:, 0].reshape(inner, dim).T.reshape(cube),
                g_wkv[:, 1].reshape(inner, dim).T.reshape(cube), g_wo.reshape(heads, hd, dim), gvec[1], g_gate, g_up, g_down)

    return jax.shard_map(device_step, mesh=mesh,
                         in_specs=(row_spec, row_spec, part_vec, row_spec) + (P(),) * 9,
                         out_specs=(row_spec, row_spec, part_vec, part_cube, part_cube, part_cube, part_cube, part_vec, part_mat, part_mat, part_mat),
                         check_vma=False)
```

```python
import functools
import math

import jax
import jax.numpy as jnp
from jax import lax
from jax.experimental import pallas as pl
from jax.experimental.pallas import tpu as pltpu
from jax.sharding import PartitionSpec as P

F32 = jnp.float32
BF16 = jnp.bfloat16
LOG2E = math.log2(math.e)
VMEM = pltpu.VMEM
MESH = pl.DeviceIdType.MESH


def mm(a, b):
    return jnp.dot(a, b, preferred_element_type=F32)


def mm_bt(a, b):
    return lax.dot_general(a, b, (((1,), (1,)), ((), ())), preferred_element_type=F32)


def mm_at(a, b):
    return lax.dot_general(a, b, (((0,), (0,)), ((), ())), preferred_element_type=F32)


def rms_norm(tensor, gain):
    mean_sq = jnp.mean(tensor * tensor, axis=-1, keepdims=True)
    return tensor * lax.rsqrt(mean_sq + 1e-6) * gain


RIGHT, LEFT = 0, 1
DMA = pltpu.SemaphoreType.DMA

FWD_ORDER = [(0, 0), (0, 1), (1, 0), (1, 1), (-3, 0), (3, 1), (4, 0), (4, 1), (3, 0), (-3, 1), (2, 0), (-2, 1), (2, 1), (-2, 0), (-1, 1), (-1, 0)]
BWD_ORDER = [0, 1, 4, 3, -3, 2, -2, -1]
BWD_FIRST = 2
FWD_PLAN = {
    ("b", 11): [("y", 1, 1, 3), ("y", 1, 0, 3), ("go", 0, 0, 1)],
    ("b", 12): [("go", 1, 1, 1)],
    ("b", 14): [("o", 1, 0, 3), ("go", 0, 1, 1)],
    ("b", 16): [("y", 0, 0, 4)],
    ("b", 17): [("o", 0, 1, 3), ("go", 1, 0, 1)],
    ("b", 19): [("go", 1, 1, 2)],
    ("b", 20): [("o", 0, 0, 4)],
    ("b", 23): [("o", 1, 1, 4)],
    ("b", 29): [("go", 0, 0, 2)],
    ("b", 30): [("go", 1, 0, 2)],
    ("b", 32): [("go", 0, 1, 2), ("go", 1, 1, 3)],
    ("b", 35): [("o", 0, 0, 3)],
    ("b", 36): [("o", 1, 1, 3)],
    ("b", 38): [("o", 0, 1, 2)],
    ("b", 39): [("go", 1, 0, 3)],
    ("b", 4): [("y", 0, 0, 2), ("y", 1, 1, 2)],
    ("b", 41): [("o", 1, 0, 2), ("go", 0, 1, 3), ("go", 1, 1, 4)],
    ("b", 7): [("y", 0, 1, 2), ("y", 1, 0, 2)],
    ("b", 8): [("go", "start")],
    ("r", 3): [("y", 0, 0, 3), ("y", 0, 1, 3)],
    ("r", 5): [("y", 1, 1, 4)],
    ("s", 1): [("y", 0, 0, 1), ("y", 1, 1, 1)],
    ("s", 2): [("y", 0, 1, 1), ("y", 1, 0, 1)],
    ("t", 1): [("o", 0, 0, 2), ("o", 1, 1, 2), ("o", 0, 1, 1), ("o", 1, 0, 1), ("o", 0, 0, 1), ("o", 1, 1, 1), ("o", 0, 1, 0), ("o", 1, 0, 0), ("o", 0, 0, 0), ("o", 1, 1, 0)],
    ("t", 2): [("go", 0, 0, 3)],
    ("t", 6): [("go", 0, 0, 4)],
}
BWD_PLAN = {
    ("b", 1): [("dh", 0, 0, 1), ("dh", 1, 1, 1)],
    ("b", 10): [("dh", 0, 1, 3), ("dh", 1, 0, 3), ("st", 0, 0, 3), ("st", 1, 1, 3)],
    ("b", 11): [("st", 0, 1, 3), ("st", 1, 0, 3)],
    ("b", 12): [("dq0", 0, 0, 4)],
    ("b", 13): [("dq0", 1, 1, 4)],
    ("b", 14): [("att", 0, 0, 1), ("att", 1, 1, 1)],
    ("b", 15): [("dq0", 0, 1, 3), ("att", 1, 0, 1)],
    ("b", 16): [("dq0", 0, 0, 3), ("dq0", 1, 0, 3), ("att", 0, 1, 1)],
    ("b", 17): [("dq0", 1, 1, 3)],
    ("b", 18): [("att", 0, 0, 2), ("att", 1, 1, 2)],
    ("b", 19): [("dq0", 0, 1, 2), ("att", 1, 0, 2), ("dq0", 0, 0, 2)],
    ("b", 2): [("dh", 0, 1, 1), ("dh", 1, 0, 1), ("st", 0, 0, 1), ("st", 1, 1, 1), ("st", 0, 1, 1), ("st", 1, 0, 1)],
    ("b", 20): [("dq0", 1, 0, 2)],
    ("b", 21): [("dq0", 1, 1, 2), ("att", 0, 1, 2)],
    ("b", 22): [("att", 0, 0, 3), ("att", 1, 1, 3)],
    ("b", 23): [("dq0", 0, 1, 1), ("dq0", 0, 0, 1), ("ar0", 0, 1, 3), ("dq0", 1, 0, 1), ("ar0", 1, 0, 3), ("ar0", 0, 0, 4), ("ar0", 1, 1, 4), ("att", 1, 0, 3)],
    ("b", 24): [("dq0", 1, 1, 1), ("dq1", 0, 0, 4), ("att", 0, 1, 3)],
    ("b", 25): [("dq1", 1, 1, 4)],
    ("b", 26): [("att", 0, 0, 4), ("att", 1, 1, 4)],
    ("b", 27): [("dq0", 0, 1, 0), ("dq0", 1, 0, 0), ("dq1", 0, 1, 3)],
    ("b", 28): [("dq0", 0, 0, 0), ("dq1", 1, 0, 3), ("ar0", 1, 0, 2), ("ar0", 1, 1, 3), ("ar0", 0, 1, 2)],
    ("b", 29): [("dq0", 1, 1, 0), ("ds0", "start"), ("ar0", 0, 0, 3)],
    ("b", 30): [("dq1", 0, 0, 3), ("dq1", 1, 1, 3)],
    ("b", 31): [("dq1", 0, 1, 2)],
    ("b", 32): [("dq1", 1, 0, 2), ("ar0", 0, 1, 1), ("ar0", 1, 0, 1), ("ds0", 0, 0, 1)],
    ("b", 33): [("ar0", 1, 1, 2), ("ds0", 0, 1, 1), ("ds0", 1, 1, 1)],
    ("b", 34): [("ar0", 0, 0, 2), ("ds0", 1, 0, 1)],
    ("b", 35): [("dq1", 0, 0, 2), ("dq1", 1, 1, 2), ("dq1", 0, 1, 1), ("dq1", 1, 0, 1), ("ar0", 0, 1, 0), ("ar0", 1, 0, 0), ("ar1", 0, 1, 3), ("ar1", 1, 0, 3), ("ar1", 0, 0, 4), ("ar1", 1, 1, 4), ("ds0", 0, 0, 2)],
    ("b", 36): [("dq2", 0, 0, 4), ("ar0", 1, 1, 1), ("ds0", 0, 1, 2), ("ds0", 1, 1, 2)],
    ("b", 37): [("dq2", 1, 1, 4), ("ar0", 0, 0, 1), ("ds0", 1, 0, 2)],
    ("b", 38): [("dq1", 0, 0, 1), ("dq1", 1, 1, 1)],
    ("b", 39): [("dq1", 0, 1, 0), ("dq1", 1, 0, 0), ("dq2", 0, 1, 3)],
    ("b", 40): [("dq2", 1, 0, 3), ("ar1", 0, 1, 2), ("ar1", 1, 0, 2), ("ar1", 0, 0, 3), ("ar1", 1, 1, 3)],
    ("b", 41): [("ar0", 1, 1, 0), ("ds0", 0, 0, 3), ("ds0", 1, 1, 3)],
    ("b", 42): [("dq2", 0, 0, 3), ("dq2", 1, 1, 3), ("ds0", 0, 1, 3)],
    ("b", 43): [("ar0", 0, 0, 0), ("as0", "start"), ("ds0", 1, 0, 3)],
    ("b", 44): [("dq1", 0, 0, 0), ("dq1", 1, 1, 0), ("ds1", "start")],
    ("b", 45): [("dq2", 0, 1, 2), ("dq2", 1, 0, 2)],
    ("b", 46): [("ar1", 0, 1, 1), ("ar1", 1, 0, 1), ("ar1", 0, 0, 2), ("ar1", 1, 1, 2)],
    ("b", 47): [("dq2", 0, 0, 2), ("dq2", 1, 1, 2), ("ar2", 0, 1, 3), ("ar2", 1, 0, 3), ("ar2", 0, 0, 4), ("ar2", 1, 1, 4), ("as0", 0, 0, 1), ("as0", 1, 1, 1), ("ds0", 0, 0, 4), ("ds0", 1, 1, 4)],
    ("b", 5): [("dh", 0, 0, 2), ("dh", 1, 1, 2)],
    ("b", 6): [("dh", 0, 1, 2), ("dh", 1, 0, 2), ("st", 0, 0, 2), ("st", 1, 1, 2)],
    ("b", 7): [("st", 0, 1, 2), ("st", 1, 0, 2)],
    ("b", 9): [("dh", 0, 0, 3), ("dh", 1, 1, 3)],
    ("f", 0): [("ar2", 0, 1, 2), ("ar2", 1, 0, 2), ("ar2", 0, 0, 3), ("ar2", 1, 1, 3)],
    ("f", 1): [("as0", 0, 0, 2), ("as0", 1, 1, 2)],
    ("f", 11): [("ar2", 0, 0, 2), ("ar2", 1, 1, 2)],
    ("f", 13): [("as0", 0, 0, 3), ("as0", 1, 1, 3)],
    ("f", 15): [("as0", 0, 1, 3), ("as0", 1, 0, 3)],
    ("f", 16): [("ds1", 0, 0, 3), ("ds1", 1, 1, 3)],
    ("f", 17): [("as1", 0, 0, 1), ("ds1", 0, 1, 3), ("ds1", 1, 0, 3), ("as1", 1, 1, 1), ("ds2", 0, 0, 1), ("ds2", 1, 1, 1), ("ds2", 0, 1, 1), ("ds2", 1, 0, 1)],
    ("f", 19): [("as1", 0, 1, 1), ("as1", 1, 0, 1)],
    ("f", 21): [("ar2", 0, 1, 0), ("ar2", 1, 0, 0)],
    ("f", 23): [("ar2", 0, 0, 1), ("ar2", 1, 1, 1)],
    ("f", 24): [("as0", 0, 0, 4), ("as0", 1, 1, 4)],
    ("f", 26): [("as1", 0, 0, 2), ("as1", 1, 1, 2), ("ds1", 0, 0, 4), ("ds1", 1, 1, 4), ("ds2", 0, 0, 2), ("ds2", 1, 1, 2), ("ds2", 0, 1, 2), ("ds2", 1, 0, 2)],
    ("f", 27): [("as1", 0, 1, 2), ("as1", 1, 0, 2)],
    ("f", 29): [("ar2", 0, 0, 0), ("ar2", 1, 1, 0), ("as2", "start")],
    ("f", 3): [("as0", 0, 1, 2), ("as0", 1, 0, 2)],
    ("f", 33): [("as1", 0, 0, 3), ("as1", 1, 1, 3)],
    ("f", 34): [("ds2", 0, 0, 3), ("ds2", 1, 1, 3)],
    ("f", 35): [("as1", 0, 1, 3), ("as1", 1, 0, 3), ("as2", 0, 0, 1), ("as2", 1, 1, 1), ("ds2", 0, 1, 3), ("ds2", 1, 0, 3)],
    ("f", 4): [("ds1", 0, 0, 2)],
    ("f", 5): [("ds1", 1, 1, 2)],
    ("f", 6): [("ds1", 0, 1, 2), ("ds1", 1, 0, 2)],
    ("f", 8): [("dq2", 0, 1, 0), ("dq2", 1, 0, 0), ("dq2", 0, 0, 0), ("dq2", 1, 1, 0), ("ds2", "start"), ("ar1", 0, 0, 0), ("ar1", 1, 1, 0), ("as1", "start")],
    ("f", 9): [("ar2", 0, 1, 1), ("ar2", 1, 0, 1)],
    ("h", 0): [("as0", 0, 1, 1), ("as0", 1, 0, 1)],
    ("h", 1): [("ds1", 0, 0, 1), ("ds1", 1, 1, 1)],
    ("h", 2): [("ds1", 0, 1, 1), ("ds1", 1, 0, 1)],
    ("h", 3): [("dq2", 0, 1, 1), ("dq2", 1, 0, 1)],
    ("h", 4): [("ar1", 0, 1, 0), ("ar1", 1, 0, 0)],
    ("h", 5): [("ar1", 0, 0, 1), ("ar1", 1, 1, 1)],
    ("h", 7): [("dq2", 0, 0, 1), ("dq2", 1, 1, 1)],
    ("m", 0): [("as2", 0, 1, 1), ("as2", 1, 0, 1)],
    ("m", 1): [("as1", 0, 0, 4), ("as1", 1, 1, 4), ("ds2", 0, 0, 4), ("ds2", 1, 1, 4)],
    ("m", 2): [("as2", 0, 0, 2), ("as2", 1, 1, 2)],
    ("m", 3): [("as2", 0, 1, 2), ("as2", 1, 0, 2)],
    ("q", 3): [("as2", 0, 0, 3), ("as2", 1, 1, 3)],
    ("q", 5): [("as2", 0, 1, 3), ("as2", 1, 0, 3)],
    ("q", 8): [("as2", 0, 0, 4), ("as2", 1, 1, 4)],
    ("r", 12): [("dh", 0, 0, 4), ("dh", 1, 1, 4), ("att", "start"), ("st", 0, 0, 4), ("st", 1, 1, 4)],
}


class Ring:
    def __init__(self, chips):
        me = lax.axis_index('seq')
        self.chips = chips
        self.far = chips // 2
        self.z = me // 2
        self.core = me - 2 * self.z
        self.partner = 2 * self.z + 1 - self.core
        self.next = (2 * self.chip(1) + self.core, 2 * self.chip(-1) + self.core)
        self.hops = {(RIGHT, 0): self.far, (LEFT, 1): self.far, (RIGHT, 1): self.far - 1, (LEFT, 0): self.far - 1}

    def chip(self, off):
        return lax.rem(self.z + off + self.chips, self.chips)

    def ahead(self, d, k):
        return self.chip(k if d == RIGHT else -k)

    def enter(self):
        barrier = pltpu.get_barrier_semaphore()
        for dev in (self.partner,) + self.next:
            pl.semaphore_signal(barrier, inc=1, device_id={'seq': dev}, device_id_type=MESH)
        pl.semaphore_wait(barrier, 3)


def remote(src, dst, ssem, rsem, dev):
    return pltpu.make_async_remote_copy(src_ref=src, dst_ref=dst, send_sem=ssem, recv_sem=rsem, device_id={'seq': dev}, device_id_type=MESH)


class Share:
    def __init__(self, ring, buf, src, sems):
        self.ring, self.buf, self.src = ring, buf, src
        self.ss, self.rs = sems

    def slot(self, chip, half):
        return self.buf.at[chip, half]

    def send(self, d, half, t):
        slot = self.slot(self.ring.ahead(d, 1 - t), half)
        src = self.src(half) if t == 1 else slot
        return remote(src, slot, self.ss.at[d, half, t - 1], self.rs.at[d, half, t - 1], self.ring.next[d])

    def recv(self, d, half, t):
        slot = self.slot(self.ring.ahead(d, -t), half)
        return remote(slot, slot, self.ss.at[d, half, t - 1], self.rs.at[d, half, t - 1], self.ring.next[d])

    def start(self):
        for d, half in self.ring.hops:
            self.send(d, half, 1).start()

    def came(self, d, half, t):
        pass

    def move(self, d, half, t):
        self.recv(d, half, t).wait_recv()
        if t < self.ring.hops[d, half]:
            self.send(d, half, t + 1).start()
        self.came(d, half, t)

    def drain(self):
        for (d, half), n in self.ring.hops.items():
            for t in range(1, n + 1):
                self.send(d, half, t).wait_send()


class Rows(Share):
    def __init__(self, ring, buf, src, sems):
        super().__init__(ring, buf, src, sems[:2])
        self.fs, self.fr, self.os, self.orr = sems[2:]

    def slot(self, chip, half):
        return self.buf.at[chip, self.ring.core, half]

    def pslot(self, chip, half):
        return self.buf.at[chip, 1 - self.ring.core, half]

    def start(self):
        super().start()
        for half in range(2):
            self.own(half).start()

    def own(self, half):
        return remote(self.src(half), self.slot(self.ring.z, half), self.os.at[half], self.orr.at[half], self.ring.partner)

    def forward(self, d, half, t):
        slot = self.slot(self.ring.ahead(d, -t), half)
        return remote(slot, slot, self.fs.at[d, half, t - 1], self.fr.at[d, half, t - 1], self.ring.partner)

    def came(self, d, half, t):
        self.forward(d, half, t).start()

    def ready(self, off):
        ring = self.ring
        if off == 0:
            for half in range(2):
                slot = self.pslot(ring.z, half)
                remote(slot, slot, self.os.at[half], self.orr.at[half], ring.partner).wait_recv()
            return
        for (d, half), n in ring.hops.items():
            t = ring.far if abs(off) == ring.far else (-off if d == RIGHT else off)
            if 1 <= t <= n:
                slot = self.pslot(ring.ahead(d, -t), half)
                remote(slot, slot, self.fs.at[d, half, t - 1], self.fr.at[d, half, t - 1], ring.partner).wait_recv()

    def drain(self):
        super().drain()
        for half in range(2):
            self.own(half).wait_send()
        for (d, half), n in self.ring.hops.items():
            for t in range(1, n + 1):
                self.forward(d, half, t).wait_send()


class Reduce:
    def __init__(self, ring, part, rbuf, merge, sems):
        self.ring, self.part, self.rbuf, self.merge = ring, part, rbuf, merge
        self.ss, self.rs = sems

    def send(self, d, half, o):
        return remote(self.part.at[self.ring.ahead(d, o), half], self.rbuf.at[d, half, o - 1], self.ss.at[d, half, o - 1], self.rs.at[d, half, o - 1], self.ring.next[d])

    def recv(self, d, half, o):
        slot = self.rbuf.at[d, half, o]
        return remote(slot, slot, self.ss.at[d, half, o], self.rs.at[d, half, o], self.ring.next[d])

    def move(self, d, half, o):
        if o < self.ring.hops[d, half]:
            self.recv(d, half, o).wait_recv()
            self.merge(self.part.at[self.ring.ahead(d, o), half], self.rbuf.at[d, half, o])
        if o > 0:
            self.send(d, half, o).start()

    def drain(self):
        for (d, half), n in self.ring.hops.items():
            for o in range(1, n + 1):
                self.send(d, half, o).wait_send()


def pick(i, values):
    out = jnp.int32(values[-1])
    for k, v in enumerate(values[:-1]):
        out = jnp.where(i == k, jnp.int32(v), out)
    return out


def mask_lanes(ref, len_ref, start):
    row = lax.broadcasted_iota(jnp.int32, ref.shape, 0) + start
    lane = lax.broadcasted_iota(jnp.int32, ref.shape, 1)
    bias = jnp.where(row < len_ref[0], 0.0, -1e30)
    ref[...] = jnp.where(lane == 0, bias, jnp.where(lane < 4, 1.0, 0.0)).astype(BF16)


def dispatch(index, table):
    def branch(keys):
        if len(keys) == 1:
            def run():
                for fn in table[keys[0]]:
                    fn()
            pl.when(index == keys[0])(run)
            return
        low, high = keys[:len(keys) // 2], keys[len(keys) // 2:]
        pl.when(index < high[0])(functools.partial(branch, low))
        pl.when(index >= high[0])(functools.partial(branch, high))
    if table:
        branch(sorted(table))


def add_into(dst, src):
    dst[...] = dst[...] + src[...]


def parts3(x):
    hi = x.astype(BF16)
    rest = x - hi.astype(F32)
    mid = rest.astype(BF16)
    lo = (rest - mid.astype(F32)).astype(BF16)
    return hi, mid, lo


def bwd_kernel(dims, len_ref, dh_ref, own_ref, gn_ref, att_ref, g1_ref, g2_ref,
               k_hbm, v_hbm, kt_hbm, qz_hbm, wo_hbm, wq_hbm, wk_hbm, wv_hbm, ma_hbm, mb_hbm, y_hbm, gog, wg_hbm, wu_hbm, wd_hbm,
               gvec_ref, dqo_ref, gmem, gwkv, gwq, gwo, gdown, ggate, gup, attg,
               k_ref, v_ref, kt_ref, qz_ref, wo_ref, wq_ref, wk_ref, wv_ref, ak_ref,
               dhg, doz, aqs, ads, stb, dk, dv, dkv, dkvp, dqp, dqr, dqa, arp, arr, ara, pvec, pdq, spb,
               msc, ybuf, abuf, wbuf, dbuf, wt, gst, gsw, gwo_s, gwq_s,
               *sems):
    chips, rows, mem, dim, hc, c, ff = dims
    QT = 2 * rows
    T = 2 * mem
    MC = min(256, mem)
    nm = T // MC
    inner = hc * 64
    np_ = hc // 2
    seg = dim // chips // 2
    fh = ff // 2
    FT = wt.shape[1]
    nf = fh // FT
    ring = Ring(chips)
    z, core, far = ring.z, ring.core, ring.far
    sems = list(sems)

    def take(n):
        out = sems[:n]
        del sems[:n]
        return out

    half_rows = rows // 2
    part_ = functools.partial
    rsrc = lambda ref: (lambda half: ref.at[pl.ds(half * half_rows, half_rows)])
    dh_g = Rows(ring, dhg, rsrc(dh_ref), take(6))
    att_g = Rows(ring, attg, rsrc(att_ref), take(6))
    st_g = Share(ring, stb, lambda half: stb.at[z, half], take(2))
    dq_r = [Reduce(ring, dqp.at[p], dqr.at[p], add_into, take(2)) for p in range(np_)]
    dq_s = [Share(ring, dqa.at[p], lambda half, p=p: dqa.at[p, z, half], take(2)) for p in range(np_)]
    ar_r = [Reduce(ring, arp.at[p], arr.at[p], add_into, take(2)) for p in range(np_)]
    ar_s = [Share(ring, ara.at[p], lambda half, p=p: ara.at[p, z, half], take(2)) for p in range(np_)]
    xs, xr, ls, gs, gr, gl, wsem, ysem, lsem = take(9)
    loads = [pltpu.make_async_copy(src, dst, lsem.at[n]) for n, (src, dst) in enumerate((
        (wo_hbm, wo_ref), (k_hbm, k_ref), (v_hbm, v_ref), (kt_hbm, kt_ref), (qz_hbm, qz_ref),
        (ma_hbm, msc.at[0, pl.ds(0, mem)]), (mb_hbm, msc.at[1, pl.ds(0, mem)]), (wq_hbm, wq_ref), (wk_hbm, wk_ref), (wv_hbm, wv_ref)))]
    for cp in loads:
        cp.start()
    ring.enter()
    dh_g.start()
    locals_ = [pltpu.make_async_copy(att_ref.at[pl.ds(half * half_rows, half_rows)], attg.at[z, core, half], ls.at[half]) for half in range(2)]
    for cp in locals_:
        cp.start()
    for half in range(2):
        dhg[z, core, half] = dh_ref[half * half_rows:(half + 1) * half_rows, :]
    doz[...] = jnp.zeros_like(doz)
    mask_lanes(ak_ref, len_ref, z * T)
    hrow = pl.ds(pl.multiple_of(core * inner, inner), inner)
    hcol = pl.ds(pl.multiple_of(core * inner, 128), inner)
    other_cols = pl.ds(pl.multiple_of((1 - core) * mem, mem), mem)
    my_cols = pl.ds(pl.multiple_of(core * mem, mem), mem)
    qmine = pl.ds(pl.multiple_of(core * rows, rows), rows)
    qother = pl.ds(pl.multiple_of((1 - core) * rows, rows), rows)

    def lanes(chip):
        return pl.ds(pl.multiple_of(chip * QT, QT), QT)

    def d_out(chip):
        return mm_bt(wo_ref[hrow, :], dhg[chip].reshape(QT, dim))

    def prepare(chip, dot=None):
        dot = d_out(chip) if dot is None else dot
        dob = dot.astype(BF16)
        q = lanes(chip)
        row = lax.broadcasted_iota(jnp.int32, (16, QT), 0)
        for h in range(hc):
            lo = h * 128 + (h % 2) * 64
            doz[lo:lo + 64, q] = dob[h * 64:(h + 1) * 64]
            for ref, half, first in ((aqs, 0, 1.0), (ads, 1, 0.0)):
                a, b, e = (x.astype(F32) for x in parts3(stb[chip, half, h:h + 1, :]))
                ref[h * 16:(h + 1) * 16, q] = jnp.where(row == 0, first, jnp.where(row == 1, a, jnp.where(row == 2, b, jnp.where(row == 3, e, 0.0)))).astype(BF16)

    dh_g.ready(0)
    loads[0].wait()
    dot0 = d_out(z)
    prod = dot0 * own_ref[:inner, :]
    for h in range(hc):
        stb[z, 0, h:h + 1, :] = -own_ref[inner + h:inner + h + 1, :]
        stb[z, 1, h:h + 1, :] = -jnp.sum(prod[h * 64:(h + 1) * 64], axis=0, keepdims=True)
    stb[z, 0, hc:8, :] = gn_ref[0:8 - hc, :]
    stb[z, 1, hc:8, :] = gn_ref[8 - hc:16 - 2 * hc, :]
    st_g.start()
    prepare(z, dot0)
    dk[...] = jnp.zeros_like(dk)
    dv[...] = jnp.zeros_like(dv)
    for cp in loads[1:]:
        cp.wait()

    def tile(h, chip):
        pair = h // 2
        q = lanes(chip)
        hz = pl.ds(pl.multiple_of(h * 128, 128), 128)
        h16 = pl.ds(pl.multiple_of(h * 16, 16), 16)
        ps = pl.ds(pl.multiple_of(pair * 128, 128), 128)
        hz64 = pl.ds(pl.multiple_of(h * 128 + (h - 2 * pair) * 64, 64), 64)
        h64 = pl.ds(pl.multiple_of(h * 64, 64), 64)
        hr = h64
        q_t = qz_ref[hz64, q]
        do_t = doz[hz64, q]
        r1 = jnp.concatenate([qz_ref[hz, q], aqs[h16, q]], axis=0)
        r2 = jnp.concatenate([doz[hz, q], ads[h16, q]], axis=0)
        stage = {}
        dq = None
        for j in range(nm + 2):
            if j < nm:
                r = slice(j * MC, (j + 1) * MC)
                ak = ak_ref[r, 0:16]
                stage["a", j] = (mm(jnp.concatenate([k_ref[r, ps], ak], axis=1), r1), mm(jnp.concatenate([v_ref[r, ps], ak], axis=1), r2))
            if 1 <= j <= nm:
                s, dp = stage.pop(("a", j - 1))
                a = jnp.exp2(s * c)
                stage["b", j - 1] = (a.astype(BF16), (a * dp).astype(BF16))
            if j >= 2:
                r = slice((j - 2) * MC, (j - 1) * MC)
                pb, ds = stage.pop(("b", j - 2))
                dv[hr, r] += mm_bt(do_t, pb)
                dk[hr, r] += mm_bt(q_t, ds)
                d = mm(kt_ref[h64, r], ds)
                dq = d if dq is None else dq + d
        dqp[pair, chip, h - 2 * pair] = dq

    scale = 0.125

    def xp(p):
        return remote(dkv.at[p, :, other_cols], dkvp.at[p], xs.at[p], xr.at[p], ring.partner)

    def xq(p):
        return remote(dqa.at[p, z, :, :, qother], pdq.at[p], xs.at[np_ + p], xr.at[np_ + p], ring.partner)

    def share_dq(p):
        for half in range(2):
            dqa[p, z, half] = (dqp[p, z, half] * scale).astype(BF16)
        dq_s[p].start()
        xq(p).start()

    def share_ar(p):
        for half in range(2):
            ara[p, z, half] = arp[p, z, half]
        ar_s[p].start()

    moves = {"dh": dh_g, "st": st_g, "att": att_g}
    begins = {"att": att_g.start}
    for p in range(np_):
        moves.update({f"dq{p}": dq_r[p], f"ds{p}": dq_s[p], f"ar{p}": ar_r[p], f"as{p}": ar_s[p]})
        begins.update({f"ds{p}": part_(share_dq, p), f"as{p}": part_(share_ar, p)})

    def acts(*point):
        return [begins[e[0]] if e[1] == "start" else part_(moves[e[0]].move, *e[1:]) for e in BWD_PLAN.get(point, [])]

    def run(*point):
        for fn in acts(*point):
            fn()

    def table(kind, n):
        return {k: acts(kind, k) for k in range(n) if acts(kind, k)}

    offs = BWD_ORDER
    first = BWD_FIRST * hc
    per = 2 * (chips - BWD_FIRST)
    needs = {k * hc: offs[k] for k in range(1, BWD_FIRST)}
    needs.update({first + 2 * (k - BWD_FIRST): offs[k] for k in range(BWD_FIRST, chips)})

    def project(p):
        r = pl.ds(pl.multiple_of(p * 128, 128), 128)
        dkv[p, 0:128, :] = (dk[r, :] * scale).astype(BF16)
        dkv[p, 128:256, :] = dv[r, :].astype(BF16)
        xp(p).start()
        g = (mm(dkv[p, :, my_cols], msc[0, 0:mem]) + mm(dkv[p, :, other_cols], msc[1, 0:mem])).T
        for n in range(2 * chips):
            arp[p, n // 2, n % 2] = g[n * seg:(n + 1) * seg]

    def body(it, carry):
        early = it < first
        b = it - first
        p = b // per
        r = b - p * per
        h = jnp.where(early, it % hc, 2 * p + r % 2)
        chip = ring.chip(pick(jnp.where(early, it // hc, BWD_FIRST + r // 2), offs))
        dispatch(it, {k: acts("r", k) + [part_(dh_g.ready, off)] for k, off in needs.items()})
        fresh = (early & (it > 0) & (it % hc == 0)) | ((b >= 0) & (b < per) & (r % 2 == 0))
        pl.when(fresh)(part_(prepare, chip))
        tile(h, chip)
        pl.when((b >= 0) & (r == per - 1))(part_(project, p))
        dispatch(it, table("b", chips * hc))
        return carry

    lax.fori_loop(0, chips * hc, body, 0)
    run("p", np_)
    near = range(1 - far, far + 1)

    for cp in locals_:
        cp.wait()
    for off in near:
        att_g.ready(off)
    gain2 = g2_ref[...].astype(F32)
    gwo_s[...] = jnp.zeros_like(gwo_s)

    def y_fetch(ch, slot):
        return pltpu.make_async_copy(y_hbm.at[ch], ybuf.at[slot], ysem.at[slot, 0])

    def fetch(ch, slot):
        return (y_fetch(ch, slot), pltpu.make_async_copy(attg.at[ch], abuf.at[slot], ysem.at[slot, 1]))

    for cp in fetch(0, 0):
        cp.start()

    def hidden(ch, carry):
        slot = ch % 2
        for cp in fetch(ch, slot):
            cp.wait()

        @pl.when(ch + 1 < chips)
        def _():
            for cp in fetch(ch + 1, 1 - slot):
                cp.start()
        att = abuf[slot].reshape(QT, dim)
        h = (ybuf[slot].reshape(QT, dim).astype(F32) + mm(att, wo_ref[...])).astype(BF16)
        qz_ref[0:dim, lanes(ch)] = rms_norm(h.astype(F32), gain2).astype(BF16).T
        ah = jnp.where(core == 0, att[:, :inner], att[:, inner:])
        gwo_s[...] += mm_at(ah, dhg[ch].reshape(QT, dim))
        dispatch(ch, table("h", chips))
        return carry

    lax.fori_loop(0, chips, hidden, 0)
    dh_g.drain()
    go_load = pltpu.make_async_copy(gog, dhg, ls.at[0])
    go_load.start()

    def partner_block(buf, dst, k):
        return pltpu.make_async_copy(buf, dst, gl.at[k]), remote(buf, dst, gs.at[k], gr.at[k], ring.partner)

    def both_start(pair):
        pair[0].start()
        pair[1].start()

    def both_wait(pair):
        pair[0].wait()
        pair[1].wait()

    wo_out = partner_block(gwo_s, gwo.at[hrow], 3 * nf)
    both_start(wo_out)

    def w_fetch(f, slot):
        cols = pl.ds(pl.multiple_of(core * fh + f * FT, FT), FT)
        return (pltpu.make_async_copy(wg_hbm.at[:, cols], wbuf.at[slot, 0], wsem.at[slot, 0]),
                pltpu.make_async_copy(wu_hbm.at[:, cols], wbuf.at[slot, 1], wsem.at[slot, 1]),
                pltpu.make_async_copy(wd_hbm.at[cols], dbuf.at[slot], wsem.at[slot, 2]))

    for cp in w_fetch(0, 0):
        cp.start()
    go_load.wait()
    f_table = table("f", 9 * nf)

    def block(f, n):
        if n == 0:
            return partner_block(gst.at[0, pl.ds(0, FT)], gdown.at[pl.ds(pl.multiple_of(core * fh + f * FT, FT), FT)], f)
        return partner_block(gsw.at[n - 1], (ggate, gup)[n - 1].at[:, pl.ds(pl.multiple_of(core * fh + f * FT, FT), FT)], n * nf + f)

    def mlp(f, carry):
        slot = f % 2
        for cp in w_fetch(f, slot):
            cp.wait()

        @pl.when(f + 1 < nf)
        def _():
            for cp in w_fetch(f + 1, 1 - slot):
                cp.start()
        for n in range(2):
            wt[n] = wbuf[slot, n].T

        def act_chunk(ch, cc):
            q = lanes(ch)
            n2t = qz_ref[0:dim, q]
            g = mm(wt[0], n2t)
            u = mm(wt[1], n2t)
            ga = mm_bt(dbuf[slot], dhg[ch].reshape(QT, dim))
            sig = jax.nn.sigmoid(g)
            si = g * sig
            doz[0:FT, q] = (si * u).astype(BF16)
            doz[FT:2 * FT, q] = (ga * u * (sig + si * (1.0 - sig))).astype(BF16)
            doz[2 * FT:3 * FT, q] = (ga * si).astype(BF16)
            dispatch(f * 9 + ch, f_table)
            return cc

        lax.fori_loop(0, chips, act_chunk, 0)

        @pl.when(f > 0)
        def _():
            for n in range(3):
                both_wait(block(f - 1, n))
        acc = [None] * 3
        for ch in range(chips):
            q = slice(ch * QT, (ch + 1) * QT)
            n2t = qz_ref[0:dim, q]
            for n, d in enumerate((mm(doz[0:FT, q], dhg[ch].reshape(QT, dim)), mm_bt(n2t, doz[FT:2 * FT, q]), mm_bt(n2t, doz[2 * FT:3 * FT, q]))):
                acc[n] = d if acc[n] is None else acc[n] + d
        gst[0, 0:FT] = acc[0]
        gsw[0] = acc[1]
        gsw[1] = acc[2]
        for n in range(3):
            both_start(block(f, n))
        dispatch(f * 9 + 8, f_table)
        return carry

    lax.fori_loop(0, nf, mlp, 0)
    for p in range(np_):
        remote(dkvp.at[p], dkvp.at[p], xs.at[p], xr.at[p], ring.partner).wait_recv()
    nb = 4
    w = mem // nb
    for n in range(3):
        both_wait(block(nf - 1, n))

    def gm(b):
        return pltpu.make_async_copy(gst.at[b % 2, pl.ds(0, w)], gmem.at[pl.ds(pl.multiple_of(b * w, w), w)], gl.at[3 * nf + 2 + b % 2])

    def memory_rows(b, carry):
        @pl.when(b > 1)
        def _():
            gm(b - 2).wait()
        cb = pl.ds(pl.multiple_of(core * mem + b * w, w), w)
        cp = pl.ds(pl.multiple_of(b * w, w), w)
        acc = None
        for p in range(np_):
            own_e = pl.ds(pl.multiple_of(core * inner + p * 128, 128), 128)
            oth_e = pl.ds(pl.multiple_of((1 - core) * inner + p * 128, 128), 128)
            for part, w_ref in ((0, wk_ref), (1, wv_ref)):
                e = slice(part * 128, (part + 1) * 128)
                lhs = jnp.concatenate([dkv[p, e, cb], dkvp[p, e, cp]], axis=0)
                rhs = jnp.concatenate([w_ref[:, own_e], w_ref[:, oth_e]], axis=1)
                d = mm_bt(lhs.T, rhs)
                acc = d if acc is None else acc + d
        gst[b % 2, 0:w] = acc
        gm(b).start()
        dispatch(b, table("m", nb))
        return carry

    lax.fori_loop(0, nb, memory_rows, 0)
    run("m", nb)

    gain = g1_ref[...].astype(F32)
    y_fetch(0, 0).start()
    spb[...] = jnp.zeros_like(spb)
    gwq_s[...] = jnp.zeros_like(gwq_s)
    wq_h = wq_ref[:, hcol]

    def query(ch, carry):
        slot = ch % 2
        y_fetch(ch, slot).wait()

        @pl.when(ch + 1 < chips)
        def _():
            y_fetch(ch + 1, 1 - slot).start()
        x = ybuf[slot].reshape(QT, dim).astype(F32)
        xhat = x * lax.rsqrt(jnp.mean(x * x, axis=-1, keepdims=True) + 1e-6)
        n1 = (xhat * gain).astype(BF16)
        dqc = jnp.concatenate([dqa[p, ch].reshape(128, QT) for p in range(np_)], axis=0)
        dn = mm_bt(dqc.T, wq_h)
        gwq_s[...] += mm(dqc, n1)
        spb[0:1, :] += jnp.sum(dn * xhat, axis=0, keepdims=True)
        dispatch(ch, table("q", chips))
        return carry

    lax.fori_loop(0, chips, query, 0)
    gvec2 = jnp.zeros((16 - 2 * hc, QT), F32)
    for ch in range(chips):
        gvec2 = gvec2 + jnp.concatenate([stb[ch, 0, hc:8, :], stb[ch, 1, hc:8, :]], axis=0)
    for n in range(dim // QT):
        spb[1:2, n * QT:(n + 1) * QT] = gvec2[n:n + 1]
    cv = remote(spb, pvec, xs.at[2 * np_], xr.at[2 * np_], ring.partner)
    cv.start()
    wq_out = partner_block(gwq_s, gwq.at[hrow], 3 * nf + 1)
    both_start(wq_out)
    for p in range(np_):
        own_r = pl.ds(pl.multiple_of(core * inner + p * 128, 128), 128)
        oth_r = pl.ds(pl.multiple_of((1 - core) * inner + p * 128, 128), 128)
        dqo_ref[own_r, :] = dqa[p, z, :, :, qmine].reshape(128, rows)
        xq(p).wait()
        dqo_ref[oth_r, :] = pdq[p].reshape(128, rows)
    run("q", chips)
    wkv_out = [pltpu.make_async_copy(ara.at[p], gwkv.at[core, p], ls.at[2 + p]) for p in range(np_)]
    wkv_out += [remote(ara.at[p], gwkv.at[core, p], xs.at[2 * np_ + 1 + p], xr.at[2 * np_ + 1 + p], ring.partner) for p in range(np_)]
    for cp in wkv_out:
        cp.start()
    for p in range(np_):
        xp(p).wait_send()
    cv.wait()
    gvec_ref[...] = spb[0:2] + pvec[0:2]
    both_wait(wo_out)
    both_wait(wq_out)
    for cp in wkv_out:
        cp.wait()
    for b in range(nb - 2, nb):
        gm(b).wait()
    for obj in [att_g, st_g] + dq_r + dq_s + ar_r + ar_s:
        obj.drain()


def bwd_call(dims, *args):
    chips, rows, mem, dim, hc, c, ff = dims
    inner = hc * 64
    QT = 2 * rows
    T = 2 * mem
    np_ = hc // 2
    h2 = chips // 2
    seg = dim // chips // 2
    FT = ff // 8
    v = pl.BlockSpec(memory_space=VMEM)
    hbm = pl.BlockSpec(memory_space=pl.ANY)
    s3 = (2, 2, h2)
    rows_sems = [DMA(s3)] * 4 + [DMA((2,))] * 2
    two = [DMA(s3)] * 2
    S = jax.ShapeDtypeStruct
    gshape = (chips, 2, 2, rows // 2, dim)
    cols = chips * QT
    wsq = VMEM((dim, 2 * inner), BF16)
    return pl.pallas_call(
        functools.partial(bwd_kernel, dims),
        out_shape=(S((2, dim), F32), S((2 * inner, rows), BF16), S((mem, dim), F32), S((2, np_, chips, 2, seg, 256), F32), S((2 * inner, dim), F32), S((2 * inner, dim), F32),
                   S((ff, dim), F32), S((dim, ff), F32), S((dim, ff), F32), S(gshape, BF16)),
        in_specs=[pl.BlockSpec(memory_space=pltpu.SMEM)] + [v] * 6 + [hbm] * 15, out_specs=(v,) * 2 + (hbm,) * 8,
        scratch_shapes=[
            VMEM((T, inner), BF16), VMEM((T, inner), BF16), VMEM((inner, T), BF16), VMEM((hc * 128, cols), BF16), VMEM((2 * inner, dim), BF16), wsq, wsq, wsq, VMEM((T, 128), BF16),
            VMEM(gshape, BF16), VMEM((max(hc * 128, 3 * FT), cols), BF16), VMEM((hc * 16, cols), BF16), VMEM((hc * 16, cols), BF16),
            VMEM((chips, 2, 8, QT), F32), VMEM((inner, T), F32), VMEM((inner, T), F32), VMEM((np_, 256, T), BF16), VMEM((np_, 256, mem), BF16),
            VMEM((np_, chips, 2, 64, QT), F32), VMEM((np_, 2, 2, h2, 64, QT), F32), VMEM((np_, chips, 2, 64, QT), BF16),
            VMEM((np_, chips, 2, seg, 256), F32), VMEM((np_, 2, 2, h2, seg, 256), F32), VMEM((np_, chips, 2, seg, 256), F32),
            VMEM((8, dim), F32), VMEM((np_, 2, 64, rows), BF16), VMEM((8, dim), F32),
            VMEM((2, mem, dim), BF16), VMEM((2, 2, 2, rows // 2, dim), BF16), VMEM((2, 2, 2, rows // 2, dim), BF16),
            VMEM((2, 2, dim, FT), BF16), VMEM((2, FT, dim), BF16), VMEM((2, FT, dim), BF16), VMEM((2, max(FT, mem // 4), dim), F32), VMEM((2, dim, FT), F32),
            VMEM((inner, dim), F32), VMEM((inner, dim), F32)]
        + rows_sems * 2 + two * (1 + 4 * np_) + [DMA((3 * np_ + 1,))] * 2 + [DMA((2 + np_,)), DMA((14,)), DMA((14,)), DMA((16,)), DMA((2, 3)), DMA((2, 2)), DMA((10,))],
        compiler_params=pltpu.CompilerParams(vmem_limit_bytes=66_900_000, collective_id=1, has_side_effects=True),
        cost_estimate=pl.CostEstimate(flops=10**10, bytes_accessed=30 << 20, transcendentals=0),
        name="attn_bwd")(*args)


def fwd_kernel(dims, len_ref, y_ref, go_ref, m_ref, g1_ref, g2_ref, wq_hbm, wk_hbm, wv_hbm, wo_hbm, wg_hbm, wu_hbm, wd_hbm,
               own, att_ref, dh_ref, gh_ref, gn_ref, k_out, v_out, kt_out, qz_out, mg_out, yall, gog,
               k_s, v_s, kt_s, qz, mg, wq_ref, wk_ref, wv_ref, ak_ref, yg, wqt, vt_s, s_scr, mx_scr, part, rbuf, patt, satt, gob, attt, wo_s, wg_s, wu_s, wd_s, n2_s, dn_s, *sems):
    chips, rows, mem, dim, hc, c, ff = dims
    QT = 2 * rows
    T = 2 * mem
    MC = min(256, mem)
    hh = hc // 2
    inner = hc * 64
    HR = hh * 64
    ring = Ring(chips)
    z, core, far = ring.z, ring.core, ring.far
    sub = rows // 2
    part_ = functools.partial
    xs, xr, ls = sems[14:]
    rsrc = lambda ref: (lambda half: ref.at[pl.ds(half * sub, sub)])
    y_g = Rows(ring, yg, rsrc(y_ref), sems[:6])
    go_g = Rows(ring, gog, rsrc(gob), sems[6:12])

    def merge(dst, src):
        for hl in range(hh):
            mr = slice(HR + hl, HR + hl + 1)
            lr = slice(HR + 8 + hl, HR + 9 + hl)
            m1, m2 = dst[mr, :], src[mr, :]
            m = jnp.maximum(m1, m2)
            a = jnp.exp2((m1 - m) * c)
            b = jnp.exp2((m2 - m) * c)
            rr = slice(hl * 64, (hl + 1) * 64)
            dst[rr, :] = dst[rr, :] * a + src[rr, :] * b
            dst[mr, :] = m
            dst[lr, :] = dst[lr, :] * a + src[lr, :] * b

    o_r = Reduce(ring, part, rbuf, merge, sems[12:14])
    loads = [pltpu.make_async_copy(src, dst, ls.at[7 + n]) for n, (src, dst) in enumerate((
        (wk_hbm, wk_ref), (wv_hbm, wv_ref), (wq_hbm, wq_ref), (wo_hbm, wo_s), (wg_hbm, wg_s), (wu_hbm, wu_s), (wd_hbm, wd_s)))]
    stores = [pltpu.make_async_copy(src, dst, ls.at[n]) for n, (src, dst) in enumerate(((k_s, k_out), (v_s, v_out), (kt_s, kt_out), (mg, mg_out), (qz, qz_out)))]
    for cp in loads[:3]:
        cp.start()
    ring.enter()
    y_g.start()
    mx_copy = remote(m_ref, mg, xs.at[0], xr.at[0], ring.partner)
    mx_copy.start()
    for cp in loads[3:]:
        cp.start()
    gob[...] = go_ref[...].astype(BF16)
    for half in range(2):
        yg[z, core, half] = y_ref[half * sub:(half + 1) * sub, :]
    hcol = pl.ds(pl.multiple_of(core * inner, 128), inner)
    qz[...] = jnp.zeros_like(qz)
    mask_lanes(ak_ref, len_ref, z * T)
    for cp in loads[:3]:
        cp.wait()
    wqt[...] = wq_ref[:, hcol].T
    wk = wk_ref[:, hcol]
    wv = wv_ref[:, hcol]

    moves = {"y": y_g, "go": go_g, "o": o_r}

    def acts(*point):
        return [go_g.start if e[1] == "start" else part_(moves[e[0]].move, *e[1:]) for e in FWD_PLAN.get(point, [])]

    def run(*point):
        for fn in acts(*point):
            fn()

    def project(src, base, blocks):
        for j in blocks:
            r = pl.ds(pl.multiple_of(base + j * MC, MC), MC)
            blk = src[j * MC:(j + 1) * MC, :]
            kb = mm(blk, wk).astype(BF16)
            vb = mm(blk, wv).astype(BF16)
            k_s[r, :] = kb
            v_s[r, :] = vb
            kt_s[:, r] = kb.T
            vt_s[:, r] = vb.T

    nb = mem // MC
    project(m_ref, core * mem, range(nb))
    run("s", 0)
    mx_copy.wait_recv()
    project(mg, (1 - core) * mem, range(nb // 2))
    run("s", 1)
    project(mg, (1 - core) * mem, range(nb // 2, nb))
    run("s", 2)
    for cp in stores[:4]:
        cp.start()
    gain = g1_ref[...].astype(F32)
    one_row = jnp.where(lax.broadcasted_iota(jnp.int32, (16, QT), 0) == 0, 1.0, 0.0).astype(BF16)

    def lanes(chip):
        return pl.ds(pl.multiple_of(chip * QT, QT), QT)

    def prep(chip):
        n1 = rms_norm(yg[chip].reshape(QT, dim).astype(F32), gain).astype(BF16)
        qt = mm_bt(wqt[...], n1).astype(BF16)
        for h in range(hc):
            lo = h * 128 + (h % 2) * 64
            qz[lo:lo + 64, lanes(chip)] = qt[h * 64:(h + 1) * 64]

    def step(new, slot, old, pslot):
        if new is not None:
            chip, h = new
            rhs = jnp.concatenate([qz[pl.ds(pl.multiple_of(h * 128, 128), 128), lanes(chip)], one_row], axis=0)
            pair = pl.ds(pl.multiple_of((h // 2) * 128, 128), 128)
            mx = None
        if old is not None:
            ochip, half, hl = old
            m = jnp.max(mx_scr[pslot], axis=0, keepdims=True)
            vrow = pl.ds(pl.multiple_of((half * hh + hl) * 64, 64), 64)
            ls_ = None
            acc = None
        for j in range(T // MC):
            r = slice(j * MC, (j + 1) * MC)
            if new is not None:
                s = mm(jnp.concatenate([k_s[r, pair], ak_ref[r, 0:16]], axis=1), rhs)
                s_scr[slot, r, :] = s
                t = jnp.max(s.reshape(MC // 8, 8, QT), axis=0)
                mx = t if mx is None else jnp.maximum(mx, t)
            if old is not None:
                pr = jnp.exp2((s_scr[pslot, r, :] - m) * c)
                t = jnp.sum(pr.reshape(MC // 8, 8, QT), axis=0)
                ls_ = t if ls_ is None else ls_ + t
                dd = mm(vt_s[vrow, r], pr.astype(BF16))
                acc = dd if acc is None else acc + dd
        if new is not None:
            mx_scr[slot] = mx
        if old is not None:
            part[ochip, half, hl * 64:(hl + 1) * 64, :] = acc
            part[ochip, half, HR + hl:HR + hl + 1, :] = m
            part[ochip, half, HR + 8 + hl:HR + 9 + hl, :] = jnp.sum(ls_, axis=0, keepdims=True)

    offs = [o for o, _ in FWD_ORDER]
    halves = [h for _, h in FWD_ORDER]
    n = len(offs)
    fresh = [int(k + 1 < n and offs[k + 1] not in offs[:k + 1]) for k in range(n)]
    run("s", 3)
    y_g.ready(0)
    prep(z)
    step((z, halves[0] * hh), 0, None, None)

    def body(pair, carry):
        for u in range(2):
            i = 2 * pair + u
            i2 = jnp.minimum(i + 1, n - 1)
            chip, half = ring.chip(pick(i, offs)), pick(i, halves)
            chip2, half2 = ring.chip(pick(i2, offs)), pick(i2, halves)
            for k in range(hh):
                slot = (u * hh + k) % 2
                if k == hh - 1:
                    dispatch(pair, {kk // 2: acts("r", kk) + [part_(y_g.ready, offs[kk + 1])] for kk in range(u, n, 2) if fresh[kk]})
                    if any(fresh[u::2]):
                        pl.when(pick(i, fresh) == 1)(part_(prep, chip2))
                    new = (chip2, half2 * hh)
                else:
                    new = (chip, half * hh + k + 1)
                step(new, 1 - slot, (chip, half, k), slot)
                dispatch(pair, {kk // 2: acts("b", kk * hh + k) for kk in range(u, n, 2) if acts("b", kk * hh + k)})
        return carry

    gl = [pltpu.make_async_copy(gob.at[pl.ds(half * sub, sub)], gog.at[z, core, half], ls.at[5 + half]) for half in range(2)]
    for cp in gl:
        cp.start()
    lax.fori_loop(0, n // 2, body, 0)
    yc = pltpu.make_async_copy(yg, yall, ls.at[14])
    yc.start()
    stores[4].start()
    run("t", 0)
    run("t", 1)
    qmine = pl.ds(pl.multiple_of(core * rows, rows), rows)
    qother = pl.ds(pl.multiple_of((1 - core) * rows, rows), rows)
    for h in range(hc):
        half, hl = h // hh, h % hh
        m = part[z, half, HR + hl:HR + hl + 1, :]
        l = part[z, half, HR + 8 + hl:HR + 9 + hl, :]
        own[h * 64:(h + 1) * 64, :] = part[z, half, hl * 64:(hl + 1) * 64, :] / l
        own[inner + h:inner + h + 1, :] = m + jnp.log2(l) / c
    satt[...] = own[:inner, qother].astype(BF16)
    xo = remote(satt, patt, xs.at[1], xr.at[1], ring.partner)
    xo.start()
    attt[pl.ds(pl.multiple_of(core * inner, inner), inner), :] = own[:inner, qmine].astype(BF16)
    for cp in loads[3:]:
        cp.wait()
    run("t", 2)
    xo.wait()
    attt[pl.ds(pl.multiple_of((1 - core) * inner, inner), inner), :] = patt[...]

    att = attt[...].T
    att_ref[...] = att
    gain2 = g2_ref[...].astype(F32)
    run("t", 3)
    hid = (y_ref[...].astype(F32) + mm(att, wo_s[...])).astype(BF16).astype(F32)
    inv = lax.rsqrt(jnp.mean(hid * hid, axis=-1, keepdims=True) + 1e-6)
    hhat = hid * inv
    n2 = (hhat * gain2).astype(BF16)
    fb = ff // 4
    n2_s[...] = n2
    dn_s[...] = jnp.zeros_like(dn_s)

    def mlp(f, carry):
        cols = pl.ds(pl.multiple_of(f * fb, fb), fb)
        wg, wu = wg_s[:, cols], wu_s[:, cols]
        g = mm(n2_s[...], wg)
        u = mm(n2_s[...], wu)
        ga = mm_bt(gob[...], wd_s[cols, :])
        sig = jax.nn.sigmoid(g)
        si = g * sig
        dn_s[...] += mm_bt((ga * u * (sig + si * (1.0 - sig))).astype(BF16), wg) + mm_bt((ga * si).astype(BF16), wu)
        dispatch(f, {n: acts("t", 4 + n) for n in range(4) if acts("t", 4 + n)})
        return carry

    lax.fori_loop(0, 4, mlp, 0)
    dn = dn_s[...]
    gsum = jnp.sum(dn * hhat, axis=0, keepdims=True)
    gn_ref[...] = jnp.zeros_like(gn_ref)
    for k in range(dim // QT):
        gn_ref[k:k + 1, :] = gsum[:, k * QT:(k + 1) * QT]
    t = dn * gain2
    gh = go_ref[...] + inv * (t - hhat * jnp.mean(t * hhat, axis=-1, keepdims=True))
    gh_ref[...] = gh
    dh_ref[...] = gh.astype(BF16)
    run("t", 8)
    for off in range(-far + 1, far + 1):
        go_g.ready(off)
    mx_copy.wait_send()
    for cp in [yc] + gl + stores:
        cp.wait()
    for obj in (y_g, go_g, o_r):
        obj.drain()


def fwd_call(dims, *args):
    chips, rows, mem, dim, hc, c, ff = dims
    hh = hc // 2
    inner = hc * 64
    QT = 2 * rows
    T = 2 * mem
    HR = hh * 64
    h2 = chips // 2
    v = pl.BlockSpec(memory_space=VMEM)
    hbm = pl.BlockSpec(memory_space=pl.ANY)
    S = jax.ShapeDtypeStruct
    s3 = (2, 2, h2)
    gshape = (chips, 2, 2, rows // 2, dim)
    rows_sems = [DMA(s3)] * 4 + [DMA((2,))] * 2
    return pl.pallas_call(
        functools.partial(fwd_kernel, dims),
        out_shape=(S((inner + 8, QT), F32), S((rows, 2 * inner), BF16), S((rows, dim), BF16), S((rows, dim), F32), S((8, QT), F32),
                   S((T, inner), BF16), S((T, inner), BF16), S((inner, T), BF16), S((hc * 128, chips * QT), BF16), S((mem, dim), BF16), S(gshape, BF16), S(gshape, BF16)),
        in_specs=[pl.BlockSpec(memory_space=pltpu.SMEM)] + [v] * 5 + [hbm] * 7, out_specs=(v,) * 5 + (hbm,) * 7,
        scratch_shapes=[
            VMEM((T, inner), BF16), VMEM((T, inner), BF16), VMEM((inner, T), BF16), VMEM((hc * 128, chips * QT), BF16), VMEM((mem, dim), BF16),
            VMEM((dim, 2 * inner), BF16), VMEM((dim, 2 * inner), BF16), VMEM((dim, 2 * inner), BF16), VMEM((T, 128), BF16),
            VMEM(gshape, BF16), VMEM((inner, dim), BF16), VMEM((inner, T), BF16), VMEM((2, T, QT), F32), VMEM((2, 8, QT), F32),
            VMEM((chips, 2, HR + 16, QT), F32), VMEM((2, 2, h2, HR + 16, QT), F32), VMEM((inner, rows), BF16), VMEM((inner, rows), BF16),
            VMEM((rows, dim), BF16), VMEM((2 * inner, rows), BF16), VMEM((2 * inner, dim), BF16), VMEM((dim, ff), BF16), VMEM((dim, ff), BF16), VMEM((ff, dim), BF16), VMEM((rows, dim), BF16), VMEM((rows, dim), F32)]
        + rows_sems * 2 + [DMA(s3)] * 2 + [DMA((2,))] * 2 + [DMA((15,))],
        compiler_params=pltpu.CompilerParams(vmem_limit_bytes=62 * 1024 * 1024, collective_id=0, has_side_effects=True),
        cost_estimate=pl.CostEstimate(flops=10**10, bytes_accessed=30 << 20, transcendentals=0),
        name="attn_fwd")(*args)


def solution(mesh):
    group = mesh.shape['seq']
    row_spec = P(('data', 'seq'), None)
    part_vec = P('data')
    part_mat = P('data', None)
    part_cube = P('data', None, None)

    def device_step(dec_in, memory, mem_len, grad_out, norm_attn, wq, wk, wv, wo, norm_mlp, w_gate, w_up, w_down):
        rows, dim = dec_in.shape
        mem = memory.shape[0]
        heads, hd = wq.shape[1], wq.shape[2]
        inner = heads * hd
        chips = group // 2
        hc = heads // 2
        c = LOG2E * hd ** -0.5
        dims = (chips, rows, mem, dim, hc, c, w_gate.shape[1])
        wq2, wk2, wv2 = (w.reshape(dim, inner) for w in (wq, wk, wv))
        wo2 = wo.reshape(inner, dim)
        gain1 = norm_attn.reshape(1, dim)
        gain2 = norm_mlp.reshape(1, dim)

        own, attended, dh, grad_hidden, gn, k_c, v_c, kt_c, qz, mem_p, y_all, go_all = fwd_call(
            dims, mem_len, dec_in, grad_out, memory, gain1, gain2, wq2, wk2, wv2, wo2, w_gate, w_up, w_down)
        gvec, dq_own, g_mem, g_wkv, g_wq, g_wo, g_down, g_gate, g_up, _ = bwd_call(
            dims, mem_len, dh, own, gn, attended, gain1, gain2,
            k_c, v_c, kt_c, qz, wo2, wq2, wk2, wv2, memory, mem_p, y_all, go_all, w_gate, w_up, w_down)
        x_in = dec_in.astype(F32)
        _, norm_pull = jax.vjp(rms_norm, x_in, norm_attn.astype(F32))
        grad_x_norm, _ = norm_pull(mm_bt(dq_own.T, wq2))
        g_dec = grad_hidden + grad_x_norm
        cube = (dim, heads, hd)
        g_wkv = g_wkv.reshape(hc, dim, 2, 2 * hd).transpose(2, 1, 0, 3).reshape((2,) + cube)
        return (g_dec, g_mem, gvec[0], g_wq.T.reshape(cube), g_wkv[0], g_wkv[1],
                g_wo.reshape(heads, hd, dim), gvec[1], g_gate, g_up, g_down)

    return jax.shard_map(device_step, mesh=mesh,
                         in_specs=(row_spec, row_spec, part_vec, row_spec) + (P(),) * 9,
                         out_specs=(row_spec, row_spec, part_vec, part_cube, part_cube, part_cube, part_cube, part_vec, part_mat, part_mat, part_mat),
                         check_vma=False)
```

```python
import functools
import math

import jax
import jax.numpy as jnp
from jax import lax
from jax.experimental import pallas as pl
from jax.experimental.pallas import tpu as pltpu
from jax.sharding import PartitionSpec as P

F32 = jnp.float32
BF16 = jnp.bfloat16
LOG2E = math.log2(math.e)
VMEM = pltpu.VMEM
MESH = pl.DeviceIdType.MESH


def mm(a, b):
    return jnp.dot(a, b, preferred_element_type=F32)


def mm_bt(a, b):
    return lax.dot_general(a, b, (((1,), (1,)), ((), ())), preferred_element_type=F32)


def mm_at(a, b):
    return lax.dot_general(a, b, (((0,), (0,)), ((), ())), preferred_element_type=F32)


def rms_norm(tensor, gain):
    mean_sq = jnp.mean(tensor * tensor, axis=-1, keepdims=True)
    return tensor * lax.rsqrt(mean_sq + 1e-6) * gain


RIGHT, LEFT = 0, 1
DMA = pltpu.SemaphoreType.DMA

FWD_ORDER = [(0, 0), (0, 1), (1, 0), (1, 1), (-3, 0), (3, 1), (4, 0), (4, 1), (3, 0), (-3, 1), (2, 0), (-2, 1), (2, 1), (-2, 0), (-1, 1), (-1, 0)]
BWD_ORDER = [0, 1, 4, 3, -3, 2, -2, -1]
BWD_FIRST = 2
FWD_PLAN = {
    ("b", 0): [("y", 0, 1, 1), ("y", 1, 0, 1)],
    ("b", 11): [("y", 1, 1, 3), ("y", 1, 0, 3)],
    ("b", 12): [("go", 0, 0, 1)],
    ("b", 13): [("go", 1, 1, 1)],
    ("b", 14): [("o", 1, 0, 3)],
    ("b", 15): [("go", 0, 1, 1)],
    ("b", 17): [("o", 0, 1, 3)],
    ("b", 18): [("go", 1, 0, 1)],
    ("b", 20): [("o", 0, 0, 4)],
    ("b", 21): [("go", 1, 1, 2)],
    ("b", 23): [("o", 1, 1, 4)],
    ("b", 31): [("go", 0, 0, 2)],
    ("b", 32): [("go", 1, 0, 2)],
    ("b", 34): [("go", 0, 1, 2)],
    ("b", 35): [("go", 1, 1, 3)],
    ("b", 36): [("o", 0, 0, 3)],
    ("b", 37): [("o", 1, 1, 3)],
    ("b", 38): [("o", 0, 1, 2)],
    ("b", 4): [("y", 0, 0, 2), ("y", 1, 1, 2)],
    ("b", 40): [("go", 1, 0, 3)],
    ("b", 41): [("o", 1, 0, 2)],
    ("b", 42): [("go", 0, 1, 3)],
    ("b", 43): [("go", 1, 1, 4)],
    ("b", 8): [("y", 0, 1, 2), ("y", 1, 0, 2)],
    ("b", 9): [("go", "start")],
    ("r", 3): [("y", 0, 0, 3), ("y", 0, 1, 3)],
    ("r", 5): [("y", 0, 0, 4), ("y", 1, 1, 4)],
    ("s", 1): [("y", 0, 0, 1), ("y", 1, 1, 1)],
    ("t", 1): [("o", 0, 0, 2), ("o", 1, 1, 2), ("o", 0, 1, 1), ("o", 1, 0, 1), ("o", 0, 0, 1), ("o", 1, 1, 1), ("o", 0, 1, 0), ("o", 1, 0, 0), ("o", 0, 0, 0), ("o", 1, 1, 0)],
    ("t", 2): [("go", 0, 0, 3)],
    ("t", 6): [("go", 0, 0, 4)],
}
BWD_PLAN = {
    ("b", 1): [("dh", 0, 0, 1), ("dh", 1, 1, 1)],
    ("b", 11): [("dh", 0, 1, 3), ("dh", 1, 0, 3), ("st", 0, 0, 3), ("st", 1, 1, 3), ("st", 0, 1, 3), ("st", 1, 0, 3)],
    ("b", 12): [("dq0", 0, 0, 4)],
    ("b", 13): [("dq0", 1, 1, 4)],
    ("b", 14): [("att", 0, 0, 1), ("att", 1, 1, 1)],
    ("b", 15): [("dq0", 0, 1, 3), ("att", 0, 1, 1), ("att", 1, 0, 1)],
    ("b", 16): [("dq0", 0, 0, 3), ("dq0", 1, 0, 3)],
    ("b", 17): [("dq0", 1, 1, 3)],
    ("b", 18): [("att", 0, 0, 2), ("att", 1, 1, 2)],
    ("b", 19): [("dq0", 0, 1, 2), ("att", 1, 0, 2)],
    ("b", 2): [("dh", 0, 1, 1), ("dh", 1, 0, 1), ("st", 0, 0, 1), ("st", 1, 1, 1)],
    ("b", 20): [("dq0", 1, 0, 2), ("att", 0, 1, 2)],
    ("b", 21): [("dq0", 0, 0, 2), ("dq0", 1, 1, 2)],
    ("b", 22): [("att", 0, 0, 3), ("att", 1, 1, 3)],
    ("b", 23): [("dq0", 0, 1, 1), ("ar0", 0, 1, 3), ("ar0", 1, 0, 3), ("ar0", 0, 0, 4), ("ar0", 1, 1, 4), ("att", 1, 0, 3)],
    ("b", 24): [("dq0", 1, 0, 1), ("dq1", 0, 0, 4), ("att", 0, 1, 3)],
    ("b", 25): [("dq0", 0, 0, 1), ("dq0", 1, 1, 1), ("dq1", 1, 1, 4)],
    ("b", 27): [("dq1", 0, 1, 3), ("att", 0, 0, 4), ("att", 1, 1, 4)],
    ("b", 28): [("dq0", 0, 1, 0), ("dq1", 1, 0, 3), ("ar0", 1, 0, 2), ("ar0", 1, 1, 3), ("ar0", 0, 1, 2)],
    ("b", 29): [("dq0", 1, 0, 0), ("ar0", 0, 0, 3)],
    ("b", 3): [("st", 0, 1, 1), ("st", 1, 0, 1)],
    ("b", 30): [("dq0", 1, 1, 0), ("dq1", 0, 0, 3)],
    ("b", 31): [("dq0", 0, 0, 0), ("ds0", "start"), ("dq1", 1, 1, 3)],
    ("b", 32): [("dq1", 0, 1, 2), ("dq1", 1, 0, 2)],
    ("b", 33): [("ar0", 0, 1, 1), ("ar0", 1, 0, 1)],
    ("b", 34): [("ar0", 0, 0, 2), ("ar0", 1, 1, 2), ("ds0", 1, 1, 1)],
    ("b", 35): [("dq1", 0, 0, 2), ("dq1", 1, 1, 2), ("ar1", 0, 1, 3), ("ar1", 1, 0, 3), ("ar1", 0, 0, 4), ("ar1", 1, 1, 4), ("ds0", 1, 0, 1), ("ds0", 0, 0, 1), ("ds0", 0, 1, 1)],
    ("b", 36): [("dq1", 0, 1, 1), ("dq1", 1, 0, 1), ("dq2", 0, 0, 4), ("ar0", 0, 1, 0), ("ar0", 1, 0, 0)],
    ("b", 37): [("dq2", 1, 1, 4), ("ar0", 0, 0, 1), ("ar0", 1, 1, 1)],
    ("b", 38): [("dq1", 0, 0, 1), ("ds0", 1, 1, 2)],
    ("b", 39): [("dq1", 1, 1, 1), ("dq2", 0, 1, 3), ("ar1", 0, 1, 2)],
    ("b", 40): [("dq2", 1, 0, 3), ("ar1", 1, 0, 2), ("ar1", 0, 0, 3), ("ar1", 1, 1, 3), ("ds0", 0, 0, 2)],
    ("b", 41): [("ds0", 0, 1, 2), ("ds0", 1, 0, 2)],
    ("b", 42): [("dq1", 0, 1, 0), ("dq1", 1, 0, 0)],
    ("b", 43): [("dq2", 0, 0, 3), ("dq2", 1, 1, 3)],
    ("b", 44): [("ar0", 0, 0, 0), ("ar0", 1, 1, 0), ("as0", "start"), ("ds0", 1, 1, 3)],
    ("b", 45): [("dq1", 0, 0, 0), ("dq1", 1, 1, 0), ("ds1", "start")],
    ("b", 46): [("dq2", 0, 1, 2), ("dq2", 1, 0, 2), ("ar1", 0, 1, 1)],
    ("b", 47): [("ar1", 1, 0, 1), ("ar1", 0, 0, 2), ("ar1", 1, 1, 2), ("ar2", 0, 1, 3), ("ar2", 1, 0, 3), ("ar2", 0, 0, 4), ("ar2", 1, 1, 4), ("ds0", 0, 0, 3), ("ds0", 0, 1, 3), ("ds0", 1, 0, 3)],
    ("b", 5): [("dh", 0, 0, 2), ("dh", 1, 1, 2)],
    ("b", 7): [("dh", 0, 1, 2), ("dh", 1, 0, 2), ("st", 0, 0, 2), ("st", 1, 1, 2), ("st", 0, 1, 2), ("st", 1, 0, 2)],
    ("b", 9): [("dh", 0, 0, 3), ("dh", 1, 1, 3)],
    ("f", 0): [("ar1", 1, 0, 0), ("ar1", 0, 0, 1), ("ar1", 1, 1, 1), ("ar2", 0, 1, 2)],
    ("f", 11): [("dq2", 0, 1, 0), ("dq2", 1, 0, 0)],
    ("f", 13): [("ar1", 0, 0, 0), ("ar1", 1, 1, 0), ("as1", "start")],
    ("f", 14): [("ar2", 0, 1, 1), ("ar2", 1, 0, 1)],
    ("f", 16): [("ar2", 0, 0, 2), ("ar2", 1, 1, 2)],
    ("f", 17): [("dq2", 0, 0, 0), ("dq2", 1, 1, 0), ("ds2", "start"), ("as0", 0, 0, 3), ("as0", 1, 1, 3)],
    ("f", 18): [("as0", 0, 1, 3), ("as0", 1, 0, 3)],
    ("f", 19): [("ds1", 0, 0, 3), ("ds1", 1, 1, 3)],
    ("f", 2): [("ar2", 1, 0, 2), ("ar2", 0, 0, 3)],
    ("f", 21): [("ds1", 0, 1, 3), ("ds1", 1, 0, 3)],
    ("f", 23): [("as1", 0, 0, 1), ("as1", 1, 1, 1)],
    ("f", 25): [("as1", 0, 1, 1), ("as1", 1, 0, 1)],
    ("f", 26): [("ar2", 0, 1, 0), ("ar2", 1, 0, 0), ("ar2", 0, 0, 1), ("ar2", 1, 1, 1), ("ds2", 0, 0, 1), ("ds2", 1, 1, 1), ("ds2", 0, 1, 1), ("ds2", 1, 0, 1)],
    ("f", 28): [("as0", 0, 0, 4), ("as0", 1, 1, 4)],
    ("f", 3): [("ar2", 1, 1, 3), ("ds0", 0, 0, 4)],
    ("f", 30): [("ds1", 0, 0, 4), ("ds1", 1, 1, 4)],
    ("f", 32): [("as1", 0, 0, 2), ("as1", 1, 1, 2)],
    ("f", 34): [("as1", 0, 1, 2), ("as1", 1, 0, 2)],
    ("f", 35): [("ar2", 0, 0, 0), ("ar2", 1, 1, 0), ("as2", "start"), ("ds2", 0, 0, 2), ("ds2", 1, 1, 2), ("ds2", 0, 1, 2), ("ds2", 1, 0, 2)],
    ("f", 6): [("dq2", 0, 0, 1), ("dq2", 1, 1, 1)],
    ("f", 8): [("as0", 0, 0, 2), ("as0", 1, 1, 2), ("as0", 0, 1, 2), ("as0", 1, 0, 2), ("ds1", 0, 0, 2), ("ds1", 1, 1, 2), ("ds1", 0, 1, 2), ("ds1", 1, 0, 2)],
    ("h", 0): [("dq2", 0, 0, 2), ("dq2", 1, 1, 2)],
    ("h", 1): [("as0", 0, 0, 1), ("as0", 1, 1, 1)],
    ("h", 3): [("as0", 0, 1, 1), ("as0", 1, 0, 1), ("ds0", 1, 1, 4), ("ds1", 0, 0, 1)],
    ("h", 4): [("ds1", 0, 1, 1), ("ds1", 1, 1, 1)],
    ("h", 5): [("ds1", 1, 0, 1)],
    ("h", 6): [("dq2", 0, 1, 1)],
    ("h", 7): [("dq2", 1, 0, 1), ("ar1", 0, 1, 0)],
    ("m", 0): [("as1", 0, 0, 3), ("as1", 1, 1, 3), ("as1", 0, 1, 3), ("as1", 1, 0, 3)],
    ("m", 2): [("as2", 0, 0, 1), ("as2", 1, 1, 1)],
    ("m", 3): [("as2", 0, 1, 1), ("as2", 1, 0, 1)],
    ("m", 4): [("ds2", 0, 0, 3), ("ds2", 1, 1, 3), ("ds2", 0, 1, 3), ("ds2", 1, 0, 3), ("ds2", 0, 0, 4), ("ds2", 1, 1, 4)],
    ("q", 0): [("as1", 0, 0, 4), ("as1", 1, 1, 4), ("as2", 0, 0, 2), ("as2", 1, 1, 2), ("as2", 0, 1, 2), ("as2", 1, 0, 2)],
    ("q", 6): [("as2", 0, 0, 3), ("as2", 1, 1, 3)],
    ("q", 8): [("as2", 0, 1, 3), ("as2", 1, 0, 3), ("as2", 0, 0, 4), ("as2", 1, 1, 4)],
    ("r", 12): [("dh", 0, 0, 4), ("dh", 1, 1, 4), ("att", "start"), ("st", 0, 0, 4), ("st", 1, 1, 4)],
}


class Ring:
    def __init__(self, chips):
        me = lax.axis_index('seq')
        self.chips = chips
        self.far = chips // 2
        self.z = me // 2
        self.core = me - 2 * self.z
        self.partner = 2 * self.z + 1 - self.core
        self.next = (2 * self.chip(1) + self.core, 2 * self.chip(-1) + self.core)
        self.hops = {(RIGHT, 0): self.far, (LEFT, 1): self.far, (RIGHT, 1): self.far - 1, (LEFT, 0): self.far - 1}

    def chip(self, off):
        return lax.rem(self.z + off + self.chips, self.chips)

    def ahead(self, d, k):
        return self.chip(k if d == RIGHT else -k)

    def enter(self):
        barrier = pltpu.get_barrier_semaphore()
        for dev in (self.partner,) + self.next:
            pl.semaphore_signal(barrier, inc=1, device_id={'seq': dev}, device_id_type=MESH)
        pl.semaphore_wait(barrier, 3)


def remote(src, dst, ssem, rsem, dev):
    return pltpu.make_async_remote_copy(src_ref=src, dst_ref=dst, send_sem=ssem, recv_sem=rsem, device_id={'seq': dev}, device_id_type=MESH)


def sent(every, ssem, rsem, dev):
    remote(every, every, ssem, rsem, dev).wait_send()


class Share:
    def __init__(self, ring, buf, src, sems):
        self.ring, self.buf, self.src = ring, buf, src
        self.ss, self.rs = sems

    def slot(self, chip, half):
        return self.buf.at[chip, half]

    def send(self, d, half, t):
        slot = self.slot(self.ring.ahead(d, 1 - t), half)
        src = self.src(half) if t == 1 else slot
        return remote(src, slot, self.ss.at[0], self.rs.at[d, half, t - 1], self.ring.next[d])

    def recv(self, d, half, t):
        slot = self.slot(self.ring.ahead(d, -t), half)
        return remote(slot, slot, self.ss.at[0], self.rs.at[d, half, t - 1], self.ring.next[d])

    def start(self):
        for d, half in self.ring.hops:
            self.send(d, half, 1).start()

    def came(self, d, half, t):
        pass

    def move(self, d, half, t):
        self.recv(d, half, t).wait_recv()
        if t < self.ring.hops[d, half]:
            self.send(d, half, t + 1).start()
        self.came(d, half, t)

    def drain(self):
        sent(self.buf.at[pl.ds(0, self.ring.chips - 1)], self.ss.at[0], self.rs.at[0, 0, 0], self.ring.next[0])


class Rows(Share):
    def __init__(self, ring, buf, src, sems):
        super().__init__(ring, buf, src, sems[:2])
        self.fs, self.fr, self.os, self.orr = sems[2:]

    def slot(self, chip, half):
        return self.buf.at[chip, self.ring.core, half]

    def pslot(self, chip, half):
        return self.buf.at[chip, 1 - self.ring.core, half]

    def start(self):
        super().start()
        for half in range(2):
            self.own(half).start()

    def own(self, half):
        return remote(self.src(half), self.slot(self.ring.z, half), self.os.at[0], self.orr.at[half], self.ring.partner)

    def forward(self, d, half, t):
        slot = self.slot(self.ring.ahead(d, -t), half)
        return remote(slot, slot, self.fs.at[0], self.fr.at[d, half, t - 1], self.ring.partner)

    def came(self, d, half, t):
        self.forward(d, half, t).start()

    def ready(self, off):
        ring = self.ring
        if off == 0:
            for half in range(2):
                slot = self.pslot(ring.z, half)
                remote(slot, slot, self.os.at[0], self.orr.at[half], ring.partner).wait_recv()
            return
        for (d, half), n in ring.hops.items():
            t = ring.far if abs(off) == ring.far else (-off if d == RIGHT else off)
            if 1 <= t <= n:
                slot = self.pslot(ring.ahead(d, -t), half)
                remote(slot, slot, self.fs.at[0], self.fr.at[d, half, t - 1], ring.partner).wait_recv()

    def drain(self):
        every = self.buf.at[pl.ds(0, self.ring.chips - 1), 0]
        sent(every, self.ss.at[0], self.rs.at[0, 0, 0], self.ring.next[0])
        sent(every, self.fs.at[0], self.fr.at[0, 0, 0], self.ring.partner)
        sent(self.buf.at[0, 0], self.os.at[0], self.orr.at[0], self.ring.partner)


class Reduce:
    def __init__(self, ring, part, rbuf, merge, sems):
        self.ring, self.part, self.rbuf, self.merge = ring, part, rbuf, merge
        self.ss, self.rs = sems

    def send(self, d, half, o):
        return remote(self.part.at[self.ring.ahead(d, o), half], self.rbuf.at[d, half, o - 1], self.ss.at[0], self.rs.at[d, half, o - 1], self.ring.next[d])

    def recv(self, d, half, o):
        slot = self.rbuf.at[d, half, o]
        return remote(slot, slot, self.ss.at[0], self.rs.at[d, half, o], self.ring.next[d])

    def move(self, d, half, o):
        if o < self.ring.hops[d, half]:
            self.recv(d, half, o).wait_recv()
            self.merge(self.part.at[self.ring.ahead(d, o), half], self.rbuf.at[d, half, o])
        if o > 0:
            self.send(d, half, o).start()

    def drain(self):
        sent(self.part.at[pl.ds(0, self.ring.chips - 1)], self.ss.at[0], self.rs.at[0, 0, 0], self.ring.next[0])


def pick(i, values):
    out = jnp.int32(values[-1])
    for k, v in enumerate(values[:-1]):
        out = jnp.where(i == k, jnp.int32(v), out)
    return out


def mask_lanes(ref, len_ref, start):
    row = lax.broadcasted_iota(jnp.int32, ref.shape, 0) + start
    lane = lax.broadcasted_iota(jnp.int32, ref.shape, 1)
    bias = jnp.where(row < len_ref[0], 0.0, -1e30)
    ref[...] = jnp.where(lane == 0, bias, jnp.where(lane < 4, 1.0, 0.0)).astype(BF16)


def dispatch(index, table):
    def branch(keys):
        if len(keys) == 1:
            def run():
                for fn in table[keys[0]]:
                    fn()
            pl.when(index == keys[0])(run)
            return
        low, high = keys[:len(keys) // 2], keys[len(keys) // 2:]
        pl.when(index < high[0])(functools.partial(branch, low))
        pl.when(index >= high[0])(functools.partial(branch, high))
    if table:
        branch(sorted(table))


def add_into(dst, src):
    dst[...] = dst[...] + src[...]


def parts3(x):
    hi = x.astype(BF16)
    rest = x - hi.astype(F32)
    mid = rest.astype(BF16)
    lo = (rest - mid.astype(F32)).astype(BF16)
    return hi, mid, lo


def bwd_kernel(dims, len_ref, dh_ref, own_ref, gn_ref, att_ref, g_ref,
               k_hbm, v_hbm, kt_hbm, qz_hbm, wo_hbm, wq_hbm, wk_hbm, wv_hbm, ma_hbm, mb_hbm, y_hbm, gog, wg_hbm, wu_hbm, wd_hbm,
               gvec_ref, dqo_ref, gmem, gwk, gwv, gwq, gwo, gdown, ggate, gup, attg,
               k_ref, v_ref, kt_ref, qz_ref, wo_ref, wq_ref, wk_ref, wv_ref, ak_ref,
               dhg, doz, aqs, ads, stb, dk, dv, dkv, dkvp, dqp, dqr, dqa, arp, arr, ara, pvec, pdq, spb,
               msc, ybuf, abuf, wbuf, dbuf, wt, gst, gsw, gwo_s, gwq_s,
               *sems):
    chips, rows, mem, dim, hc, c, ff = dims
    QT = 2 * rows
    T = 2 * mem
    MC = min(256, mem)
    nm = T // MC
    inner = hc * 64
    np_ = hc // 2
    seg = 256 // chips // 2
    fh = ff // 2
    FT = wt.shape[1]
    nf = fh // FT
    ring = Ring(chips)
    z, core, far = ring.z, ring.core, ring.far
    sems = list(sems)

    def take(n):
        out = sems[:n]
        del sems[:n]
        return out

    half_rows = rows // 2
    part_ = functools.partial
    rsrc = lambda ref: (lambda half: ref.at[pl.ds(half * half_rows, half_rows)])
    dh_g = Rows(ring, dhg, rsrc(dh_ref), take(6))
    att_g = Rows(ring, attg, rsrc(att_ref), take(6))
    st_g = Share(ring, stb, lambda half: stb.at[z, half], take(2))
    dq_r = [Reduce(ring, dqp.at[p], dqr.at[p], add_into, take(2)) for p in range(np_)]
    dq_s = [Share(ring, dqa.at[p], lambda half, p=p: dqa.at[p, z, half], take(2)) for p in range(np_)]
    ar_r = [Reduce(ring, arp.at[p], arr.at[p], add_into, take(2)) for p in range(np_)]
    ar_s = [Share(ring, ara.at[p], lambda half, p=p: ara.at[p, z, half], take(2)) for p in range(np_)]
    xs, xr, ls, gs, gr, gl, wsem, ysem, lsem = take(9)
    loads = [pltpu.make_async_copy(src, dst, lsem.at[n]) for n, (src, dst) in enumerate((
        (wo_hbm, wo_ref), (k_hbm, k_ref), (v_hbm, v_ref), (kt_hbm, kt_ref), (qz_hbm, qz_ref),
        (ma_hbm, msc.at[0, pl.ds(0, mem)]), (mb_hbm, msc.at[1, pl.ds(0, mem)]), (wq_hbm, wq_ref), (wk_hbm, wk_ref), (wv_hbm, wv_ref)))]
    for cp in loads:
        cp.start()
    ring.enter()
    dh_g.start()
    locals_ = [pltpu.make_async_copy(att_ref.at[pl.ds(half * half_rows, half_rows)], attg.at[z, core, half], ls.at[half]) for half in range(2)]
    for cp in locals_:
        cp.start()
    for half in range(2):
        dhg[z, core, half] = dh_ref[half * half_rows:(half + 1) * half_rows, :]
    doz[...] = jnp.zeros_like(doz)
    mask_lanes(ak_ref, len_ref, z * T)
    hrow = pl.ds(pl.multiple_of(core * inner, inner), inner)
    hcol = pl.ds(pl.multiple_of(core * inner, 128), inner)
    other_cols = pl.ds(pl.multiple_of((1 - core) * mem, mem), mem)
    my_cols = pl.ds(pl.multiple_of(core * mem, mem), mem)
    qmine = pl.ds(pl.multiple_of(core * rows, rows), rows)
    qother = pl.ds(pl.multiple_of((1 - core) * rows, rows), rows)

    def lanes(chip):
        return pl.ds(pl.multiple_of(chip * QT, QT), QT)

    def d_out(chip):
        return mm_bt(wo_ref[hrow, :], dhg[chip].reshape(QT, dim))

    def prepare(chip, dot=None):
        dot = d_out(chip) if dot is None else dot
        dob = dot.astype(BF16)
        q = lanes(chip)
        row = lax.broadcasted_iota(jnp.int32, (16, QT), 0)
        for h in range(hc):
            lo = h * 128 + (h % 2) * 64
            doz[lo:lo + 64, q] = dob[h * 64:(h + 1) * 64]
            for ref, half, first in ((aqs, 0, 1.0), (ads, 1, 0.0)):
                a, b, e = (x.astype(F32) for x in parts3(stb[chip, half, h:h + 1, :]))
                ref[h * 16:(h + 1) * 16, q] = jnp.where(row == 0, first, jnp.where(row == 1, a, jnp.where(row == 2, b, jnp.where(row == 3, e, 0.0)))).astype(BF16)

    dh_g.ready(0)
    loads[0].wait()
    dot0 = d_out(z)
    prod = dot0 * own_ref[:inner, :]
    for h in range(hc):
        stb[z, 0, h:h + 1, :] = -own_ref[inner + h:inner + h + 1, :]
        stb[z, 1, h:h + 1, :] = -jnp.sum(prod[h * 64:(h + 1) * 64], axis=0, keepdims=True)
    stb[z, 0, hc:8, :] = gn_ref[0:8 - hc, :]
    stb[z, 1, hc:8, :] = gn_ref[8 - hc:16 - 2 * hc, :]
    st_g.start()
    prepare(z, dot0)
    dk[...] = jnp.zeros_like(dk)
    dv[...] = jnp.zeros_like(dv)
    for cp in loads[1:]:
        cp.wait()

    def tile(h, chip):
        pair = h // 2
        q = lanes(chip)
        hz = pl.ds(pl.multiple_of(h * 128, 128), 128)
        h16 = pl.ds(pl.multiple_of(h * 16, 16), 16)
        ps = pl.ds(pl.multiple_of(pair * 128, 128), 128)
        hz64 = pl.ds(pl.multiple_of(h * 128 + (h - 2 * pair) * 64, 64), 64)
        h64 = pl.ds(pl.multiple_of(h * 64, 64), 64)
        hr = h64
        q_t = qz_ref[hz64, q]
        do_t = doz[hz64, q]
        r1 = jnp.concatenate([qz_ref[hz, q], aqs[h16, q]], axis=0)
        r2 = jnp.concatenate([doz[hz, q], ads[h16, q]], axis=0)
        stage = {}
        dq = None
        for j in range(nm + 2):
            if j < nm:
                r = slice(j * MC, (j + 1) * MC)
                ak = ak_ref[r, 0:16]
                stage["a", j] = (mm(jnp.concatenate([k_ref[r, ps], ak], axis=1), r1), mm(jnp.concatenate([v_ref[r, ps], ak], axis=1), r2))
            if 1 <= j <= nm:
                s, dp = stage.pop(("a", j - 1))
                a = jnp.exp2(s * c)
                stage["b", j - 1] = (a.astype(BF16), (a * dp).astype(BF16))
            if j >= 2:
                r = slice((j - 2) * MC, (j - 1) * MC)
                pb, ds = stage.pop(("b", j - 2))
                dv[hr, r] += mm_bt(do_t, pb)
                dk[hr, r] += mm_bt(q_t, ds)
                d = mm(kt_ref[h64, r], ds)
                dq = d if dq is None else dq + d
        dqp[pair, chip, h - 2 * pair] = dq

    scale = 0.125

    def xp(p):
        return remote(dkv.at[p, :, other_cols], dkvp.at[p], xs.at[p], xr.at[p], ring.partner)

    def xq(p):
        return remote(dqa.at[p, z, :, :, qother], pdq.at[p], xs.at[np_ + p], xr.at[np_ + p], ring.partner)

    def share_dq(p):
        for half in range(2):
            dqa[p, z, half] = (dqp[p, z, half] * scale).astype(BF16)
        dq_s[p].start()
        xq(p).start()

    def share_ar(p):
        for half in range(2):
            ara[p, z, half] = arp[p, z, half]
        ar_s[p].start()

    moves = {"dh": dh_g, "st": st_g, "att": att_g}
    begins = {"att": att_g.start}
    for p in range(np_):
        moves.update({f"dq{p}": dq_r[p], f"ds{p}": dq_s[p], f"ar{p}": ar_r[p], f"as{p}": ar_s[p]})
        begins.update({f"ds{p}": part_(share_dq, p), f"as{p}": part_(share_ar, p)})

    def acts(*point):
        return [begins[e[0]] if e[1] == "start" else part_(moves[e[0]].move, *e[1:]) for e in BWD_PLAN.get(point, [])]

    def run(*point):
        for fn in acts(*point):
            fn()

    def table(kind, n):
        return {k: acts(kind, k) for k in range(n) if acts(kind, k)}

    offs = BWD_ORDER
    first = BWD_FIRST * hc
    per = 2 * (chips - BWD_FIRST)
    needs = {k * hc: offs[k] for k in range(1, BWD_FIRST)}
    needs.update({first + 2 * (k - BWD_FIRST): offs[k] for k in range(BWD_FIRST, chips)})

    def project(p):
        r = pl.ds(pl.multiple_of(p * 128, 128), 128)
        dkv[p, 0:128, :] = (dk[r, :] * scale).astype(BF16)
        dkv[p, 128:256, :] = dv[r, :].astype(BF16)
        xp(p).start()
        g = mm(dkv[p, :, my_cols], msc[0, 0:mem]) + mm(dkv[p, :, other_cols], msc[1, 0:mem])
        for n in range(2 * chips):
            arp[p, n // 2, n % 2] = g[n * seg:(n + 1) * seg]

    def body(it, carry):
        early = it < first
        b = it - first
        p = b // per
        r = b - p * per
        h = jnp.where(early, it % hc, 2 * p + r % 2)
        chip = ring.chip(pick(jnp.where(early, it // hc, BWD_FIRST + r // 2), offs))
        dispatch(it, {k: acts("r", k) + [part_(dh_g.ready, off)] for k, off in needs.items()})
        fresh = (early & (it > 0) & (it % hc == 0)) | ((b >= 0) & (b < per) & (r % 2 == 0))
        pl.when(fresh)(part_(prepare, chip))
        tile(h, chip)
        pl.when((b >= 0) & (r == per - 1))(part_(project, p))
        dispatch(it, table("b", chips * hc))
        return carry

    lax.fori_loop(0, chips * hc, body, 0)
    run("p", np_)
    near = range(1 - far, far + 1)

    for cp in locals_:
        cp.wait()
    for off in near:
        att_g.ready(off)
    gain2 = g_ref[1:2, :].astype(F32)
    gwo_s[...] = jnp.zeros_like(gwo_s)

    def y_fetch(ch, slot):
        return pltpu.make_async_copy(y_hbm.at[ch], ybuf.at[slot], ysem.at[slot, 0])

    def fetch(ch, slot):
        return (y_fetch(ch, slot), pltpu.make_async_copy(attg.at[ch], abuf.at[slot], ysem.at[slot, 1]))

    for cp in fetch(0, 0):
        cp.start()

    def hidden(ch, carry):
        slot = ch % 2
        for cp in fetch(ch, slot):
            cp.wait()

        @pl.when(ch + 1 < chips)
        def _():
            for cp in fetch(ch + 1, 1 - slot):
                cp.start()
        att = abuf[slot].reshape(QT, dim)
        h = (ybuf[slot].reshape(QT, dim).astype(F32) + mm(att, wo_ref[...])).astype(BF16)
        qz_ref[0:dim, lanes(ch)] = rms_norm(h.astype(F32), gain2).astype(BF16).T
        ah = jnp.where(core == 0, att[:, :inner], att[:, inner:])
        gwo_s[...] += mm_at(ah, dhg[ch].reshape(QT, dim))
        dispatch(ch, table("h", chips))
        return carry

    lax.fori_loop(0, chips, hidden, 0)
    dh_g.drain()
    go_load = pltpu.make_async_copy(gog, dhg, ls.at[0])
    go_load.start()

    def partner_block(buf, dst, k):
        return pltpu.make_async_copy(buf, dst, gl.at[k]), remote(buf, dst, gs.at[k], gr.at[k], ring.partner)

    def both_start(pair):
        pair[0].start()
        pair[1].start()

    def both_wait(pair):
        pair[0].wait()
        pair[1].wait()

    wo_out = partner_block(gwo_s, gwo.at[hrow], 3 * nf)
    both_start(wo_out)

    def w_fetch(f, slot):
        cols = pl.ds(pl.multiple_of(core * fh + f * FT, FT), FT)
        return (pltpu.make_async_copy(wg_hbm.at[:, cols], wbuf.at[slot, 0], wsem.at[slot, 0]),
                pltpu.make_async_copy(wu_hbm.at[:, cols], wbuf.at[slot, 1], wsem.at[slot, 1]),
                pltpu.make_async_copy(wd_hbm.at[cols], dbuf.at[slot], wsem.at[slot, 2]))

    for cp in w_fetch(0, 0):
        cp.start()
    go_load.wait()
    f_table = table("f", 9 * nf)

    def block(f, n):
        if n == 0:
            return partner_block(gst.at[0, pl.ds(0, FT)], gdown.at[pl.ds(pl.multiple_of(core * fh + f * FT, FT), FT)], f)
        return partner_block(gsw.at[n - 1], (ggate, gup)[n - 1].at[:, pl.ds(pl.multiple_of(core * fh + f * FT, FT), FT)], n * nf + f)

    def mlp(f, carry):
        slot = f % 2
        for cp in w_fetch(f, slot):
            cp.wait()

        @pl.when(f + 1 < nf)
        def _():
            for cp in w_fetch(f + 1, 1 - slot):
                cp.start()
        for n in range(2):
            wt[n] = wbuf[slot, n].T

        def act_chunk(ch, cc):
            q = lanes(ch)
            n2t = qz_ref[0:dim, q]
            g = mm(wt[0], n2t)
            u = mm(wt[1], n2t)
            ga = mm_bt(dbuf[slot], dhg[ch].reshape(QT, dim))
            sig = jax.nn.sigmoid(g)
            si = g * sig
            doz[0:FT, q] = (si * u).astype(BF16)
            doz[FT:2 * FT, q] = (ga * u * (sig + si * (1.0 - sig))).astype(BF16)
            doz[2 * FT:3 * FT, q] = (ga * si).astype(BF16)
            dispatch(f * 9 + ch, f_table)
            return cc

        lax.fori_loop(0, chips, act_chunk, 0)

        @pl.when(f > 0)
        def _():
            for n in range(3):
                both_wait(block(f - 1, n))
        acc = [None] * 3
        for ch in range(chips):
            q = slice(ch * QT, (ch + 1) * QT)
            n2t = qz_ref[0:dim, q]
            for n, d in enumerate((mm(doz[0:FT, q], dhg[ch].reshape(QT, dim)), mm_bt(n2t, doz[FT:2 * FT, q]), mm_bt(n2t, doz[2 * FT:3 * FT, q]))):
                acc[n] = d if acc[n] is None else acc[n] + d
        gst[0, 0:FT] = acc[0]
        gsw[0] = acc[1]
        gsw[1] = acc[2]
        for n in range(3):
            both_start(block(f, n))
        dispatch(f * 9 + 8, f_table)
        return carry

    lax.fori_loop(0, nf, mlp, 0)
    for p in range(np_):
        remote(dkvp.at[p], dkvp.at[p], xs.at[p], xr.at[p], ring.partner).wait_recv()
    nb = 4
    w = mem // nb
    for n in range(3):
        both_wait(block(nf - 1, n))

    def gm(b):
        return pltpu.make_async_copy(gst.at[b % 2, pl.ds(0, w)], gmem.at[pl.ds(pl.multiple_of(b * w, w), w)], gl.at[3 * nf + 2 + b % 2])

    def memory_rows(b, carry):
        @pl.when(b > 1)
        def _():
            gm(b - 2).wait()
        cb = pl.ds(pl.multiple_of(core * mem + b * w, w), w)
        cp = pl.ds(pl.multiple_of(b * w, w), w)
        acc = None
        for p in range(np_):
            own_e = pl.ds(pl.multiple_of(core * inner + p * 128, 128), 128)
            oth_e = pl.ds(pl.multiple_of((1 - core) * inner + p * 128, 128), 128)
            for part, w_ref in ((0, wk_ref), (1, wv_ref)):
                e = slice(part * 128, (part + 1) * 128)
                lhs = jnp.concatenate([dkv[p, e, cb], dkvp[p, e, cp]], axis=0)
                rhs = jnp.concatenate([w_ref[:, own_e], w_ref[:, oth_e]], axis=1)
                d = mm_bt(lhs.T, rhs)
                acc = d if acc is None else acc + d
        gst[b % 2, 0:w] = acc
        gm(b).start()
        dispatch(b, table("m", nb))
        return carry

    lax.fori_loop(0, nb, memory_rows, 0)
    run("m", nb)

    gain = g_ref[0:1, :].astype(F32)
    y_fetch(0, 0).start()
    spb[...] = jnp.zeros_like(spb)
    gwq_s[...] = jnp.zeros_like(gwq_s)
    wq_h = wq_ref[:, hcol]

    def query(ch, carry):
        slot = ch % 2
        y_fetch(ch, slot).wait()

        @pl.when(ch + 1 < chips)
        def _():
            y_fetch(ch + 1, 1 - slot).start()
        x = ybuf[slot].reshape(QT, dim).astype(F32)
        xhat = x * lax.rsqrt(jnp.mean(x * x, axis=-1, keepdims=True) + 1e-6)
        n1 = (xhat * gain).astype(BF16)
        dqc = jnp.concatenate([dqa[p, ch].reshape(128, QT) for p in range(np_)], axis=0)
        dn = mm_bt(dqc.T, wq_h)
        gwq_s[...] += mm(dqc, n1)
        spb[0:1, :] += jnp.sum(dn * xhat, axis=0, keepdims=True)
        dispatch(ch, table("q", chips))
        return carry

    lax.fori_loop(0, chips, query, 0)
    gvec2 = jnp.zeros((16 - 2 * hc, QT), F32)
    for ch in range(chips):
        gvec2 = gvec2 + jnp.concatenate([stb[ch, 0, hc:8, :], stb[ch, 1, hc:8, :]], axis=0)
    for n in range(dim // QT):
        spb[1:2, n * QT:(n + 1) * QT] = gvec2[n:n + 1]
    cv = remote(spb, pvec, xs.at[2 * np_], xr.at[2 * np_], ring.partner)
    cv.start()
    wq_out = partner_block(gwq_s, gwq.at[hrow], 3 * nf + 1)
    both_start(wq_out)
    for p in range(np_):
        own_r = pl.ds(pl.multiple_of(core * inner + p * 128, 128), 128)
        oth_r = pl.ds(pl.multiple_of((1 - core) * inner + p * 128, 128), 128)
        dqo_ref[own_r, :] = dqa[p, z, :, :, qmine].reshape(128, rows)
        xq(p).wait()
        dqo_ref[oth_r, :] = pdq[p].reshape(128, rows)
    run("q", chips)
    wkv_out = []
    for p in range(np_):
        for k, out in enumerate((gwk, gwv)):
            n = 2 * p + k
            src = ara.at[p, pl.ds(k * (chips // 2), chips // 2)]
            wkv_out.append(pltpu.make_async_copy(src, out.at[core, p], ls.at[2 + n]))
            wkv_out.append(remote(src, out.at[core, p], xs.at[2 * np_ + 1 + n], xr.at[2 * np_ + 1 + n], ring.partner))
    for cp in wkv_out:
        cp.start()
    for p in range(np_):
        xp(p).wait_send()
    cv.wait()
    gvec_ref[...] = spb[0:2] + pvec[0:2]
    both_wait(wo_out)
    both_wait(wq_out)
    for cp in wkv_out:
        cp.wait()
    for b in range(nb - 2, nb):
        gm(b).wait()
    for obj in [att_g, st_g] + dq_r + dq_s + ar_r + ar_s:
        obj.drain()


def bwd_call(dims, *args):
    chips, rows, mem, dim, hc, c, ff = dims
    inner = hc * 64
    QT = 2 * rows
    T = 2 * mem
    np_ = hc // 2
    h2 = chips // 2
    seg = 256 // chips // 2
    FT = ff // 8
    v = pl.BlockSpec(memory_space=VMEM)
    hbm = pl.BlockSpec(memory_space=pl.ANY)
    s3 = (2, 2, h2)
    rows_sems = [DMA((1,)), DMA(s3)] * 2 + [DMA((1,)), DMA((2,))]
    two = [DMA((1,)), DMA(s3)]
    S = jax.ShapeDtypeStruct
    gshape = (chips, 2, 2, rows // 2, dim)
    cols = chips * QT
    wsq = VMEM((dim, 2 * inner), BF16)
    return pl.pallas_call(
        functools.partial(bwd_kernel, dims),
        out_shape=(S((2, dim), F32), S((2 * inner, rows), BF16), S((mem, dim), F32), S((2, np_, chips // 2, 2, seg, dim), F32), S((2, np_, chips // 2, 2, seg, dim), F32), S((2 * inner, dim), F32), S((2 * inner, dim), F32),
                   S((ff, dim), F32), S((dim, ff), F32), S((dim, ff), F32), S(gshape, BF16)),
        in_specs=[pl.BlockSpec(memory_space=pltpu.SMEM)] + [v] * 5 + [hbm] * 15, out_specs=(v,) * 2 + (hbm,) * 9,
        scratch_shapes=[
            VMEM((T, inner), BF16), VMEM((T, inner), BF16), VMEM((inner, T), BF16), VMEM((hc * 128, cols), BF16), VMEM((2 * inner, dim), BF16), wsq, wsq, wsq, VMEM((T, 128), BF16),
            VMEM(gshape, BF16), VMEM((max(hc * 128, 3 * FT), cols), BF16), VMEM((hc * 16, cols), BF16), VMEM((hc * 16, cols), BF16),
            VMEM((chips, 2, 8, QT), F32), VMEM((inner, T), F32), VMEM((inner, T), F32), VMEM((np_, 256, T), BF16), VMEM((np_, 256, mem), BF16),
            VMEM((np_, chips, 2, 64, QT), F32), VMEM((np_, 2, 2, h2, 64, QT), F32), VMEM((np_, chips, 2, 64, QT), BF16),
            VMEM((np_, chips, 2, seg, dim), F32), VMEM((np_, 2, 2, h2, seg, dim), F32), VMEM((np_, chips, 2, seg, dim), F32),
            VMEM((8, dim), F32), VMEM((np_, 2, 64, rows), BF16), VMEM((8, dim), F32),
            VMEM((2, mem, dim), BF16), VMEM((2, 2, 2, rows // 2, dim), BF16), VMEM((2, 2, 2, rows // 2, dim), BF16),
            VMEM((2, 2, dim, FT), BF16), VMEM((2, FT, dim), BF16), VMEM((2, FT, dim), BF16), VMEM((2, max(FT, mem // 4), dim), F32), VMEM((2, dim, FT), F32),
            VMEM((inner, dim), F32), VMEM((inner, dim), F32)]
        + rows_sems * 2 + two * (1 + 4 * np_) + [DMA((4 * np_ + 1,))] * 2 + [DMA((2 + 2 * np_,)), DMA((14,)), DMA((14,)), DMA((16,)), DMA((2, 3)), DMA((2, 2)), DMA((10,))],
        compiler_params=pltpu.CompilerParams(vmem_limit_bytes=66_900_000, collective_id=1, has_side_effects=True),
        cost_estimate=pl.CostEstimate(flops=10**10, bytes_accessed=30 << 20, transcendentals=0),
        name="attn_bwd")(*args)


def fwd_kernel(dims, len_ref, y_ref, go_ref, m_ref, g_ref, wq_hbm, wk_hbm, wv_hbm, wo_hbm, wg_hbm, wu_hbm, wd_hbm,
               own, att_ref, dh_ref, gh_ref, gn_ref, k_out, v_out, kt_out, qz_out, mg_out, yall, gog,
               k_s, v_s, kt_s, qz, mg, wq_ref, wk_ref, wv_ref, ak_ref, yg, wqt, vt_s, s_scr, mx_scr, part, rbuf, patt, satt, gob, attt, wo_s, wg_s, wu_s, wd_s, n2_s, dn_s, *sems):
    chips, rows, mem, dim, hc, c, ff = dims
    QT = 2 * rows
    T = 2 * mem
    MC = min(256, mem)
    hh = hc // 2
    inner = hc * 64
    HR = hh * 64
    ring = Ring(chips)
    z, core, far = ring.z, ring.core, ring.far
    sub = rows // 2
    part_ = functools.partial
    xs, xr, ls = sems[14:]
    rsrc = lambda ref: (lambda half: ref.at[pl.ds(half * sub, sub)])
    y_g = Rows(ring, yg, rsrc(y_ref), sems[:6])
    go_g = Rows(ring, gog, rsrc(gob), sems[6:12])

    def merge(dst, src):
        for hl in range(hh):
            mr = slice(HR + hl, HR + hl + 1)
            lr = slice(HR + 8 + hl, HR + 9 + hl)
            m1, m2 = dst[mr, :], src[mr, :]
            m = jnp.maximum(m1, m2)
            a = jnp.exp2((m1 - m) * c)
            b = jnp.exp2((m2 - m) * c)
            rr = slice(hl * 64, (hl + 1) * 64)
            dst[rr, :] = dst[rr, :] * a + src[rr, :] * b
            dst[mr, :] = m
            dst[lr, :] = dst[lr, :] * a + src[lr, :] * b

    o_r = Reduce(ring, part, rbuf, merge, sems[12:14])
    loads = [pltpu.make_async_copy(src, dst, ls.at[7 + n]) for n, (src, dst) in enumerate((
        (wk_hbm, wk_ref), (wv_hbm, wv_ref), (wq_hbm, wq_ref), (wo_hbm, wo_s), (wg_hbm, wg_s), (wu_hbm, wu_s), (wd_hbm, wd_s)))]
    stores = [pltpu.make_async_copy(src, dst, ls.at[n]) for n, (src, dst) in enumerate(((k_s, k_out), (v_s, v_out), (kt_s, kt_out), (mg, mg_out), (qz, qz_out)))]
    for cp in loads[:3]:
        cp.start()
    ring.enter()
    y_g.start()
    mx_copy = remote(m_ref, mg, xs.at[0], xr.at[0], ring.partner)
    mx_copy.start()
    for cp in loads[3:]:
        cp.start()
    gob[...] = go_ref[...].astype(BF16)
    for half in range(2):
        yg[z, core, half] = y_ref[half * sub:(half + 1) * sub, :]
    hcol = pl.ds(pl.multiple_of(core * inner, 128), inner)
    qz[...] = jnp.zeros_like(qz)
    mask_lanes(ak_ref, len_ref, z * T)
    for cp in loads[:3]:
        cp.wait()
    wqt[...] = wq_ref[:, hcol].T
    wk = wk_ref[:, hcol]
    wv = wv_ref[:, hcol]

    moves = {"y": y_g, "go": go_g, "o": o_r}

    def acts(*point):
        return [go_g.start if e[1] == "start" else part_(moves[e[0]].move, *e[1:]) for e in FWD_PLAN.get(point, [])]

    def run(*point):
        for fn in acts(*point):
            fn()

    def project(src, base, blocks):
        for j in blocks:
            r = pl.ds(pl.multiple_of(base + j * MC, MC), MC)
            blk = src[j * MC:(j + 1) * MC, :]
            kb = mm(blk, wk).astype(BF16)
            vb = mm(blk, wv).astype(BF16)
            k_s[r, :] = kb
            v_s[r, :] = vb
            kt_s[:, r] = kb.T
            vt_s[:, r] = vb.T

    nb = mem // MC
    project(m_ref, core * mem, range(nb))
    run("s", 0)
    mx_copy.wait_recv()
    project(mg, (1 - core) * mem, range(nb // 2))
    run("s", 1)
    project(mg, (1 - core) * mem, range(nb // 2, nb))
    run("s", 2)
    for cp in stores[:4]:
        cp.start()
    gain = g_ref[0:1, :].astype(F32)
    one_row = jnp.where(lax.broadcasted_iota(jnp.int32, (16, QT), 0) == 0, 1.0, 0.0).astype(BF16)

    def lanes(chip):
        return pl.ds(pl.multiple_of(chip * QT, QT), QT)

    def prep(chip):
        n1 = rms_norm(yg[chip].reshape(QT, dim).astype(F32), gain).astype(BF16)
        qt = mm_bt(wqt[...], n1).astype(BF16)
        for h in range(hc):
            lo = h * 128 + (h % 2) * 64
            qz[lo:lo + 64, lanes(chip)] = qt[h * 64:(h + 1) * 64]

    def step(new, slot, old, pslot):
        if new is not None:
            chip, h = new
            rhs = jnp.concatenate([qz[pl.ds(pl.multiple_of(h * 128, 128), 128), lanes(chip)], one_row], axis=0)
            pair = pl.ds(pl.multiple_of((h // 2) * 128, 128), 128)
            mx = None
        if old is not None:
            ochip, half, hl = old
            m = jnp.max(mx_scr[pslot], axis=0, keepdims=True)
            vrow = pl.ds(pl.multiple_of((half * hh + hl) * 64, 64), 64)
            ls_ = None
            acc = None
        for j in range(T // MC):
            r = slice(j * MC, (j + 1) * MC)
            if new is not None:
                s = mm(jnp.concatenate([k_s[r, pair], ak_ref[r, 0:16]], axis=1), rhs)
                s_scr[slot, r, :] = s
                t = jnp.max(s.reshape(MC // 8, 8, QT), axis=0)
                mx = t if mx is None else jnp.maximum(mx, t)
            if old is not None:
                pr = jnp.exp2((s_scr[pslot, r, :] - m) * c)
                t = jnp.sum(pr.reshape(MC // 8, 8, QT), axis=0)
                ls_ = t if ls_ is None else ls_ + t
                dd = mm(vt_s[vrow, r], pr.astype(BF16))
                acc = dd if acc is None else acc + dd
        if new is not None:
            mx_scr[slot] = mx
        if old is not None:
            part[ochip, half, hl * 64:(hl + 1) * 64, :] = acc
            part[ochip, half, HR + hl:HR + hl + 1, :] = m
            part[ochip, half, HR + 8 + hl:HR + 9 + hl, :] = jnp.sum(ls_, axis=0, keepdims=True)

    offs = [o for o, _ in FWD_ORDER]
    halves = [h for _, h in FWD_ORDER]
    n = len(offs)
    fresh = [int(k + 1 < n and offs[k + 1] not in offs[:k + 1]) for k in range(n)]
    run("s", 3)
    y_g.ready(0)
    prep(z)
    step((z, halves[0] * hh), 0, None, None)

    def body(pair, carry):
        for u in range(2):
            i = 2 * pair + u
            i2 = jnp.minimum(i + 1, n - 1)
            chip, half = ring.chip(pick(i, offs)), pick(i, halves)
            chip2, half2 = ring.chip(pick(i2, offs)), pick(i2, halves)
            for k in range(hh):
                slot = (u * hh + k) % 2
                if k == hh - 1:
                    dispatch(pair, {kk // 2: acts("r", kk) + [part_(y_g.ready, offs[kk + 1])] for kk in range(u, n, 2) if fresh[kk]})
                    if any(fresh[u::2]):
                        pl.when(pick(i, fresh) == 1)(part_(prep, chip2))
                    new = (chip2, half2 * hh)
                else:
                    new = (chip, half * hh + k + 1)
                step(new, 1 - slot, (chip, half, k), slot)
                dispatch(pair, {kk // 2: acts("b", kk * hh + k) for kk in range(u, n, 2) if acts("b", kk * hh + k)})
        return carry

    gl = [pltpu.make_async_copy(gob.at[pl.ds(half * sub, sub)], gog.at[z, core, half], ls.at[5 + half]) for half in range(2)]
    for cp in gl:
        cp.start()
    lax.fori_loop(0, n // 2, body, 0)
    yc = pltpu.make_async_copy(yg, yall, ls.at[14])
    yc.start()
    stores[4].start()
    run("t", 0)
    run("t", 1)
    qmine = pl.ds(pl.multiple_of(core * rows, rows), rows)
    qother = pl.ds(pl.multiple_of((1 - core) * rows, rows), rows)
    for h in range(hc):
        half, hl = h // hh, h % hh
        m = part[z, half, HR + hl:HR + hl + 1, :]
        l = part[z, half, HR + 8 + hl:HR + 9 + hl, :]
        own[h * 64:(h + 1) * 64, :] = part[z, half, hl * 64:(hl + 1) * 64, :] / l
        own[inner + h:inner + h + 1, :] = m + jnp.log2(l) / c
    satt[...] = own[:inner, qother].astype(BF16)
    xo = remote(satt, patt, xs.at[1], xr.at[1], ring.partner)
    xo.start()
    attt[pl.ds(pl.multiple_of(core * inner, inner), inner), :] = own[:inner, qmine].astype(BF16)
    for cp in loads[3:]:
        cp.wait()
    run("t", 2)
    xo.wait()
    attt[pl.ds(pl.multiple_of((1 - core) * inner, inner), inner), :] = patt[...]

    att = attt[...].T
    att_ref[...] = att
    gain2 = g_ref[1:2, :].astype(F32)
    run("t", 3)
    hid = (y_ref[...].astype(F32) + mm(att, wo_s[...])).astype(BF16).astype(F32)
    inv = lax.rsqrt(jnp.mean(hid * hid, axis=-1, keepdims=True) + 1e-6)
    hhat = hid * inv
    n2 = (hhat * gain2).astype(BF16)
    fb = ff // 4
    n2_s[...] = n2
    dn_s[...] = jnp.zeros_like(dn_s)

    def mlp(f, carry):
        cols = pl.ds(pl.multiple_of(f * fb, fb), fb)
        wg, wu = wg_s[:, cols], wu_s[:, cols]
        g = mm(n2_s[...], wg)
        u = mm(n2_s[...], wu)
        ga = mm_bt(gob[...], wd_s[cols, :])
        sig = jax.nn.sigmoid(g)
        si = g * sig
        dn_s[...] += mm_bt((ga * u * (sig + si * (1.0 - sig))).astype(BF16), wg) + mm_bt((ga * si).astype(BF16), wu)
        dispatch(f, {n: acts("t", 4 + n) for n in range(4) if acts("t", 4 + n)})
        return carry

    lax.fori_loop(0, 4, mlp, 0)
    dn = dn_s[...]
    gsum = jnp.sum(dn * hhat, axis=0, keepdims=True)
    gn_ref[...] = jnp.zeros_like(gn_ref)
    for k in range(dim // QT):
        gn_ref[k:k + 1, :] = gsum[:, k * QT:(k + 1) * QT]
    t = dn * gain2
    gh = go_ref[...] + inv * (t - hhat * jnp.mean(t * hhat, axis=-1, keepdims=True))
    gh_ref[...] = gh
    dh_ref[...] = gh.astype(BF16)
    run("t", 8)
    for off in range(-far + 1, far + 1):
        go_g.ready(off)
    mx_copy.wait_send()
    for cp in [yc] + gl + stores:
        cp.wait()
    for obj in (y_g, go_g, o_r):
        obj.drain()


def fwd_call(dims, *args):
    chips, rows, mem, dim, hc, c, ff = dims
    hh = hc // 2
    inner = hc * 64
    QT = 2 * rows
    T = 2 * mem
    HR = hh * 64
    h2 = chips // 2
    v = pl.BlockSpec(memory_space=VMEM)
    hbm = pl.BlockSpec(memory_space=pl.ANY)
    S = jax.ShapeDtypeStruct
    s3 = (2, 2, h2)
    gshape = (chips, 2, 2, rows // 2, dim)
    rows_sems = [DMA((1,)), DMA(s3)] * 2 + [DMA((1,)), DMA((2,))]
    return pl.pallas_call(
        functools.partial(fwd_kernel, dims),
        out_shape=(S((inner + 8, QT), F32), S((rows, 2 * inner), BF16), S((rows, dim), BF16), S((rows, dim), F32), S((8, QT), F32),
                   S((T, inner), BF16), S((T, inner), BF16), S((inner, T), BF16), S((hc * 128, chips * QT), BF16), S((mem, dim), BF16), S(gshape, BF16), S(gshape, BF16)),
        in_specs=[pl.BlockSpec(memory_space=pltpu.SMEM)] + [v] * 4 + [hbm] * 7, out_specs=(v,) * 5 + (hbm,) * 7,
        scratch_shapes=[
            VMEM((T, inner), BF16), VMEM((T, inner), BF16), VMEM((inner, T), BF16), VMEM((hc * 128, chips * QT), BF16), VMEM((mem, dim), BF16),
            VMEM((dim, 2 * inner), BF16), VMEM((dim, 2 * inner), BF16), VMEM((dim, 2 * inner), BF16), VMEM((T, 128), BF16),
            VMEM(gshape, BF16), VMEM((inner, dim), BF16), VMEM((inner, T), BF16), VMEM((2, T, QT), F32), VMEM((2, 8, QT), F32),
            VMEM((chips, 2, HR + 16, QT), F32), VMEM((2, 2, h2, HR + 16, QT), F32), VMEM((inner, rows), BF16), VMEM((inner, rows), BF16),
            VMEM((rows, dim), BF16), VMEM((2 * inner, rows), BF16), VMEM((2 * inner, dim), BF16), VMEM((dim, ff), BF16), VMEM((dim, ff), BF16), VMEM((ff, dim), BF16), VMEM((rows, dim), BF16), VMEM((rows, dim), F32)]
        + rows_sems * 2 + [DMA((1,)), DMA(s3)] + [DMA((2,))] * 2 + [DMA((15,))],
        compiler_params=pltpu.CompilerParams(vmem_limit_bytes=62 * 1024 * 1024, collective_id=0, has_side_effects=True),
        cost_estimate=pl.CostEstimate(flops=10**10, bytes_accessed=30 << 20, transcendentals=0),
        name="attn_fwd")(*args)


def solution(mesh):
    group = mesh.shape['seq']
    row_spec = P(('data', 'seq'), None)
    part_vec = P('data')
    part_mat = P('data', None)
    part_cube = P('data', None, None)

    def device_step(dec_in, memory, mem_len, grad_out, norm_attn, wq, wk, wv, wo, norm_mlp, w_gate, w_up, w_down):
        rows, dim = dec_in.shape
        mem = memory.shape[0]
        heads, hd = wq.shape[1], wq.shape[2]
        inner = heads * hd
        chips = group // 2
        hc = heads // 2
        c = LOG2E * hd ** -0.5
        dims = (chips, rows, mem, dim, hc, c, w_gate.shape[1])
        wq2, wk2, wv2 = (w.reshape(dim, inner) for w in (wq, wk, wv))
        wo2 = wo.reshape(inner, dim)
        gains = jnp.stack([norm_attn, norm_mlp])

        own, attended, dh, grad_hidden, gn, k_c, v_c, kt_c, qz, mem_p, y_all, go_all = fwd_call(
            dims, mem_len, dec_in, grad_out, memory, gains, wq2, wk2, wv2, wo2, w_gate, w_up, w_down)
        gvec, dq_own, g_mem, g_wk, g_wv, g_wq, g_wo, g_down, g_gate, g_up, _ = bwd_call(
            dims, mem_len, dh, own, gn, attended, gains,
            k_c, v_c, kt_c, qz, wo2, wq2, wk2, wv2, memory, mem_p, y_all, go_all, w_gate, w_up, w_down)
        x_in = dec_in.astype(F32)
        _, norm_pull = jax.vjp(rms_norm, x_in, norm_attn.astype(F32))
        grad_x_norm, _ = norm_pull(mm_bt(dq_own.T, wq2))
        g_dec = grad_hidden + grad_x_norm
        cube = (dim, heads, hd)
        g_wq, g_wk, g_wv = (g.reshape(inner, dim).T.reshape(cube) for g in (g_wq, g_wk, g_wv))
        return (g_dec, g_mem, gvec[0], g_wq, g_wk, g_wv, g_wo.reshape(heads, hd, dim), gvec[1], g_gate, g_up, g_down)

    return jax.shard_map(device_step, mesh=mesh,
                         in_specs=(row_spec, row_spec, part_vec, row_spec) + (P(),) * 9,
                         out_specs=(row_spec, row_spec, part_vec, part_cube, part_cube, part_cube, part_cube, part_vec, part_mat, part_mat, part_mat),
                         check_vma=False)
```

```python
import functools
import math

import jax
import jax.numpy as jnp
from jax import lax
from jax.experimental import pallas as pl
from jax.experimental.pallas import tpu as pltpu
from jax.sharding import PartitionSpec as P

F32 = jnp.float32
BF16 = jnp.bfloat16
LOG2E = math.log2(math.e)
VMEM = pltpu.VMEM
MESH = pl.DeviceIdType.MESH


def mm(a, b):
    return jnp.dot(a, b, preferred_element_type=F32)


def mm_bt(a, b):
    return lax.dot_general(a, b, (((1,), (1,)), ((), ())), preferred_element_type=F32)


def mm_at(a, b):
    return lax.dot_general(a, b, (((0,), (0,)), ((), ())), preferred_element_type=F32)


def rms_norm(tensor, gain):
    mean_sq = jnp.mean(tensor * tensor, axis=-1, keepdims=True)
    return tensor * lax.rsqrt(mean_sq + 1e-6) * gain


RIGHT, LEFT = 0, 1
DMA = pltpu.SemaphoreType.DMA

FWD_ORDER = [(0, 0), (0, 1), (1, 0), (1, 1), (-3, 0), (3, 1), (4, 0), (4, 1), (3, 0), (-3, 1), (2, 0), (-2, 1), (2, 1), (-2, 0), (-1, 1), (-1, 0)]
BWD_ORDER = [0, 1, 4, 3, -3, 2, -2, -1]
BWD_FIRST = 2
FWD_PLAN = {
    ("b", 0): [("y", 0, 1, 1), ("y", 1, 0, 1)],
    ("b", 11): [("y", 1, 1, 3), ("y", 1, 0, 3)],
    ("b", 12): [("go", 0, 0, 1)],
    ("b", 13): [("go", 1, 1, 1)],
    ("b", 14): [("o", 1, 0, 3)],
    ("b", 15): [("go", 0, 1, 1)],
    ("b", 17): [("o", 0, 1, 3)],
    ("b", 18): [("go", 1, 0, 1)],
    ("b", 20): [("o", 0, 0, 4)],
    ("b", 21): [("go", 1, 1, 2)],
    ("b", 23): [("o", 1, 1, 4)],
    ("b", 31): [("go", 0, 0, 2)],
    ("b", 32): [("go", 1, 0, 2)],
    ("b", 34): [("go", 0, 1, 2)],
    ("b", 35): [("go", 1, 1, 3)],
    ("b", 36): [("o", 0, 0, 3)],
    ("b", 37): [("o", 1, 1, 3)],
    ("b", 38): [("o", 0, 1, 2)],
    ("b", 4): [("y", 0, 0, 2), ("y", 1, 1, 2)],
    ("b", 40): [("go", 1, 0, 3)],
    ("b", 41): [("o", 1, 0, 2)],
    ("b", 42): [("go", 0, 1, 3)],
    ("b", 43): [("go", 1, 1, 4)],
    ("b", 8): [("y", 0, 1, 2), ("y", 1, 0, 2)],
    ("b", 9): [("go", "start")],
    ("r", 3): [("y", 0, 0, 3), ("y", 0, 1, 3)],
    ("r", 5): [("y", 0, 0, 4), ("y", 1, 1, 4)],
    ("s", 1): [("y", 0, 0, 1), ("y", 1, 1, 1)],
    ("t", 1): [("o", 0, 0, 2), ("o", 1, 1, 2), ("o", 0, 1, 1), ("o", 1, 0, 1), ("o", 0, 0, 1), ("o", 1, 1, 1), ("o", 0, 1, 0), ("o", 1, 0, 0), ("o", 0, 0, 0), ("o", 1, 1, 0)],
    ("t", 2): [("go", 0, 0, 3)],
    ("t", 6): [("go", 0, 0, 4)],
}
BWD_PLAN = {
    ("b", 1): [("dh", 0, 0, 1), ("dh", 1, 1, 1)],
    ("b", 10): [("dh", 0, 1, 3), ("dh", 1, 0, 3), ("st", 0, 0, 3), ("st", 1, 1, 3)],
    ("b", 11): [("st", 0, 1, 3), ("st", 1, 0, 3)],
    ("b", 12): [("dq0", 0, 0, 4)],
    ("b", 13): [("dq0", 1, 1, 4)],
    ("b", 14): [("att", 0, 0, 1), ("att", 1, 1, 1)],
    ("b", 15): [("dq0", 0, 1, 3), ("att", 0, 1, 1), ("att", 1, 0, 1)],
    ("b", 16): [("dq0", 0, 0, 3), ("dq0", 1, 0, 3)],
    ("b", 17): [("dq0", 1, 1, 3)],
    ("b", 18): [("att", 0, 0, 2), ("att", 1, 1, 2)],
    ("b", 19): [("dq0", 0, 1, 2), ("att", 1, 0, 2)],
    ("b", 2): [("dh", 0, 1, 1), ("dh", 1, 0, 1), ("st", 0, 0, 1), ("st", 1, 1, 1), ("st", 0, 1, 1), ("st", 1, 0, 1)],
    ("b", 20): [("dq0", 1, 0, 2), ("att", 0, 1, 2)],
    ("b", 21): [("dq0", 0, 0, 2), ("dq0", 1, 1, 2)],
    ("b", 22): [("att", 0, 0, 3), ("att", 1, 1, 3)],
    ("b", 23): [("dq0", 0, 1, 1), ("ar0", 0, 1, 3), ("ar0", 1, 0, 3), ("ar0", 0, 0, 4), ("ar0", 1, 1, 4), ("att", 1, 0, 3)],
    ("b", 24): [("dq0", 1, 0, 1), ("dq1", 0, 0, 4), ("att", 0, 1, 3)],
    ("b", 25): [("dq0", 0, 0, 1), ("dq0", 1, 1, 1), ("dq1", 1, 1, 4)],
    ("b", 26): [("att", 0, 0, 4), ("att", 1, 1, 4)],
    ("b", 27): [("dq0", 0, 1, 0), ("dq1", 0, 1, 3), ("ar0", 1, 0, 2)],
    ("b", 28): [("dq1", 1, 0, 3), ("ar0", 1, 1, 3), ("ar0", 0, 1, 2)],
    ("b", 29): [("dq0", 1, 0, 0), ("ar0", 0, 0, 3)],
    ("b", 30): [("dq0", 1, 1, 0), ("dq1", 0, 0, 3)],
    ("b", 31): [("dq0", 0, 0, 0), ("ds0", "start"), ("dq1", 1, 1, 3), ("ar0", 1, 0, 1)],
    ("b", 32): [("dq1", 0, 1, 2), ("dq1", 1, 0, 2), ("ar0", 0, 1, 1)],
    ("b", 33): [("ar0", 0, 0, 2), ("ar0", 1, 1, 2)],
    ("b", 34): [("dq1", 0, 0, 2), ("ds0", 1, 1, 1), ("ds0", 1, 0, 1)],
    ("b", 35): [("dq1", 1, 1, 2), ("dq1", 0, 1, 1), ("ar0", 1, 0, 0), ("ar1", 0, 1, 3), ("ar1", 1, 0, 3), ("ar1", 0, 0, 4), ("ar1", 1, 1, 4), ("ds0", 0, 0, 1), ("ds0", 0, 1, 1)],
    ("b", 36): [("dq1", 1, 0, 1), ("dq2", 0, 0, 4), ("ar0", 0, 1, 0), ("ar0", 0, 0, 1), ("ar0", 1, 1, 1)],
    ("b", 37): [("dq1", 0, 0, 1), ("dq2", 1, 1, 4), ("ds0", 1, 1, 2), ("ds0", 1, 0, 2)],
    ("b", 38): [("dq1", 0, 1, 0), ("dq1", 1, 1, 1)],
    ("b", 39): [("dq2", 0, 1, 3), ("ar1", 0, 1, 2), ("ar1", 1, 0, 2)],
    ("b", 40): [("dq2", 1, 0, 3), ("ar1", 0, 0, 3), ("ar1", 1, 1, 3), ("ds0", 0, 0, 2)],
    ("b", 41): [("dq1", 1, 0, 0), ("ds0", 0, 1, 2)],
    ("b", 42): [("dq2", 0, 0, 3), ("ar0", 1, 1, 0)],
    ("b", 43): [("dq2", 1, 1, 3), ("ar0", 0, 0, 0), ("as0", "start"), ("ds0", 1, 1, 3), ("dq1", 0, 0, 0), ("ds0", 1, 0, 3)],
    ("b", 45): [("dq1", 1, 1, 0), ("ds1", "start"), ("dq2", 0, 1, 2), ("ar1", 0, 1, 1), ("ar1", 1, 0, 1)],
    ("b", 46): [("dq2", 1, 0, 2), ("ar1", 0, 0, 2), ("ds0", 0, 0, 3)],
    ("b", 47): [("dq2", 0, 0, 2), ("dq2", 1, 1, 2), ("ar1", 1, 1, 2), ("ar2", 0, 1, 3), ("ar2", 1, 0, 3), ("ar2", 0, 0, 4), ("ar2", 1, 1, 4), ("ds0", 0, 1, 3)],
    ("b", 5): [("dh", 0, 0, 2), ("dh", 1, 1, 2)],
    ("b", 6): [("dh", 0, 1, 2), ("dh", 1, 0, 2), ("st", 0, 0, 2), ("st", 1, 1, 2)],
    ("b", 7): [("st", 0, 1, 2), ("st", 1, 0, 2)],
    ("b", 9): [("dh", 0, 0, 3), ("dh", 1, 1, 3)],
    ("f", 1): [("dq2", 0, 0, 1), ("ar1", 1, 1, 1), ("ar2", 0, 1, 2), ("ar2", 1, 0, 2)],
    ("f", 10): [("dq2", 1, 1, 0), ("ar1", 0, 0, 0)],
    ("f", 12): [("dq2", 0, 0, 0), ("ds2", "start"), ("ar1", 1, 1, 0), ("as1", "start")],
    ("f", 14): [("ar2", 0, 1, 1), ("ar2", 1, 0, 1)],
    ("f", 16): [("ar2", 0, 0, 2), ("ar2", 1, 1, 2)],
    ("f", 17): [("as0", 0, 0, 3), ("as0", 1, 1, 3), ("as0", 0, 1, 3), ("as0", 1, 0, 3), ("ds1", 0, 0, 3), ("ds1", 1, 1, 3), ("ds1", 0, 1, 3), ("ds1", 1, 0, 3)],
    ("f", 19): [("ds2", 0, 0, 1), ("ds2", 1, 1, 1)],
    ("f", 21): [("ds2", 0, 1, 1), ("ds2", 1, 0, 1)],
    ("f", 23): [("as1", 0, 0, 1), ("as1", 1, 1, 1)],
    ("f", 25): [("as1", 0, 1, 1), ("as1", 1, 0, 1)],
    ("f", 26): [("ar2", 0, 1, 0), ("ar2", 1, 0, 0), ("ar2", 0, 0, 1), ("ar2", 1, 1, 1), ("as0", 0, 0, 4), ("as0", 1, 1, 4), ("ds1", 0, 0, 4), ("ds1", 1, 1, 4)],
    ("f", 28): [("ds2", 0, 0, 2), ("ds2", 1, 1, 2)],
    ("f", 3): [("ar2", 0, 0, 3), ("ar2", 1, 1, 3)],
    ("f", 30): [("ds2", 0, 1, 2), ("ds2", 1, 0, 2)],
    ("f", 32): [("as1", 0, 0, 2), ("as1", 1, 1, 2)],
    ("f", 34): [("as1", 0, 1, 2), ("as1", 1, 0, 2)],
    ("f", 35): [("ar2", 0, 0, 0), ("ar2", 1, 1, 0), ("as2", "start"), ("ds2", 0, 0, 3), ("as1", 0, 0, 3), ("ds2", 1, 1, 3), ("as1", 1, 1, 3), ("ds2", 0, 1, 3), ("ds2", 1, 0, 3)],
    ("f", 5): [("as0", 0, 0, 2), ("as0", 1, 1, 2)],
    ("f", 7): [("as0", 0, 1, 2), ("as0", 1, 0, 2)],
    ("f", 8): [("dq2", 0, 1, 0), ("dq2", 1, 0, 0), ("ds1", 0, 0, 2), ("ds1", 1, 1, 2), ("ds1", 0, 1, 2), ("ds1", 1, 0, 2)],
    ("h", 0): [("as0", 0, 0, 1), ("as0", 1, 1, 1)],
    ("h", 1): [("as0", 0, 1, 1), ("as0", 1, 0, 1), ("ds1", 0, 0, 1), ("ds0", 1, 1, 4)],
    ("h", 2): [("ds1", 0, 1, 1), ("ds1", 1, 1, 1)],
    ("h", 3): [("ds1", 1, 0, 1)],
    ("h", 4): [("dq2", 0, 1, 1), ("ar1", 1, 0, 0)],
    ("h", 5): [("ar1", 0, 1, 0), ("dq2", 1, 0, 1)],
    ("h", 6): [("ar1", 0, 0, 1), ("ds0", 0, 0, 4)],
    ("h", 7): [("dq2", 1, 1, 1)],
    ("m", 1): [("as1", 0, 1, 3), ("as1", 1, 0, 3)],
    ("m", 3): [("as2", 0, 0, 1), ("as2", 1, 1, 1)],
    ("m", 4): [("ds2", 0, 0, 4), ("ds2", 1, 1, 4)],
    ("q", 0): [("as2", 0, 1, 1), ("as2", 1, 0, 1)],
    ("q", 1): [("as1", 0, 0, 4), ("as1", 1, 1, 4)],
    ("q", 3): [("as2", 0, 0, 2), ("as2", 1, 1, 2)],
    ("q", 6): [("as2", 0, 1, 2), ("as2", 1, 0, 2)],
    ("q", 8): [("as2", 0, 0, 3), ("as2", 1, 1, 3), ("as2", 0, 1, 3), ("as2", 1, 0, 3), ("as2", 0, 0, 4), ("as2", 1, 1, 4)],
    ("r", 12): [("dh", 0, 0, 4), ("dh", 1, 1, 4), ("att", "start"), ("st", 0, 0, 4), ("st", 1, 1, 4)],
}


class Ring:
    def __init__(self, chips):
        me = lax.axis_index('seq')
        self.chips = chips
        self.far = chips // 2
        self.z = me // 2
        self.core = me - 2 * self.z
        self.partner = 2 * self.z + 1 - self.core
        self.next = (2 * self.chip(1) + self.core, 2 * self.chip(-1) + self.core)
        self.hops = {(RIGHT, 0): self.far, (LEFT, 1): self.far, (RIGHT, 1): self.far - 1, (LEFT, 0): self.far - 1}

    def chip(self, off):
        return lax.rem(self.z + off + self.chips, self.chips)

    def ahead(self, d, k):
        return self.chip(k if d == RIGHT else -k)

    def enter(self):
        barrier = pltpu.get_barrier_semaphore()
        for dev in (self.partner,) + self.next:
            pl.semaphore_signal(barrier, inc=1, device_id={'seq': dev}, device_id_type=MESH)
        pl.semaphore_wait(barrier, 3)


def remote(src, dst, ssem, rsem, dev):
    return pltpu.make_async_remote_copy(src_ref=src, dst_ref=dst, send_sem=ssem, recv_sem=rsem, device_id={'seq': dev}, device_id_type=MESH)


def sent(every, ssem, rsem, dev):
    remote(every, every, ssem, rsem, dev).wait_send()


class Share:
    def __init__(self, ring, buf, src, sems):
        self.ring, self.buf, self.src = ring, buf, src
        self.ss, self.rs = sems

    def slot(self, chip, half):
        return self.buf.at[chip, half]

    def send(self, d, half, t):
        slot = self.slot(self.ring.ahead(d, 1 - t), half)
        src = self.src(half) if t == 1 else slot
        return remote(src, slot, self.ss.at[0], self.rs.at[d, half, t - 1], self.ring.next[d])

    def recv(self, d, half, t):
        slot = self.slot(self.ring.ahead(d, -t), half)
        return remote(slot, slot, self.ss.at[0], self.rs.at[d, half, t - 1], self.ring.next[d])

    def start(self):
        for d, half in self.ring.hops:
            self.send(d, half, 1).start()

    def came(self, d, half, t):
        pass

    def move(self, d, half, t):
        self.recv(d, half, t).wait_recv()
        if t < self.ring.hops[d, half]:
            self.send(d, half, t + 1).start()
        self.came(d, half, t)

    def drain(self):
        sent(self.buf.at[pl.ds(0, self.ring.chips - 1)], self.ss.at[0], self.rs.at[0, 0, 0], self.ring.next[0])


class Rows(Share):
    def __init__(self, ring, buf, src, sems):
        super().__init__(ring, buf, src, sems[:2])
        self.fs, self.fr, self.os, self.orr = sems[2:]

    def slot(self, chip, half):
        return self.buf.at[chip, self.ring.core, half]

    def pslot(self, chip, half):
        return self.buf.at[chip, 1 - self.ring.core, half]

    def start(self):
        super().start()
        for half in range(2):
            self.own(half).start()

    def own(self, half):
        return remote(self.src(half), self.slot(self.ring.z, half), self.os.at[0], self.orr.at[half], self.ring.partner)

    def forward(self, d, half, t):
        slot = self.slot(self.ring.ahead(d, -t), half)
        return remote(slot, slot, self.fs.at[0], self.fr.at[d, half, t - 1], self.ring.partner)

    def came(self, d, half, t):
        self.forward(d, half, t).start()

    def ready(self, off):
        ring = self.ring
        if off == 0:
            for half in range(2):
                slot = self.pslot(ring.z, half)
                remote(slot, slot, self.os.at[0], self.orr.at[half], ring.partner).wait_recv()
            return
        for (d, half), n in ring.hops.items():
            t = ring.far if abs(off) == ring.far else (-off if d == RIGHT else off)
            if 1 <= t <= n:
                slot = self.pslot(ring.ahead(d, -t), half)
                remote(slot, slot, self.fs.at[0], self.fr.at[d, half, t - 1], ring.partner).wait_recv()

    def drain(self):
        every = self.buf.at[pl.ds(0, self.ring.chips - 1), 0]
        sent(every, self.ss.at[0], self.rs.at[0, 0, 0], self.ring.next[0])
        sent(every, self.fs.at[0], self.fr.at[0, 0, 0], self.ring.partner)
        sent(self.buf.at[0, 0], self.os.at[0], self.orr.at[0], self.ring.partner)


class Reduce:
    def __init__(self, ring, part, rbuf, merge, sems):
        self.ring, self.part, self.rbuf, self.merge = ring, part, rbuf, merge
        self.ss, self.rs = sems

    def send(self, d, half, o):
        return remote(self.part.at[self.ring.ahead(d, o), half], self.rbuf.at[d, half, o - 1], self.ss.at[0], self.rs.at[d, half, o - 1], self.ring.next[d])

    def recv(self, d, half, o):
        slot = self.rbuf.at[d, half, o]
        return remote(slot, slot, self.ss.at[0], self.rs.at[d, half, o], self.ring.next[d])

    def move(self, d, half, o):
        if o < self.ring.hops[d, half]:
            self.recv(d, half, o).wait_recv()
            self.merge(self.part.at[self.ring.ahead(d, o), half], self.rbuf.at[d, half, o])
        if o > 0:
            self.send(d, half, o).start()

    def drain(self):
        sent(self.part.at[pl.ds(0, self.ring.chips - 1)], self.ss.at[0], self.rs.at[0, 0, 0], self.ring.next[0])


def pick(i, values):
    out = jnp.int32(values[-1])
    for k, v in enumerate(values[:-1]):
        out = jnp.where(i == k, jnp.int32(v), out)
    return out


def mask_lanes(ref, len_ref, start):
    row = lax.broadcasted_iota(jnp.int32, ref.shape, 0) + start
    lane = lax.broadcasted_iota(jnp.int32, ref.shape, 1)
    bias = jnp.where(row < len_ref[0], 0.0, -1e30)
    ref[...] = jnp.where(lane == 0, bias, jnp.where(lane < 4, 1.0, 0.0)).astype(BF16)


def dispatch(index, table):
    def branch(keys):
        if len(keys) == 1:
            def run():
                for fn in table[keys[0]]:
                    fn()
            pl.when(index == keys[0])(run)
            return
        low, high = keys[:len(keys) // 2], keys[len(keys) // 2:]
        pl.when(index < high[0])(functools.partial(branch, low))
        pl.when(index >= high[0])(functools.partial(branch, high))
    if table:
        branch(sorted(table))


def add_into(dst, src):
    dst[...] = dst[...] + src[...]


def parts3(x):
    hi = x.astype(BF16)
    rest = x - hi.astype(F32)
    mid = rest.astype(BF16)
    lo = (rest - mid.astype(F32)).astype(BF16)
    return hi, mid, lo


def bwd_kernel(dims, len_ref, dh_ref, own_ref, gn_ref, att_ref, y_ref, gh_ref, g_ref,
               k_hbm, v_hbm, kt_hbm, qz_hbm, wo_hbm, wq_hbm, wk_hbm, wv_hbm, ma_hbm, mb_hbm, y_hbm, gog, wg_hbm, wu_hbm, wd_hbm,
               gvec_ref, gdec_ref, gmem, gwk, gwv, gwq, gwo, gdown, ggate, gup, attg,
               dqo_ref, k_ref, v_ref, kt_ref, qz_ref, wo_ref, wq_ref, wk_ref, wv_ref, ak_ref,
               dhg, doz, aqs, ads, stb, dk, dv, dkv, dkvp, dqp, dqr, dqa, arp, arr, ara, pvec, pdq, spb,
               msc, ybuf, abuf, wbuf, dbuf, wt, gst, gsw, gwo_s, gwq_s,
               *sems):
    chips, rows, mem, dim, hc, c, ff = dims
    QT = 2 * rows
    T = 2 * mem
    MC = min(256, mem)
    nm = T // MC
    inner = hc * 64
    np_ = hc // 2
    seg = 256 // chips // 2
    fh = ff // 2
    FT = wt.shape[1]
    nf = fh // FT
    ring = Ring(chips)
    z, core, far = ring.z, ring.core, ring.far
    sems = list(sems)

    def take(n):
        out = sems[:n]
        del sems[:n]
        return out

    half_rows = rows // 2
    part_ = functools.partial
    rsrc = lambda ref: (lambda half: ref.at[pl.ds(half * half_rows, half_rows)])
    dh_g = Rows(ring, dhg, rsrc(dh_ref), take(6))
    att_g = Rows(ring, attg, rsrc(att_ref), take(6))
    st_g = Share(ring, stb, lambda half: stb.at[z, half], take(2))
    dq_r = [Reduce(ring, dqp.at[p], dqr.at[p], add_into, take(2)) for p in range(np_)]
    dq_s = [Share(ring, dqa.at[p], lambda half, p=p: dqa.at[p, z, half], take(2)) for p in range(np_)]
    ar_r = [Reduce(ring, arp.at[p], arr.at[p], add_into, take(2)) for p in range(np_)]
    ar_s = [Share(ring, ara.at[p], lambda half, p=p: ara.at[p, z, half], take(2)) for p in range(np_)]
    xs, xr, ls, gs, gr, gl, wsem, ysem, lsem = take(9)
    loads = [pltpu.make_async_copy(src, dst, lsem.at[n]) for n, (src, dst) in enumerate((
        (wo_hbm, wo_ref), (k_hbm, k_ref), (v_hbm, v_ref), (kt_hbm, kt_ref), (qz_hbm, qz_ref),
        (ma_hbm, msc.at[0, pl.ds(0, mem)]), (mb_hbm, msc.at[1, pl.ds(0, mem)]), (wq_hbm, wq_ref), (wk_hbm, wk_ref), (wv_hbm, wv_ref)))]
    for cp in loads:
        cp.start()
    ring.enter()
    dh_g.start()
    locals_ = [pltpu.make_async_copy(att_ref.at[pl.ds(half * half_rows, half_rows)], attg.at[z, core, half], ls.at[half]) for half in range(2)]
    for cp in locals_:
        cp.start()
    for half in range(2):
        dhg[z, core, half] = dh_ref[half * half_rows:(half + 1) * half_rows, :]
    doz[...] = jnp.zeros_like(doz)
    mask_lanes(ak_ref, len_ref, z * T)
    hrow = pl.ds(pl.multiple_of(core * inner, inner), inner)
    hcol = pl.ds(pl.multiple_of(core * inner, 128), inner)
    other_cols = pl.ds(pl.multiple_of((1 - core) * mem, mem), mem)
    my_cols = pl.ds(pl.multiple_of(core * mem, mem), mem)
    qmine = pl.ds(pl.multiple_of(core * rows, rows), rows)
    qother = pl.ds(pl.multiple_of((1 - core) * rows, rows), rows)

    def lanes(chip):
        return pl.ds(pl.multiple_of(chip * QT, QT), QT)

    def d_out(chip):
        return mm_bt(wo_ref[hrow, :], dhg[chip].reshape(QT, dim))

    def prepare(chip, dot=None):
        dot = d_out(chip) if dot is None else dot
        dob = dot.astype(BF16)
        q = lanes(chip)
        row = lax.broadcasted_iota(jnp.int32, (16, QT), 0)
        for h in range(hc):
            lo = h * 128 + (h % 2) * 64
            doz[lo:lo + 64, q] = dob[h * 64:(h + 1) * 64]
            for ref, half, first in ((aqs, 0, 1.0), (ads, 1, 0.0)):
                a, b, e = (x.astype(F32) for x in parts3(stb[chip, half, h:h + 1, :]))
                ref[h * 16:(h + 1) * 16, q] = jnp.where(row == 0, first, jnp.where(row == 1, a, jnp.where(row == 2, b, jnp.where(row == 3, e, 0.0)))).astype(BF16)

    dh_g.ready(0)
    loads[0].wait()
    dot0 = d_out(z)
    prod = dot0 * own_ref[:inner, :]
    for h in range(hc):
        stb[z, 0, h:h + 1, :] = -own_ref[inner + h:inner + h + 1, :]
        stb[z, 1, h:h + 1, :] = -jnp.sum(prod[h * 64:(h + 1) * 64], axis=0, keepdims=True)
    stb[z, 0, hc:8, :] = gn_ref[0:8 - hc, :]
    stb[z, 1, hc:8, :] = gn_ref[8 - hc:16 - 2 * hc, :]
    st_g.start()
    prepare(z, dot0)
    dk[...] = jnp.zeros_like(dk)
    dv[...] = jnp.zeros_like(dv)
    for cp in loads[1:]:
        cp.wait()

    def tile(h, chip):
        pair = h // 2
        q = lanes(chip)
        hz = pl.ds(pl.multiple_of(h * 128, 128), 128)
        h16 = pl.ds(pl.multiple_of(h * 16, 16), 16)
        ps = pl.ds(pl.multiple_of(pair * 128, 128), 128)
        hz64 = pl.ds(pl.multiple_of(h * 128 + (h - 2 * pair) * 64, 64), 64)
        h64 = pl.ds(pl.multiple_of(h * 64, 64), 64)
        hr = h64
        q_t = qz_ref[hz64, q]
        do_t = doz[hz64, q]
        r1 = jnp.concatenate([qz_ref[hz, q], aqs[h16, q]], axis=0)
        r2 = jnp.concatenate([doz[hz, q], ads[h16, q]], axis=0)
        stage = {}
        dq = None
        for j in range(nm + 2):
            if j < nm:
                r = slice(j * MC, (j + 1) * MC)
                ak = ak_ref[r, 0:16]
                stage["a", j] = (mm(jnp.concatenate([k_ref[r, ps], ak], axis=1), r1), mm(jnp.concatenate([v_ref[r, ps], ak], axis=1), r2))
            if 1 <= j <= nm:
                s, dp = stage.pop(("a", j - 1))
                a = jnp.exp2(s * c)
                stage["b", j - 1] = (a.astype(BF16), (a * dp).astype(BF16))
            if j >= 2:
                r = slice((j - 2) * MC, (j - 1) * MC)
                pb, ds = stage.pop(("b", j - 2))
                dv[hr, r] += mm_bt(do_t, pb)
                dk[hr, r] += mm_bt(q_t, ds)
                d = mm(kt_ref[h64, r], ds)
                dq = d if dq is None else dq + d
        dqp[pair, chip, h - 2 * pair] = dq

    scale = 0.125

    def xp(p):
        return remote(dkv.at[p, :, other_cols], dkvp.at[p], xs.at[p], xr.at[p], ring.partner)

    def xq(p):
        return remote(dqa.at[p, z, :, :, qother], pdq.at[p], xs.at[np_ + p], xr.at[np_ + p], ring.partner)

    def share_dq(p):
        for half in range(2):
            dqa[p, z, half] = (dqp[p, z, half] * scale).astype(BF16)
        dq_s[p].start()
        xq(p).start()

    def share_ar(p):
        for half in range(2):
            ara[p, z, half] = arp[p, z, half]
        ar_s[p].start()

    moves = {"dh": dh_g, "st": st_g, "att": att_g}
    begins = {"att": att_g.start}
    for p in range(np_):
        moves.update({f"dq{p}": dq_r[p], f"ds{p}": dq_s[p], f"ar{p}": ar_r[p], f"as{p}": ar_s[p]})
        begins.update({f"ds{p}": part_(share_dq, p), f"as{p}": part_(share_ar, p)})

    def acts(*point):
        return [begins[e[0]] if e[1] == "start" else part_(moves[e[0]].move, *e[1:]) for e in BWD_PLAN.get(point, [])]

    def run(*point):
        for fn in acts(*point):
            fn()

    def table(kind, n):
        return {k: acts(kind, k) for k in range(n) if acts(kind, k)}

    offs = BWD_ORDER
    first = BWD_FIRST * hc
    per = 2 * (chips - BWD_FIRST)
    needs = {k * hc: offs[k] for k in range(1, BWD_FIRST)}
    needs.update({first + 2 * (k - BWD_FIRST): offs[k] for k in range(BWD_FIRST, chips)})

    def project(p):
        r = pl.ds(pl.multiple_of(p * 128, 128), 128)
        dkv[p, 0:128, :] = (dk[r, :] * scale).astype(BF16)
        dkv[p, 128:256, :] = dv[r, :].astype(BF16)
        xp(p).start()
        g = mm(dkv[p, :, my_cols], msc[0, 0:mem]) + mm(dkv[p, :, other_cols], msc[1, 0:mem])
        for n in range(2 * chips):
            arp[p, n // 2, n % 2] = g[n * seg:(n + 1) * seg]

    def body(it, carry):
        early = it < first
        b = it - first
        p = b // per
        r = b - p * per
        h = jnp.where(early, it % hc, 2 * p + r % 2)
        chip = ring.chip(pick(jnp.where(early, it // hc, BWD_FIRST + r // 2), offs))
        dispatch(it, {k: acts("r", k) + [part_(dh_g.ready, off)] for k, off in needs.items()})
        fresh = (early & (it > 0) & (it % hc == 0)) | ((b >= 0) & (b < per) & (r % 2 == 0))
        pl.when(fresh)(part_(prepare, chip))
        tile(h, chip)
        pl.when((b >= 0) & (r == per - 1))(part_(project, p))
        dispatch(it, table("b", chips * hc))
        return carry

    lax.fori_loop(0, chips * hc, body, 0)
    run("p", np_)
    near = range(1 - far, far + 1)

    for cp in locals_:
        cp.wait()
    for off in near:
        att_g.ready(off)
    gain2 = g_ref[1:2, :].astype(F32)
    gwo_s[...] = jnp.zeros_like(gwo_s)

    def y_fetch(ch, slot):
        return pltpu.make_async_copy(y_hbm.at[ch], ybuf.at[slot], ysem.at[slot, 0])

    def fetch(ch, slot):
        return (y_fetch(ch, slot), pltpu.make_async_copy(attg.at[ch], abuf.at[slot], ysem.at[slot, 1]))

    for cp in fetch(0, 0):
        cp.start()

    def hidden(ch, carry):
        slot = ch % 2
        for cp in fetch(ch, slot):
            cp.wait()

        @pl.when(ch + 1 < chips)
        def _():
            for cp in fetch(ch + 1, 1 - slot):
                cp.start()
        att = abuf[slot].reshape(QT, dim)
        h = (ybuf[slot].reshape(QT, dim).astype(F32) + mm(att, wo_ref[...])).astype(BF16)
        qz_ref[0:dim, lanes(ch)] = rms_norm(h.astype(F32), gain2).astype(BF16).T
        ah = jnp.where(core == 0, att[:, :inner], att[:, inner:])
        gwo_s[...] += mm_at(ah, dhg[ch].reshape(QT, dim))
        dispatch(ch, table("h", chips))
        return carry

    lax.fori_loop(0, chips, hidden, 0)
    dh_g.drain()
    go_load = pltpu.make_async_copy(gog, dhg, ls.at[0])
    go_load.start()

    def partner_block(buf, dst, k):
        return pltpu.make_async_copy(buf, dst, gl.at[k]), remote(buf, dst, gs.at[k], gr.at[k], ring.partner)

    def both_start(pair):
        pair[0].start()
        pair[1].start()

    def both_wait(pair):
        pair[0].wait()
        pair[1].wait()

    wo_out = partner_block(gwo_s, gwo.at[hrow], 3 * nf)
    both_start(wo_out)

    def w_fetch(f, slot):
        cols = pl.ds(pl.multiple_of(core * fh + f * FT, FT), FT)
        return (pltpu.make_async_copy(wg_hbm.at[:, cols], wbuf.at[0], wsem.at[slot, 0]),
                pltpu.make_async_copy(wu_hbm.at[:, cols], wbuf.at[1], wsem.at[slot, 1]),
                pltpu.make_async_copy(wd_hbm.at[cols], dbuf.at[slot], wsem.at[slot, 2]))

    for cp in w_fetch(0, 0):
        cp.start()
    go_load.wait()
    f_table = table("f", 9 * nf)

    def block(f, n):
        if n == 0:
            return partner_block(gst.at[f % 2, pl.ds(0, FT)], gdown.at[pl.ds(pl.multiple_of(core * fh + f * FT, FT), FT)], f)
        return partner_block(gsw.at[f % 2, n - 1], (ggate, gup)[n - 1].at[:, pl.ds(pl.multiple_of(core * fh + f * FT, FT), FT)], n * nf + f)

    def mlp(f, carry):
        slot = f % 2
        for cp in w_fetch(f, slot):
            cp.wait()

        for n in range(2):
            wt[n] = wbuf[n].T

        @pl.when(f + 1 < nf)
        def _():
            for cp in w_fetch(f + 1, 1 - slot):
                cp.start()

        def act_pair(k, cc):
            for ch in (2 * k, 2 * k + 1):
                q = lanes(ch)
                n2t = qz_ref[0:dim, q]
                g = mm(wt[0], n2t)
                u = mm(wt[1], n2t)
                ga = mm_bt(dbuf[slot], dhg[ch].reshape(QT, dim))
                sig = jax.nn.sigmoid(g)
                si = g * sig
                doz[0:FT, q] = (si * u).astype(BF16)
                doz[FT:2 * FT, q] = (ga * u * (sig + si * (1.0 - sig))).astype(BF16)
                doz[2 * FT:3 * FT, q] = (ga * si).astype(BF16)
            dispatch(f * 9 + 2 * k + 1, f_table)
            return cc

        lax.fori_loop(0, chips // 2, act_pair, 0)

        @pl.when(f > 1)
        def _():
            for n in range(3):
                both_wait(block(f - 2, n))
        acc = [None] * 3
        for ch in range(chips):
            q = slice(ch * QT, (ch + 1) * QT)
            n2t = qz_ref[0:dim, q]
            for n, d in enumerate((mm(doz[0:FT, q], dhg[ch].reshape(QT, dim)), mm_bt(n2t, doz[FT:2 * FT, q]), mm_bt(n2t, doz[2 * FT:3 * FT, q]))):
                acc[n] = d if acc[n] is None else acc[n] + d
        gst[slot, 0:FT] = acc[0]
        gsw[slot, 0] = acc[1]
        gsw[slot, 1] = acc[2]
        for n in range(3):
            both_start(block(f, n))
        dispatch(f * 9 + 8, f_table)
        return carry

    lax.fori_loop(0, nf, mlp, 0)
    for p in range(np_):
        remote(dkvp.at[p], dkvp.at[p], xs.at[p], xr.at[p], ring.partner).wait_recv()
    nb = 4
    w = mem // nb
    for f in (nf - 2, nf - 1):
        for n in range(3):
            both_wait(block(f, n))

    def gm(b):
        return pltpu.make_async_copy(gst.at[b % 2, pl.ds(0, w)], gmem.at[pl.ds(pl.multiple_of(b * w, w), w)], gl.at[3 * nf + 2 + b % 2])

    def memory_rows(b, carry):
        @pl.when(b > 1)
        def _():
            gm(b - 2).wait()
        cb = pl.ds(pl.multiple_of(core * mem + b * w, w), w)
        cp = pl.ds(pl.multiple_of(b * w, w), w)
        acc = None
        for p in range(np_):
            own_e = pl.ds(pl.multiple_of(core * inner + p * 128, 128), 128)
            oth_e = pl.ds(pl.multiple_of((1 - core) * inner + p * 128, 128), 128)
            for part, w_ref in ((0, wk_ref), (1, wv_ref)):
                e = slice(part * 128, (part + 1) * 128)
                lhs = jnp.concatenate([dkv[p, e, cb], dkvp[p, e, cp]], axis=0)
                rhs = jnp.concatenate([w_ref[:, own_e], w_ref[:, oth_e]], axis=1)
                d = mm_bt(lhs.T, rhs)
                acc = d if acc is None else acc + d
        gst[b % 2, 0:w] = acc
        gm(b).start()
        dispatch(b, table("m", nb))
        return carry

    lax.fori_loop(0, nb, memory_rows, 0)
    run("m", nb)

    gain = g_ref[0:1, :].astype(F32)
    y_fetch(0, 0).start()
    spb[...] = jnp.zeros_like(spb)
    gwq_s[...] = jnp.zeros_like(gwq_s)
    wq_h = wq_ref[:, hcol]

    def query(ch, carry):
        slot = ch % 2
        y_fetch(ch, slot).wait()

        @pl.when(ch + 1 < chips)
        def _():
            y_fetch(ch + 1, 1 - slot).start()
        x = ybuf[slot].reshape(QT, dim).astype(F32)
        xhat = x * lax.rsqrt(jnp.mean(x * x, axis=-1, keepdims=True) + 1e-6)
        n1 = (xhat * gain).astype(BF16)
        dqc = jnp.concatenate([dqa[p, ch].reshape(128, QT) for p in range(np_)], axis=0)
        dn = mm_bt(dqc.T, wq_h)
        gwq_s[...] += mm(dqc, n1)
        spb[0:1, :] += jnp.sum(dn * xhat, axis=0, keepdims=True)
        dispatch(ch, table("q", chips))
        return carry

    lax.fori_loop(0, chips, query, 0)
    gvec2 = jnp.zeros((16 - 2 * hc, QT), F32)
    for ch in range(chips):
        gvec2 = gvec2 + jnp.concatenate([stb[ch, 0, hc:8, :], stb[ch, 1, hc:8, :]], axis=0)
    for n in range(dim // QT):
        spb[1:2, n * QT:(n + 1) * QT] = gvec2[n:n + 1]
    cv = remote(spb, pvec, xs.at[2 * np_], xr.at[2 * np_], ring.partner)
    cv.start()
    wq_out = partner_block(gwq_s, gwq.at[hrow], 3 * nf + 1)
    both_start(wq_out)
    for p in range(np_):
        own_r = pl.ds(pl.multiple_of(core * inner + p * 128, 128), 128)
        oth_r = pl.ds(pl.multiple_of((1 - core) * inner + p * 128, 128), 128)
        dqo_ref[own_r, :] = dqa[p, z, :, :, qmine].reshape(128, rows)
        xq(p).wait()
        dqo_ref[oth_r, :] = pdq[p].reshape(128, rows)
    x = y_ref[...].astype(F32)
    inv = lax.rsqrt(jnp.mean(x * x, axis=-1, keepdims=True) + 1e-6)
    xhat = x * inv
    t = mm_bt(dqo_ref[...].T, wq_ref[...]) * gain
    gdec_ref[...] = gh_ref[...] + inv * (t - xhat * jnp.mean(t * xhat, axis=-1, keepdims=True))
    run("q", chips)
    wkv_out = []
    for p in range(np_):
        for k, out in enumerate((gwk, gwv)):
            n = 2 * p + k
            src = ara.at[p, pl.ds(k * (chips // 2), chips // 2)]
            wkv_out.append(pltpu.make_async_copy(src, out.at[core, p], ls.at[2 + n]))
            wkv_out.append(remote(src, out.at[core, p], xs.at[2 * np_ + 1 + n], xr.at[2 * np_ + 1 + n], ring.partner))
    for cp in wkv_out:
        cp.start()
    for p in range(np_):
        xp(p).wait_send()
    cv.wait()
    gvec_ref[...] = spb[0:2] + pvec[0:2]
    both_wait(wo_out)
    both_wait(wq_out)
    for cp in wkv_out:
        cp.wait()
    for b in range(nb - 2, nb):
        gm(b).wait()
    for obj in [att_g, st_g] + dq_r + dq_s + ar_r + ar_s:
        obj.drain()


def bwd_call(dims, *args):
    chips, rows, mem, dim, hc, c, ff = dims
    inner = hc * 64
    QT = 2 * rows
    T = 2 * mem
    np_ = hc // 2
    h2 = chips // 2
    seg = 256 // chips // 2
    FT = ff // 8
    v = pl.BlockSpec(memory_space=VMEM)
    hbm = pl.BlockSpec(memory_space=pl.ANY)
    s3 = (2, 2, h2)
    rows_sems = [DMA((1,)), DMA(s3)] * 2 + [DMA((1,)), DMA((2,))]
    two = [DMA((1,)), DMA(s3)]
    S = jax.ShapeDtypeStruct
    gshape = (chips, 2, 2, rows // 2, dim)
    cols = chips * QT
    wsq = VMEM((dim, 2 * inner), BF16)
    return pl.pallas_call(
        functools.partial(bwd_kernel, dims),
        out_shape=(S((2, dim), F32), S((rows, dim), F32), S((mem, dim), F32), S((2, np_, chips // 2, 2, seg, dim), F32), S((2, np_, chips // 2, 2, seg, dim), F32), S((2 * inner, dim), F32), S((2 * inner, dim), F32),
                   S((ff, dim), F32), S((dim, ff), F32), S((dim, ff), F32), S(gshape, BF16)),
        in_specs=[pl.BlockSpec(memory_space=pltpu.SMEM)] + [v] * 7 + [hbm] * 15, out_specs=(v,) * 2 + (hbm,) * 9,
        scratch_shapes=[
            VMEM((2 * inner, rows), BF16), VMEM((T, inner), BF16), VMEM((T, inner), BF16), VMEM((inner, T), BF16), VMEM((hc * 128, cols), BF16), VMEM((2 * inner, dim), BF16), wsq, wsq, wsq, VMEM((T, 128), BF16),
            VMEM(gshape, BF16), VMEM((max(hc * 128, 3 * FT), cols), BF16), VMEM((hc * 16, cols), BF16), VMEM((hc * 16, cols), BF16),
            VMEM((chips, 2, 8, QT), F32), VMEM((inner, T), F32), VMEM((inner, T), F32), VMEM((np_, 256, T), BF16), VMEM((np_, 256, mem), BF16),
            VMEM((np_, chips, 2, 64, QT), F32), VMEM((np_, 2, 2, h2, 64, QT), F32), VMEM((np_, chips, 2, 64, QT), BF16),
            VMEM((np_, chips, 2, seg, dim), F32), VMEM((np_, 2, 2, h2, seg, dim), F32), VMEM((np_, chips, 2, seg, dim), F32),
            VMEM((8, dim), F32), VMEM((np_, 2, 64, rows), BF16), VMEM((8, dim), F32),
            VMEM((2, mem, dim), BF16), VMEM((2, 2, 2, rows // 2, dim), BF16), VMEM((2, 2, 2, rows // 2, dim), BF16),
            VMEM((2, dim, FT), BF16), VMEM((2, FT, dim), BF16), VMEM((2, FT, dim), BF16), VMEM((2, max(FT, mem // 4), dim), F32), VMEM((2, 2, dim, FT), F32),
            VMEM((inner, dim), F32), VMEM((inner, dim), F32)]
        + rows_sems * 2 + two * (1 + 4 * np_) + [DMA((4 * np_ + 1,))] * 2 + [DMA((2 + 2 * np_,)), DMA((14,)), DMA((14,)), DMA((16,)), DMA((2, 3)), DMA((2, 2)), DMA((10,))],
        compiler_params=pltpu.CompilerParams(vmem_limit_bytes=67_043_328, collective_id=1, has_side_effects=True),
        cost_estimate=pl.CostEstimate(flops=10**10, bytes_accessed=30 << 20, transcendentals=0),
        name="attn_bwd")(*args)


def fwd_kernel(dims, len_ref, y_ref, go_ref, m_ref, g_ref, wq_hbm, wk_hbm, wv_hbm, wo_hbm, wg_hbm, wu_hbm, wd_hbm,
               own, att_ref, dh_ref, gh_ref, gn_ref, k_out, v_out, kt_out, qz_out, mg_out, yall, gog,
               k_s, v_s, kt_s, qz, mg, wq_ref, wk_ref, wv_ref, ak_ref, yg, wqt, vt_s, s_scr, mx_scr, part, rbuf, patt, satt, gob, attt, wo_s, wg_s, wu_s, wd_s, n2_s, dn_s, *sems):
    chips, rows, mem, dim, hc, c, ff = dims
    QT = 2 * rows
    T = 2 * mem
    MC = min(256, mem)
    hh = hc // 2
    inner = hc * 64
    HR = hh * 64
    ring = Ring(chips)
    z, core, far = ring.z, ring.core, ring.far
    sub = rows // 2
    part_ = functools.partial
    xs, xr, ls = sems[14:]
    rsrc = lambda ref: (lambda half: ref.at[pl.ds(half * sub, sub)])
    y_g = Rows(ring, yg, rsrc(y_ref), sems[:6])
    go_g = Rows(ring, gog, rsrc(gob), sems[6:12])

    def merge(dst, src):
        for hl in range(hh):
            mr = slice(HR + hl, HR + hl + 1)
            lr = slice(HR + 8 + hl, HR + 9 + hl)
            m1, m2 = dst[mr, :], src[mr, :]
            m = jnp.maximum(m1, m2)
            a = jnp.exp2((m1 - m) * c)
            b = jnp.exp2((m2 - m) * c)
            rr = slice(hl * 64, (hl + 1) * 64)
            dst[rr, :] = dst[rr, :] * a + src[rr, :] * b
            dst[mr, :] = m
            dst[lr, :] = dst[lr, :] * a + src[lr, :] * b

    o_r = Reduce(ring, part, rbuf, merge, sems[12:14])
    loads = [pltpu.make_async_copy(src, dst, ls.at[7 + n]) for n, (src, dst) in enumerate((
        (wk_hbm, wk_ref), (wv_hbm, wv_ref), (wq_hbm, wq_ref), (wo_hbm, wo_s), (wg_hbm, wg_s), (wu_hbm, wu_s), (wd_hbm, wd_s)))]
    stores = [pltpu.make_async_copy(src, dst, ls.at[n]) for n, (src, dst) in enumerate(((k_s, k_out), (v_s, v_out), (kt_s, kt_out), (mg, mg_out), (qz, qz_out)))]
    for cp in loads[:3]:
        cp.start()
    ring.enter()
    y_g.start()
    mx_copy = remote(m_ref, mg, xs.at[0], xr.at[0], ring.partner)
    mx_copy.start()
    for cp in loads[3:]:
        cp.start()
    gob[...] = go_ref[...].astype(BF16)
    for half in range(2):
        yg[z, core, half] = y_ref[half * sub:(half + 1) * sub, :]
    hcol = pl.ds(pl.multiple_of(core * inner, 128), inner)
    qz[...] = jnp.zeros_like(qz)
    mask_lanes(ak_ref, len_ref, z * T)
    for cp in loads[:3]:
        cp.wait()
    wqt[...] = wq_ref[:, hcol].T
    wk = wk_ref[:, hcol]
    wv = wv_ref[:, hcol]

    moves = {"y": y_g, "go": go_g, "o": o_r}

    def acts(*point):
        return [go_g.start if e[1] == "start" else part_(moves[e[0]].move, *e[1:]) for e in FWD_PLAN.get(point, [])]

    def run(*point):
        for fn in acts(*point):
            fn()

    def project(src, base, blocks):
        for j in blocks:
            r = pl.ds(pl.multiple_of(base + j * MC, MC), MC)
            blk = src[j * MC:(j + 1) * MC, :]
            kb = mm(blk, wk).astype(BF16)
            vb = mm(blk, wv).astype(BF16)
            k_s[r, :] = kb
            v_s[r, :] = vb
            kt_s[:, r] = kb.T
            vt_s[:, r] = vb.T

    nb = mem // MC
    project(m_ref, core * mem, range(nb))
    run("s", 0)
    mx_copy.wait_recv()
    project(mg, (1 - core) * mem, range(nb // 2))
    run("s", 1)
    project(mg, (1 - core) * mem, range(nb // 2, nb))
    run("s", 2)
    for cp in stores[:4]:
        cp.start()
    gain = g_ref[0:1, :].astype(F32)
    one_row = jnp.where(lax.broadcasted_iota(jnp.int32, (16, QT), 0) == 0, 1.0, 0.0).astype(BF16)

    def lanes(chip):
        return pl.ds(pl.multiple_of(chip * QT, QT), QT)

    def prep(chip):
        n1 = rms_norm(yg[chip].reshape(QT, dim).astype(F32), gain).astype(BF16)
        qt = mm_bt(wqt[...], n1).astype(BF16)
        for h in range(hc):
            lo = h * 128 + (h % 2) * 64
            qz[lo:lo + 64, lanes(chip)] = qt[h * 64:(h + 1) * 64]

    def step(new, slot, old, pslot):
        if new is not None:
            chip, h = new
            rhs = jnp.concatenate([qz[pl.ds(pl.multiple_of(h * 128, 128), 128), lanes(chip)], one_row], axis=0)
            pair = pl.ds(pl.multiple_of((h // 2) * 128, 128), 128)
            mx = None
        if old is not None:
            ochip, half, hl = old
            m = jnp.max(mx_scr[pslot], axis=0, keepdims=True)
            vrow = pl.ds(pl.multiple_of((half * hh + hl) * 64, 64), 64)
            ls_ = None
            acc = None
        for j in range(T // MC):
            r = slice(j * MC, (j + 1) * MC)
            if new is not None:
                s = mm(jnp.concatenate([k_s[r, pair], ak_ref[r, 0:16]], axis=1), rhs)
                s_scr[slot, r, :] = s
                t = jnp.max(s.reshape(MC // 8, 8, QT), axis=0)
                mx = t if mx is None else jnp.maximum(mx, t)
            if old is not None:
                pr = jnp.exp2((s_scr[pslot, r, :] - m) * c)
                t = jnp.sum(pr.reshape(MC // 8, 8, QT), axis=0)
                ls_ = t if ls_ is None else ls_ + t
                dd = mm(vt_s[vrow, r], pr.astype(BF16))
                acc = dd if acc is None else acc + dd
        if new is not None:
            mx_scr[slot] = mx
        if old is not None:
            part[ochip, half, hl * 64:(hl + 1) * 64, :] = acc
            part[ochip, half, HR + hl:HR + hl + 1, :] = m
            part[ochip, half, HR + 8 + hl:HR + 9 + hl, :] = jnp.sum(ls_, axis=0, keepdims=True)

    offs = [o for o, _ in FWD_ORDER]
    halves = [h for _, h in FWD_ORDER]
    n = len(offs)
    fresh = [int(k + 1 < n and offs[k + 1] not in offs[:k + 1]) for k in range(n)]
    run("s", 3)
    y_g.ready(0)
    prep(z)
    step((z, halves[0] * hh), 0, None, None)

    def body(pair, carry):
        for u in range(2):
            i = 2 * pair + u
            i2 = jnp.minimum(i + 1, n - 1)
            chip, half = ring.chip(pick(i, offs)), pick(i, halves)
            chip2, half2 = ring.chip(pick(i2, offs)), pick(i2, halves)
            for k in range(hh):
                slot = (u * hh + k) % 2
                if k == hh - 1:
                    dispatch(pair, {kk // 2: acts("r", kk) + [part_(y_g.ready, offs[kk + 1])] for kk in range(u, n, 2) if fresh[kk]})
                    if any(fresh[u::2]):
                        pl.when(pick(i, fresh) == 1)(part_(prep, chip2))
                    new = (chip2, half2 * hh)
                else:
                    new = (chip, half * hh + k + 1)
                step(new, 1 - slot, (chip, half, k), slot)
                dispatch(pair, {kk // 2: acts("b", kk * hh + k) for kk in range(u, n, 2) if acts("b", kk * hh + k)})
        return carry

    gl = [pltpu.make_async_copy(gob.at[pl.ds(half * sub, sub)], gog.at[z, core, half], ls.at[5 + half]) for half in range(2)]
    for cp in gl:
        cp.start()
    lax.fori_loop(0, n // 2, body, 0)
    yc = pltpu.make_async_copy(yg, yall, ls.at[14])
    yc.start()
    stores[4].start()
    run("t", 0)
    run("t", 1)
    qmine = pl.ds(pl.multiple_of(core * rows, rows), rows)
    qother = pl.ds(pl.multiple_of((1 - core) * rows, rows), rows)
    for h in range(hc):
        half, hl = h // hh, h % hh
        m = part[z, half, HR + hl:HR + hl + 1, :]
        l = part[z, half, HR + 8 + hl:HR + 9 + hl, :]
        own[h * 64:(h + 1) * 64, :] = part[z, half, hl * 64:(hl + 1) * 64, :] / l
        own[inner + h:inner + h + 1, :] = m + jnp.log2(l) / c
    satt[...] = own[:inner, qother].astype(BF16)
    xo = remote(satt, patt, xs.at[1], xr.at[1], ring.partner)
    xo.start()
    attt[pl.ds(pl.multiple_of(core * inner, inner), inner), :] = own[:inner, qmine].astype(BF16)
    for cp in loads[3:]:
        cp.wait()
    run("t", 2)
    xo.wait()
    attt[pl.ds(pl.multiple_of((1 - core) * inner, inner), inner), :] = patt[...]

    att = attt[...].T
    att_ref[...] = att
    gain2 = g_ref[1:2, :].astype(F32)
    run("t", 3)
    hid = (y_ref[...].astype(F32) + mm(att, wo_s[...])).astype(BF16).astype(F32)
    inv = lax.rsqrt(jnp.mean(hid * hid, axis=-1, keepdims=True) + 1e-6)
    hhat = hid * inv
    n2 = (hhat * gain2).astype(BF16)
    fb = ff // 4
    n2_s[...] = n2
    dn_s[...] = jnp.zeros_like(dn_s)

    def mlp(f, carry):
        cols = pl.ds(pl.multiple_of(f * fb, fb), fb)
        wg, wu = wg_s[:, cols], wu_s[:, cols]
        g = mm(n2_s[...], wg)
        u = mm(n2_s[...], wu)
        ga = mm_bt(gob[...], wd_s[cols, :])
        sig = jax.nn.sigmoid(g)
        si = g * sig
        dn_s[...] += mm_bt((ga * u * (sig + si * (1.0 - sig))).astype(BF16), wg) + mm_bt((ga * si).astype(BF16), wu)
        dispatch(f, {n: acts("t", 4 + n) for n in range(4) if acts("t", 4 + n)})
        return carry

    lax.fori_loop(0, 4, mlp, 0)
    dn = dn_s[...]
    gsum = jnp.sum(dn * hhat, axis=0, keepdims=True)
    gn_ref[...] = jnp.zeros_like(gn_ref)
    for k in range(dim // QT):
        gn_ref[k:k + 1, :] = gsum[:, k * QT:(k + 1) * QT]
    t = dn * gain2
    gh = go_ref[...] + inv * (t - hhat * jnp.mean(t * hhat, axis=-1, keepdims=True))
    gh_ref[...] = gh
    dh_ref[...] = gh.astype(BF16)
    run("t", 8)
    for off in range(-far + 1, far + 1):
        go_g.ready(off)
    mx_copy.wait_send()
    for cp in [yc] + gl + stores:
        cp.wait()
    for obj in (y_g, go_g, o_r):
        obj.drain()


def fwd_call(dims, *args):
    chips, rows, mem, dim, hc, c, ff = dims
    hh = hc // 2
    inner = hc * 64
    QT = 2 * rows
    T = 2 * mem
    HR = hh * 64
    h2 = chips // 2
    v = pl.BlockSpec(memory_space=VMEM)
    hbm = pl.BlockSpec(memory_space=pl.ANY)
    S = jax.ShapeDtypeStruct
    s3 = (2, 2, h2)
    gshape = (chips, 2, 2, rows // 2, dim)
    rows_sems = [DMA((1,)), DMA(s3)] * 2 + [DMA((1,)), DMA((2,))]
    return pl.pallas_call(
        functools.partial(fwd_kernel, dims),
        out_shape=(S((inner + 8, QT), F32), S((rows, 2 * inner), BF16), S((rows, dim), BF16), S((rows, dim), F32), S((8, QT), F32),
                   S((T, inner), BF16), S((T, inner), BF16), S((inner, T), BF16), S((hc * 128, chips * QT), BF16), S((mem, dim), BF16), S(gshape, BF16), S(gshape, BF16)),
        in_specs=[pl.BlockSpec(memory_space=pltpu.SMEM)] + [v] * 4 + [hbm] * 7, out_specs=(v,) * 5 + (hbm,) * 7,
        scratch_shapes=[
            VMEM((T, inner), BF16), VMEM((T, inner), BF16), VMEM((inner, T), BF16), VMEM((hc * 128, chips * QT), BF16), VMEM((mem, dim), BF16),
            VMEM((dim, 2 * inner), BF16), VMEM((dim, 2 * inner), BF16), VMEM((dim, 2 * inner), BF16), VMEM((T, 128), BF16),
            VMEM(gshape, BF16), VMEM((inner, dim), BF16), VMEM((inner, T), BF16), VMEM((2, T, QT), F32), VMEM((2, 8, QT), F32),
            VMEM((chips, 2, HR + 16, QT), F32), VMEM((2, 2, h2, HR + 16, QT), F32), VMEM((inner, rows), BF16), VMEM((inner, rows), BF16),
            VMEM((rows, dim), BF16), VMEM((2 * inner, rows), BF16), VMEM((2 * inner, dim), BF16), VMEM((dim, ff), BF16), VMEM((dim, ff), BF16), VMEM((ff, dim), BF16), VMEM((rows, dim), BF16), VMEM((rows, dim), F32)]
        + rows_sems * 2 + [DMA((1,)), DMA(s3)] + [DMA((2,))] * 2 + [DMA((15,))],
        compiler_params=pltpu.CompilerParams(vmem_limit_bytes=62 * 1024 * 1024, collective_id=0, has_side_effects=True),
        cost_estimate=pl.CostEstimate(flops=10**10, bytes_accessed=30 << 20, transcendentals=0),
        name="attn_fwd")(*args)


def solution(mesh):
    group = mesh.shape['seq']
    row_spec = P(('data', 'seq'), None)
    part_vec = P('data')
    part_mat = P('data', None)
    part_cube = P('data', None, None)

    def device_step(dec_in, memory, mem_len, grad_out, norm_attn, wq, wk, wv, wo, norm_mlp, w_gate, w_up, w_down):
        rows, dim = dec_in.shape
        mem = memory.shape[0]
        heads, hd = wq.shape[1], wq.shape[2]
        inner = heads * hd
        chips = group // 2
        hc = heads // 2
        c = LOG2E * hd ** -0.5
        dims = (chips, rows, mem, dim, hc, c, w_gate.shape[1])
        wq2, wk2, wv2 = (w.reshape(dim, inner) for w in (wq, wk, wv))
        wo2 = wo.reshape(inner, dim)
        gains = jnp.stack([norm_attn, norm_mlp])

        own, attended, dh, grad_hidden, gn, k_c, v_c, kt_c, qz, mem_p, y_all, go_all = fwd_call(
            dims, mem_len, dec_in, grad_out, memory, gains, wq2, wk2, wv2, wo2, w_gate, w_up, w_down)
        gvec, g_dec, g_mem, g_wk, g_wv, g_wq, g_wo, g_down, g_gate, g_up, _ = bwd_call(
            dims, mem_len, dh, own, gn, attended, dec_in, grad_hidden, gains,
            k_c, v_c, kt_c, qz, wo2, wq2, wk2, wv2, memory, mem_p, y_all, go_all, w_gate, w_up, w_down)
        cube = (dim, heads, hd)
        g_wq, g_wk, g_wv = (g.reshape(inner, dim).T.reshape(cube) for g in (g_wq, g_wk, g_wv))
        return (g_dec, g_mem, gvec[0], g_wq, g_wk, g_wv, g_wo.reshape(heads, hd, dim), gvec[1], g_gate, g_up, g_down)

    return jax.shard_map(device_step, mesh=mesh,
                         in_specs=(row_spec, row_spec, part_vec, row_spec) + (P(),) * 9,
                         out_specs=(row_spec, row_spec, part_vec, part_cube, part_cube, part_cube, part_cube, part_vec, part_mat, part_mat, part_mat),
                         check_vma=False)
```

```python
import functools
import math

import jax
import jax.numpy as jnp
from jax import lax
from jax.experimental import pallas as pl
from jax.experimental.pallas import tpu as pltpu
from jax.sharding import PartitionSpec as P

F32 = jnp.float32
BF16 = jnp.bfloat16
LOG2E = math.log2(math.e)
VMEM = pltpu.VMEM
MESH = pl.DeviceIdType.MESH


def mm(a, b):
    return jnp.dot(a, b, preferred_element_type=F32)


def mm_bt(a, b):
    return lax.dot_general(a, b, (((1,), (1,)), ((), ())), preferred_element_type=F32)


def mm_at(a, b):
    return lax.dot_general(a, b, (((0,), (0,)), ((), ())), preferred_element_type=F32)


def rms_norm(tensor, gain):
    mean_sq = jnp.mean(tensor * tensor, axis=-1, keepdims=True)
    return tensor * lax.rsqrt(mean_sq + 1e-6) * gain


RIGHT, LEFT = 0, 1
DMA = pltpu.SemaphoreType.DMA

FWD_ORDER = [(0, 0), (0, 1), (1, 0), (1, 1), (-3, 0), (3, 1), (4, 0), (4, 1), (3, 0), (-3, 1), (2, 0), (-2, 1), (2, 1), (-2, 0), (-1, 1), (-1, 0)]
BWD_ORDER = [0, 1, 4, 3, -3, 2, -2, -1]
BWD_FIRST = 2
FWD_PLAN = {
    ("b", 0): [("y", 0, 1, 1), ("y", 1, 0, 1)],
    ("b", 11): [("y", 1, 1, 3), ("y", 1, 0, 3)],
    ("b", 12): [("go", 0, 0, 1)],
    ("b", 13): [("go", 1, 1, 1)],
    ("b", 14): [("o", 1, 0, 3)],
    ("b", 15): [("go", 0, 1, 1)],
    ("b", 17): [("o", 0, 1, 3)],
    ("b", 18): [("go", 1, 0, 1)],
    ("b", 20): [("o", 0, 0, 4)],
    ("b", 21): [("go", 1, 1, 2)],
    ("b", 23): [("o", 1, 1, 4)],
    ("b", 31): [("go", 0, 0, 2)],
    ("b", 32): [("go", 1, 0, 2)],
    ("b", 34): [("go", 0, 1, 2)],
    ("b", 35): [("go", 1, 1, 3)],
    ("b", 36): [("o", 0, 0, 3)],
    ("b", 37): [("o", 1, 1, 3)],
    ("b", 38): [("o", 0, 1, 2)],
    ("b", 4): [("y", 0, 0, 2), ("y", 1, 1, 2)],
    ("b", 40): [("go", 1, 0, 3)],
    ("b", 41): [("o", 1, 0, 2)],
    ("b", 42): [("go", 0, 1, 3)],
    ("b", 43): [("go", 1, 1, 4)],
    ("b", 8): [("y", 0, 1, 2), ("y", 1, 0, 2)],
    ("b", 9): [("go", "start")],
    ("r", 3): [("y", 0, 0, 3), ("y", 0, 1, 3)],
    ("r", 5): [("y", 0, 0, 4), ("y", 1, 1, 4)],
    ("s", 1): [("y", 0, 0, 1), ("y", 1, 1, 1)],
    ("t", 1): [("o", 0, 0, 2), ("o", 1, 1, 2), ("o", 0, 1, 1), ("o", 1, 0, 1), ("o", 0, 0, 1), ("o", 1, 1, 1), ("o", 0, 1, 0), ("o", 1, 0, 0), ("o", 0, 0, 0), ("o", 1, 1, 0)],
    ("t", 2): [("go", 0, 0, 3)],
    ("t", 6): [("go", 0, 0, 4)],
}
BWD_PLAN = {
    ("b", 1): [("dh", 0, 0, 1), ("dh", 1, 1, 1)],
    ("b", 10): [("dh", 0, 1, 3), ("dh", 1, 0, 3), ("st", 0, 0, 3), ("st", 1, 1, 3)],
    ("b", 11): [("st", 0, 1, 3), ("st", 1, 0, 3)],
    ("b", 12): [("dq0", 0, 0, 4)],
    ("b", 13): [("dq0", 1, 1, 4)],
    ("b", 14): [("att", 0, 0, 1), ("att", 1, 1, 1)],
    ("b", 15): [("dq0", 0, 1, 3), ("att", 0, 1, 1), ("att", 1, 0, 1)],
    ("b", 16): [("dq0", 0, 0, 3), ("dq0", 1, 0, 3)],
    ("b", 17): [("dq0", 1, 1, 3)],
    ("b", 18): [("att", 0, 0, 2), ("att", 1, 1, 2)],
    ("b", 19): [("dq0", 0, 1, 2), ("att", 1, 0, 2)],
    ("b", 2): [("dh", 0, 1, 1), ("dh", 1, 0, 1), ("st", 0, 0, 1), ("st", 1, 1, 1), ("st", 0, 1, 1), ("st", 1, 0, 1)],
    ("b", 20): [("dq0", 1, 0, 2), ("att", 0, 1, 2)],
    ("b", 21): [("dq0", 0, 0, 2), ("dq0", 1, 1, 2)],
    ("b", 22): [("att", 0, 0, 3), ("att", 1, 1, 3)],
    ("b", 23): [("dq0", 0, 1, 1), ("att", 1, 0, 3), ("ar0", 0, 1, 3), ("ar0", 1, 0, 3), ("ar0", 0, 0, 4), ("ar0", 1, 1, 4)],
    ("b", 24): [("dq1", 0, 0, 4), ("dq0", 1, 0, 1), ("att", 0, 1, 3)],
    ("b", 25): [("dq1", 1, 1, 4), ("dq0", 0, 0, 1), ("dq0", 1, 1, 1)],
    ("b", 26): [("att", 0, 0, 4), ("att", 1, 1, 4)],
    ("b", 27): [("dq1", 0, 1, 3), ("dq0", 0, 1, 0), ("ar0", 1, 0, 2)],
    ("b", 28): [("dq1", 1, 0, 3), ("ar0", 1, 1, 3), ("ar0", 0, 1, 2)],
    ("b", 29): [("dq0", 1, 0, 0), ("ar0", 0, 0, 3)],
    ("b", 30): [("dq1", 0, 0, 3), ("dq1", 1, 1, 3)],
    ("b", 31): [("dq0", 0, 0, 0), ("dq0", 1, 1, 0), ("ds0", "start"), ("ar0", 1, 0, 1)],
    ("b", 32): [("dq1", 0, 1, 2), ("dq1", 1, 0, 2), ("ar0", 0, 1, 1)],
    ("b", 33): [("ar0", 0, 0, 2), ("ar0", 1, 1, 2)],
    ("b", 34): [("dq1", 0, 0, 2), ("dq1", 1, 1, 2)],
    ("b", 35): [("dq1", 0, 1, 1), ("ds0", 0, 0, 1), ("ds0", 1, 1, 1), ("ds0", 0, 1, 1), ("ds0", 1, 0, 1), ("ar1", 0, 1, 3), ("ar1", 1, 0, 3), ("ar1", 0, 0, 4), ("ar1", 1, 1, 4), ("ar0", 1, 0, 0)],
    ("b", 36): [("dq2", 0, 0, 4), ("dq1", 1, 0, 1), ("ar0", 0, 1, 0), ("ar0", 0, 0, 1), ("ar0", 1, 1, 1)],
    ("b", 37): [("dq2", 1, 1, 4), ("dq1", 0, 0, 1), ("dq1", 1, 1, 1)],
    ("b", 38): [("dq1", 0, 1, 0), ("ds0", 1, 1, 2), ("ds0", 1, 0, 2)],
    ("b", 39): [("dq2", 0, 1, 3), ("ds0", 0, 0, 2), ("ds0", 0, 1, 2), ("ar1", 1, 0, 2)],
    ("b", 40): [("dq2", 1, 0, 3), ("ar1", 1, 1, 3), ("ar1", 0, 1, 2)],
    ("b", 41): [("dq1", 1, 0, 0), ("ar1", 0, 0, 3)],
    ("b", 42): [("dq2", 0, 0, 3), ("ar0", 1, 1, 0)],
    ("b", 43): [("dq2", 1, 1, 3), ("ar0", 0, 0, 0), ("as0", "start")],
    ("b", 44): [("dq1", 0, 0, 0), ("dq1", 1, 1, 0), ("ds1", "start"), ("ds0", 1, 1, 3)],
    ("b", 45): [("dq2", 0, 1, 2), ("ds0", 1, 0, 3), ("ds0", 0, 0, 3), ("ar1", 1, 0, 1), ("ds0", 0, 1, 3)],
    ("b", 46): [("dq2", 1, 0, 2), ("ar1", 0, 1, 1)],
    ("b", 47): [("dq2", 0, 0, 2), ("dq2", 1, 1, 2), ("ar2", 0, 1, 3), ("ar2", 1, 0, 3), ("ar2", 0, 0, 4), ("ar2", 1, 1, 4), ("ar1", 0, 0, 2), ("ar1", 1, 1, 2)],
    ("b", 5): [("dh", 0, 0, 2), ("dh", 1, 1, 2)],
    ("b", 6): [("dh", 0, 1, 2), ("dh", 1, 0, 2), ("st", 0, 0, 2), ("st", 1, 1, 2)],
    ("b", 7): [("st", 0, 1, 2), ("st", 1, 0, 2)],
    ("b", 9): [("dh", 0, 0, 3), ("dh", 1, 1, 3)],
    ("f", 1): [("ar2", 0, 1, 2), ("ar2", 1, 0, 2), ("ar2", 0, 0, 3), ("ar2", 1, 1, 3)],
    ("f", 10): [("dq2", 0, 0, 0), ("dq2", 1, 1, 0), ("ds2", "start")],
    ("f", 12): [("ar2", 0, 1, 1), ("ar2", 1, 0, 1)],
    ("f", 14): [("ar2", 0, 0, 2), ("ar2", 1, 1, 2)],
    ("f", 17): [("ds1", 0, 0, 3), ("ds1", 1, 1, 3), ("ar1", 0, 0, 0), ("ar1", 1, 1, 0), ("as1", "start"), ("as0", 0, 0, 3), ("as0", 1, 1, 3), ("as0", 0, 1, 3), ("as0", 1, 0, 3)],
    ("f", 19): [("ds1", 0, 1, 3), ("ds1", 1, 0, 3), ("ds2", 0, 0, 1), ("ds2", 1, 1, 1)],
    ("f", 21): [("ds2", 0, 1, 1), ("ds2", 1, 0, 1)],
    ("f", 23): [("ar2", 0, 1, 0), ("ar2", 1, 0, 0)],
    ("f", 25): [("ar2", 0, 0, 1), ("ar2", 1, 1, 1)],
    ("f", 26): [("ds1", 0, 0, 4), ("ds1", 1, 1, 4), ("as1", 0, 0, 1), ("as1", 1, 1, 1), ("as1", 0, 1, 1), ("as1", 1, 0, 1)],
    ("f", 28): [("as0", 0, 0, 4), ("as0", 1, 1, 4)],
    ("f", 3): [("ar1", 0, 0, 1), ("ar1", 1, 1, 1)],
    ("f", 30): [("ds2", 0, 0, 2), ("ds2", 1, 1, 2)],
    ("f", 32): [("ds2", 0, 1, 2), ("ds2", 1, 0, 2)],
    ("f", 34): [("ar2", 0, 0, 0), ("ar2", 1, 1, 0), ("as2", "start")],
    ("f", 35): [("ds2", 0, 0, 3), ("ds2", 1, 1, 3), ("ds2", 0, 1, 3), ("ds2", 1, 0, 3), ("as1", 0, 0, 2), ("as1", 1, 1, 2), ("as1", 0, 1, 2), ("as1", 1, 0, 2)],
    ("f", 5): [("as0", 0, 0, 2), ("as0", 1, 1, 2)],
    ("f", 7): [("as0", 0, 1, 2), ("as0", 1, 0, 2)],
    ("f", 8): [("dq2", 0, 1, 0), ("dq2", 1, 0, 0), ("ds1", 0, 0, 2), ("ds1", 1, 1, 2), ("ds1", 0, 1, 2), ("ds1", 1, 0, 2)],
    ("h", 0): [("as0", 0, 0, 1), ("as0", 1, 1, 1)],
    ("h", 1): [("as0", 0, 1, 1), ("as0", 1, 0, 1)],
    ("h", 2): [("ds1", 0, 0, 1), ("ds1", 1, 1, 1), ("ds1", 0, 1, 1), ("ds1", 1, 0, 1)],
    ("h", 3): [("ds0", 1, 1, 4)],
    ("h", 4): [("dq2", 0, 1, 1), ("ar1", 1, 0, 0), ("ds0", 0, 0, 4)],
    ("h", 6): [("dq2", 1, 0, 1), ("ar1", 0, 1, 0)],
    ("h", 7): [("dq2", 0, 0, 1), ("dq2", 1, 1, 1)],
    ("m", 0): [("as2", 0, 0, 1), ("as2", 1, 1, 1)],
    ("m", 1): [("as2", 0, 1, 1), ("as2", 1, 0, 1)],
    ("m", 3): [("ds2", 0, 0, 4), ("ds2", 1, 1, 4)],
    ("q", 0): [("as1", 0, 0, 3), ("as1", 1, 1, 3)],
    ("q", 2): [("as1", 0, 1, 3), ("as1", 1, 0, 3)],
    ("q", 3): [("as2", 0, 0, 2), ("as2", 1, 1, 2)],
    ("q", 5): [("as2", 0, 1, 2), ("as2", 1, 0, 2)],
    ("q", 7): [("as1", 0, 0, 4), ("as1", 1, 1, 4)],
    ("q", 8): [("as2", 0, 0, 3), ("as2", 1, 1, 3), ("as2", 0, 1, 3), ("as2", 1, 0, 3), ("as2", 0, 0, 4), ("as2", 1, 1, 4)],
    ("r", 12): [("dh", 0, 0, 4), ("dh", 1, 1, 4), ("att", "start"), ("st", 0, 0, 4), ("st", 1, 1, 4)],
}


class Ring:
    def __init__(self, chips):
        me = lax.axis_index('seq')
        self.chips = chips
        self.far = chips // 2
        self.z = me // 2
        self.core = me - 2 * self.z
        self.partner = 2 * self.z + 1 - self.core
        self.next = (2 * self.chip(1) + self.core, 2 * self.chip(-1) + self.core)
        self.hops = {(RIGHT, 0): self.far, (LEFT, 1): self.far, (RIGHT, 1): self.far - 1, (LEFT, 0): self.far - 1}

    def chip(self, off):
        return lax.rem(self.z + off + self.chips, self.chips)

    def ahead(self, d, k):
        return self.chip(k if d == RIGHT else -k)

    def enter(self):
        barrier = pltpu.get_barrier_semaphore()
        for dev in (self.partner,) + self.next:
            pl.semaphore_signal(barrier, inc=1, device_id={'seq': dev}, device_id_type=MESH)
        pl.semaphore_wait(barrier, 3)


def remote(src, dst, ssem, rsem, dev):
    return pltpu.make_async_remote_copy(src_ref=src, dst_ref=dst, send_sem=ssem, recv_sem=rsem, device_id={'seq': dev}, device_id_type=MESH)


def sent(every, ssem, rsem, dev):
    remote(every, every, ssem, rsem, dev).wait_send()


class Share:
    def __init__(self, ring, buf, src, sems):
        self.ring, self.buf, self.src = ring, buf, src
        self.ss, self.rs = sems

    def slot(self, chip, half):
        return self.buf.at[chip, half]

    def send(self, d, half, t):
        slot = self.slot(self.ring.ahead(d, 1 - t), half)
        src = self.src(half) if t == 1 else slot
        return remote(src, slot, self.ss.at[0], self.rs.at[d, half, t - 1], self.ring.next[d])

    def recv(self, d, half, t):
        slot = self.slot(self.ring.ahead(d, -t), half)
        return remote(slot, slot, self.ss.at[0], self.rs.at[d, half, t - 1], self.ring.next[d])

    def start(self):
        for d, half in self.ring.hops:
            self.send(d, half, 1).start()

    def came(self, d, half, t):
        pass

    def move(self, d, half, t):
        self.recv(d, half, t).wait_recv()
        if t < self.ring.hops[d, half]:
            self.send(d, half, t + 1).start()
        self.came(d, half, t)

    def drain(self):
        sent(self.buf.at[pl.ds(0, self.ring.chips - 1)], self.ss.at[0], self.rs.at[0, 0, 0], self.ring.next[0])


class Rows(Share):
    def __init__(self, ring, buf, src, sems):
        super().__init__(ring, buf, src, sems[:2])
        self.fs, self.fr, self.os, self.orr = sems[2:]

    def slot(self, chip, half):
        return self.buf.at[chip, self.ring.core, half]

    def pslot(self, chip, half):
        return self.buf.at[chip, 1 - self.ring.core, half]

    def start(self):
        super().start()
        for half in range(2):
            self.own(half).start()

    def own(self, half):
        return remote(self.src(half), self.slot(self.ring.z, half), self.os.at[0], self.orr.at[half], self.ring.partner)

    def forward(self, d, half, t):
        slot = self.slot(self.ring.ahead(d, -t), half)
        return remote(slot, slot, self.fs.at[0], self.fr.at[d, half, t - 1], self.ring.partner)

    def came(self, d, half, t):
        self.forward(d, half, t).start()

    def ready(self, off):
        ring = self.ring
        if off == 0:
            for half in range(2):
                slot = self.pslot(ring.z, half)
                remote(slot, slot, self.os.at[0], self.orr.at[half], ring.partner).wait_recv()
            return
        for (d, half), n in ring.hops.items():
            t = ring.far if abs(off) == ring.far else (-off if d == RIGHT else off)
            if 1 <= t <= n:
                slot = self.pslot(ring.ahead(d, -t), half)
                remote(slot, slot, self.fs.at[0], self.fr.at[d, half, t - 1], ring.partner).wait_recv()

    def drain(self):
        every = self.buf.at[pl.ds(0, self.ring.chips - 1), 0]
        sent(every, self.ss.at[0], self.rs.at[0, 0, 0], self.ring.next[0])
        sent(every, self.fs.at[0], self.fr.at[0, 0, 0], self.ring.partner)
        sent(self.buf.at[0, 0], self.os.at[0], self.orr.at[0], self.ring.partner)


class Reduce:
    def __init__(self, ring, part, rbuf, merge, sems):
        self.ring, self.part, self.rbuf, self.merge = ring, part, rbuf, merge
        self.ss, self.rs = sems

    def send(self, d, half, o):
        return remote(self.part.at[self.ring.ahead(d, o), half], self.rbuf.at[d, half, o - 1], self.ss.at[0], self.rs.at[d, half, o - 1], self.ring.next[d])

    def recv(self, d, half, o):
        slot = self.rbuf.at[d, half, o]
        return remote(slot, slot, self.ss.at[0], self.rs.at[d, half, o], self.ring.next[d])

    def move(self, d, half, o):
        if o < self.ring.hops[d, half]:
            self.recv(d, half, o).wait_recv()
            self.merge(self.part.at[self.ring.ahead(d, o), half], self.rbuf.at[d, half, o])
        if o > 0:
            self.send(d, half, o).start()

    def drain(self):
        sent(self.part.at[pl.ds(0, self.ring.chips - 1)], self.ss.at[0], self.rs.at[0, 0, 0], self.ring.next[0])


def pick(i, values):
    out = jnp.int32(values[-1])
    for k, v in enumerate(values[:-1]):
        out = jnp.where(i == k, jnp.int32(v), out)
    return out


def mask_lanes(ref, len_ref, start):
    row = lax.broadcasted_iota(jnp.int32, ref.shape, 0) + start
    lane = lax.broadcasted_iota(jnp.int32, ref.shape, 1)
    bias = jnp.where(row < len_ref[0], 0.0, -1e30)
    ref[...] = jnp.where(lane == 0, bias, jnp.where(lane < 4, 1.0, 0.0)).astype(BF16)


def dispatch(index, table):
    def branch(keys):
        if len(keys) == 1:
            def run():
                for fn in table[keys[0]]:
                    fn()
            pl.when(index == keys[0])(run)
            return
        low, high = keys[:len(keys) // 2], keys[len(keys) // 2:]
        pl.when(index < high[0])(functools.partial(branch, low))
        pl.when(index >= high[0])(functools.partial(branch, high))
    if table:
        branch(sorted(table))


def add_into(dst, src):
    dst[...] = dst[...] + src[...]


def parts3(x):
    hi = x.astype(BF16)
    rest = x - hi.astype(F32)
    mid = rest.astype(BF16)
    lo = (rest - mid.astype(F32)).astype(BF16)
    return hi, mid, lo


def bwd_kernel(dims, len_ref, dh_ref, own_ref, gn_ref, att_ref, y_ref, gh_ref, g1_ref, g2_ref,
               k_hbm, v_hbm, kt_hbm, qz_hbm, wo_hbm, wq_hbm, wk_hbm, wv_hbm, ma_hbm, mb_hbm, y_hbm, gog, wg_hbm, wu_hbm, wd_hbm,
               gvec_ref, gdec_ref, gmem, gwk, gwv, gwq, gwo, gdown, ggate, gup, attg,
               dqo_ref, k_ref, v_ref, kt_ref, qz_ref, wo_ref, wq_ref, wk_ref, wv_ref, ak_ref,
               dhg, doz, aqs, ads, stb, dk, dv, dkv, dkvp, dqp, dqr, dqa, arp, arr, ara, pvec, pdq, spb,
               msc, ybuf, abuf, wbuf, dbuf, wt, gst, gsw, gwo_s,
               *sems):
    chips, rows, mem, dim, hc, c, ff = dims
    QT = 2 * rows
    T = 2 * mem
    MC = min(256, mem)
    nm = T // MC
    inner = hc * 64
    np_ = hc // 2
    seg = 256 // chips // 2
    fh = ff // 2
    FT = wt.shape[1]
    nf = fh // FT
    ring = Ring(chips)
    z, core, far = ring.z, ring.core, ring.far
    sems = list(sems)

    def take(n):
        out = sems[:n]
        del sems[:n]
        return out

    half_rows = rows // 2
    part_ = functools.partial
    rsrc = lambda ref: (lambda half: ref.at[pl.ds(half * half_rows, half_rows)])
    dh_g = Rows(ring, dhg, rsrc(dh_ref), take(6))
    att_g = Rows(ring, attg, rsrc(att_ref), take(6))
    st_g = Share(ring, stb, lambda half: stb.at[z, half], take(2))
    dq_r = [Reduce(ring, dqp.at[p], dqr.at[p], add_into, take(2)) for p in range(np_)]
    dq_s = [Share(ring, dqa.at[p], lambda half, p=p: dqa.at[p, z, half], take(2)) for p in range(np_)]
    ar_r = [Reduce(ring, arp.at[p], arr.at[p], add_into, take(2)) for p in range(np_)]
    ar_s = [Share(ring, ara.at[p], lambda half, p=p: ara.at[p, z, half], take(2)) for p in range(np_)]
    xs, xr, ls, gs, gr, gl, wsem, ysem, lsem = take(9)
    loads = [pltpu.make_async_copy(src, dst, lsem.at[n]) for n, (src, dst) in enumerate((
        (wo_hbm, wo_ref), (k_hbm, k_ref), (v_hbm, v_ref), (kt_hbm, kt_ref), (qz_hbm, qz_ref),
        (ma_hbm, msc.at[0, pl.ds(0, mem)]), (mb_hbm, msc.at[1, pl.ds(0, mem)]), (wq_hbm, wq_ref), (wk_hbm, wk_ref), (wv_hbm, wv_ref)))]
    for cp in loads:
        cp.start()
    ring.enter()
    dh_g.start()
    locals_ = [pltpu.make_async_copy(att_ref.at[pl.ds(half * half_rows, half_rows)], attg.at[z, core, half], ls.at[half]) for half in range(2)]
    for cp in locals_:
        cp.start()
    for half in range(2):
        dhg[z, core, half] = dh_ref[half * half_rows:(half + 1) * half_rows, :]
    doz[...] = jnp.zeros_like(doz)
    mask_lanes(ak_ref, len_ref, z * T)
    hrow = pl.ds(pl.multiple_of(core * inner, inner), inner)
    hcol = pl.ds(pl.multiple_of(core * inner, 128), inner)
    other_cols = pl.ds(pl.multiple_of((1 - core) * mem, mem), mem)
    my_cols = pl.ds(pl.multiple_of(core * mem, mem), mem)
    qmine = pl.ds(pl.multiple_of(core * rows, rows), rows)
    qother = pl.ds(pl.multiple_of((1 - core) * rows, rows), rows)

    def lanes(chip):
        return pl.ds(pl.multiple_of(chip * QT, QT), QT)

    def d_out(chip):
        return mm_bt(wo_ref[hrow, :], dhg[chip].reshape(QT, dim))

    def prepare(chip, dot=None):
        dot = d_out(chip) if dot is None else dot
        dob = dot.astype(BF16)
        q = lanes(chip)
        row = lax.broadcasted_iota(jnp.int32, (16, QT), 0)
        for h in range(hc):
            lo = h * 128 + (h % 2) * 64
            doz[lo:lo + 64, q] = dob[h * 64:(h + 1) * 64]
            for ref, half, first in ((aqs, 0, 1.0), (ads, 1, 0.0)):
                a, b, e = (x.astype(F32) for x in parts3(stb[chip, half, h:h + 1, :]))
                ref[h * 16:(h + 1) * 16, q] = jnp.where(row == 0, first, jnp.where(row == 1, a, jnp.where(row == 2, b, jnp.where(row == 3, e, 0.0)))).astype(BF16)

    dh_g.ready(0)
    loads[0].wait()
    dot0 = d_out(z)
    prod = dot0 * own_ref[:inner, :]
    for h in range(hc):
        stb[z, 0, h:h + 1, :] = -own_ref[inner + h:inner + h + 1, :]
        stb[z, 1, h:h + 1, :] = -jnp.sum(prod[h * 64:(h + 1) * 64], axis=0, keepdims=True)
    stb[z, 0, hc:8, :] = gn_ref[0:8 - hc, :]
    stb[z, 1, hc:8, :] = gn_ref[8 - hc:16 - 2 * hc, :]
    st_g.start()
    prepare(z, dot0)
    dk[...] = jnp.zeros_like(dk)
    dv[...] = jnp.zeros_like(dv)
    for cp in loads[1:]:
        cp.wait()

    def tile(h, chip):
        pair = h // 2
        q = lanes(chip)
        hz = pl.ds(pl.multiple_of(h * 128, 128), 128)
        h16 = pl.ds(pl.multiple_of(h * 16, 16), 16)
        ps = pl.ds(pl.multiple_of(pair * 128, 128), 128)
        hz64 = pl.ds(pl.multiple_of(h * 128 + (h - 2 * pair) * 64, 64), 64)
        h64 = pl.ds(pl.multiple_of(h * 64, 64), 64)
        hr = h64
        q_t = qz_ref[hz64, q]
        do_t = doz[hz64, q]
        r1 = jnp.concatenate([qz_ref[hz, q], aqs[h16, q]], axis=0)
        r2 = jnp.concatenate([doz[hz, q], ads[h16, q]], axis=0)
        stage = {}
        dq = None
        for j in range(nm + 2):
            if j < nm:
                r = slice(j * MC, (j + 1) * MC)
                ak = ak_ref[r, 0:16]
                stage["a", j] = (mm(jnp.concatenate([k_ref[r, ps], ak], axis=1), r1), mm(jnp.concatenate([v_ref[r, ps], ak], axis=1), r2))
            if 1 <= j <= nm:
                s, dp = stage.pop(("a", j - 1))
                a = jnp.exp2(s * c)
                stage["b", j - 1] = (a.astype(BF16), (a * dp).astype(BF16))
            if j >= 2:
                r = slice((j - 2) * MC, (j - 1) * MC)
                pb, ds = stage.pop(("b", j - 2))
                dv[hr, r] += mm_bt(do_t, pb)
                dk[hr, r] += mm_bt(q_t, ds)
                d = mm(kt_ref[h64, r], ds)
                dq = d if dq is None else dq + d
        dqp[pair, chip, h - 2 * pair] = dq

    scale = 0.125

    def xp(p):
        return remote(dkv.at[p, :, other_cols], dkvp.at[p], xs.at[p], xr.at[p], ring.partner)

    def xq(p):
        return remote(dqa.at[p, z, :, :, qother], pdq.at[p], xs.at[np_ + p], xr.at[np_ + p], ring.partner)

    def share_dq(p):
        for half in range(2):
            dqa[p, z, half] = (dqp[p, z, half] * scale).astype(BF16)
        dq_s[p].start()
        xq(p).start()

    def share_ar(p):
        for half in range(2):
            ara[p, z, half] = arp[p, z, half]
        ar_s[p].start()

    moves = {"dh": dh_g, "st": st_g, "att": att_g}
    begins = {"att": att_g.start}
    for p in range(np_):
        moves.update({f"dq{p}": dq_r[p], f"ds{p}": dq_s[p], f"ar{p}": ar_r[p], f"as{p}": ar_s[p]})
        begins.update({f"ds{p}": part_(share_dq, p), f"as{p}": part_(share_ar, p)})

    def acts(*point):
        return [begins[e[0]] if e[1] == "start" else part_(moves[e[0]].move, *e[1:]) for e in BWD_PLAN.get(point, [])]

    def run(*point):
        for fn in acts(*point):
            fn()

    def table(kind, n):
        return {k: acts(kind, k) for k in range(n) if acts(kind, k)}

    offs = BWD_ORDER
    first = BWD_FIRST * hc
    per = 2 * (chips - BWD_FIRST)
    needs = {k * hc: offs[k] for k in range(1, BWD_FIRST)}
    needs.update({first + 2 * (k - BWD_FIRST): offs[k] for k in range(BWD_FIRST, chips)})

    def project(p):
        r = pl.ds(pl.multiple_of(p * 128, 128), 128)
        dkv[p, 0:128, :] = (dk[r, :] * scale).astype(BF16)
        dkv[p, 128:256, :] = dv[r, :].astype(BF16)
        xp(p).start()
        g = mm(dkv[p, :, my_cols], msc[0, 0:mem]) + mm(dkv[p, :, other_cols], msc[1, 0:mem])
        for n in range(2 * chips):
            arp[p, n // 2, n % 2] = g[n * seg:(n + 1) * seg]

    def body(it, carry):
        early = it < first
        b = it - first
        p = b // per
        r = b - p * per
        h = jnp.where(early, it % hc, 2 * p + r % 2)
        chip = ring.chip(pick(jnp.where(early, it // hc, BWD_FIRST + r // 2), offs))
        dispatch(it, {k: acts("r", k) + [part_(dh_g.ready, off)] for k, off in needs.items()})
        fresh = (early & (it > 0) & (it % hc == 0)) | ((b >= 0) & (b < per) & (r % 2 == 0))
        pl.when(fresh)(part_(prepare, chip))
        tile(h, chip)
        pl.when((b >= 0) & (r == per - 1))(part_(project, p))
        dispatch(it, table("b", chips * hc))
        return carry

    lax.fori_loop(0, chips * hc, body, 0)
    run("p", np_)
    near = range(1 - far, far + 1)

    for cp in locals_:
        cp.wait()
    for off in near:
        att_g.ready(off)
    gain2 = g2_ref[...].astype(F32)[None, :]
    gwo_s[...] = jnp.zeros_like(gwo_s)

    def y_fetch(ch, slot):
        return pltpu.make_async_copy(y_hbm.at[ch], ybuf.at[slot], ysem.at[slot, 0])

    def fetch(ch, slot):
        return (y_fetch(ch, slot), pltpu.make_async_copy(attg.at[ch], abuf.at[slot], ysem.at[slot, 1]))

    for cp in fetch(0, 0):
        cp.start()

    def hidden(ch, carry):
        slot = ch % 2
        for cp in fetch(ch, slot):
            cp.wait()

        @pl.when(ch + 1 < chips)
        def _():
            for cp in fetch(ch + 1, 1 - slot):
                cp.start()
        att = abuf[slot].reshape(QT, dim)
        h = (ybuf[slot].reshape(QT, dim).astype(F32) + mm(att, wo_ref[...])).astype(BF16)
        qz_ref[0:dim, lanes(ch)] = rms_norm(h.astype(F32), gain2).astype(BF16).T
        ah = jnp.where(core == 0, att[:, :inner], att[:, inner:])
        gwo_s[...] += mm_at(ah, dhg[ch].reshape(QT, dim))
        dispatch(ch, table("h", chips))
        return carry

    lax.fori_loop(0, chips, hidden, 0)
    dh_g.drain()
    go_load = pltpu.make_async_copy(gog, dhg, ls.at[0])
    go_load.start()

    def partner_block(buf, dst, k):
        return pltpu.make_async_copy(buf, dst, gl.at[k]), remote(buf, dst, gs.at[k], gr.at[k], ring.partner)

    def both_start(pair):
        pair[0].start()
        pair[1].start()

    def both_wait(pair):
        pair[0].wait()
        pair[1].wait()

    wo_out = partner_block(gwo_s, gwo.at[hrow], 3 * nf)
    both_start(wo_out)

    def w_fetch(f, slot):
        cols = pl.ds(pl.multiple_of(core * fh + f * FT, FT), FT)
        return (pltpu.make_async_copy(wg_hbm.at[:, cols], wbuf.at[0], wsem.at[slot, 0]),
                pltpu.make_async_copy(wu_hbm.at[:, cols], wbuf.at[1], wsem.at[slot, 1]),
                pltpu.make_async_copy(wd_hbm.at[cols], dbuf.at[slot], wsem.at[slot, 2]))

    for cp in w_fetch(0, 0):
        cp.start()
    go_load.wait()
    f_table = table("f", 9 * nf)

    def block(f, n):
        if n == 0:
            return partner_block(gst.at[f % 2, pl.ds(0, FT)], gdown.at[pl.ds(pl.multiple_of(core * fh + f * FT, FT), FT)], f)
        return partner_block(gsw.at[f % 2, n - 1], (ggate, gup)[n - 1].at[:, pl.ds(pl.multiple_of(core * fh + f * FT, FT), FT)], n * nf + f)

    def mlp(f, carry):
        slot = f % 2
        for cp in w_fetch(f, slot):
            cp.wait()

        for n in range(2):
            wt[n] = wbuf[n].T

        @pl.when(f + 1 < nf)
        def _():
            for cp in w_fetch(f + 1, 1 - slot):
                cp.start()

        def act_pair(k, cc):
            for ch in (2 * k, 2 * k + 1):
                q = lanes(ch)
                n2t = qz_ref[0:dim, q]
                g = mm(wt[0], n2t)
                u = mm(wt[1], n2t)
                ga = mm_bt(dbuf[slot], dhg[ch].reshape(QT, dim))
                sig = jax.nn.sigmoid(g)
                si = g * sig
                doz[0:FT, q] = (si * u).astype(BF16)
                doz[FT:2 * FT, q] = (ga * u * (sig + si * (1.0 - sig))).astype(BF16)
                doz[2 * FT:3 * FT, q] = (ga * si).astype(BF16)
            dispatch(f * 9 + 2 * k + 1, f_table)
            return cc

        lax.fori_loop(0, chips // 2, act_pair, 0)

        @pl.when(f > 1)
        def _():
            for n in range(3):
                both_wait(block(f - 2, n))
        acc = [None] * 3
        for ch in range(chips):
            q = slice(ch * QT, (ch + 1) * QT)
            n2t = qz_ref[0:dim, q]
            for n, d in enumerate((mm(doz[0:FT, q], dhg[ch].reshape(QT, dim)), mm_bt(n2t, doz[FT:2 * FT, q]), mm_bt(n2t, doz[2 * FT:3 * FT, q]))):
                acc[n] = d if acc[n] is None else acc[n] + d
        gst[slot, 0:FT] = acc[0]
        gsw[slot, 0] = acc[1]
        gsw[slot, 1] = acc[2]
        for n in range(3):
            both_start(block(f, n))
        dispatch(f * 9 + 8, f_table)
        return carry

    lax.fori_loop(0, nf, mlp, 0)
    for p in range(np_):
        remote(dkvp.at[p], dkvp.at[p], xs.at[p], xr.at[p], ring.partner).wait_recv()
    nb = 4
    w = mem // nb
    for f in (nf - 2, nf - 1):
        for n in range(3):
            both_wait(block(f, n))

    def gm(b):
        return pltpu.make_async_copy(gst.at[b % 2, pl.ds(0, w)], gmem.at[pl.ds(pl.multiple_of(b * w, w), w)], gl.at[3 * nf + 2 + b % 2])

    def memory_rows(b, carry):
        @pl.when(b > 1)
        def _():
            gm(b - 2).wait()
        cb = pl.ds(pl.multiple_of(core * mem + b * w, w), w)
        cp = pl.ds(pl.multiple_of(b * w, w), w)
        acc = None
        for p in range(np_):
            own_e = pl.ds(pl.multiple_of(core * inner + p * 128, 128), 128)
            oth_e = pl.ds(pl.multiple_of((1 - core) * inner + p * 128, 128), 128)
            for part, w_ref in ((0, wk_ref), (1, wv_ref)):
                e = slice(part * 128, (part + 1) * 128)
                lhs = jnp.concatenate([dkv[p, e, cb], dkvp[p, e, cp]], axis=0)
                rhs = jnp.concatenate([w_ref[:, own_e], w_ref[:, oth_e]], axis=1)
                d = mm_bt(lhs.T, rhs)
                acc = d if acc is None else acc + d
        gst[b % 2, 0:w] = acc
        gm(b).start()
        dispatch(b, table("m", nb))
        return carry

    lax.fori_loop(0, nb, memory_rows, 0)
    run("m", nb)

    gain = g1_ref[...].astype(F32)[None, :]
    y_fetch(0, 0).start()
    spb[...] = jnp.zeros_like(spb)
    both_wait(wo_out)
    gwq_s = gwo_s
    gwq_s[...] = jnp.zeros_like(gwq_s)
    wq_h = wq_ref[:, hcol]

    def query(ch, carry):
        slot = ch % 2
        y_fetch(ch, slot).wait()

        @pl.when(ch + 1 < chips)
        def _():
            y_fetch(ch + 1, 1 - slot).start()
        x = ybuf[slot].reshape(QT, dim).astype(F32)
        xhat = x * lax.rsqrt(jnp.mean(x * x, axis=-1, keepdims=True) + 1e-6)
        n1 = (xhat * gain).astype(BF16)
        dqc = jnp.concatenate([dqa[p, ch].reshape(128, QT) for p in range(np_)], axis=0)
        dn = mm_bt(dqc.T, wq_h)
        gwq_s[...] += mm(dqc, n1)
        spb[0:1, :] += jnp.sum(dn * xhat, axis=0, keepdims=True)
        dispatch(ch, table("q", chips))
        return carry

    lax.fori_loop(0, chips, query, 0)
    gvec2 = jnp.zeros((16 - 2 * hc, QT), F32)
    for ch in range(chips):
        gvec2 = gvec2 + jnp.concatenate([stb[ch, 0, hc:8, :], stb[ch, 1, hc:8, :]], axis=0)
    for n in range(dim // QT):
        spb[1:2, n * QT:(n + 1) * QT] = gvec2[n:n + 1]
    cv = remote(spb, pvec, xs.at[2 * np_], xr.at[2 * np_], ring.partner)
    cv.start()
    wq_out = partner_block(gwq_s, gwq.at[hrow], 3 * nf + 1)
    both_start(wq_out)
    for p in range(np_):
        own_r = pl.ds(pl.multiple_of(core * inner + p * 128, 128), 128)
        oth_r = pl.ds(pl.multiple_of((1 - core) * inner + p * 128, 128), 128)
        dqo_ref[own_r, :] = dqa[p, z, :, :, qmine].reshape(128, rows)
        xq(p).wait()
        dqo_ref[oth_r, :] = pdq[p].reshape(128, rows)
    x = y_ref[...].astype(F32)
    inv = lax.rsqrt(jnp.mean(x * x, axis=-1, keepdims=True) + 1e-6)
    xhat = x * inv
    t = mm_bt(dqo_ref[...].T, wq_ref[...]) * gain
    gdec_ref[...] = gh_ref[...] + inv * (t - xhat * jnp.mean(t * xhat, axis=-1, keepdims=True))
    run("q", chips)
    wkv_out = []
    for p in range(np_):
        for k, out in enumerate((gwk, gwv)):
            n = 2 * p + k
            src = ara.at[p, pl.ds(k * (chips // 2), chips // 2)]
            wkv_out.append(pltpu.make_async_copy(src, out.at[core, p], ls.at[2 + n]))
            wkv_out.append(remote(src, out.at[core, p], xs.at[2 * np_ + 1 + n], xr.at[2 * np_ + 1 + n], ring.partner))
    for cp in wkv_out:
        cp.start()
    for p in range(np_):
        xp(p).wait_send()
    cv.wait()
    gvec_ref[...] = spb[0:2] + pvec[0:2]
    both_wait(wq_out)
    for cp in wkv_out:
        cp.wait()
    for b in range(nb - 2, nb):
        gm(b).wait()
    for obj in [att_g, st_g] + dq_r + dq_s + ar_r + ar_s:
        obj.drain()


def bwd_call(dims, *args):
    chips, rows, mem, dim, hc, c, ff = dims
    inner = hc * 64
    QT = 2 * rows
    T = 2 * mem
    np_ = hc // 2
    h2 = chips // 2
    seg = 256 // chips // 2
    FT = ff // 8
    v = pl.BlockSpec(memory_space=VMEM)
    hbm = pl.BlockSpec(memory_space=pl.ANY)
    s3 = (2, 2, h2)
    rows_sems = [DMA((1,)), DMA(s3)] * 2 + [DMA((1,)), DMA((2,))]
    two = [DMA((1,)), DMA(s3)]
    S = jax.ShapeDtypeStruct
    gshape = (chips, 2, 2, rows // 2, dim)
    cols = chips * QT
    wsq = VMEM((dim, 2 * inner), BF16)
    return pl.pallas_call(
        functools.partial(bwd_kernel, dims),
        out_shape=(S((2, dim), F32), S((rows, dim), F32), S((mem, dim), F32), S((2, np_, chips // 2, 2, seg, dim), F32), S((2, np_, chips // 2, 2, seg, dim), F32), S((2 * inner, dim), F32), S((2 * inner, dim), F32),
                   S((ff, dim), F32), S((dim, ff), F32), S((dim, ff), F32), S(gshape, BF16)),
        in_specs=[pl.BlockSpec(memory_space=pltpu.SMEM)] + [v] * 8 + [hbm] * 15, out_specs=(v,) * 2 + (hbm,) * 9,
        scratch_shapes=[
            VMEM((2 * inner, rows), BF16), VMEM((T, inner), BF16), VMEM((T, inner), BF16), VMEM((inner, T), BF16), VMEM((hc * 128, cols), BF16), VMEM((2 * inner, dim), BF16), wsq, wsq, wsq, VMEM((T, 128), BF16),
            VMEM(gshape, BF16), VMEM((max(hc * 128, 3 * FT), cols), BF16), VMEM((hc * 16, cols), BF16), VMEM((hc * 16, cols), BF16),
            VMEM((chips, 2, 8, QT), F32), VMEM((inner, T), F32), VMEM((inner, T), F32), VMEM((np_, 256, T), BF16), VMEM((np_, 256, mem), BF16),
            VMEM((np_, chips, 2, 64, QT), F32), VMEM((np_, 2, 2, h2, 64, QT), F32), VMEM((np_, chips, 2, 64, QT), BF16),
            VMEM((np_, chips, 2, seg, dim), F32), VMEM((np_, 2, 2, h2, seg, dim), F32), VMEM((np_, chips, 2, seg, dim), F32),
            VMEM((8, dim), F32), VMEM((np_, 2, 64, rows), BF16), VMEM((8, dim), F32),
            VMEM((2, mem, dim), BF16), VMEM((2, 2, 2, rows // 2, dim), BF16), VMEM((2, 2, 2, rows // 2, dim), BF16),
            VMEM((2, dim, FT), BF16), VMEM((2, FT, dim), BF16), VMEM((2, FT, dim), BF16), VMEM((2, max(FT, mem // 4), dim), F32), VMEM((2, 2, dim, FT), F32),
            VMEM((inner, dim), F32)]
        + rows_sems * 2 + two * (1 + 4 * np_) + [DMA((4 * np_ + 1,))] * 2 + [DMA((2 + 2 * np_,)), DMA((14,)), DMA((14,)), DMA((16,)), DMA((2, 3)), DMA((2, 2)), DMA((10,))],
        compiler_params=pltpu.CompilerParams(vmem_limit_bytes=67_043_328, collective_id=1, has_side_effects=True),
        cost_estimate=pl.CostEstimate(flops=10**10, bytes_accessed=30 << 20, transcendentals=0),
        name="attn_bwd")(*args)


def finish_kernel(slots, *refs):
    n = (len(refs) - 3) // 2
    srcs, dsts, (buf, si, so) = refs[:n], refs[n:2 * n], refs[2 * n:]
    rows = buf.shape[1]
    moves = []
    for src, dst in zip(srcs, dsts):
        for c in range(0, src.shape[1], buf.shape[2]):
            wide = min(buf.shape[2], src.shape[1] - c)
            cols = pl.ds(c, wide)
            for r in range(0, src.shape[0], rows):
                k = len(moves) % slots
                w = min(rows, src.shape[0] - r)
                b = buf.at[k, pl.ds(0, w), pl.ds(0, wide)]
                moves.append((pltpu.make_async_copy(src.at[pl.ds(r, w), cols], b, si.at[k]), pltpu.make_async_copy(b, dst.at[pl.ds(r, w), cols], so.at[k])))
    lag = slots // 2
    for i in range(len(moves) + lag):
        if i < len(moves):
            if i >= slots:
                moves[i - slots][1].wait()
            moves[i][0].start()
        if i >= lag:
            moves[i - lag][0].wait()
            moves[i - lag][1].start()
    for m in moves[-slots:]:
        m[1].wait()


def finish_call(*arrays):
    slots, rows, cols = 16, 256, 1024
    hbm = pl.BlockSpec(memory_space=pl.ANY)
    return pl.pallas_call(
        functools.partial(finish_kernel, slots),
        out_shape=tuple(jax.ShapeDtypeStruct(a.shape, a.dtype) for a in arrays),
        in_specs=[hbm] * len(arrays), out_specs=(hbm,) * len(arrays),
        scratch_shapes=[VMEM((slots, rows, cols), F32), DMA((slots,)), DMA((slots,))],
        compiler_params=pltpu.CompilerParams(vmem_limit_bytes=32 * 1024 * 1024),
        name="finish")(*arrays)


def fwd_kernel(dims, len_ref, y_ref, go_ref, m_ref, g1_ref, g2_ref, wq_hbm, wk_hbm, wv_hbm, wo_hbm, wg_hbm, wu_hbm, wd_hbm,
               own, att_ref, dh_ref, gh_ref, gn_ref, k_out, v_out, kt_out, qz_out, mg_out, yall, gog,
               k_s, v_s, kt_s, qz, mg, wq_ref, wk_ref, wv_ref, ak_ref, yg, wqt, vt_s, s_scr, mx_scr, part, rbuf, patt, satt, gob, attt, wo_s, wg_s, wu_s, wd_s, n2_s, dn_s, *sems):
    chips, rows, mem, dim, hc, c, ff = dims
    QT = 2 * rows
    T = 2 * mem
    MC = min(256, mem)
    hh = hc // 2
    inner = hc * 64
    HR = hh * 64
    ring = Ring(chips)
    z, core, far = ring.z, ring.core, ring.far
    sub = rows // 2
    part_ = functools.partial
    xs, xr, ls = sems[14:]
    rsrc = lambda ref: (lambda half: ref.at[pl.ds(half * sub, sub)])
    y_g = Rows(ring, yg, rsrc(y_ref), sems[:6])
    go_g = Rows(ring, gog, rsrc(gob), sems[6:12])

    def merge(dst, src):
        for hl in range(hh):
            mr = slice(HR + hl, HR + hl + 1)
            lr = slice(HR + 8 + hl, HR + 9 + hl)
            m1, m2 = dst[mr, :], src[mr, :]
            m = jnp.maximum(m1, m2)
            a = jnp.exp2((m1 - m) * c)
            b = jnp.exp2((m2 - m) * c)
            rr = slice(hl * 64, (hl + 1) * 64)
            dst[rr, :] = dst[rr, :] * a + src[rr, :] * b
            dst[mr, :] = m
            dst[lr, :] = dst[lr, :] * a + src[lr, :] * b

    o_r = Reduce(ring, part, rbuf, merge, sems[12:14])
    loads = [pltpu.make_async_copy(src, dst, ls.at[7 + n]) for n, (src, dst) in enumerate((
        (wk_hbm, wk_ref), (wv_hbm, wv_ref), (wq_hbm, wq_ref), (wo_hbm, wo_s), (wg_hbm, wg_s), (wu_hbm, wu_s), (wd_hbm, wd_s)))]
    stores = [pltpu.make_async_copy(src, dst, ls.at[n]) for n, (src, dst) in enumerate(((k_s, k_out), (v_s, v_out), (kt_s, kt_out), (mg, mg_out), (qz, qz_out)))]
    for cp in loads[:3]:
        cp.start()
    ring.enter()
    y_g.start()
    mx_copy = remote(m_ref, mg, xs.at[0], xr.at[0], ring.partner)
    mx_copy.start()
    for cp in loads[3:]:
        cp.start()
    gob[...] = go_ref[...].astype(BF16)
    for half in range(2):
        yg[z, core, half] = y_ref[half * sub:(half + 1) * sub, :]
    hcol = pl.ds(pl.multiple_of(core * inner, 128), inner)
    qz[...] = jnp.zeros_like(qz)
    mask_lanes(ak_ref, len_ref, z * T)
    for cp in loads[:3]:
        cp.wait()
    wqt[...] = wq_ref[:, hcol].T
    wk = wk_ref[:, hcol]
    wv = wv_ref[:, hcol]

    moves = {"y": y_g, "go": go_g, "o": o_r}

    def acts(*point):
        return [go_g.start if e[1] == "start" else part_(moves[e[0]].move, *e[1:]) for e in FWD_PLAN.get(point, [])]

    def run(*point):
        for fn in acts(*point):
            fn()

    def project(src, base, blocks):
        for j in blocks:
            r = pl.ds(pl.multiple_of(base + j * MC, MC), MC)
            blk = src[j * MC:(j + 1) * MC, :]
            kb = mm(blk, wk).astype(BF16)
            vb = mm(blk, wv).astype(BF16)
            k_s[r, :] = kb
            v_s[r, :] = vb
            kt_s[:, r] = kb.T
            vt_s[:, r] = vb.T

    nb = mem // MC
    project(m_ref, core * mem, range(nb))
    run("s", 0)
    mx_copy.wait_recv()
    project(mg, (1 - core) * mem, range(nb // 2))
    run("s", 1)
    project(mg, (1 - core) * mem, range(nb // 2, nb))
    run("s", 2)
    for cp in stores[:4]:
        cp.start()
    gain = g1_ref[...].astype(F32)[None, :]
    one_row = jnp.where(lax.broadcasted_iota(jnp.int32, (16, QT), 0) == 0, 1.0, 0.0).astype(BF16)

    def lanes(chip):
        return pl.ds(pl.multiple_of(chip * QT, QT), QT)

    def prep(chip):
        n1 = rms_norm(yg[chip].reshape(QT, dim).astype(F32), gain).astype(BF16)
        qt = mm_bt(wqt[...], n1).astype(BF16)
        for h in range(hc):
            lo = h * 128 + (h % 2) * 64
            qz[lo:lo + 64, lanes(chip)] = qt[h * 64:(h + 1) * 64]

    def step(new, slot, old, pslot):
        if new is not None:
            chip, h = new
            rhs = jnp.concatenate([qz[pl.ds(pl.multiple_of(h * 128, 128), 128), lanes(chip)], one_row], axis=0)
            pair = pl.ds(pl.multiple_of((h // 2) * 128, 128), 128)
            mx = None
        if old is not None:
            ochip, half, hl = old
            m = jnp.max(mx_scr[pslot], axis=0, keepdims=True)
            vrow = pl.ds(pl.multiple_of((half * hh + hl) * 64, 64), 64)
            ls_ = None
            acc = None
        for j in range(T // MC):
            r = slice(j * MC, (j + 1) * MC)
            if new is not None:
                s = mm(jnp.concatenate([k_s[r, pair], ak_ref[r, 0:16]], axis=1), rhs)
                s_scr[slot, r, :] = s
                t = jnp.max(s.reshape(MC // 8, 8, QT), axis=0)
                mx = t if mx is None else jnp.maximum(mx, t)
            if old is not None:
                pr = jnp.exp2((s_scr[pslot, r, :] - m) * c)
                t = jnp.sum(pr.reshape(MC // 8, 8, QT), axis=0)
                ls_ = t if ls_ is None else ls_ + t
                dd = mm(vt_s[vrow, r], pr.astype(BF16))
                acc = dd if acc is None else acc + dd
        if new is not None:
            mx_scr[slot] = mx
        if old is not None:
            part[ochip, half, hl * 64:(hl + 1) * 64, :] = acc
            part[ochip, half, HR + hl:HR + hl + 1, :] = m
            part[ochip, half, HR + 8 + hl:HR + 9 + hl, :] = jnp.sum(ls_, axis=0, keepdims=True)

    offs = [o for o, _ in FWD_ORDER]
    halves = [h for _, h in FWD_ORDER]
    n = len(offs)
    fresh = [int(k + 1 < n and offs[k + 1] not in offs[:k + 1]) for k in range(n)]
    run("s", 3)
    y_g.ready(0)
    prep(z)
    step((z, halves[0] * hh), 0, None, None)

    def body(pair, carry):
        for u in range(2):
            i = 2 * pair + u
            i2 = jnp.minimum(i + 1, n - 1)
            chip, half = ring.chip(pick(i, offs)), pick(i, halves)
            chip2, half2 = ring.chip(pick(i2, offs)), pick(i2, halves)
            for k in range(hh):
                slot = (u * hh + k) % 2
                if k == hh - 1:
                    dispatch(pair, {kk // 2: acts("r", kk) + [part_(y_g.ready, offs[kk + 1])] for kk in range(u, n, 2) if fresh[kk]})
                    if any(fresh[u::2]):
                        pl.when(pick(i, fresh) == 1)(part_(prep, chip2))
                    new = (chip2, half2 * hh)
                else:
                    new = (chip, half * hh + k + 1)
                step(new, 1 - slot, (chip, half, k), slot)
                dispatch(pair, {kk // 2: acts("b", kk * hh + k) for kk in range(u, n, 2) if acts("b", kk * hh + k)})
        return carry

    gl = [pltpu.make_async_copy(gob.at[pl.ds(half * sub, sub)], gog.at[z, core, half], ls.at[5 + half]) for half in range(2)]
    for cp in gl:
        cp.start()
    lax.fori_loop(0, n // 2, body, 0)
    yc = pltpu.make_async_copy(yg, yall, ls.at[14])
    yc.start()
    stores[4].start()
    run("t", 0)
    run("t", 1)
    qmine = pl.ds(pl.multiple_of(core * rows, rows), rows)
    qother = pl.ds(pl.multiple_of((1 - core) * rows, rows), rows)
    for h in range(hc):
        half, hl = h // hh, h % hh
        m = part[z, half, HR + hl:HR + hl + 1, :]
        l = part[z, half, HR + 8 + hl:HR + 9 + hl, :]
        own[h * 64:(h + 1) * 64, :] = part[z, half, hl * 64:(hl + 1) * 64, :] / l
        own[inner + h:inner + h + 1, :] = m + jnp.log2(l) / c
    satt[...] = own[:inner, qother].astype(BF16)
    xo = remote(satt, patt, xs.at[1], xr.at[1], ring.partner)
    xo.start()
    attt[pl.ds(pl.multiple_of(core * inner, inner), inner), :] = own[:inner, qmine].astype(BF16)
    for cp in loads[3:]:
        cp.wait()
    run("t", 2)
    xo.wait()
    attt[pl.ds(pl.multiple_of((1 - core) * inner, inner), inner), :] = patt[...]

    att = attt[...].T
    att_ref[...] = att
    gain2 = g2_ref[...].astype(F32)[None, :]
    run("t", 3)
    hid = (y_ref[...].astype(F32) + mm(att, wo_s[...])).astype(BF16).astype(F32)
    inv = lax.rsqrt(jnp.mean(hid * hid, axis=-1, keepdims=True) + 1e-6)
    hhat = hid * inv
    n2 = (hhat * gain2).astype(BF16)
    fb = ff // 4
    n2_s[...] = n2
    dn_s[...] = jnp.zeros_like(dn_s)

    def mlp(f, carry):
        cols = pl.ds(pl.multiple_of(f * fb, fb), fb)
        wg, wu = wg_s[:, cols], wu_s[:, cols]
        g = mm(n2_s[...], wg)
        u = mm(n2_s[...], wu)
        ga = mm_bt(gob[...], wd_s[cols, :])
        sig = jax.nn.sigmoid(g)
        si = g * sig
        dn_s[...] += mm_bt((ga * u * (sig + si * (1.0 - sig))).astype(BF16), wg) + mm_bt((ga * si).astype(BF16), wu)
        dispatch(f, {n: acts("t", 4 + n) for n in range(4) if acts("t", 4 + n)})
        return carry

    lax.fori_loop(0, 4, mlp, 0)
    dn = dn_s[...]
    gsum = jnp.sum(dn * hhat, axis=0, keepdims=True)
    gn_ref[...] = jnp.zeros_like(gn_ref)
    for k in range(dim // QT):
        gn_ref[k:k + 1, :] = gsum[:, k * QT:(k + 1) * QT]
    t = dn * gain2
    gh = go_ref[...] + inv * (t - hhat * jnp.mean(t * hhat, axis=-1, keepdims=True))
    gh_ref[...] = gh
    dh_ref[...] = gh.astype(BF16)
    run("t", 8)
    for off in range(-far + 1, far + 1):
        go_g.ready(off)
    mx_copy.wait_send()
    for cp in [yc] + gl + stores:
        cp.wait()
    for obj in (y_g, go_g, o_r):
        obj.drain()


def fwd_call(dims, *args):
    chips, rows, mem, dim, hc, c, ff = dims
    hh = hc // 2
    inner = hc * 64
    QT = 2 * rows
    T = 2 * mem
    HR = hh * 64
    h2 = chips // 2
    v = pl.BlockSpec(memory_space=VMEM)
    hbm = pl.BlockSpec(memory_space=pl.ANY)
    S = jax.ShapeDtypeStruct
    s3 = (2, 2, h2)
    gshape = (chips, 2, 2, rows // 2, dim)
    rows_sems = [DMA((1,)), DMA(s3)] * 2 + [DMA((1,)), DMA((2,))]
    return pl.pallas_call(
        functools.partial(fwd_kernel, dims),
        out_shape=(S((inner + 8, QT), F32), S((rows, 2 * inner), BF16), S((rows, dim), BF16), S((rows, dim), F32), S((8, QT), F32),
                   S((T, inner), BF16), S((T, inner), BF16), S((inner, T), BF16), S((hc * 128, chips * QT), BF16), S((mem, dim), BF16), S(gshape, BF16), S(gshape, BF16)),
        in_specs=[pl.BlockSpec(memory_space=pltpu.SMEM)] + [v] * 5 + [hbm] * 7, out_specs=(v,) * 5 + (hbm,) * 7,
        scratch_shapes=[
            VMEM((T, inner), BF16), VMEM((T, inner), BF16), VMEM((inner, T), BF16), VMEM((hc * 128, chips * QT), BF16), VMEM((mem, dim), BF16),
            VMEM((dim, 2 * inner), BF16), VMEM((dim, 2 * inner), BF16), VMEM((dim, 2 * inner), BF16), VMEM((T, 128), BF16),
            VMEM(gshape, BF16), VMEM((inner, dim), BF16), VMEM((inner, T), BF16), VMEM((2, T, QT), F32), VMEM((2, 8, QT), F32),
            VMEM((chips, 2, HR + 16, QT), F32), VMEM((2, 2, h2, HR + 16, QT), F32), VMEM((inner, rows), BF16), VMEM((inner, rows), BF16),
            VMEM((rows, dim), BF16), VMEM((2 * inner, rows), BF16), VMEM((2 * inner, dim), BF16), VMEM((dim, ff), BF16), VMEM((dim, ff), BF16), VMEM((ff, dim), BF16), VMEM((rows, dim), BF16), VMEM((rows, dim), F32)]
        + rows_sems * 2 + [DMA((1,)), DMA(s3)] + [DMA((2,))] * 2 + [DMA((15,))],
        compiler_params=pltpu.CompilerParams(vmem_limit_bytes=62 * 1024 * 1024, collective_id=0, has_side_effects=True),
        cost_estimate=pl.CostEstimate(flops=10**10, bytes_accessed=30 << 20, transcendentals=0),
        name="attn_fwd")(*args)


def solution(mesh):
    group = mesh.shape['seq']
    row_spec = P(('data', 'seq'), None)
    part_vec = P('data')
    part_mat = P('data', None)
    part_cube = P('data', None, None)

    def device_step(dec_in, memory, mem_len, grad_out, norm_attn, wq, wk, wv, wo, norm_mlp, w_gate, w_up, w_down):
        rows, dim = dec_in.shape
        mem = memory.shape[0]
        heads, hd = wq.shape[1], wq.shape[2]
        inner = heads * hd
        chips = group // 2
        hc = heads // 2
        c = LOG2E * hd ** -0.5
        dims = (chips, rows, mem, dim, hc, c, w_gate.shape[1])
        wq2, wk2, wv2 = (w.reshape(dim, inner) for w in (wq, wk, wv))
        wo2 = wo.reshape(inner, dim)

        own, attended, dh, grad_hidden, gn, k_c, v_c, kt_c, qz, mem_p, y_all, go_all = fwd_call(
            dims, mem_len, dec_in, grad_out, memory, norm_attn, norm_mlp, wq2, wk2, wv2, wo2, w_gate, w_up, w_down)
        gvec, g_dec, g_mem, g_wk, g_wv, g_wq, g_wo, g_down, g_gate, g_up, _ = bwd_call(
            dims, mem_len, dh, own, gn, attended, dec_in, grad_hidden, norm_attn, norm_mlp,
            k_c, v_c, kt_c, qz, wo2, wq2, wk2, wv2, memory, mem_p, y_all, go_all, w_gate, w_up, w_down)
        cube = (dim, heads, hd)
        g_wk, g_wv = (g.reshape(inner, dim) for g in (g_wk, g_wv))
        g_mem, g_wq, g_wk, g_wv, g_wo, g_down, g_gate, g_up = finish_call(g_mem, g_wq, g_wk, g_wv, g_wo, g_down, g_gate, g_up)
        g_wq, g_wk, g_wv = (g.T.reshape(cube) for g in (g_wq, g_wk, g_wv))
        return (g_dec, g_mem, gvec[0], g_wq, g_wk, g_wv, g_wo.reshape(heads, hd, dim), gvec[1], g_gate, g_up, g_down)

    return jax.shard_map(device_step, mesh=mesh,
                         in_specs=(row_spec, row_spec, part_vec, row_spec) + (P(),) * 9,
                         out_specs=(row_spec, row_spec, part_vec, part_cube, part_cube, part_cube, part_cube, part_vec, part_mat, part_mat, part_mat),
                         check_vma=False)
```

```python
import functools
import math

import jax
import jax.numpy as jnp
from jax import lax
from jax.experimental import pallas as pl
from jax.experimental.pallas import tpu as pltpu
from jax.sharding import PartitionSpec as P

F32 = jnp.float32
BF16 = jnp.bfloat16
LOG2E = math.log2(math.e)
VMEM = pltpu.VMEM
MESH = pl.DeviceIdType.MESH


def mm(a, b):
    return jnp.dot(a, b, preferred_element_type=F32)


def mm_bt(a, b):
    return lax.dot_general(a, b, (((1,), (1,)), ((), ())), preferred_element_type=F32)


def mm_at(a, b):
    return lax.dot_general(a, b, (((0,), (0,)), ((), ())), preferred_element_type=F32)


def rms_norm(tensor, gain):
    mean_sq = jnp.mean(tensor * tensor, axis=-1, keepdims=True)
    return tensor * lax.rsqrt(mean_sq + 1e-6) * gain


RIGHT, LEFT = 0, 1
DMA = pltpu.SemaphoreType.DMA

FWD_ORDER = [(0, 0), (0, 1), (1, 0), (1, 1), (-3, 0), (3, 1), (4, 0), (4, 1), (3, 0), (-3, 1), (2, 0), (-2, 1), (2, 1), (-2, 0), (-1, 1), (-1, 0)]
BWD_ORDER = [0, 1, 4, 3, -3, 2, -2, -1]
BWD_FIRST = 2
FWD_PLAN = {
    ("b", 0): [("y", 0, 1, 1), ("y", 1, 0, 1)],
    ("b", 11): [("y", 1, 1, 3), ("y", 1, 0, 3)],
    ("b", 12): [("go", 0, 0, 1)],
    ("b", 13): [("go", 1, 1, 1)],
    ("b", 14): [("o", 1, 0, 3)],
    ("b", 15): [("go", 0, 1, 1)],
    ("b", 17): [("o", 0, 1, 3)],
    ("b", 18): [("go", 1, 0, 1)],
    ("b", 20): [("o", 0, 0, 4)],
    ("b", 21): [("go", 1, 1, 2)],
    ("b", 23): [("o", 1, 1, 4)],
    ("b", 31): [("go", 0, 0, 2)],
    ("b", 32): [("go", 1, 0, 2)],
    ("b", 34): [("go", 0, 1, 2)],
    ("b", 35): [("go", 1, 1, 3)],
    ("b", 36): [("o", 0, 0, 3)],
    ("b", 37): [("o", 1, 1, 3)],
    ("b", 38): [("o", 0, 1, 2)],
    ("b", 4): [("y", 0, 0, 2), ("y", 1, 1, 2)],
    ("b", 40): [("go", 1, 0, 3)],
    ("b", 41): [("o", 1, 0, 2)],
    ("b", 42): [("go", 0, 1, 3)],
    ("b", 43): [("go", 1, 1, 4)],
    ("b", 8): [("y", 0, 1, 2), ("y", 1, 0, 2)],
    ("b", 9): [("go", "start")],
    ("r", 3): [("y", 0, 0, 3), ("y", 0, 1, 3)],
    ("r", 5): [("y", 0, 0, 4), ("y", 1, 1, 4)],
    ("s", 1): [("y", 0, 0, 1), ("y", 1, 1, 1)],
    ("t", 1): [("o", 0, 0, 2), ("o", 1, 1, 2), ("o", 0, 1, 1), ("o", 1, 0, 1), ("o", 0, 0, 1), ("o", 1, 1, 1), ("o", 0, 1, 0), ("o", 1, 0, 0), ("o", 0, 0, 0), ("o", 1, 1, 0)],
    ("t", 2): [("go", 0, 0, 3)],
    ("t", 6): [("go", 0, 0, 4)],
}
BWD_PLAN = {
    ("b", 1): [("dh", 0, 0, 1), ("dh", 1, 1, 1)],
    ("b", 10): [("dh", 0, 1, 3), ("dh", 1, 0, 3), ("st", 0, 0, 3), ("st", 1, 1, 3)],
    ("b", 11): [("st", 0, 1, 3), ("st", 1, 0, 3)],
    ("b", 12): [("dq0", 0, 0, 4)],
    ("b", 13): [("dq0", 1, 1, 4)],
    ("b", 14): [("att", 0, 0, 1), ("att", 1, 1, 1)],
    ("b", 15): [("dq0", 0, 1, 3), ("att", 0, 1, 1), ("att", 1, 0, 1)],
    ("b", 16): [("dq0", 0, 0, 3), ("dq0", 1, 0, 3)],
    ("b", 17): [("dq0", 1, 1, 3)],
    ("b", 18): [("att", 0, 0, 2), ("att", 1, 1, 2)],
    ("b", 19): [("dq0", 0, 1, 2), ("att", 1, 0, 2)],
    ("b", 2): [("dh", 0, 1, 1), ("dh", 1, 0, 1), ("st", 0, 0, 1), ("st", 1, 1, 1), ("st", 0, 1, 1), ("st", 1, 0, 1)],
    ("b", 20): [("dq0", 1, 0, 2), ("att", 0, 1, 2)],
    ("b", 21): [("dq0", 0, 0, 2), ("dq0", 1, 1, 2)],
    ("b", 22): [("att", 0, 0, 3), ("att", 1, 1, 3)],
    ("b", 23): [("dq0", 0, 1, 1), ("att", 1, 0, 3), ("ar0", 0, 1, 3), ("ar0", 1, 0, 3), ("ar0", 0, 0, 4), ("ar0", 1, 1, 4)],
    ("b", 24): [("dq1", 0, 0, 4), ("dq0", 1, 0, 1), ("att", 0, 1, 3)],
    ("b", 25): [("dq1", 1, 1, 4), ("dq0", 0, 0, 1), ("dq0", 1, 1, 1)],
    ("b", 26): [("att", 0, 0, 4), ("att", 1, 1, 4)],
    ("b", 27): [("dq1", 0, 1, 3), ("dq0", 0, 1, 0), ("ar0", 1, 0, 2)],
    ("b", 28): [("dq1", 1, 0, 3), ("ar0", 1, 1, 3), ("ar0", 0, 1, 2)],
    ("b", 29): [("dq0", 1, 0, 0), ("ar0", 0, 0, 3)],
    ("b", 30): [("dq1", 0, 0, 3), ("dq1", 1, 1, 3)],
    ("b", 31): [("dq0", 0, 0, 0), ("dq0", 1, 1, 0), ("ds0", "start"), ("ar0", 1, 0, 1)],
    ("b", 32): [("dq1", 0, 1, 2), ("dq1", 1, 0, 2), ("ar0", 0, 1, 1)],
    ("b", 33): [("ar0", 0, 0, 2), ("ar0", 1, 1, 2)],
    ("b", 34): [("dq1", 0, 0, 2), ("dq1", 1, 1, 2)],
    ("b", 35): [("dq1", 0, 1, 1), ("ds0", 0, 0, 1), ("ds0", 1, 1, 1), ("ds0", 0, 1, 1), ("ds0", 1, 0, 1), ("ar1", 0, 1, 3), ("ar1", 1, 0, 3), ("ar1", 0, 0, 4), ("ar1", 1, 1, 4), ("ar0", 1, 0, 0)],
    ("b", 36): [("dq2", 0, 0, 4), ("dq1", 1, 0, 1), ("ar0", 0, 1, 0), ("ar0", 0, 0, 1), ("ar0", 1, 1, 1)],
    ("b", 37): [("dq2", 1, 1, 4), ("dq1", 0, 0, 1), ("dq1", 1, 1, 1)],
    ("b", 38): [("dq1", 0, 1, 0), ("ds0", 1, 1, 2), ("ds0", 1, 0, 2)],
    ("b", 39): [("dq2", 0, 1, 3), ("ds0", 0, 0, 2), ("ds0", 0, 1, 2), ("ar1", 1, 0, 2)],
    ("b", 40): [("dq2", 1, 0, 3), ("ar1", 1, 1, 3), ("ar1", 0, 1, 2)],
    ("b", 41): [("dq1", 1, 0, 0), ("ar1", 0, 0, 3)],
    ("b", 42): [("dq2", 0, 0, 3), ("ar0", 1, 1, 0)],
    ("b", 43): [("dq2", 1, 1, 3), ("ar0", 0, 0, 0), ("as0", "start")],
    ("b", 44): [("dq1", 0, 0, 0), ("dq1", 1, 1, 0), ("ds1", "start"), ("ds0", 1, 1, 3)],
    ("b", 45): [("dq2", 0, 1, 2), ("ds0", 1, 0, 3), ("ds0", 0, 0, 3), ("ar1", 1, 0, 1), ("ds0", 0, 1, 3)],
    ("b", 46): [("dq2", 1, 0, 2), ("ar1", 0, 1, 1)],
    ("b", 47): [("dq2", 0, 0, 2), ("dq2", 1, 1, 2), ("ar2", 0, 1, 3), ("ar2", 1, 0, 3), ("ar2", 0, 0, 4), ("ar2", 1, 1, 4), ("ar1", 0, 0, 2), ("ar1", 1, 1, 2)],
    ("b", 5): [("dh", 0, 0, 2), ("dh", 1, 1, 2)],
    ("b", 6): [("dh", 0, 1, 2), ("dh", 1, 0, 2), ("st", 0, 0, 2), ("st", 1, 1, 2)],
    ("b", 7): [("st", 0, 1, 2), ("st", 1, 0, 2)],
    ("b", 9): [("dh", 0, 0, 3), ("dh", 1, 1, 3)],
    ("f", 1): [("ar2", 0, 1, 2), ("ar2", 1, 0, 2), ("ar2", 0, 0, 3), ("ar2", 1, 1, 3)],
    ("f", 10): [("dq2", 0, 0, 0), ("dq2", 1, 1, 0), ("ds2", "start")],
    ("f", 12): [("ar2", 0, 1, 1), ("ar2", 1, 0, 1)],
    ("f", 14): [("ar2", 0, 0, 2), ("ar2", 1, 1, 2)],
    ("f", 17): [("ds1", 0, 0, 3), ("ds1", 1, 1, 3), ("ar1", 0, 0, 0), ("ar1", 1, 1, 0), ("as1", "start"), ("as0", 0, 0, 3), ("as0", 1, 1, 3), ("as0", 0, 1, 3), ("as0", 1, 0, 3)],
    ("f", 19): [("ds1", 0, 1, 3), ("ds1", 1, 0, 3), ("ds2", 0, 0, 1), ("ds2", 1, 1, 1)],
    ("f", 21): [("ds2", 0, 1, 1), ("ds2", 1, 0, 1)],
    ("f", 23): [("ar2", 0, 1, 0), ("ar2", 1, 0, 0)],
    ("f", 25): [("ar2", 0, 0, 1), ("ar2", 1, 1, 1)],
    ("f", 26): [("ds1", 0, 0, 4), ("ds1", 1, 1, 4), ("as1", 0, 0, 1), ("as1", 1, 1, 1), ("as1", 0, 1, 1), ("as1", 1, 0, 1)],
    ("f", 28): [("as0", 0, 0, 4), ("as0", 1, 1, 4)],
    ("f", 3): [("ar1", 0, 0, 1), ("ar1", 1, 1, 1)],
    ("f", 30): [("ds2", 0, 0, 2), ("ds2", 1, 1, 2)],
    ("f", 32): [("ds2", 0, 1, 2), ("ds2", 1, 0, 2)],
    ("f", 34): [("ar2", 0, 0, 0), ("ar2", 1, 1, 0), ("as2", "start")],
    ("f", 35): [("ds2", 0, 0, 3), ("ds2", 1, 1, 3), ("ds2", 0, 1, 3), ("ds2", 1, 0, 3), ("as1", 0, 0, 2), ("as1", 1, 1, 2), ("as1", 0, 1, 2), ("as1", 1, 0, 2)],
    ("f", 5): [("as0", 0, 0, 2), ("as0", 1, 1, 2)],
    ("f", 7): [("as0", 0, 1, 2), ("as0", 1, 0, 2)],
    ("f", 8): [("dq2", 0, 1, 0), ("dq2", 1, 0, 0), ("ds1", 0, 0, 2), ("ds1", 1, 1, 2), ("ds1", 0, 1, 2), ("ds1", 1, 0, 2)],
    ("h", 0): [("as0", 0, 0, 1), ("as0", 1, 1, 1)],
    ("h", 1): [("as0", 0, 1, 1), ("as0", 1, 0, 1)],
    ("h", 2): [("ds1", 0, 0, 1), ("ds1", 1, 1, 1), ("ds1", 0, 1, 1), ("ds1", 1, 0, 1)],
    ("h", 3): [("ds0", 1, 1, 4)],
    ("h", 4): [("dq2", 0, 1, 1), ("ar1", 1, 0, 0), ("ds0", 0, 0, 4)],
    ("h", 6): [("dq2", 1, 0, 1), ("ar1", 0, 1, 0)],
    ("h", 7): [("dq2", 0, 0, 1), ("dq2", 1, 1, 1)],
    ("m", 0): [("as2", 0, 0, 1), ("as2", 1, 1, 1)],
    ("m", 1): [("as2", 0, 1, 1), ("as2", 1, 0, 1)],
    ("m", 3): [("ds2", 0, 0, 4), ("ds2", 1, 1, 4)],
    ("q", 0): [("as1", 0, 0, 3), ("as1", 1, 1, 3)],
    ("q", 2): [("as1", 0, 1, 3), ("as1", 1, 0, 3)],
    ("q", 3): [("as2", 0, 0, 2), ("as2", 1, 1, 2)],
    ("q", 5): [("as2", 0, 1, 2), ("as2", 1, 0, 2)],
    ("q", 7): [("as1", 0, 0, 4), ("as1", 1, 1, 4)],
    ("q", 8): [("as2", 0, 0, 3), ("as2", 1, 1, 3), ("as2", 0, 1, 3), ("as2", 1, 0, 3), ("as2", 0, 0, 4), ("as2", 1, 1, 4)],
    ("r", 12): [("dh", 0, 0, 4), ("dh", 1, 1, 4), ("att", "start"), ("st", 0, 0, 4), ("st", 1, 1, 4)],
}


class Ring:
    def __init__(self, chips):
        me = lax.axis_index('seq')
        self.chips = chips
        self.far = chips // 2
        self.z = me // 2
        self.core = me - 2 * self.z
        self.partner = 2 * self.z + 1 - self.core
        self.next = (2 * self.chip(1) + self.core, 2 * self.chip(-1) + self.core)
        self.hops = {(RIGHT, 0): self.far, (LEFT, 1): self.far, (RIGHT, 1): self.far - 1, (LEFT, 0): self.far - 1}

    def chip(self, off):
        return lax.rem(self.z + off + self.chips, self.chips)

    def ahead(self, d, k):
        return self.chip(k if d == RIGHT else -k)

    def enter(self):
        barrier = pltpu.get_barrier_semaphore()
        for dev in (self.partner,) + self.next:
            pl.semaphore_signal(barrier, inc=1, device_id={'seq': dev}, device_id_type=MESH)
        pl.semaphore_wait(barrier, 3)


def remote(src, dst, ssem, rsem, dev):
    return pltpu.make_async_remote_copy(src_ref=src, dst_ref=dst, send_sem=ssem, recv_sem=rsem, device_id={'seq': dev}, device_id_type=MESH)


def sent(every, ssem, rsem, dev):
    remote(every, every, ssem, rsem, dev).wait_send()


class Share:
    def __init__(self, ring, buf, src, sems):
        self.ring, self.buf, self.src = ring, buf, src
        self.ss, self.rs = sems

    def slot(self, chip, half):
        return self.buf.at[chip, half]

    def send(self, d, half, t):
        slot = self.slot(self.ring.ahead(d, 1 - t), half)
        src = self.src(half) if t == 1 else slot
        return remote(src, slot, self.ss.at[0], self.rs.at[d, half, t - 1], self.ring.next[d])

    def recv(self, d, half, t):
        slot = self.slot(self.ring.ahead(d, -t), half)
        return remote(slot, slot, self.ss.at[0], self.rs.at[d, half, t - 1], self.ring.next[d])

    def start(self):
        for d, half in self.ring.hops:
            self.send(d, half, 1).start()

    def came(self, d, half, t):
        pass

    def move(self, d, half, t):
        self.recv(d, half, t).wait_recv()
        if t < self.ring.hops[d, half]:
            self.send(d, half, t + 1).start()
        self.came(d, half, t)

    def drain(self):
        sent(self.buf.at[pl.ds(0, self.ring.chips - 1)], self.ss.at[0], self.rs.at[0, 0, 0], self.ring.next[0])


class Rows(Share):
    def __init__(self, ring, buf, src, sems):
        super().__init__(ring, buf, src, sems[:2])
        self.fs, self.fr, self.os, self.orr = sems[2:]

    def slot(self, chip, half):
        return self.buf.at[chip, self.ring.core, half]

    def pslot(self, chip, half):
        return self.buf.at[chip, 1 - self.ring.core, half]

    def start(self):
        super().start()
        for half in range(2):
            self.own(half).start()

    def own(self, half):
        return remote(self.src(half), self.slot(self.ring.z, half), self.os.at[0], self.orr.at[half], self.ring.partner)

    def forward(self, d, half, t):
        slot = self.slot(self.ring.ahead(d, -t), half)
        return remote(slot, slot, self.fs.at[0], self.fr.at[d, half, t - 1], self.ring.partner)

    def came(self, d, half, t):
        self.forward(d, half, t).start()

    def ready(self, off):
        ring = self.ring
        if off == 0:
            for half in range(2):
                slot = self.pslot(ring.z, half)
                remote(slot, slot, self.os.at[0], self.orr.at[half], ring.partner).wait_recv()
            return
        for (d, half), n in ring.hops.items():
            t = ring.far if abs(off) == ring.far else (-off if d == RIGHT else off)
            if 1 <= t <= n:
                slot = self.pslot(ring.ahead(d, -t), half)
                remote(slot, slot, self.fs.at[0], self.fr.at[d, half, t - 1], ring.partner).wait_recv()

    def drain(self):
        every = self.buf.at[pl.ds(0, self.ring.chips - 1), 0]
        sent(every, self.ss.at[0], self.rs.at[0, 0, 0], self.ring.next[0])
        sent(every, self.fs.at[0], self.fr.at[0, 0, 0], self.ring.partner)
        sent(self.buf.at[0, 0], self.os.at[0], self.orr.at[0], self.ring.partner)


class Reduce:
    def __init__(self, ring, part, rbuf, merge, sems):
        self.ring, self.part, self.rbuf, self.merge = ring, part, rbuf, merge
        self.ss, self.rs = sems

    def send(self, d, half, o):
        return remote(self.part.at[self.ring.ahead(d, o), half], self.rbuf.at[d, half, o - 1], self.ss.at[0], self.rs.at[d, half, o - 1], self.ring.next[d])

    def recv(self, d, half, o):
        slot = self.rbuf.at[d, half, o]
        return remote(slot, slot, self.ss.at[0], self.rs.at[d, half, o], self.ring.next[d])

    def move(self, d, half, o):
        if o < self.ring.hops[d, half]:
            self.recv(d, half, o).wait_recv()
            self.merge(self.part.at[self.ring.ahead(d, o), half], self.rbuf.at[d, half, o])
        if o > 0:
            self.send(d, half, o).start()

    def drain(self):
        sent(self.part.at[pl.ds(0, self.ring.chips - 1)], self.ss.at[0], self.rs.at[0, 0, 0], self.ring.next[0])


def pick(i, values):
    out = jnp.int32(values[-1])
    for k, v in enumerate(values[:-1]):
        out = jnp.where(i == k, jnp.int32(v), out)
    return out


def mask_lanes(ref, len_ref, start):
    row = lax.broadcasted_iota(jnp.int32, ref.shape, 0) + start
    lane = lax.broadcasted_iota(jnp.int32, ref.shape, 1)
    bias = jnp.where(row < len_ref[0], 0.0, -1e30)
    ref[...] = jnp.where(lane == 0, bias, jnp.where(lane < 4, 1.0, 0.0)).astype(BF16)


def dispatch(index, table):
    def branch(keys):
        if len(keys) == 1:
            def run():
                for fn in table[keys[0]]:
                    fn()
            pl.when(index == keys[0])(run)
            return
        low, high = keys[:len(keys) // 2], keys[len(keys) // 2:]
        pl.when(index < high[0])(functools.partial(branch, low))
        pl.when(index >= high[0])(functools.partial(branch, high))
    if table:
        branch(sorted(table))


def add_into(dst, src):
    dst[...] = dst[...] + src[...]


def parts3(x):
    hi = x.astype(BF16)
    rest = x - hi.astype(F32)
    mid = rest.astype(BF16)
    lo = (rest - mid.astype(F32)).astype(BF16)
    return hi, mid, lo


def bwd_kernel(dims, len_ref, dh_ref, own_ref, gn_ref, att_ref, y_ref, gh_ref, g1_ref, g2_ref,
               k_hbm, v_hbm, kt_hbm, qz_hbm, wo_hbm, wq_hbm, wk_hbm, wv_hbm, ma_hbm, mb_hbm, y_hbm, gog, wg_hbm, wu_hbm, wd_hbm,
               gvec_ref, gdec_ref, gmem, gwk, gwv, gwq, gwo, gdown, ggate, gup, attg,
               dqo_ref, k_ref, v_ref, kt_ref, qz_ref, wo_ref, wq_ref, wk_ref, wv_ref, ak_ref,
               dhg, doz, aqs, ads, stb, dk, dv, dkv, dkvp, dqp, dqr, dqa, arp, arr, ara, pvec, pdq, spb,
               msc, ybuf, abuf, wbuf, dbuf, wt, gst, gsw, gwo_s,
               *sems):
    chips, rows, mem, dim, hc, c, ff = dims
    QT = 2 * rows
    T = 2 * mem
    MC = min(256, mem)
    nm = T // MC
    inner = hc * 64
    np_ = hc // 2
    seg = 256 // chips // 2
    fh = ff // 2
    FT = wt.shape[1]
    nf = fh // FT
    ring = Ring(chips)
    z, core, far = ring.z, ring.core, ring.far
    sems = list(sems)

    def take(n):
        out = sems[:n]
        del sems[:n]
        return out

    half_rows = rows // 2
    part_ = functools.partial
    rsrc = lambda ref: (lambda half: ref.at[pl.ds(half * half_rows, half_rows)])
    dh_g = Rows(ring, dhg, rsrc(dh_ref), take(6))
    att_g = Rows(ring, attg, rsrc(att_ref), take(6))
    st_g = Share(ring, stb, lambda half: stb.at[z, half], take(2))
    dq_r = [Reduce(ring, dqp.at[p], dqr.at[p], add_into, take(2)) for p in range(np_)]
    dq_s = [Share(ring, dqa.at[p], lambda half, p=p: dqa.at[p, z, half], take(2)) for p in range(np_)]
    ar_r = [Reduce(ring, arp.at[p], arr.at[p], add_into, take(2)) for p in range(np_)]
    ar_s = [Share(ring, ara.at[p], lambda half, p=p: ara.at[p, z, half], take(2)) for p in range(np_)]
    xs, xr, ls, gs, gr, gl, wsem, ysem, lsem = take(9)
    loads = [pltpu.make_async_copy(src, dst, lsem.at[n]) for n, (src, dst) in enumerate((
        (wo_hbm, wo_ref), (k_hbm, k_ref), (v_hbm, v_ref), (kt_hbm, kt_ref), (qz_hbm, qz_ref),
        (ma_hbm, msc.at[0, pl.ds(0, mem)]), (mb_hbm, msc.at[1, pl.ds(0, mem)]), (wq_hbm, wq_ref), (wk_hbm, wk_ref), (wv_hbm, wv_ref)))]
    for cp in loads:
        cp.start()
    ring.enter()
    dh_g.start()
    locals_ = [pltpu.make_async_copy(att_ref.at[pl.ds(half * half_rows, half_rows)], attg.at[z, core, half], ls.at[half]) for half in range(2)]
    for cp in locals_:
        cp.start()
    for half in range(2):
        dhg[z, core, half] = dh_ref[half * half_rows:(half + 1) * half_rows, :]
    doz[...] = jnp.zeros_like(doz)
    mask_lanes(ak_ref, len_ref, z * T)
    hrow = pl.ds(pl.multiple_of(core * inner, inner), inner)
    hcol = pl.ds(pl.multiple_of(core * inner, 128), inner)
    other_cols = pl.ds(pl.multiple_of((1 - core) * mem, mem), mem)
    my_cols = pl.ds(pl.multiple_of(core * mem, mem), mem)
    qmine = pl.ds(pl.multiple_of(core * rows, rows), rows)
    qother = pl.ds(pl.multiple_of((1 - core) * rows, rows), rows)

    def lanes(chip):
        return pl.ds(pl.multiple_of(chip * QT, QT), QT)

    def d_out(chip):
        return mm_bt(wo_ref[hrow, :], dhg[chip].reshape(QT, dim))

    def prepare(chip, dot=None):
        dot = d_out(chip) if dot is None else dot
        dob = dot.astype(BF16)
        q = lanes(chip)
        row = lax.broadcasted_iota(jnp.int32, (16, QT), 0)
        for h in range(hc):
            lo = h * 128 + (h % 2) * 64
            doz[lo:lo + 64, q] = dob[h * 64:(h + 1) * 64]
            for ref, half, first in ((aqs, 0, 1.0), (ads, 1, 0.0)):
                a, b, e = (x.astype(F32) for x in parts3(stb[chip, half, h:h + 1, :]))
                ref[h * 16:(h + 1) * 16, q] = jnp.where(row == 0, first, jnp.where(row == 1, a, jnp.where(row == 2, b, jnp.where(row == 3, e, 0.0)))).astype(BF16)

    dh_g.ready(0)
    loads[0].wait()
    dot0 = d_out(z)
    prod = dot0 * own_ref[:inner, :]
    for h in range(hc):
        stb[z, 0, h:h + 1, :] = -own_ref[inner + h:inner + h + 1, :]
        stb[z, 1, h:h + 1, :] = -jnp.sum(prod[h * 64:(h + 1) * 64], axis=0, keepdims=True)
    stb[z, 0, hc:8, :] = gn_ref[0:8 - hc, :]
    stb[z, 1, hc:8, :] = gn_ref[8 - hc:16 - 2 * hc, :]
    st_g.start()
    prepare(z, dot0)
    dk[...] = jnp.zeros_like(dk)
    dv[...] = jnp.zeros_like(dv)
    for cp in loads[1:]:
        cp.wait()

    def tile(h, chip):
        pair = h // 2
        q = lanes(chip)
        hz = pl.ds(pl.multiple_of(h * 128, 128), 128)
        h16 = pl.ds(pl.multiple_of(h * 16, 16), 16)
        ps = pl.ds(pl.multiple_of(pair * 128, 128), 128)
        hz64 = pl.ds(pl.multiple_of(h * 128 + (h - 2 * pair) * 64, 64), 64)
        h64 = pl.ds(pl.multiple_of(h * 64, 64), 64)
        hr = h64
        q_t = qz_ref[hz64, q]
        do_t = doz[hz64, q]
        r1 = jnp.concatenate([qz_ref[hz, q], aqs[h16, q]], axis=0)
        r2 = jnp.concatenate([doz[hz, q], ads[h16, q]], axis=0)
        stage = {}
        dq = None
        for j in range(nm + 2):
            if j < nm:
                r = slice(j * MC, (j + 1) * MC)
                ak = ak_ref[r, 0:16]
                stage["a", j] = (mm(jnp.concatenate([k_ref[r, ps], ak], axis=1), r1), mm(jnp.concatenate([v_ref[r, ps], ak], axis=1), r2))
            if 1 <= j <= nm:
                s, dp = stage.pop(("a", j - 1))
                a = jnp.exp2(s * c)
                stage["b", j - 1] = (a.astype(BF16), (a * dp).astype(BF16))
            if j >= 2:
                r = slice((j - 2) * MC, (j - 1) * MC)
                pb, ds = stage.pop(("b", j - 2))
                dv[hr, r] += mm_bt(do_t, pb)
                dk[hr, r] += mm_bt(q_t, ds)
                d = mm(kt_ref[h64, r], ds)
                dq = d if dq is None else dq + d
        dqp[pair, chip, h - 2 * pair] = dq

    scale = 0.125

    def xp(p):
        return remote(dkv.at[p, :, other_cols], dkvp.at[p], xs.at[p], xr.at[p], ring.partner)

    def xq(p):
        return remote(dqa.at[p, z, :, :, qother], pdq.at[p], xs.at[np_ + p], xr.at[np_ + p], ring.partner)

    def share_dq(p):
        for half in range(2):
            dqa[p, z, half] = (dqp[p, z, half] * scale).astype(BF16)
        dq_s[p].start()
        xq(p).start()

    def share_ar(p):
        for half in range(2):
            ara[p, z, half] = arp[p, z, half]
        ar_s[p].start()

    moves = {"dh": dh_g, "st": st_g, "att": att_g}
    begins = {"att": att_g.start}
    for p in range(np_):
        moves.update({f"dq{p}": dq_r[p], f"ds{p}": dq_s[p], f"ar{p}": ar_r[p], f"as{p}": ar_s[p]})
        begins.update({f"ds{p}": part_(share_dq, p), f"as{p}": part_(share_ar, p)})

    def acts(*point):
        return [begins[e[0]] if e[1] == "start" else part_(moves[e[0]].move, *e[1:]) for e in BWD_PLAN.get(point, [])]

    def run(*point):
        for fn in acts(*point):
            fn()

    def table(kind, n):
        return {k: acts(kind, k) for k in range(n) if acts(kind, k)}

    offs = BWD_ORDER
    first = BWD_FIRST * hc
    per = 2 * (chips - BWD_FIRST)
    needs = {k * hc: offs[k] for k in range(1, BWD_FIRST)}
    needs.update({first + 2 * (k - BWD_FIRST): offs[k] for k in range(BWD_FIRST, chips)})

    def project(p):
        r = pl.ds(pl.multiple_of(p * 128, 128), 128)
        dkv[p, 0:128, :] = (dk[r, :] * scale).astype(BF16)
        dkv[p, 128:256, :] = dv[r, :].astype(BF16)
        xp(p).start()
        g = mm(dkv[p, :, my_cols], msc[0, 0:mem]) + mm(dkv[p, :, other_cols], msc[1, 0:mem])
        for n in range(2 * chips):
            arp[p, n // 2, n % 2] = g[n * seg:(n + 1) * seg]

    def body(it, carry):
        early = it < first
        b = it - first
        p = b // per
        r = b - p * per
        h = jnp.where(early, it % hc, 2 * p + r % 2)
        chip = ring.chip(pick(jnp.where(early, it // hc, BWD_FIRST + r // 2), offs))
        dispatch(it, {k: acts("r", k) + [part_(dh_g.ready, off)] for k, off in needs.items()})
        fresh = (early & (it > 0) & (it % hc == 0)) | ((b >= 0) & (b < per) & (r % 2 == 0))
        pl.when(fresh)(part_(prepare, chip))
        tile(h, chip)
        pl.when((b >= 0) & (r == per - 1))(part_(project, p))
        dispatch(it, table("b", chips * hc))
        return carry

    lax.fori_loop(0, chips * hc, body, 0)
    run("p", np_)
    near = range(1 - far, far + 1)

    for cp in locals_:
        cp.wait()
    for off in near:
        att_g.ready(off)
    gain2 = g2_ref[...].astype(F32)[None, :]
    gwo_s[...] = jnp.zeros_like(gwo_s)

    def y_fetch(ch, slot):
        return pltpu.make_async_copy(y_hbm.at[ch], ybuf.at[slot], ysem.at[slot, 0])

    def fetch(ch, slot):
        return (y_fetch(ch, slot), pltpu.make_async_copy(attg.at[ch], abuf.at[slot], ysem.at[slot, 1]))

    for cp in fetch(0, 0):
        cp.start()

    def hidden(ch, carry):
        slot = ch % 2
        for cp in fetch(ch, slot):
            cp.wait()

        @pl.when(ch + 1 < chips)
        def _():
            for cp in fetch(ch + 1, 1 - slot):
                cp.start()
        att = abuf[slot].reshape(QT, dim)
        h = (ybuf[slot].reshape(QT, dim).astype(F32) + mm(att, wo_ref[...])).astype(BF16)
        qz_ref[0:dim, lanes(ch)] = rms_norm(h.astype(F32), gain2).astype(BF16).T
        ah = jnp.where(core == 0, att[:, :inner], att[:, inner:])
        gwo_s[...] += mm_at(ah, dhg[ch].reshape(QT, dim))
        dispatch(ch, table("h", chips))
        return carry

    lax.fori_loop(0, chips, hidden, 0)
    dh_g.drain()
    go_load = pltpu.make_async_copy(gog, dhg, ls.at[0])
    go_load.start()

    def partner_block(buf, dst, k):
        return pltpu.make_async_copy(buf, dst, gl.at[k]), remote(buf, dst, gs.at[k], gr.at[k], ring.partner)

    def both_start(pair):
        pair[0].start()
        pair[1].start()

    def both_wait(pair):
        pair[0].wait()
        pair[1].wait()

    wo_out = partner_block(gwo_s, gwo.at[hrow], 3 * nf)
    both_start(wo_out)

    def w_fetch(f, slot):
        cols = pl.ds(pl.multiple_of(core * fh + f * FT, FT), FT)
        return (pltpu.make_async_copy(wg_hbm.at[:, cols], wbuf.at[0], wsem.at[slot, 0]),
                pltpu.make_async_copy(wu_hbm.at[:, cols], wbuf.at[1], wsem.at[slot, 1]),
                pltpu.make_async_copy(wd_hbm.at[cols], dbuf.at[slot], wsem.at[slot, 2]))

    for cp in w_fetch(0, 0):
        cp.start()
    go_load.wait()
    f_table = table("f", 9 * nf)

    def block(f, n):
        if n == 0:
            return partner_block(gst.at[f % 2, pl.ds(0, FT)], gdown.at[pl.ds(pl.multiple_of(core * fh + f * FT, FT), FT)], f)
        return partner_block(gsw.at[f % 2, n - 1], (ggate, gup)[n - 1].at[:, pl.ds(pl.multiple_of(core * fh + f * FT, FT), FT)], n * nf + f)

    def mlp(f, carry):
        slot = f % 2
        for cp in w_fetch(f, slot):
            cp.wait()

        for n in range(2):
            wt[n] = wbuf[n].T

        @pl.when(f + 1 < nf)
        def _():
            for cp in w_fetch(f + 1, 1 - slot):
                cp.start()

        def act_pair(k, cc):
            for ch in (2 * k, 2 * k + 1):
                q = lanes(ch)
                n2t = qz_ref[0:dim, q]
                g = mm(wt[0], n2t)
                u = mm(wt[1], n2t)
                ga = mm_bt(dbuf[slot], dhg[ch].reshape(QT, dim))
                sig = jax.nn.sigmoid(g)
                si = g * sig
                doz[0:FT, q] = (si * u).astype(BF16)
                doz[FT:2 * FT, q] = (ga * u * (sig + si * (1.0 - sig))).astype(BF16)
                doz[2 * FT:3 * FT, q] = (ga * si).astype(BF16)
            dispatch(f * 9 + 2 * k + 1, f_table)
            return cc

        lax.fori_loop(0, chips // 2, act_pair, 0)

        @pl.when(f > 1)
        def _():
            for n in range(3):
                both_wait(block(f - 2, n))
        acc = [None] * 3
        for ch in range(chips):
            q = slice(ch * QT, (ch + 1) * QT)
            n2t = qz_ref[0:dim, q]
            for n, d in enumerate((mm(doz[0:FT, q], dhg[ch].reshape(QT, dim)), mm_bt(n2t, doz[FT:2 * FT, q]), mm_bt(n2t, doz[2 * FT:3 * FT, q]))):
                acc[n] = d if acc[n] is None else acc[n] + d
        gst[slot, 0:FT] = acc[0]
        gsw[slot, 0] = acc[1]
        gsw[slot, 1] = acc[2]
        for n in range(3):
            both_start(block(f, n))
        dispatch(f * 9 + 8, f_table)
        return carry

    lax.fori_loop(0, nf, mlp, 0)
    for p in range(np_):
        remote(dkvp.at[p], dkvp.at[p], xs.at[p], xr.at[p], ring.partner).wait_recv()
    nb = 4
    w = mem // nb
    for f in (nf - 2, nf - 1):
        for n in range(3):
            both_wait(block(f, n))

    def gm(b):
        return pltpu.make_async_copy(gst.at[b % 2, pl.ds(0, w)], gmem.at[pl.ds(pl.multiple_of(b * w, w), w)], gl.at[3 * nf + 2 + b % 2])

    def memory_rows(b, carry):
        @pl.when(b > 1)
        def _():
            gm(b - 2).wait()
        cb = pl.ds(pl.multiple_of(core * mem + b * w, w), w)
        cp = pl.ds(pl.multiple_of(b * w, w), w)
        acc = None
        for p in range(np_):
            own_e = pl.ds(pl.multiple_of(core * inner + p * 128, 128), 128)
            oth_e = pl.ds(pl.multiple_of((1 - core) * inner + p * 128, 128), 128)
            for part, w_ref in ((0, wk_ref), (1, wv_ref)):
                e = slice(part * 128, (part + 1) * 128)
                lhs = jnp.concatenate([dkv[p, e, cb], dkvp[p, e, cp]], axis=0)
                rhs = jnp.concatenate([w_ref[:, own_e], w_ref[:, oth_e]], axis=1)
                d = mm_bt(lhs.T, rhs)
                acc = d if acc is None else acc + d
        gst[b % 2, 0:w] = acc
        gm(b).start()
        dispatch(b, table("m", nb))
        return carry

    lax.fori_loop(0, nb, memory_rows, 0)
    run("m", nb)

    gain = g1_ref[...].astype(F32)[None, :]
    y_fetch(0, 0).start()
    spb[...] = jnp.zeros_like(spb)
    both_wait(wo_out)
    gwq_s = gwo_s
    gwq_s[...] = jnp.zeros_like(gwq_s)
    wq_h = wq_ref[:, hcol]

    def query(ch, carry):
        slot = ch % 2
        y_fetch(ch, slot).wait()

        @pl.when(ch + 1 < chips)
        def _():
            y_fetch(ch + 1, 1 - slot).start()
        x = ybuf[slot].reshape(QT, dim).astype(F32)
        xhat = x * lax.rsqrt(jnp.mean(x * x, axis=-1, keepdims=True) + 1e-6)
        n1 = (xhat * gain).astype(BF16)
        dqc = jnp.concatenate([dqa[p, ch].reshape(128, QT) for p in range(np_)], axis=0)
        dn = mm_bt(dqc.T, wq_h)
        gwq_s[...] += mm(dqc, n1)
        spb[0:1, :] += jnp.sum(dn * xhat, axis=0, keepdims=True)
        dispatch(ch, table("q", chips))
        return carry

    lax.fori_loop(0, chips, query, 0)
    gvec2 = jnp.zeros((16 - 2 * hc, QT), F32)
    for ch in range(chips):
        gvec2 = gvec2 + jnp.concatenate([stb[ch, 0, hc:8, :], stb[ch, 1, hc:8, :]], axis=0)
    for n in range(dim // QT):
        spb[1:2, n * QT:(n + 1) * QT] = gvec2[n:n + 1]
    cv = remote(spb, pvec, xs.at[2 * np_], xr.at[2 * np_], ring.partner)
    cv.start()
    wq_out = partner_block(gwq_s, gwq.at[hrow], 3 * nf + 1)
    both_start(wq_out)
    for p in range(np_):
        own_r = pl.ds(pl.multiple_of(core * inner + p * 128, 128), 128)
        oth_r = pl.ds(pl.multiple_of((1 - core) * inner + p * 128, 128), 128)
        dqo_ref[own_r, :] = dqa[p, z, :, :, qmine].reshape(128, rows)
        xq(p).wait()
        dqo_ref[oth_r, :] = pdq[p].reshape(128, rows)
    x = y_ref[...].astype(F32)
    inv = lax.rsqrt(jnp.mean(x * x, axis=-1, keepdims=True) + 1e-6)
    xhat = x * inv
    t = mm_bt(dqo_ref[...].T, wq_ref[...]) * gain
    gdec_ref[...] = gh_ref[...] + inv * (t - xhat * jnp.mean(t * xhat, axis=-1, keepdims=True))
    run("q", chips)
    wkv_out = []
    for p in range(np_):
        for k, out in enumerate((gwk, gwv)):
            n = 2 * p + k
            src = ara.at[p, pl.ds(k * (chips // 2), chips // 2)]
            wkv_out.append(pltpu.make_async_copy(src, out.at[core, p], ls.at[2 + n]))
            wkv_out.append(remote(src, out.at[core, p], xs.at[2 * np_ + 1 + n], xr.at[2 * np_ + 1 + n], ring.partner))
    for cp in wkv_out:
        cp.start()
    for p in range(np_):
        xp(p).wait_send()
    cv.wait()
    gvec_ref[...] = spb[0:2] + pvec[0:2]
    both_wait(wq_out)
    for cp in wkv_out:
        cp.wait()
    for b in range(nb - 2, nb):
        gm(b).wait()
    for obj in [att_g, st_g] + dq_r + dq_s + ar_r + ar_s:
        obj.drain()


def bwd_call(dims, *args):
    chips, rows, mem, dim, hc, c, ff = dims
    inner = hc * 64
    QT = 2 * rows
    T = 2 * mem
    np_ = hc // 2
    h2 = chips // 2
    seg = 256 // chips // 2
    FT = ff // 8
    v = pl.BlockSpec(memory_space=VMEM)
    hbm = pl.BlockSpec(memory_space=pl.ANY)
    s3 = (2, 2, h2)
    rows_sems = [DMA((1,)), DMA(s3)] * 2 + [DMA((1,)), DMA((2,))]
    two = [DMA((1,)), DMA(s3)]
    S = jax.ShapeDtypeStruct
    gshape = (chips, 2, 2, rows // 2, dim)
    cols = chips * QT
    wsq = VMEM((dim, 2 * inner), BF16)
    return pl.pallas_call(
        functools.partial(bwd_kernel, dims),
        out_shape=(S((2, dim), F32), S((rows, dim), F32), S((mem, dim), F32), S((2, np_, chips // 2, 2, seg, dim), F32), S((2, np_, chips // 2, 2, seg, dim), F32), S((2 * inner, dim), F32), S((2 * inner, dim), F32),
                   S((ff, dim), F32), S((dim, ff), F32), S((dim, ff), F32), S(gshape, BF16)),
        in_specs=[pl.BlockSpec(memory_space=pltpu.SMEM)] + [v] * 8 + [hbm] * 15, out_specs=(v,) * 2 + (hbm,) * 9,
        scratch_shapes=[
            VMEM((2 * inner, rows), BF16), VMEM((T, inner), BF16), VMEM((T, inner), BF16), VMEM((inner, T), BF16), VMEM((hc * 128, cols), BF16), VMEM((2 * inner, dim), BF16), wsq, wsq, wsq, VMEM((T, 128), BF16),
            VMEM(gshape, BF16), VMEM((max(hc * 128, 3 * FT), cols), BF16), VMEM((hc * 16, cols), BF16), VMEM((hc * 16, cols), BF16),
            VMEM((chips, 2, 8, QT), F32), VMEM((inner, T), F32), VMEM((inner, T), F32), VMEM((np_, 256, T), BF16), VMEM((np_, 256, mem), BF16),
            VMEM((np_, chips, 2, 64, QT), F32), VMEM((np_, 2, 2, h2, 64, QT), F32), VMEM((np_, chips, 2, 64, QT), BF16),
            VMEM((np_, chips, 2, seg, dim), F32), VMEM((np_, 2, 2, h2, seg, dim), F32), VMEM((np_, chips, 2, seg, dim), F32),
            VMEM((8, dim), F32), VMEM((np_, 2, 64, rows), BF16), VMEM((8, dim), F32),
            VMEM((2, mem, dim), BF16), VMEM((2, 2, 2, rows // 2, dim), BF16), VMEM((2, 2, 2, rows // 2, dim), BF16),
            VMEM((2, dim, FT), BF16), VMEM((2, FT, dim), BF16), VMEM((2, FT, dim), BF16), VMEM((2, max(FT, mem // 4), dim), F32), VMEM((2, 2, dim, FT), F32),
            VMEM((inner, dim), F32)]
        + rows_sems * 2 + two * (1 + 4 * np_) + [DMA((4 * np_ + 1,))] * 2 + [DMA((2 + 2 * np_,)), DMA((14,)), DMA((14,)), DMA((16,)), DMA((2, 3)), DMA((2, 2)), DMA((10,))],
        compiler_params=pltpu.CompilerParams(vmem_limit_bytes=67_043_328, collective_id=1, has_side_effects=True),
        cost_estimate=pl.CostEstimate(flops=10**10, bytes_accessed=30 << 20, transcendentals=0),
        name="attn_bwd")(*args)


def finish_kernel(slots, *refs):
    n = (len(refs) - 3) // 2
    srcs, dsts, (buf, si, so) = refs[:n], refs[n:2 * n], refs[2 * n:]
    rows = buf.shape[1]
    moves = []
    for src, dst in zip(srcs, dsts):
        for c in range(0, src.shape[1], buf.shape[2]):
            wide = min(buf.shape[2], src.shape[1] - c)
            cols = pl.ds(c, wide)
            for r in range(0, src.shape[0], rows):
                k = len(moves) % slots
                w = min(rows, src.shape[0] - r)
                b = buf.at[k, pl.ds(0, w), pl.ds(0, wide)]
                moves.append((pltpu.make_async_copy(src.at[pl.ds(r, w), cols], b, si.at[k]), pltpu.make_async_copy(b, dst.at[pl.ds(r, w), cols], so.at[k])))
    lag = slots // 2
    for i in range(len(moves) + lag):
        if i < len(moves):
            if i >= slots:
                moves[i - slots][1].wait()
            moves[i][0].start()
        if i >= lag:
            moves[i - lag][0].wait()
            moves[i - lag][1].start()
    for m in moves[-slots:]:
        m[1].wait()


def finish_call(*arrays):
    slots, rows, cols = 24, 256, 1024
    hbm = pl.BlockSpec(memory_space=pl.ANY)
    return pl.pallas_call(
        functools.partial(finish_kernel, slots),
        out_shape=tuple(jax.ShapeDtypeStruct(a.shape, a.dtype) for a in arrays),
        in_specs=[hbm] * len(arrays), out_specs=(hbm,) * len(arrays),
        scratch_shapes=[VMEM((slots, rows, cols), F32), DMA((slots,)), DMA((slots,))],
        compiler_params=pltpu.CompilerParams(vmem_limit_bytes=67_043_328),
        name="finish")(*arrays)


def fwd_kernel(dims, len_ref, y_ref, go_ref, m_ref, g1_ref, g2_ref, wq_hbm, wk_hbm, wv_hbm, wo_hbm, wg_hbm, wu_hbm, wd_hbm,
               own, att_ref, dh_ref, gh_ref, gn_ref, k_out, v_out, kt_out, qz_out, mg_out, yall, gog,
               k_s, v_s, kt_s, qz, mg, wq_ref, wk_ref, wv_ref, ak_ref, yg, wqt, vt_s, s_scr, mx_scr, part, rbuf, patt, satt, gob, attt, wo_s, wg_s, wu_s, wd_s, n2_s, dn_s, *sems):
    chips, rows, mem, dim, hc, c, ff = dims
    QT = 2 * rows
    T = 2 * mem
    MC = min(256, mem)
    hh = hc // 2
    inner = hc * 64
    HR = hh * 64
    ring = Ring(chips)
    z, core, far = ring.z, ring.core, ring.far
    sub = rows // 2
    part_ = functools.partial
    xs, xr, ls = sems[14:]
    rsrc = lambda ref: (lambda half: ref.at[pl.ds(half * sub, sub)])
    y_g = Rows(ring, yg, rsrc(y_ref), sems[:6])
    go_g = Rows(ring, gog, rsrc(gob), sems[6:12])

    def merge(dst, src):
        for hl in range(hh):
            mr = slice(HR + hl, HR + hl + 1)
            lr = slice(HR + 8 + hl, HR + 9 + hl)
            m1, m2 = dst[mr, :], src[mr, :]
            m = jnp.maximum(m1, m2)
            a = jnp.exp2((m1 - m) * c)
            b = jnp.exp2((m2 - m) * c)
            rr = slice(hl * 64, (hl + 1) * 64)
            dst[rr, :] = dst[rr, :] * a + src[rr, :] * b
            dst[mr, :] = m
            dst[lr, :] = dst[lr, :] * a + src[lr, :] * b

    o_r = Reduce(ring, part, rbuf, merge, sems[12:14])
    loads = [pltpu.make_async_copy(src, dst, ls.at[7 + n]) for n, (src, dst) in enumerate((
        (wk_hbm, wk_ref), (wv_hbm, wv_ref), (wq_hbm, wq_ref), (wo_hbm, wo_s), (wg_hbm, wg_s), (wu_hbm, wu_s), (wd_hbm, wd_s)))]
    stores = [pltpu.make_async_copy(src, dst, ls.at[n]) for n, (src, dst) in enumerate(((k_s, k_out), (v_s, v_out), (kt_s, kt_out), (mg, mg_out), (qz, qz_out)))]
    for cp in loads[:3]:
        cp.start()
    ring.enter()
    y_g.start()
    mx_copy = remote(m_ref, mg, xs.at[0], xr.at[0], ring.partner)
    mx_copy.start()
    for cp in loads[3:]:
        cp.start()
    gob[...] = go_ref[...].astype(BF16)
    for half in range(2):
        yg[z, core, half] = y_ref[half * sub:(half + 1) * sub, :]
    hcol = pl.ds(pl.multiple_of(core * inner, 128), inner)
    qz[...] = jnp.zeros_like(qz)
    mask_lanes(ak_ref, len_ref, z * T)
    for cp in loads[:3]:
        cp.wait()
    wqt[...] = wq_ref[:, hcol].T
    wk = wk_ref[:, hcol]
    wv = wv_ref[:, hcol]

    moves = {"y": y_g, "go": go_g, "o": o_r}

    def acts(*point):
        return [go_g.start if e[1] == "start" else part_(moves[e[0]].move, *e[1:]) for e in FWD_PLAN.get(point, [])]

    def run(*point):
        for fn in acts(*point):
            fn()

    def project(src, base, blocks):
        for j in blocks:
            r = pl.ds(pl.multiple_of(base + j * MC, MC), MC)
            blk = src[j * MC:(j + 1) * MC, :]
            kb = mm(blk, wk).astype(BF16)
            vb = mm(blk, wv).astype(BF16)
            k_s[r, :] = kb
            v_s[r, :] = vb
            kt_s[:, r] = kb.T
            vt_s[:, r] = vb.T

    nb = mem // MC
    project(m_ref, core * mem, range(nb))
    run("s", 0)
    mx_copy.wait_recv()
    project(mg, (1 - core) * mem, range(nb // 2))
    run("s", 1)
    project(mg, (1 - core) * mem, range(nb // 2, nb))
    run("s", 2)
    for cp in stores[:4]:
        cp.start()
    gain = g1_ref[...].astype(F32)[None, :]
    one_row = jnp.where(lax.broadcasted_iota(jnp.int32, (16, QT), 0) == 0, 1.0, 0.0).astype(BF16)

    def lanes(chip):
        return pl.ds(pl.multiple_of(chip * QT, QT), QT)

    def prep(chip):
        n1 = rms_norm(yg[chip].reshape(QT, dim).astype(F32), gain).astype(BF16)
        qt = mm_bt(wqt[...], n1).astype(BF16)
        for h in range(hc):
            lo = h * 128 + (h % 2) * 64
            qz[lo:lo + 64, lanes(chip)] = qt[h * 64:(h + 1) * 64]

    def step(new, slot, old, pslot):
        if new is not None:
            chip, h = new
            rhs = jnp.concatenate([qz[pl.ds(pl.multiple_of(h * 128, 128), 128), lanes(chip)], one_row], axis=0)
            pair = pl.ds(pl.multiple_of((h // 2) * 128, 128), 128)
            mx = None
        if old is not None:
            ochip, half, hl = old
            m = jnp.max(mx_scr[pslot], axis=0, keepdims=True)
            vrow = pl.ds(pl.multiple_of((half * hh + hl) * 64, 64), 64)
            ls_ = None
            acc = None
        for j in range(T // MC):
            r = slice(j * MC, (j + 1) * MC)
            if new is not None:
                s = mm(jnp.concatenate([k_s[r, pair], ak_ref[r, 0:16]], axis=1), rhs)
                s_scr[slot, r, :] = s
                t = jnp.max(s.reshape(MC // 8, 8, QT), axis=0)
                mx = t if mx is None else jnp.maximum(mx, t)
            if old is not None:
                pr = jnp.exp2((s_scr[pslot, r, :] - m) * c)
                t = jnp.sum(pr.reshape(MC // 8, 8, QT), axis=0)
                ls_ = t if ls_ is None else ls_ + t
                dd = mm(vt_s[vrow, r], pr.astype(BF16))
                acc = dd if acc is None else acc + dd
        if new is not None:
            mx_scr[slot] = mx
        if old is not None:
            part[ochip, half, hl * 64:(hl + 1) * 64, :] = acc
            part[ochip, half, HR + hl:HR + hl + 1, :] = m
            part[ochip, half, HR + 8 + hl:HR + 9 + hl, :] = jnp.sum(ls_, axis=0, keepdims=True)

    offs = [o for o, _ in FWD_ORDER]
    halves = [h for _, h in FWD_ORDER]
    n = len(offs)
    fresh = [int(k + 1 < n and offs[k + 1] not in offs[:k + 1]) for k in range(n)]
    run("s", 3)
    y_g.ready(0)
    prep(z)
    step((z, halves[0] * hh), 0, None, None)

    def body(pair, carry):
        for u in range(2):
            i = 2 * pair + u
            i2 = jnp.minimum(i + 1, n - 1)
            chip, half = ring.chip(pick(i, offs)), pick(i, halves)
            chip2, half2 = ring.chip(pick(i2, offs)), pick(i2, halves)
            for k in range(hh):
                slot = (u * hh + k) % 2
                if k == hh - 1:
                    dispatch(pair, {kk // 2: acts("r", kk) + [part_(y_g.ready, offs[kk + 1])] for kk in range(u, n, 2) if fresh[kk]})
                    if any(fresh[u::2]):
                        pl.when(pick(i, fresh) == 1)(part_(prep, chip2))
                    new = (chip2, half2 * hh)
                else:
                    new = (chip, half * hh + k + 1)
                step(new, 1 - slot, (chip, half, k), slot)
                dispatch(pair, {kk // 2: acts("b", kk * hh + k) for kk in range(u, n, 2) if acts("b", kk * hh + k)})
        return carry

    gl = [pltpu.make_async_copy(gob.at[pl.ds(half * sub, sub)], gog.at[z, core, half], ls.at[5 + half]) for half in range(2)]
    for cp in gl:
        cp.start()
    lax.fori_loop(0, n // 2, body, 0)
    yc = pltpu.make_async_copy(yg, yall, ls.at[14])
    yc.start()
    stores[4].start()
    run("t", 0)
    run("t", 1)
    qmine = pl.ds(pl.multiple_of(core * rows, rows), rows)
    qother = pl.ds(pl.multiple_of((1 - core) * rows, rows), rows)
    for h in range(hc):
        half, hl = h // hh, h % hh
        m = part[z, half, HR + hl:HR + hl + 1, :]
        l = part[z, half, HR + 8 + hl:HR + 9 + hl, :]
        own[h * 64:(h + 1) * 64, :] = part[z, half, hl * 64:(hl + 1) * 64, :] / l
        own[inner + h:inner + h + 1, :] = m + jnp.log2(l) / c
    satt[...] = own[:inner, qother].astype(BF16)
    xo = remote(satt, patt, xs.at[1], xr.at[1], ring.partner)
    xo.start()
    attt[pl.ds(pl.multiple_of(core * inner, inner), inner), :] = own[:inner, qmine].astype(BF16)
    for cp in loads[3:]:
        cp.wait()
    run("t", 2)
    xo.wait()
    attt[pl.ds(pl.multiple_of((1 - core) * inner, inner), inner), :] = patt[...]

    att = attt[...].T
    att_ref[...] = att
    gain2 = g2_ref[...].astype(F32)[None, :]
    run("t", 3)
    hid = (y_ref[...].astype(F32) + mm(att, wo_s[...])).astype(BF16).astype(F32)
    inv = lax.rsqrt(jnp.mean(hid * hid, axis=-1, keepdims=True) + 1e-6)
    hhat = hid * inv
    n2 = (hhat * gain2).astype(BF16)
    fb = ff // 4
    n2_s[...] = n2
    dn_s[...] = jnp.zeros_like(dn_s)

    def mlp(f, carry):
        cols = pl.ds(pl.multiple_of(f * fb, fb), fb)
        wg, wu = wg_s[:, cols], wu_s[:, cols]
        g = mm(n2_s[...], wg)
        u = mm(n2_s[...], wu)
        ga = mm_bt(gob[...], wd_s[cols, :])
        sig = jax.nn.sigmoid(g)
        si = g * sig
        dn_s[...] += mm_bt((ga * u * (sig + si * (1.0 - sig))).astype(BF16), wg) + mm_bt((ga * si).astype(BF16), wu)
        dispatch(f, {n: acts("t", 4 + n) for n in range(4) if acts("t", 4 + n)})
        return carry

    lax.fori_loop(0, 4, mlp, 0)
    dn = dn_s[...]
    gsum = jnp.sum(dn * hhat, axis=0, keepdims=True)
    gn_ref[...] = jnp.zeros_like(gn_ref)
    for k in range(dim // QT):
        gn_ref[k:k + 1, :] = gsum[:, k * QT:(k + 1) * QT]
    t = dn * gain2
    gh = go_ref[...] + inv * (t - hhat * jnp.mean(t * hhat, axis=-1, keepdims=True))
    gh_ref[...] = gh
    dh_ref[...] = gh.astype(BF16)
    run("t", 8)
    for off in range(-far + 1, far + 1):
        go_g.ready(off)
    mx_copy.wait_send()
    for cp in [yc] + gl + stores:
        cp.wait()
    for obj in (y_g, go_g, o_r):
        obj.drain()


def fwd_call(dims, *args):
    chips, rows, mem, dim, hc, c, ff = dims
    hh = hc // 2
    inner = hc * 64
    QT = 2 * rows
    T = 2 * mem
    HR = hh * 64
    h2 = chips // 2
    v = pl.BlockSpec(memory_space=VMEM)
    hbm = pl.BlockSpec(memory_space=pl.ANY)
    S = jax.ShapeDtypeStruct
    s3 = (2, 2, h2)
    gshape = (chips, 2, 2, rows // 2, dim)
    rows_sems = [DMA((1,)), DMA(s3)] * 2 + [DMA((1,)), DMA((2,))]
    return pl.pallas_call(
        functools.partial(fwd_kernel, dims),
        out_shape=(S((inner + 8, QT), F32), S((rows, 2 * inner), BF16), S((rows, dim), BF16), S((rows, dim), F32), S((8, QT), F32),
                   S((T, inner), BF16), S((T, inner), BF16), S((inner, T), BF16), S((hc * 128, chips * QT), BF16), S((mem, dim), BF16), S(gshape, BF16), S(gshape, BF16)),
        in_specs=[pl.BlockSpec(memory_space=pltpu.SMEM)] + [v] * 5 + [hbm] * 7, out_specs=(v,) * 5 + (hbm,) * 7,
        scratch_shapes=[
            VMEM((T, inner), BF16), VMEM((T, inner), BF16), VMEM((inner, T), BF16), VMEM((hc * 128, chips * QT), BF16), VMEM((mem, dim), BF16),
            VMEM((dim, 2 * inner), BF16), VMEM((dim, 2 * inner), BF16), VMEM((dim, 2 * inner), BF16), VMEM((T, 128), BF16),
            VMEM(gshape, BF16), VMEM((inner, dim), BF16), VMEM((inner, T), BF16), VMEM((2, T, QT), F32), VMEM((2, 8, QT), F32),
            VMEM((chips, 2, HR + 16, QT), F32), VMEM((2, 2, h2, HR + 16, QT), F32), VMEM((inner, rows), BF16), VMEM((inner, rows), BF16),
            VMEM((rows, dim), BF16), VMEM((2 * inner, rows), BF16), VMEM((2 * inner, dim), BF16), VMEM((dim, ff), BF16), VMEM((dim, ff), BF16), VMEM((ff, dim), BF16), VMEM((rows, dim), BF16), VMEM((rows, dim), F32)]
        + rows_sems * 2 + [DMA((1,)), DMA(s3)] + [DMA((2,))] * 2 + [DMA((15,))],
        compiler_params=pltpu.CompilerParams(vmem_limit_bytes=62 * 1024 * 1024, collective_id=0, has_side_effects=True),
        cost_estimate=pl.CostEstimate(flops=10**10, bytes_accessed=30 << 20, transcendentals=0),
        name="attn_fwd")(*args)


def solution(mesh):
    group = mesh.shape['seq']
    row_spec = P(('data', 'seq'), None)
    part_vec = P('data')
    part_mat = P('data', None)
    part_cube = P('data', None, None)

    def device_step(dec_in, memory, mem_len, grad_out, norm_attn, wq, wk, wv, wo, norm_mlp, w_gate, w_up, w_down):
        rows, dim = dec_in.shape
        mem = memory.shape[0]
        heads, hd = wq.shape[1], wq.shape[2]
        inner = heads * hd
        chips = group // 2
        hc = heads // 2
        c = LOG2E * hd ** -0.5
        dims = (chips, rows, mem, dim, hc, c, w_gate.shape[1])
        wq2, wk2, wv2 = (w.reshape(dim, inner) for w in (wq, wk, wv))
        wo2 = wo.reshape(inner, dim)

        own, attended, dh, grad_hidden, gn, k_c, v_c, kt_c, qz, mem_p, y_all, go_all = fwd_call(
            dims, mem_len, dec_in, grad_out, memory, norm_attn, norm_mlp, wq2, wk2, wv2, wo2, w_gate, w_up, w_down)
        gvec, g_dec, g_mem, g_wk, g_wv, g_wq, g_wo, g_down, g_gate, g_up, _ = bwd_call(
            dims, mem_len, dh, own, gn, attended, dec_in, grad_hidden, norm_attn, norm_mlp,
            k_c, v_c, kt_c, qz, wo2, wq2, wk2, wv2, memory, mem_p, y_all, go_all, w_gate, w_up, w_down)
        cube = (dim, heads, hd)
        g_wk, g_wv = (g.reshape(inner, dim) for g in (g_wk, g_wv))
        g_mem, g_wq, g_wk, g_wv, g_wo, g_down, g_gate, g_up = finish_call(g_mem, g_wq, g_wk, g_wv, g_wo, g_down, g_gate, g_up)
        g_wq, g_wk, g_wv = (g.T.reshape(cube) for g in (g_wq, g_wk, g_wv))
        return (g_dec, g_mem, gvec[0], g_wq, g_wk, g_wv, g_wo.reshape(heads, hd, dim), gvec[1], g_gate, g_up, g_down)

    return jax.shard_map(device_step, mesh=mesh,
                         in_specs=(row_spec, row_spec, part_vec, row_spec) + (P(),) * 9,
                         out_specs=(row_spec, row_spec, part_vec, part_cube, part_cube, part_cube, part_cube, part_vec, part_mat, part_mat, part_mat),
                         check_vma=False)
```

```python
import functools
import math

import jax
import jax.numpy as jnp
from jax import lax
from jax.experimental import pallas as pl
from jax.experimental.pallas import tpu as pltpu
from jax.sharding import PartitionSpec as P

F32 = jnp.float32
BF16 = jnp.bfloat16
LOG2E = math.log2(math.e)
VMEM = pltpu.VMEM
MESH = pl.DeviceIdType.MESH


def mm(a, b):
    return jnp.dot(a, b, preferred_element_type=F32)


def mm_bt(a, b):
    return lax.dot_general(a, b, (((1,), (1,)), ((), ())), preferred_element_type=F32)


def mm_at(a, b):
    return lax.dot_general(a, b, (((0,), (0,)), ((), ())), preferred_element_type=F32)


def rms_norm(tensor, gain):
    mean_sq = jnp.mean(tensor * tensor, axis=-1, keepdims=True)
    return tensor * lax.rsqrt(mean_sq + 1e-6) * gain


RIGHT, LEFT = 0, 1
DMA = pltpu.SemaphoreType.DMA

FWD_ORDER = [(0, 0), (0, 1), (1, 0), (1, 1), (-3, 0), (3, 1), (4, 0), (4, 1), (3, 0), (-3, 1), (2, 0), (-2, 1), (2, 1), (-2, 0), (-1, 1), (-1, 0)]
BWD_ORDER = [0, 1, -1, 4, 3, -3, 2, -2]
BWD_FIRST = 2
FWD_PLAN = {
    ("b", 0): [("y", 0, 1, 1), ("y", 1, 0, 1)],
    ("b", 11): [("y", 1, 1, 3), ("y", 1, 0, 3)],
    ("b", 13): [("go", 0, 0, 1), ("go", 1, 1, 1)],
    ("b", 14): [("o", 1, 0, 3)],
    ("b", 16): [("go", 0, 1, 1)],
    ("b", 17): [("o", 0, 1, 3)],
    ("b", 18): [("go", 1, 0, 1)],
    ("b", 20): [("o", 0, 0, 4)],
    ("b", 21): [("go", 1, 1, 2)],
    ("b", 23): [("o", 1, 1, 4)],
    ("b", 31): [("go", 0, 0, 2)],
    ("b", 32): [("go", 1, 0, 2)],
    ("b", 34): [("go", 0, 1, 2)],
    ("b", 35): [("go", 1, 1, 3)],
    ("b", 36): [("o", 0, 0, 3)],
    ("b", 37): [("o", 1, 1, 3)],
    ("b", 38): [("o", 0, 1, 2)],
    ("b", 4): [("y", 0, 0, 2), ("y", 1, 1, 2)],
    ("b", 41): [("o", 1, 0, 2)],
    ("b", 42): [("go", 1, 0, 3)],
    ("b", 44): [("go", 0, 1, 3)],
    ("b", 45): [("go", 1, 1, 4)],
    ("b", 8): [("y", 0, 1, 2), ("y", 1, 0, 2)],
    ("b", 9): [("go", "start")],
    ("r", 3): [("y", 0, 0, 3), ("y", 0, 1, 3)],
    ("r", 5): [("y", 0, 0, 4), ("y", 1, 1, 4)],
    ("s", 1): [("y", 0, 0, 1), ("y", 1, 1, 1)],
    ("t", 1): [("o", 0, 0, 2), ("o", 1, 1, 2), ("o", 0, 1, 1), ("o", 1, 0, 1), ("o", 0, 0, 1), ("o", 1, 1, 1), ("o", 0, 1, 0), ("o", 1, 0, 0), ("o", 0, 0, 0), ("o", 1, 1, 0)],
    ("t", 2): [("go", 0, 0, 3)],
    ("t", 7): [("go", 0, 0, 4)],
}
BWD_PLAN = {
    ("b", 1): [("dh", 0, 0, 1), ("dh", 1, 1, 1)],
    ("b", 10): [("dh", 0, 1, 3), ("dh", 1, 0, 3), ("st", 0, 0, 3), ("st", 1, 1, 3)],
    ("b", 11): [("st", 0, 1, 3), ("st", 1, 0, 3)],
    ("b", 13): [("dh", 0, 0, 4), ("dh", 1, 1, 4), ("att", "start"), ("st", 0, 0, 4), ("st", 1, 1, 4)],
    ("b", 14): [("dq0", 0, 0, 4)],
    ("b", 15): [("dq0", 1, 1, 4)],
    ("b", 16): [("att", 0, 0, 1), ("att", 1, 1, 1)],
    ("b", 17): [("dq0", 0, 1, 3)],
    ("b", 18): [("dq0", 0, 0, 3), ("dq0", 1, 0, 3), ("att", 1, 0, 1), ("att", 0, 1, 1)],
    ("b", 19): [("dq0", 1, 1, 3)],
    ("b", 2): [("dh", 0, 1, 1), ("dh", 1, 0, 1), ("st", 0, 0, 1), ("st", 1, 1, 1), ("st", 0, 1, 1), ("st", 1, 0, 1)],
    ("b", 20): [("att", 0, 0, 2)],
    ("b", 21): [("dq0", 0, 1, 2), ("att", 1, 1, 2)],
    ("b", 22): [("dq0", 1, 0, 2), ("dq0", 0, 0, 2)],
    ("b", 23): [("dq0", 1, 1, 2), ("att", 1, 0, 2), ("att", 0, 1, 2), ("ar0", 0, 1, 3), ("ar0", 1, 0, 3), ("ar0", 0, 0, 4), ("ar0", 1, 1, 4)],
    ("b", 24): [("dq0", 0, 1, 1)],
    ("b", 25): [("dq0", 1, 0, 1), ("dq0", 0, 0, 1)],
    ("b", 26): [("dq0", 1, 1, 1), ("dq1", 0, 0, 4)],
    ("b", 27): [("dq1", 1, 1, 4)],
    ("b", 28): [("att", 0, 1, 3), ("ar0", 0, 1, 2)],
    ("b", 29): [("dq1", 0, 1, 3), ("att", 1, 1, 3), ("att", 1, 0, 3), ("ar0", 0, 0, 3), ("ar0", 1, 0, 2), ("dq0", 0, 1, 0), ("ar0", 1, 1, 3)],
    ("b", 30): [("dq0", 1, 0, 0), ("dq0", 0, 0, 0), ("dq1", 1, 0, 3)],
    ("b", 31): [("dq0", 1, 1, 0), ("ds0", "start"), ("dq1", 0, 0, 3)],
    ("b", 32): [("dq1", 1, 1, 3), ("ar0", 0, 1, 1)],
    ("b", 33): [("dq1", 0, 1, 2)],
    ("b", 34): [("ar0", 0, 0, 2), ("ar0", 1, 0, 1), ("ds0", 0, 0, 1)],
    ("b", 35): [("dq1", 0, 0, 2), ("dq1", 1, 0, 2), ("att", 1, 1, 4), ("ar1", 0, 1, 3), ("ar1", 1, 0, 3), ("ar1", 0, 0, 4), ("ar1", 1, 1, 4), ("ar0", 1, 1, 2), ("ds0", 0, 1, 1)],
    ("b", 36): [("ar0", 0, 1, 0), ("ds0", 1, 1, 1), ("ds0", 1, 0, 1)],
    ("b", 37): [("dq1", 0, 1, 1), ("dq1", 1, 1, 2), ("ar0", 0, 0, 1)],
    ("b", 38): [("dq2", 0, 0, 4), ("ar0", 1, 0, 0), ("ds0", 0, 0, 2)],
    ("b", 39): [("dq1", 0, 0, 1), ("dq1", 1, 0, 1), ("dq2", 1, 1, 4), ("ar1", 0, 1, 2), ("ar1", 1, 0, 2)],
    ("b", 40): [("ar1", 0, 0, 3), ("ar1", 1, 1, 3)],
    ("b", 41): [("dq2", 0, 1, 3), ("ar0", 1, 1, 1), ("ds0", 0, 1, 2), ("ds0", 1, 1, 2)],
    ("b", 42): [("dq1", 0, 1, 0), ("dq2", 1, 0, 3), ("ar0", 0, 0, 0), ("ds0", 1, 0, 2)],
    ("b", 43): [("dq1", 1, 1, 1), ("dq2", 0, 0, 3)],
    ("b", 44): [("dq1", 1, 0, 0), ("ds0", 0, 0, 3)],
    ("b", 45): [("dq1", 0, 0, 0), ("dq2", 1, 1, 3)],
    ("b", 46): [("att", 0, 0, 3), ("ar1", 0, 1, 1), ("ar1", 1, 0, 1), ("ar1", 0, 0, 2), ("ar1", 1, 1, 2)],
    ("b", 47): [("dq2", 0, 1, 2), ("ar2", 0, 1, 3), ("ar2", 1, 0, 3), ("ar2", 0, 0, 4), ("ar2", 1, 1, 4), ("ar0", 1, 1, 0), ("as0", "start"), ("ds0", 1, 1, 3), ("dq2", 1, 0, 2), ("ds0", 0, 1, 3)],
    ("b", 5): [("dh", 0, 0, 2), ("dh", 1, 1, 2)],
    ("b", 6): [("dh", 0, 1, 2), ("dh", 1, 0, 2), ("st", 0, 0, 2), ("st", 1, 1, 2)],
    ("b", 7): [("st", 0, 1, 2), ("st", 1, 0, 2)],
    ("b", 9): [("dh", 0, 0, 3), ("dh", 1, 1, 3)],
    ("f", 1): [("dq2", 1, 1, 1), ("dq2", 0, 1, 0), ("ar2", 1, 0, 1), ("ar1", 0, 0, 0)],
    ("f", 10): [("dq2", 0, 0, 0), ("ds1", 1, 0, 2)],
    ("f", 12): [("dq2", 1, 1, 0), ("ds2", "start"), ("ar2", 0, 1, 0)],
    ("f", 14): [("ar2", 1, 0, 0), ("as1", 0, 0, 1)],
    ("f", 16): [("as1", 0, 1, 1), ("as1", 1, 1, 1)],
    ("f", 17): [("ar2", 0, 0, 1), ("ar2", 1, 1, 1), ("as1", 1, 0, 1), ("as0", 0, 0, 3), ("as0", 0, 1, 3), ("as0", 1, 1, 3)],
    ("f", 19): [("ds1", 0, 0, 3), ("as0", 1, 0, 3)],
    ("f", 21): [("ds1", 0, 1, 3), ("ds1", 1, 1, 3)],
    ("f", 23): [("ds2", 0, 0, 1), ("ds1", 1, 0, 3), ("ds2", 0, 1, 1)],
    ("f", 25): [("ds2", 1, 1, 1)],
    ("f", 26): [("ar2", 0, 0, 0), ("ar2", 1, 1, 0), ("as2", "start"), ("as1", 0, 0, 2), ("as1", 0, 1, 2), ("as1", 1, 1, 2), ("as0", 0, 0, 4), ("as1", 1, 0, 2), ("ds2", 1, 0, 1)],
    ("f", 28): [("ds1", 0, 0, 4)],
    ("f", 3): [("ar2", 0, 1, 1), ("ar1", 1, 1, 0), ("as1", "start")],
    ("f", 30): [("as0", 1, 1, 4), ("ds2", 0, 0, 2), ("ds1", 1, 1, 4)],
    ("f", 32): [("ds2", 0, 1, 2), ("ds2", 1, 1, 2)],
    ("f", 34): [("as2", 0, 0, 1), ("as2", 1, 1, 1)],
    ("f", 35): [("as2", 0, 1, 1), ("as2", 1, 0, 1), ("as1", 0, 0, 3), ("as1", 1, 1, 3), ("as1", 0, 1, 3), ("as1", 1, 0, 3)],
    ("f", 5): [("ar2", 1, 1, 2), ("ar2", 0, 0, 2)],
    ("f", 7): [("as0", 1, 1, 2), ("as0", 0, 0, 2)],
    ("f", 8): [("dq2", 1, 0, 0), ("as0", 1, 0, 2), ("as0", 0, 1, 2), ("ds1", 0, 0, 2), ("ds1", 0, 1, 2), ("ds1", 1, 1, 2)],
    ("h", 0): [("dq1", 1, 1, 0), ("ds1", "start"), ("dq2", 0, 0, 2), ("dq2", 1, 1, 2), ("dq2", 0, 1, 1), ("ar2", 1, 0, 2), ("ar1", 0, 1, 0), ("ar1", 1, 0, 0), ("ar1", 0, 0, 1), ("ar1", 1, 1, 1), ("ds0", 1, 0, 3), ("ds0", 0, 0, 4)],
    ("h", 1): [("ar2", 0, 1, 2), ("ar2", 1, 1, 3)],
    ("h", 2): [("ar2", 0, 0, 3), ("as0", 1, 1, 1)],
    ("h", 3): [("as0", 0, 0, 1), ("as0", 1, 0, 1)],
    ("h", 4): [("as0", 0, 1, 1), ("ds0", 1, 1, 4)],
    ("h", 5): [("dq2", 1, 0, 1), ("ds1", 0, 0, 1), ("ds1", 0, 1, 1)],
    ("h", 6): [("ds1", 1, 1, 1), ("ds1", 1, 0, 1)],
    ("h", 7): [("dq2", 0, 0, 1)],
    ("m", 0): [("ds2", 0, 0, 3), ("ds2", 1, 0, 2)],
    ("m", 1): [("ds2", 0, 1, 3), ("ds2", 1, 1, 3)],
    ("m", 2): [("as2", 0, 0, 2), ("as2", 1, 1, 2)],
    ("m", 3): [("as2", 0, 1, 2), ("as2", 1, 0, 2)],
    ("m", 4): [("ds2", 0, 0, 4), ("ds2", 1, 0, 3), ("ds2", 1, 1, 4)],
    ("p", 3): [("att", 0, 0, 4)],
    ("q", 0): [("as1", 0, 0, 4), ("as1", 1, 1, 4), ("as2", 0, 0, 3)],
    ("q", 1): [("as2", 1, 1, 3)],
    ("q", 2): [("as2", 0, 1, 3)],
    ("q", 3): [("as2", 1, 0, 3)],
    ("q", 6): [("as2", 0, 0, 4)],
    ("q", 7): [("as2", 1, 1, 4)],
}


class Ring:
    def __init__(self, chips):
        me = lax.axis_index('seq')
        self.chips = chips
        self.far = chips // 2
        self.z = me // 2
        self.core = me - 2 * self.z
        self.partner = 2 * self.z + 1 - self.core
        self.next = (2 * self.chip(1) + self.core, 2 * self.chip(-1) + self.core)
        self.hops = {(RIGHT, 0): self.far, (LEFT, 1): self.far, (RIGHT, 1): self.far - 1, (LEFT, 0): self.far - 1}

    def chip(self, off):
        return lax.rem(self.z + off + self.chips, self.chips)

    def ahead(self, d, k):
        return self.chip(k if d == RIGHT else -k)

    def enter(self):
        barrier = pltpu.get_barrier_semaphore()
        for dev in (self.partner,) + self.next:
            pl.semaphore_signal(barrier, inc=1, device_id={'seq': dev}, device_id_type=MESH)
        pl.semaphore_wait(barrier, 3)


def remote(src, dst, ssem, rsem, dev):
    return pltpu.make_async_remote_copy(src_ref=src, dst_ref=dst, send_sem=ssem, recv_sem=rsem, device_id={'seq': dev}, device_id_type=MESH)


def sent(every, ssem, rsem, dev):
    remote(every, every, ssem, rsem, dev).wait_send()


class Share:
    def __init__(self, ring, buf, src, sems):
        self.ring, self.buf, self.src = ring, buf, src
        self.ss, self.rs = sems

    def slot(self, chip, half):
        return self.buf.at[chip, half]

    def send(self, d, half, t):
        slot = self.slot(self.ring.ahead(d, 1 - t), half)
        src = self.src(half) if t == 1 else slot
        return remote(src, slot, self.ss.at[0], self.rs.at[d, half, t - 1], self.ring.next[d])

    def recv(self, d, half, t):
        slot = self.slot(self.ring.ahead(d, -t), half)
        return remote(slot, slot, self.ss.at[0], self.rs.at[d, half, t - 1], self.ring.next[d])

    def start(self):
        for d, half in self.ring.hops:
            self.send(d, half, 1).start()

    def came(self, d, half, t):
        pass

    def move(self, d, half, t):
        self.recv(d, half, t).wait_recv()
        if t < self.ring.hops[d, half]:
            self.send(d, half, t + 1).start()
        self.came(d, half, t)

    def drain(self):
        sent(self.buf.at[pl.ds(0, self.ring.chips - 1)], self.ss.at[0], self.rs.at[0, 0, 0], self.ring.next[0])


class Rows(Share):
    def __init__(self, ring, buf, src, sems):
        super().__init__(ring, buf, src, sems[:2])
        self.fs, self.fr, self.os, self.orr = sems[2:]

    def slot(self, chip, half):
        return self.buf.at[chip, self.ring.core, half]

    def pslot(self, chip, half):
        return self.buf.at[chip, 1 - self.ring.core, half]

    def start(self):
        super().start()
        for half in range(2):
            self.own(half).start()

    def own(self, half):
        return remote(self.src(half), self.slot(self.ring.z, half), self.os.at[0], self.orr.at[half], self.ring.partner)

    def forward(self, d, half, t):
        slot = self.slot(self.ring.ahead(d, -t), half)
        return remote(slot, slot, self.fs.at[0], self.fr.at[d, half, t - 1], self.ring.partner)

    def came(self, d, half, t):
        self.forward(d, half, t).start()

    def ready(self, off):
        ring = self.ring
        if off == 0:
            for half in range(2):
                slot = self.pslot(ring.z, half)
                remote(slot, slot, self.os.at[0], self.orr.at[half], ring.partner).wait_recv()
            return
        for (d, half), n in ring.hops.items():
            t = ring.far if abs(off) == ring.far else (-off if d == RIGHT else off)
            if 1 <= t <= n:
                slot = self.pslot(ring.ahead(d, -t), half)
                remote(slot, slot, self.fs.at[0], self.fr.at[d, half, t - 1], ring.partner).wait_recv()

    def drain(self):
        every = self.buf.at[pl.ds(0, self.ring.chips - 1), 0]
        sent(every, self.ss.at[0], self.rs.at[0, 0, 0], self.ring.next[0])
        sent(every, self.fs.at[0], self.fr.at[0, 0, 0], self.ring.partner)
        sent(self.buf.at[0, 0], self.os.at[0], self.orr.at[0], self.ring.partner)


class Reduce:
    def __init__(self, ring, part, rbuf, merge, sems):
        self.ring, self.part, self.rbuf, self.merge = ring, part, rbuf, merge
        self.ss, self.rs = sems

    def send(self, d, half, o):
        return remote(self.part.at[self.ring.ahead(d, o), half], self.rbuf.at[d, half, o - 1], self.ss.at[0], self.rs.at[d, half, o - 1], self.ring.next[d])

    def recv(self, d, half, o):
        slot = self.rbuf.at[d, half, o]
        return remote(slot, slot, self.ss.at[0], self.rs.at[d, half, o], self.ring.next[d])

    def move(self, d, half, o):
        if o < self.ring.hops[d, half]:
            self.recv(d, half, o).wait_recv()
            self.merge(self.part.at[self.ring.ahead(d, o), half], self.rbuf.at[d, half, o])
        if o > 0:
            self.send(d, half, o).start()

    def drain(self):
        sent(self.part.at[pl.ds(0, self.ring.chips - 1)], self.ss.at[0], self.rs.at[0, 0, 0], self.ring.next[0])


def pick(i, values):
    out = jnp.int32(values[-1])
    for k, v in enumerate(values[:-1]):
        out = jnp.where(i == k, jnp.int32(v), out)
    return out


def mask_lanes(ref, len_ref, start):
    row = lax.broadcasted_iota(jnp.int32, ref.shape, 0) + start
    lane = lax.broadcasted_iota(jnp.int32, ref.shape, 1)
    bias = jnp.where(row < len_ref[0], 0.0, -1e30)
    ref[...] = jnp.where(lane == 0, bias, jnp.where(lane < 4, 1.0, 0.0)).astype(BF16)


def dispatch(index, table):
    def branch(keys):
        if len(keys) == 1:
            def run():
                for fn in table[keys[0]]:
                    fn()
            pl.when(index == keys[0])(run)
            return
        low, high = keys[:len(keys) // 2], keys[len(keys) // 2:]
        pl.when(index < high[0])(functools.partial(branch, low))
        pl.when(index >= high[0])(functools.partial(branch, high))
    if table:
        branch(sorted(table))


def add_into(dst, src):
    dst[...] = dst[...] + src[...]


def parts3(x):
    hi = x.astype(BF16)
    rest = x - hi.astype(F32)
    mid = rest.astype(BF16)
    lo = (rest - mid.astype(F32)).astype(BF16)
    return hi, mid, lo


def bwd_kernel(dims, len_ref, dh_ref, own_ref, gn_ref, att_ref, y_ref, gh_ref, g1_ref, g2_ref,
               k_hbm, v_hbm, kt_hbm, qz_hbm, wo_hbm, wq_hbm, wk_hbm, wv_hbm, ma_hbm, mb_hbm, y_hbm, gog, wg_hbm, wu_hbm, wd_hbm,
               gvec_ref, gdec_ref, gmem, gwk, gwv, gwq, gwo, gdown, ggate, gup, attg,
               dqo_ref, k_ref, v_ref, kt_ref, qz_ref, wo_ref, wq_ref, wk_ref, wv_ref, ak_ref,
               dhg, doz, aqs, ads, stb, dk, dv, dkv, dkvp, dqp, dqr, dqa, arp, arr, ara, pvec, pdq, spb,
               msc, ybuf, abuf, wbuf, dbuf, wt, gst, gsw, gwo_s,
               *sems):
    chips, rows, mem, dim, hc, c, ff = dims
    QT = 2 * rows
    T = 2 * mem
    MC = min(256, mem)
    nm = T // MC
    inner = hc * 64
    np_ = hc // 2
    seg = 256 // chips // 2
    fh = ff // 2
    FT = wt.shape[1]
    nf = fh // FT
    ring = Ring(chips)
    z, core, far = ring.z, ring.core, ring.far
    sems = list(sems)

    def take(n):
        out = sems[:n]
        del sems[:n]
        return out

    half_rows = rows // 2
    part_ = functools.partial
    rsrc = lambda ref: (lambda half: ref.at[pl.ds(half * half_rows, half_rows)])
    dh_g = Rows(ring, dhg, rsrc(dh_ref), take(6))
    att_g = Rows(ring, attg, rsrc(att_ref), take(6))
    st_g = Share(ring, stb, lambda half: stb.at[z, half], take(2))
    dq_r = [Reduce(ring, dqp.at[p], dqr.at[p], add_into, take(2)) for p in range(np_)]
    dq_s = [Share(ring, dqa.at[p], lambda half, p=p: dqa.at[p, z, half], take(2)) for p in range(np_)]
    ar_r = [Reduce(ring, arp.at[p], arr.at[p], add_into, take(2)) for p in range(np_)]
    ar_s = [Share(ring, ara.at[p], lambda half, p=p: ara.at[p, z, half], take(2)) for p in range(np_)]
    xs, xr, ls, gs, gr, gl, wsem, ysem, lsem = take(9)
    loads = [pltpu.make_async_copy(src, dst, lsem.at[n]) for n, (src, dst) in enumerate((
        (wo_hbm, wo_ref), (k_hbm, k_ref), (v_hbm, v_ref), (kt_hbm, kt_ref), (qz_hbm, qz_ref),
        (ma_hbm, msc.at[0, pl.ds(0, mem)]), (mb_hbm, msc.at[1, pl.ds(0, mem)]), (wq_hbm, wq_ref), (wk_hbm, wk_ref), (wv_hbm, wv_ref)))]
    for cp in loads:
        cp.start()
    ring.enter()
    dh_g.start()
    locals_ = [pltpu.make_async_copy(att_ref.at[pl.ds(half * half_rows, half_rows)], attg.at[z, core, half], ls.at[half]) for half in range(2)]
    for cp in locals_:
        cp.start()
    for half in range(2):
        dhg[z, core, half] = dh_ref[half * half_rows:(half + 1) * half_rows, :]
    doz[...] = jnp.zeros_like(doz)
    mask_lanes(ak_ref, len_ref, z * T)
    hrow = pl.ds(pl.multiple_of(core * inner, inner), inner)
    hcol = pl.ds(pl.multiple_of(core * inner, 128), inner)
    other_cols = pl.ds(pl.multiple_of((1 - core) * mem, mem), mem)
    my_cols = pl.ds(pl.multiple_of(core * mem, mem), mem)
    qmine = pl.ds(pl.multiple_of(core * rows, rows), rows)
    qother = pl.ds(pl.multiple_of((1 - core) * rows, rows), rows)

    def lanes(chip):
        return pl.ds(pl.multiple_of(chip * QT, QT), QT)

    def d_out(chip):
        return mm_bt(wo_ref[hrow, :], dhg[chip].reshape(QT, dim))

    def prepare(chip, dot=None):
        dot = d_out(chip) if dot is None else dot
        dob = dot.astype(BF16)
        q = lanes(chip)
        row = lax.broadcasted_iota(jnp.int32, (16, QT), 0)
        for h in range(hc):
            lo = h * 128 + (h % 2) * 64
            doz[lo:lo + 64, q] = dob[h * 64:(h + 1) * 64]
            for ref, half, first in ((aqs, 0, 1.0), (ads, 1, 0.0)):
                a, b, e = (x.astype(F32) for x in parts3(stb[chip, half, h:h + 1, :]))
                ref[h * 16:(h + 1) * 16, q] = jnp.where(row == 0, first, jnp.where(row == 1, a, jnp.where(row == 2, b, jnp.where(row == 3, e, 0.0)))).astype(BF16)

    dh_g.ready(0)
    loads[0].wait()
    dot0 = d_out(z)
    prod = dot0 * own_ref[:inner, :]
    for h in range(hc):
        stb[z, 0, h:h + 1, :] = -own_ref[inner + h:inner + h + 1, :]
        stb[z, 1, h:h + 1, :] = -jnp.sum(prod[h * 64:(h + 1) * 64], axis=0, keepdims=True)
    stb[z, 0, hc:8, :] = gn_ref[0:8 - hc, :]
    stb[z, 1, hc:8, :] = gn_ref[8 - hc:16 - 2 * hc, :]
    st_g.start()
    prepare(z, dot0)
    dk[...] = jnp.zeros_like(dk)
    dv[...] = jnp.zeros_like(dv)
    for cp in loads[1:]:
        cp.wait()

    def tile(h, chip):
        pair = h // 2
        q = lanes(chip)
        hz = pl.ds(pl.multiple_of(h * 128, 128), 128)
        h16 = pl.ds(pl.multiple_of(h * 16, 16), 16)
        ps = pl.ds(pl.multiple_of(pair * 128, 128), 128)
        hz64 = pl.ds(pl.multiple_of(h * 128 + (h - 2 * pair) * 64, 64), 64)
        h64 = pl.ds(pl.multiple_of(h * 64, 64), 64)
        hr = h64
        q_t = qz_ref[hz64, q]
        do_t = doz[hz64, q]
        r1 = jnp.concatenate([qz_ref[hz, q], aqs[h16, q]], axis=0)
        r2 = jnp.concatenate([doz[hz, q], ads[h16, q]], axis=0)
        stage = {}
        dq = None
        for j in range(nm + 2):
            if j < nm:
                r = slice(j * MC, (j + 1) * MC)
                ak = ak_ref[r, 0:16]
                stage["a", j] = (mm(jnp.concatenate([k_ref[r, ps], ak], axis=1), r1), mm(jnp.concatenate([v_ref[r, ps], ak], axis=1), r2))
            if 1 <= j <= nm:
                s, dp = stage.pop(("a", j - 1))
                a = jnp.exp2(s * c)
                stage["b", j - 1] = (a.astype(BF16), (a * dp).astype(BF16))
            if j >= 2:
                r = slice((j - 2) * MC, (j - 1) * MC)
                pb, ds = stage.pop(("b", j - 2))
                dv[hr, r] += mm_bt(do_t, pb)
                dk[hr, r] += mm_bt(q_t, ds)
                d = mm(kt_ref[h64, r], ds)
                dq = d if dq is None else dq + d
        dqp[pair, chip, h - 2 * pair] = dq

    scale = 0.125

    def xp(p):
        return remote(dkv.at[p, :, other_cols], dkvp.at[p], xs.at[p], xr.at[p], ring.partner)

    def xq(p):
        return remote(dqa.at[p, z, :, :, qother], pdq.at[p], xs.at[np_ + p], xr.at[np_ + p], ring.partner)

    def share_dq(p):
        for half in range(2):
            dqa[p, z, half] = (dqp[p, z, half] * scale).astype(BF16)
        dq_s[p].start()
        xq(p).start()

    def share_ar(p):
        for half in range(2):
            ara[p, z, half] = arp[p, z, half]
        ar_s[p].start()

    moves = {"dh": dh_g, "st": st_g, "att": att_g}
    begins = {"att": att_g.start}
    for p in range(np_):
        moves.update({f"dq{p}": dq_r[p], f"ds{p}": dq_s[p], f"ar{p}": ar_r[p], f"as{p}": ar_s[p]})
        begins.update({f"ds{p}": part_(share_dq, p), f"as{p}": part_(share_ar, p)})

    def acts(*point):
        return [begins[e[0]] if e[1] == "start" else part_(moves[e[0]].move, *e[1:]) for e in BWD_PLAN.get(point, [])]

    def run(*point):
        for fn in acts(*point):
            fn()

    def table(kind, n):
        return {k: acts(kind, k) for k in range(n) if acts(kind, k)}

    offs = BWD_ORDER
    first = BWD_FIRST * hc
    per = 2 * (chips - BWD_FIRST)
    needs = {k * hc: offs[k] for k in range(1, BWD_FIRST)}
    needs.update({first + 2 * (k - BWD_FIRST): offs[k] for k in range(BWD_FIRST, chips)})

    def project(p):
        r = pl.ds(pl.multiple_of(p * 128, 128), 128)
        dkv[p, 0:128, :] = (dk[r, :] * scale).astype(BF16)
        dkv[p, 128:256, :] = dv[r, :].astype(BF16)
        xp(p).start()
        g = mm(dkv[p, :, my_cols], msc[0, 0:mem]) + mm(dkv[p, :, other_cols], msc[1, 0:mem])
        for n in range(2 * chips):
            arp[p, n // 2, n % 2] = g[n * seg:(n + 1) * seg]

    def body(it, carry):
        early = it < first
        b = it - first
        p = b // per
        r = b - p * per
        h = jnp.where(early, it % hc, 2 * p + r % 2)
        chip = ring.chip(pick(jnp.where(early, it // hc, BWD_FIRST + r // 2), offs))
        dispatch(it, {k: acts("r", k) + [part_(dh_g.ready, off)] for k, off in needs.items()})
        fresh = (early & (it > 0) & (it % hc == 0)) | ((b >= 0) & (b < per) & (r % 2 == 0))
        pl.when(fresh)(part_(prepare, chip))
        tile(h, chip)
        pl.when((b >= 0) & (r == per - 1))(part_(project, p))
        dispatch(it, table("b", chips * hc))
        return carry

    lax.fori_loop(0, chips * hc, body, 0)
    run("p", np_)
    near = range(1 - far, far + 1)

    for cp in locals_:
        cp.wait()
    for off in near:
        att_g.ready(off)
    gain2 = g2_ref[...].astype(F32)[None, :]
    gwo_s[...] = jnp.zeros_like(gwo_s)

    def y_fetch(ch, slot):
        return pltpu.make_async_copy(y_hbm.at[ch], ybuf.at[slot], ysem.at[slot, 0])

    def fetch(ch, slot):
        return (y_fetch(ch, slot), pltpu.make_async_copy(attg.at[ch], abuf.at[slot], ysem.at[slot, 1]))

    for cp in fetch(0, 0):
        cp.start()

    def hidden(ch, carry):
        slot = ch % 2
        for cp in fetch(ch, slot):
            cp.wait()

        @pl.when(ch + 1 < chips)
        def _():
            for cp in fetch(ch + 1, 1 - slot):
                cp.start()
        att = abuf[slot].reshape(QT, dim)
        h = (ybuf[slot].reshape(QT, dim).astype(F32) + mm(att, wo_ref[...])).astype(BF16)
        qz_ref[0:dim, lanes(ch)] = rms_norm(h.astype(F32), gain2).astype(BF16).T
        ah = jnp.where(core == 0, att[:, :inner], att[:, inner:])
        gwo_s[...] += mm_at(ah, dhg[ch].reshape(QT, dim))
        dispatch(ch, table("h", chips))
        return carry

    lax.fori_loop(0, chips, hidden, 0)
    dh_g.drain()
    go_load = pltpu.make_async_copy(gog, dhg, ls.at[0])
    go_load.start()

    def partner_block(buf, dst, k):
        return pltpu.make_async_copy(buf, dst, gl.at[k]), remote(buf, dst, gs.at[k], gr.at[k], ring.partner)

    def both_start(pair):
        pair[0].start()
        pair[1].start()

    def both_wait(pair):
        pair[0].wait()
        pair[1].wait()

    wo_out = partner_block(gwo_s, gwo.at[hrow], 3 * nf)
    both_start(wo_out)

    def w_fetch(f, slot):
        cols = pl.ds(pl.multiple_of(core * fh + f * FT, FT), FT)
        return (pltpu.make_async_copy(wg_hbm.at[:, cols], wbuf.at[0], wsem.at[slot, 0]),
                pltpu.make_async_copy(wu_hbm.at[:, cols], wbuf.at[1], wsem.at[slot, 1]),
                pltpu.make_async_copy(wd_hbm.at[cols], dbuf.at[slot], wsem.at[slot, 2]))

    for cp in w_fetch(0, 0):
        cp.start()
    go_load.wait()
    f_table = table("f", 9 * nf)

    def block(f, n):
        if n == 0:
            return partner_block(gst.at[f % 2, pl.ds(0, FT)], gdown.at[pl.ds(pl.multiple_of(core * fh + f * FT, FT), FT)], f)
        return partner_block(gsw.at[f % 2, n - 1], (ggate, gup)[n - 1].at[:, pl.ds(pl.multiple_of(core * fh + f * FT, FT), FT)], n * nf + f)

    def mlp(f, carry):
        slot = f % 2
        for cp in w_fetch(f, slot):
            cp.wait()

        for n in range(2):
            wt[n] = wbuf[n].T

        @pl.when(f + 1 < nf)
        def _():
            for cp in w_fetch(f + 1, 1 - slot):
                cp.start()

        def act_pair(k, cc):
            for ch in (2 * k, 2 * k + 1):
                q = lanes(ch)
                n2t = qz_ref[0:dim, q]
                g = mm(wt[0], n2t)
                u = mm(wt[1], n2t)
                ga = mm_bt(dbuf[slot], dhg[ch].reshape(QT, dim))
                sig = jax.nn.sigmoid(g)
                si = g * sig
                doz[0:FT, q] = (si * u).astype(BF16)
                doz[FT:2 * FT, q] = (ga * u * (sig + si * (1.0 - sig))).astype(BF16)
                doz[2 * FT:3 * FT, q] = (ga * si).astype(BF16)
            dispatch(f * 9 + 2 * k + 1, f_table)
            return cc

        lax.fori_loop(0, chips // 2, act_pair, 0)

        @pl.when(f > 1)
        def _():
            for n in range(3):
                both_wait(block(f - 2, n))
        acc = [None] * 3
        for ch in range(chips):
            q = slice(ch * QT, (ch + 1) * QT)
            n2t = qz_ref[0:dim, q]
            for n, d in enumerate((mm(doz[0:FT, q], dhg[ch].reshape(QT, dim)), mm_bt(n2t, doz[FT:2 * FT, q]), mm_bt(n2t, doz[2 * FT:3 * FT, q]))):
                acc[n] = d if acc[n] is None else acc[n] + d
        gst[slot, 0:FT] = acc[0]
        gsw[slot, 0] = acc[1]
        gsw[slot, 1] = acc[2]
        for n in range(3):
            both_start(block(f, n))
        dispatch(f * 9 + 8, f_table)
        return carry

    lax.fori_loop(0, nf, mlp, 0)
    for p in range(np_):
        remote(dkvp.at[p], dkvp.at[p], xs.at[p], xr.at[p], ring.partner).wait_recv()
    nb = 4
    w = mem // nb
    for f in (nf - 2, nf - 1):
        for n in range(3):
            both_wait(block(f, n))

    def gm(b):
        return pltpu.make_async_copy(gst.at[b % 2, pl.ds(0, w)], gmem.at[pl.ds(pl.multiple_of(b * w, w), w)], gl.at[3 * nf + 2 + b % 2])

    def memory_rows(b, carry):
        @pl.when(b > 1)
        def _():
            gm(b - 2).wait()
        cb = pl.ds(pl.multiple_of(core * mem + b * w, w), w)
        cp = pl.ds(pl.multiple_of(b * w, w), w)
        acc = None
        for p in range(np_):
            own_e = pl.ds(pl.multiple_of(core * inner + p * 128, 128), 128)
            oth_e = pl.ds(pl.multiple_of((1 - core) * inner + p * 128, 128), 128)
            for part, w_ref in ((0, wk_ref), (1, wv_ref)):
                e = slice(part * 128, (part + 1) * 128)
                lhs = jnp.concatenate([dkv[p, e, cb], dkvp[p, e, cp]], axis=0)
                rhs = jnp.concatenate([w_ref[:, own_e], w_ref[:, oth_e]], axis=1)
                d = mm_bt(lhs.T, rhs)
                acc = d if acc is None else acc + d
        gst[b % 2, 0:w] = acc
        gm(b).start()
        dispatch(b, table("m", nb))
        return carry

    lax.fori_loop(0, nb, memory_rows, 0)
    run("m", nb)

    gain = g1_ref[...].astype(F32)[None, :]
    y_fetch(0, 0).start()
    spb[...] = jnp.zeros_like(spb)
    both_wait(wo_out)
    gwq_s = gwo_s
    gwq_s[...] = jnp.zeros_like(gwq_s)
    wq_h = wq_ref[:, hcol]

    def query(ch, carry):
        slot = ch % 2
        y_fetch(ch, slot).wait()

        @pl.when(ch + 1 < chips)
        def _():
            y_fetch(ch + 1, 1 - slot).start()
        x = ybuf[slot].reshape(QT, dim).astype(F32)
        xhat = x * lax.rsqrt(jnp.mean(x * x, axis=-1, keepdims=True) + 1e-6)
        n1 = (xhat * gain).astype(BF16)
        dqc = jnp.concatenate([dqa[p, ch].reshape(128, QT) for p in range(np_)], axis=0)
        dn = mm_bt(dqc.T, wq_h)
        gwq_s[...] += mm(dqc, n1)
        spb[0:1, :] += jnp.sum(dn * xhat, axis=0, keepdims=True)
        dispatch(ch, table("q", chips))
        return carry

    lax.fori_loop(0, chips, query, 0)
    gvec2 = jnp.zeros((16 - 2 * hc, QT), F32)
    for ch in range(chips):
        gvec2 = gvec2 + jnp.concatenate([stb[ch, 0, hc:8, :], stb[ch, 1, hc:8, :]], axis=0)
    for n in range(dim // QT):
        spb[1:2, n * QT:(n + 1) * QT] = gvec2[n:n + 1]
    cv = remote(spb, pvec, xs.at[2 * np_], xr.at[2 * np_], ring.partner)
    cv.start()
    wq_out = partner_block(gwq_s, gwq.at[hrow], 3 * nf + 1)
    both_start(wq_out)
    for p in range(np_):
        own_r = pl.ds(pl.multiple_of(core * inner + p * 128, 128), 128)
        oth_r = pl.ds(pl.multiple_of((1 - core) * inner + p * 128, 128), 128)
        dqo_ref[own_r, :] = dqa[p, z, :, :, qmine].reshape(128, rows)
        xq(p).wait()
        dqo_ref[oth_r, :] = pdq[p].reshape(128, rows)
    x = y_ref[...].astype(F32)
    inv = lax.rsqrt(jnp.mean(x * x, axis=-1, keepdims=True) + 1e-6)
    xhat = x * inv
    t = mm_bt(dqo_ref[...].T, wq_ref[...]) * gain
    gdec_ref[...] = gh_ref[...] + inv * (t - xhat * jnp.mean(t * xhat, axis=-1, keepdims=True))
    run("q", chips)
    wkv_out = []
    for p in range(np_):
        for k, out in enumerate((gwk, gwv)):
            n = 2 * p + k
            src = ara.at[p, pl.ds(k * (chips // 2), chips // 2)]
            wkv_out.append(pltpu.make_async_copy(src, out.at[core, p], ls.at[2 + n]))
            wkv_out.append(remote(src, out.at[core, p], xs.at[2 * np_ + 1 + n], xr.at[2 * np_ + 1 + n], ring.partner))
    for cp in wkv_out:
        cp.start()
    for p in range(np_):
        xp(p).wait_send()
    cv.wait()
    gvec_ref[...] = spb[0:2] + pvec[0:2]
    both_wait(wq_out)
    for cp in wkv_out:
        cp.wait()
    for b in range(nb - 2, nb):
        gm(b).wait()
    for obj in [att_g, st_g] + dq_r + dq_s + ar_r + ar_s:
        obj.drain()


def bwd_call(dims, *args):
    chips, rows, mem, dim, hc, c, ff = dims
    inner = hc * 64
    QT = 2 * rows
    T = 2 * mem
    np_ = hc // 2
    h2 = chips // 2
    seg = 256 // chips // 2
    FT = ff // 8
    v = pl.BlockSpec(memory_space=VMEM)
    hbm = pl.BlockSpec(memory_space=pl.ANY)
    s3 = (2, 2, h2)
    rows_sems = [DMA((1,)), DMA(s3)] * 2 + [DMA((1,)), DMA((2,))]
    two = [DMA((1,)), DMA(s3)]
    S = jax.ShapeDtypeStruct
    gshape = (chips, 2, 2, rows // 2, dim)
    cols = chips * QT
    wsq = VMEM((dim, 2 * inner), BF16)
    return pl.pallas_call(
        functools.partial(bwd_kernel, dims),
        out_shape=(S((2, dim), F32), S((rows, dim), F32), S((mem, dim), F32), S((2, np_, chips // 2, 2, seg, dim), F32), S((2, np_, chips // 2, 2, seg, dim), F32), S((2 * inner, dim), F32), S((2 * inner, dim), F32),
                   S((ff, dim), F32), S((dim, ff), F32), S((dim, ff), F32), S(gshape, BF16)),
        in_specs=[pl.BlockSpec(memory_space=pltpu.SMEM)] + [v] * 8 + [hbm] * 15, out_specs=(v,) * 2 + (hbm,) * 9,
        scratch_shapes=[
            VMEM((2 * inner, rows), BF16), VMEM((T, inner), BF16), VMEM((T, inner), BF16), VMEM((inner, T), BF16), VMEM((hc * 128, cols), BF16), VMEM((2 * inner, dim), BF16), wsq, wsq, wsq, VMEM((T, 128), BF16),
            VMEM(gshape, BF16), VMEM((max(hc * 128, 3 * FT), cols), BF16), VMEM((hc * 16, cols), BF16), VMEM((hc * 16, cols), BF16),
            VMEM((chips, 2, 8, QT), F32), VMEM((inner, T), F32), VMEM((inner, T), F32), VMEM((np_, 256, T), BF16), VMEM((np_, 256, mem), BF16),
            VMEM((np_, chips, 2, 64, QT), F32), VMEM((np_, 2, 2, h2, 64, QT), F32), VMEM((np_, chips, 2, 64, QT), BF16),
            VMEM((np_, chips, 2, seg, dim), F32), VMEM((np_, 2, 2, h2, seg, dim), F32), VMEM((np_, chips, 2, seg, dim), F32),
            VMEM((8, dim), F32), VMEM((np_, 2, 64, rows), BF16), VMEM((8, dim), F32),
            VMEM((2, mem, dim), BF16), VMEM((2, 2, 2, rows // 2, dim), BF16), VMEM((2, 2, 2, rows // 2, dim), BF16),
            VMEM((2, dim, FT), BF16), VMEM((2, FT, dim), BF16), VMEM((2, FT, dim), BF16), VMEM((2, max(FT, mem // 4), dim), F32), VMEM((2, 2, dim, FT), F32),
            VMEM((inner, dim), F32)]
        + rows_sems * 2 + two * (1 + 4 * np_) + [DMA((4 * np_ + 1,))] * 2 + [DMA((2 + 2 * np_,)), DMA((14,)), DMA((14,)), DMA((16,)), DMA((2, 3)), DMA((2, 2)), DMA((10,))],
        compiler_params=pltpu.CompilerParams(vmem_limit_bytes=67_043_328, collective_id=1, has_side_effects=True),
        cost_estimate=pl.CostEstimate(flops=10**10, bytes_accessed=30 << 20, transcendentals=0),
        name="attn_bwd")(*args)


def finish_kernel(slots, *refs):
    n = (len(refs) - 3) // 2
    srcs, dsts, (buf, si, so) = refs[:n], refs[n:2 * n], refs[2 * n:]
    rows = buf.shape[1]
    moves = []
    for src, dst in zip(srcs, dsts):
        for c in range(0, src.shape[1], buf.shape[2]):
            wide = min(buf.shape[2], src.shape[1] - c)
            cols = pl.ds(c, wide)
            for r in range(0, src.shape[0], rows):
                k = len(moves) % slots
                w = min(rows, src.shape[0] - r)
                b = buf.at[k, pl.ds(0, w), pl.ds(0, wide)]
                moves.append((pltpu.make_async_copy(src.at[pl.ds(r, w), cols], b, si.at[k]), pltpu.make_async_copy(b, dst.at[pl.ds(r, w), cols], so.at[k])))
    lag = slots // 2
    for i in range(len(moves) + lag):
        if i < len(moves):
            if i >= slots:
                moves[i - slots][1].wait()
            moves[i][0].start()
        if i >= lag:
            moves[i - lag][0].wait()
            moves[i - lag][1].start()
    for m in moves[-slots:]:
        m[1].wait()


def finish_call(*arrays):
    slots, rows, cols = 24, 256, 1024
    hbm = pl.BlockSpec(memory_space=pl.ANY)
    return pl.pallas_call(
        functools.partial(finish_kernel, slots),
        out_shape=tuple(jax.ShapeDtypeStruct(a.shape, a.dtype) for a in arrays),
        in_specs=[hbm] * len(arrays), out_specs=(hbm,) * len(arrays),
        scratch_shapes=[VMEM((slots, rows, cols), F32), DMA((slots,)), DMA((slots,))],
        compiler_params=pltpu.CompilerParams(vmem_limit_bytes=67_043_328),
        name="finish")(*arrays)


def fwd_kernel(dims, len_ref, y_ref, go_ref, m_ref, g1_ref, g2_ref, wq_hbm, wk_hbm, wv_hbm, wo_hbm, wg_hbm, wu_hbm, wd_hbm,
               own, att_ref, dh_ref, gh_ref, gn_ref, k_out, v_out, kt_out, qz_out, mg_out, yall, gog,
               k_s, v_s, kt_s, qz, mg, wq_ref, wk_ref, wv_ref, ak_ref, yg, wqt, vt_s, s_scr, mx_scr, part, rbuf, patt, satt, gob, attt, wo_s, wg_s, wu_s, wd_s, n2_s, dn_s, *sems):
    chips, rows, mem, dim, hc, c, ff = dims
    QT = 2 * rows
    T = 2 * mem
    MC = min(256, mem)
    hh = hc // 2
    inner = hc * 64
    HR = hh * 64
    ring = Ring(chips)
    z, core, far = ring.z, ring.core, ring.far
    sub = rows // 2
    part_ = functools.partial
    xs, xr, ls = sems[14:]
    rsrc = lambda ref: (lambda half: ref.at[pl.ds(half * sub, sub)])
    y_g = Rows(ring, yg, rsrc(y_ref), sems[:6])
    go_g = Rows(ring, gog, rsrc(gob), sems[6:12])

    def merge(dst, src):
        for hl in range(hh):
            mr = slice(HR + hl, HR + hl + 1)
            lr = slice(HR + 8 + hl, HR + 9 + hl)
            m1, m2 = dst[mr, :], src[mr, :]
            m = jnp.maximum(m1, m2)
            a = jnp.exp2((m1 - m) * c)
            b = jnp.exp2((m2 - m) * c)
            rr = slice(hl * 64, (hl + 1) * 64)
            dst[rr, :] = dst[rr, :] * a + src[rr, :] * b
            dst[mr, :] = m
            dst[lr, :] = dst[lr, :] * a + src[lr, :] * b

    o_r = Reduce(ring, part, rbuf, merge, sems[12:14])
    loads = [pltpu.make_async_copy(src, dst, ls.at[7 + n]) for n, (src, dst) in enumerate((
        (wk_hbm, wk_ref), (wv_hbm, wv_ref), (wq_hbm, wq_ref), (wo_hbm, wo_s), (wg_hbm, wg_s), (wu_hbm, wu_s), (wd_hbm, wd_s)))]
    stores = [pltpu.make_async_copy(src, dst, ls.at[n]) for n, (src, dst) in enumerate(((k_s, k_out), (v_s, v_out), (kt_s, kt_out), (mg, mg_out), (qz, qz_out)))]
    for cp in loads[:3]:
        cp.start()
    ring.enter()
    y_g.start()
    mx_copy = remote(m_ref, mg, xs.at[0], xr.at[0], ring.partner)
    mx_copy.start()
    for cp in loads[3:]:
        cp.start()
    gob[...] = go_ref[...].astype(BF16)
    for half in range(2):
        yg[z, core, half] = y_ref[half * sub:(half + 1) * sub, :]
    hcol = pl.ds(pl.multiple_of(core * inner, 128), inner)
    qz[...] = jnp.zeros_like(qz)
    mask_lanes(ak_ref, len_ref, z * T)
    for cp in loads[:3]:
        cp.wait()
    wqt[...] = wq_ref[:, hcol].T
    wk = wk_ref[:, hcol]
    wv = wv_ref[:, hcol]

    moves = {"y": y_g, "go": go_g, "o": o_r}

    def acts(*point):
        return [go_g.start if e[1] == "start" else part_(moves[e[0]].move, *e[1:]) for e in FWD_PLAN.get(point, [])]

    def run(*point):
        for fn in acts(*point):
            fn()

    def project(src, base, blocks):
        for j in blocks:
            r = pl.ds(pl.multiple_of(base + j * MC, MC), MC)
            blk = src[j * MC:(j + 1) * MC, :]
            kb = mm(blk, wk).astype(BF16)
            vb = mm(blk, wv).astype(BF16)
            k_s[r, :] = kb
            v_s[r, :] = vb
            kt_s[:, r] = kb.T
            vt_s[:, r] = vb.T

    nb = mem // MC
    project(m_ref, core * mem, range(nb))
    run("s", 0)
    mx_copy.wait_recv()
    project(mg, (1 - core) * mem, range(nb // 2))
    run("s", 1)
    project(mg, (1 - core) * mem, range(nb // 2, nb))
    run("s", 2)
    for cp in stores[:4]:
        cp.start()
    gain = g1_ref[...].astype(F32)[None, :]
    one_row = jnp.where(lax.broadcasted_iota(jnp.int32, (16, QT), 0) == 0, 1.0, 0.0).astype(BF16)

    def lanes(chip):
        return pl.ds(pl.multiple_of(chip * QT, QT), QT)

    def prep(chip):
        n1 = rms_norm(yg[chip].reshape(QT, dim).astype(F32), gain).astype(BF16)
        qt = mm_bt(wqt[...], n1).astype(BF16)
        for h in range(hc):
            lo = h * 128 + (h % 2) * 64
            qz[lo:lo + 64, lanes(chip)] = qt[h * 64:(h + 1) * 64]

    def step(new, slot, old, pslot):
        if new is not None:
            chip, h = new
            rhs = jnp.concatenate([qz[pl.ds(pl.multiple_of(h * 128, 128), 128), lanes(chip)], one_row], axis=0)
            pair = pl.ds(pl.multiple_of((h // 2) * 128, 128), 128)
            mx = None
        if old is not None:
            ochip, half, hl = old
            m = jnp.max(mx_scr[pslot], axis=0, keepdims=True)
            vrow = pl.ds(pl.multiple_of((half * hh + hl) * 64, 64), 64)
            ls_ = None
            acc = None
        for j in range(T // MC):
            r = slice(j * MC, (j + 1) * MC)
            if new is not None:
                s = mm(jnp.concatenate([k_s[r, pair], ak_ref[r, 0:16]], axis=1), rhs)
                s_scr[slot, r, :] = s
                t = jnp.max(s.reshape(MC // 8, 8, QT), axis=0)
                mx = t if mx is None else jnp.maximum(mx, t)
            if old is not None:
                pr = jnp.exp2((s_scr[pslot, r, :] - m) * c)
                t = jnp.sum(pr.reshape(MC // 8, 8, QT), axis=0)
                ls_ = t if ls_ is None else ls_ + t
                dd = mm(vt_s[vrow, r], pr.astype(BF16))
                acc = dd if acc is None else acc + dd
        if new is not None:
            mx_scr[slot] = mx
        if old is not None:
            part[ochip, half, hl * 64:(hl + 1) * 64, :] = acc
            part[ochip, half, HR + hl:HR + hl + 1, :] = m
            part[ochip, half, HR + 8 + hl:HR + 9 + hl, :] = jnp.sum(ls_, axis=0, keepdims=True)

    offs = [o for o, _ in FWD_ORDER]
    halves = [h for _, h in FWD_ORDER]
    n = len(offs)
    fresh = [int(k + 1 < n and offs[k + 1] not in offs[:k + 1]) for k in range(n)]
    run("s", 3)
    y_g.ready(0)
    prep(z)
    step((z, halves[0] * hh), 0, None, None)

    def body(pair, carry):
        for u in range(2):
            i = 2 * pair + u
            i2 = jnp.minimum(i + 1, n - 1)
            chip, half = ring.chip(pick(i, offs)), pick(i, halves)
            chip2, half2 = ring.chip(pick(i2, offs)), pick(i2, halves)
            for k in range(hh):
                slot = (u * hh + k) % 2
                if k == hh - 1:
                    dispatch(pair, {kk // 2: acts("r", kk) + [part_(y_g.ready, offs[kk + 1])] for kk in range(u, n, 2) if fresh[kk]})
                    if any(fresh[u::2]):
                        pl.when(pick(i, fresh) == 1)(part_(prep, chip2))
                    new = (chip2, half2 * hh)
                else:
                    new = (chip, half * hh + k + 1)
                step(new, 1 - slot, (chip, half, k), slot)
                dispatch(pair, {kk // 2: acts("b", kk * hh + k) for kk in range(u, n, 2) if acts("b", kk * hh + k)})
        return carry

    gl = [pltpu.make_async_copy(gob.at[pl.ds(half * sub, sub)], gog.at[z, core, half], ls.at[5 + half]) for half in range(2)]
    for cp in gl:
        cp.start()
    lax.fori_loop(0, n // 2, body, 0)
    yc = pltpu.make_async_copy(yg, yall, ls.at[14])
    yc.start()
    stores[4].start()
    run("t", 0)
    run("t", 1)
    qmine = pl.ds(pl.multiple_of(core * rows, rows), rows)
    qother = pl.ds(pl.multiple_of((1 - core) * rows, rows), rows)
    for h in range(hc):
        half, hl = h // hh, h % hh
        m = part[z, half, HR + hl:HR + hl + 1, :]
        l = part[z, half, HR + 8 + hl:HR + 9 + hl, :]
        own[h * 64:(h + 1) * 64, :] = part[z, half, hl * 64:(hl + 1) * 64, :] / l
        own[inner + h:inner + h + 1, :] = m + jnp.log2(l) / c
    satt[...] = own[:inner, qother].astype(BF16)
    xo = remote(satt, patt, xs.at[1], xr.at[1], ring.partner)
    xo.start()
    attt[pl.ds(pl.multiple_of(core * inner, inner), inner), :] = own[:inner, qmine].astype(BF16)
    for cp in loads[3:]:
        cp.wait()
    run("t", 2)
    xo.wait()
    attt[pl.ds(pl.multiple_of((1 - core) * inner, inner), inner), :] = patt[...]

    att = attt[...].T
    att_ref[...] = att
    gain2 = g2_ref[...].astype(F32)[None, :]
    run("t", 3)
    hid = (y_ref[...].astype(F32) + mm(att, wo_s[...])).astype(BF16).astype(F32)
    inv = lax.rsqrt(jnp.mean(hid * hid, axis=-1, keepdims=True) + 1e-6)
    hhat = hid * inv
    n2 = (hhat * gain2).astype(BF16)
    fb = ff // 4
    n2_s[...] = n2
    dn_s[...] = jnp.zeros_like(dn_s)

    def mlp(f, carry):
        cols = pl.ds(pl.multiple_of(f * fb, fb), fb)
        wg, wu = wg_s[:, cols], wu_s[:, cols]
        g = mm(n2_s[...], wg)
        u = mm(n2_s[...], wu)
        ga = mm_bt(gob[...], wd_s[cols, :])
        sig = jax.nn.sigmoid(g)
        si = g * sig
        dn_s[...] += mm_bt((ga * u * (sig + si * (1.0 - sig))).astype(BF16), wg) + mm_bt((ga * si).astype(BF16), wu)
        dispatch(f, {n: acts("t", 4 + n) for n in range(4) if acts("t", 4 + n)})
        return carry

    lax.fori_loop(0, 4, mlp, 0)
    dn = dn_s[...]
    gsum = jnp.sum(dn * hhat, axis=0, keepdims=True)
    gn_ref[...] = jnp.zeros_like(gn_ref)
    for k in range(dim // QT):
        gn_ref[k:k + 1, :] = gsum[:, k * QT:(k + 1) * QT]
    t = dn * gain2
    gh = go_ref[...] + inv * (t - hhat * jnp.mean(t * hhat, axis=-1, keepdims=True))
    gh_ref[...] = gh
    dh_ref[...] = gh.astype(BF16)
    run("t", 8)
    for off in range(-far + 1, far + 1):
        go_g.ready(off)
    mx_copy.wait_send()
    for cp in [yc] + gl + stores:
        cp.wait()
    for obj in (y_g, go_g, o_r):
        obj.drain()


def fwd_call(dims, *args):
    chips, rows, mem, dim, hc, c, ff = dims
    hh = hc // 2
    inner = hc * 64
    QT = 2 * rows
    T = 2 * mem
    HR = hh * 64
    h2 = chips // 2
    v = pl.BlockSpec(memory_space=VMEM)
    hbm = pl.BlockSpec(memory_space=pl.ANY)
    S = jax.ShapeDtypeStruct
    s3 = (2, 2, h2)
    gshape = (chips, 2, 2, rows // 2, dim)
    rows_sems = [DMA((1,)), DMA(s3)] * 2 + [DMA((1,)), DMA((2,))]
    return pl.pallas_call(
        functools.partial(fwd_kernel, dims),
        out_shape=(S((inner + 8, QT), F32), S((rows, 2 * inner), BF16), S((rows, dim), BF16), S((rows, dim), F32), S((8, QT), F32),
                   S((T, inner), BF16), S((T, inner), BF16), S((inner, T), BF16), S((hc * 128, chips * QT), BF16), S((mem, dim), BF16), S(gshape, BF16), S(gshape, BF16)),
        in_specs=[pl.BlockSpec(memory_space=pltpu.SMEM)] + [v] * 5 + [hbm] * 7, out_specs=(v,) * 5 + (hbm,) * 7,
        scratch_shapes=[
            VMEM((T, inner), BF16), VMEM((T, inner), BF16), VMEM((inner, T), BF16), VMEM((hc * 128, chips * QT), BF16), VMEM((mem, dim), BF16),
            VMEM((dim, 2 * inner), BF16), VMEM((dim, 2 * inner), BF16), VMEM((dim, 2 * inner), BF16), VMEM((T, 128), BF16),
            VMEM(gshape, BF16), VMEM((inner, dim), BF16), VMEM((inner, T), BF16), VMEM((2, T, QT), F32), VMEM((2, 8, QT), F32),
            VMEM((chips, 2, HR + 16, QT), F32), VMEM((2, 2, h2, HR + 16, QT), F32), VMEM((inner, rows), BF16), VMEM((inner, rows), BF16),
            VMEM((rows, dim), BF16), VMEM((2 * inner, rows), BF16), VMEM((2 * inner, dim), BF16), VMEM((dim, ff), BF16), VMEM((dim, ff), BF16), VMEM((ff, dim), BF16), VMEM((rows, dim), BF16), VMEM((rows, dim), F32)]
        + rows_sems * 2 + [DMA((1,)), DMA(s3)] + [DMA((2,))] * 2 + [DMA((15,))],
        compiler_params=pltpu.CompilerParams(vmem_limit_bytes=62 * 1024 * 1024, collective_id=0, has_side_effects=True),
        cost_estimate=pl.CostEstimate(flops=10**10, bytes_accessed=30 << 20, transcendentals=0),
        name="attn_fwd")(*args)


def solution(mesh):
    group = mesh.shape['seq']
    row_spec = P(('data', 'seq'), None)
    part_vec = P('data')
    part_mat = P('data', None)
    part_cube = P('data', None, None)

    def device_step(dec_in, memory, mem_len, grad_out, norm_attn, wq, wk, wv, wo, norm_mlp, w_gate, w_up, w_down):
        rows, dim = dec_in.shape
        mem = memory.shape[0]
        heads, hd = wq.shape[1], wq.shape[2]
        inner = heads * hd
        chips = group // 2
        hc = heads // 2
        c = LOG2E * hd ** -0.5
        dims = (chips, rows, mem, dim, hc, c, w_gate.shape[1])
        wq2, wk2, wv2 = (w.reshape(dim, inner) for w in (wq, wk, wv))
        wo2 = wo.reshape(inner, dim)

        own, attended, dh, grad_hidden, gn, k_c, v_c, kt_c, qz, mem_p, y_all, go_all = fwd_call(
            dims, mem_len, dec_in, grad_out, memory, norm_attn, norm_mlp, wq2, wk2, wv2, wo2, w_gate, w_up, w_down)
        gvec, g_dec, g_mem, g_wk, g_wv, g_wq, g_wo, g_down, g_gate, g_up, _ = bwd_call(
            dims, mem_len, dh, own, gn, attended, dec_in, grad_hidden, norm_attn, norm_mlp,
            k_c, v_c, kt_c, qz, wo2, wq2, wk2, wv2, memory, mem_p, y_all, go_all, w_gate, w_up, w_down)
        cube = (dim, heads, hd)
        g_wk, g_wv = (g.reshape(inner, dim) for g in (g_wk, g_wv))
        g_dec, g_mem, g_wq, g_wk, g_wv, g_wo, g_down, g_gate, g_up = finish_call(g_dec, g_mem, g_wq, g_wk, g_wv, g_wo, g_down, g_gate, g_up)
        g_wq, g_wk, g_wv = (g.T.reshape(cube) for g in (g_wq, g_wk, g_wv))
        return (g_dec, g_mem, gvec[0], g_wq, g_wk, g_wv, g_wo.reshape(heads, hd, dim), gvec[1], g_gate, g_up, g_down)

    return jax.shard_map(device_step, mesh=mesh,
                         in_specs=(row_spec, row_spec, part_vec, row_spec) + (P(),) * 9,
                         out_specs=(row_spec, row_spec, part_vec, part_cube, part_cube, part_cube, part_cube, part_vec, part_mat, part_mat, part_mat),
                         check_vma=False)
```
